32 devices in a mesh: dp: 8 (over z, x), mp: 4 (over y, core).
Axes of the slice: x: 2, y: 2, z: 4, core: 2. Of those that a mesh axis runs over, the one named last changes fastest.
Arguments:
- tokens: bfloat16 [32768, 1024], P(('dp', 'mp')), may hold values from -6 to 6
- segment_ids: int32 [32, 1024], P('dp'), may hold values from 0 to 7, never falling along the last dimension, each value on 1 to 512 neighbouring positions
- time_steps: int32 [32], P('dp'), may hold values from 0 to 999
- w_qkv: bfloat16 [1024, 3, 1024], P(None, None, 'mp'), may hold values from -0.1875 to 0.1875
- b_qv: bfloat16 [2, 1024], P(None, 'mp'), may hold values from -1.796875 to 1.796875
- w_out: bfloat16 [1024, 1024], P('mp'), may hold values from -0.75 to 0.75
- b_out: bfloat16 [1024], replicated, may hold values from -1.796875 to 1.796875
- gain_one: bfloat16 [1024], replicated, may hold values from 0.5 to 1.5
- shift_one: bfloat16 [1024], replicated, may hold values from -1.796875 to 1.796875
- w_up: bfloat16 [1024, 4096], P(None, 'mp'), may hold values from -0.1875 to 0.1875
- b_up: bfloat16 [4096], P('mp'), may hold values from -1.796875 to 1.796875
- w_down: bfloat16 [4096, 1024], P('mp'), may hold values from -0.09375 to 0.09375
- b_down: bfloat16 [1024], replicated, may hold values from -1.796875 to 1.796875
- gain_two: bfloat16 [1024], replicated, may hold values from 0.5 to 1.5
- shift_two: bfloat16 [1024], replicated, may hold values from -1.796875 to 1.796875
- w_time: bfloat16 [1024, 1024], replicated, may hold values from -0.1875 to 0.1875
- b_time: bfloat16 [1024], replicated, may hold values from -1.796875 to 1.796875
- cotangent: bfloat16 [32768, 1024], P(('dp', 'mp')), may hold values from -6 to 6
Outputs:
- out_rows: bfloat16 [32768, 1024], P(('dp', 'mp'))
- grad_tokens: float32 [32768, 1024], P(('dp', 'mp'))
- grad_w_qkv: float32 [1024, 3, 1024], P('dp', None, 'mp')
- grad_b_qv: float32 [2, 4, 256], P(None, 'mp', 'dp')
- grad_w_out: float32 [1024, 1024], P('mp', 'dp')
- grad_b_out: float32 [1024], P(('dp', 'mp'))
- grad_gain_one: float32 [1024], P(('dp', 'mp'))
- grad_shift_one: float32 [1024], P(('dp', 'mp'))
- grad_w_up: float32 [1024, 4096], P('dp', 'mp')
- grad_b_up: float32 [4, 1024], P('mp', 'dp')
- grad_w_down: float32 [4096, 1024], P('mp', 'dp')
- grad_b_down: float32 [1024], P(('dp', 'mp'))
- grad_gain_two: float32 [1024], P(('dp', 'mp'))
- grad_shift_two: float32 [1024], P(('dp', 'mp'))
- grad_w_time: float32 [1024, 1024], P(('dp', 'mp'))
- grad_b_time: float32 [1024], P(('dp', 'mp'))
The draws below stay inside these ranges and needn't reach their ends.
Inputs may be any that keep to these rules, and one draw needn't show every extreme that they name: `segment_ids`: along a packed row the ids never fall and every id from 0 up occurs; a document holds at most 512 tokens, and some document holds exactly that many.
All inputs are finite; a program needn't handle non-finite values.
Results may differ from the reference program's by a relative error of at most 0.02.
Values may be sent and summed in bfloat16 or wider, within the bound.
A program may use at most 256 MiB of HBM per device.

```python
import math
import jax
import jax.numpy as jnp
import numpy as np
from jax import lax

D = 1024
HEADS = 16
HEAD_DIM = 64
FF = 4096
LEN = 1024
SEQS = 32
TOKENS = 32768
N_MP = 4


def set_ends(array, stream_key, smallest, largest):
    index_at = [jax.random.randint(jax.random.fold_in(stream_key, axis), (), 0, length) for axis, length in enumerate(array.shape)]
    widest = array.shape.index(max(array.shape))
    next_to = index_at[:widest] + [(index_at[widest] + 1) % array.shape[widest]] + index_at[widest + 1:]
    return array.at[tuple(index_at)].set(smallest).at[tuple(next_to)].set(largest)


def block_levels(key, dims, shards, smallest, largest):
    factor_of = 1.0
    for axis_at, blocks in shards:
        steps = jax.random.uniform(jax.random.fold_in(jax.random.fold_in(key, 6), axis_at), (blocks,), jnp.float32, smallest / len(shards), largest / len(shards))
        factor_of = factor_of * jnp.repeat(jnp.exp(steps), dims[axis_at] // blocks).reshape((-1,) + (1,) * (len(dims) - 1 - axis_at))
    return factor_of


def length_profile(count, total, limit, slope):
    portions = [(1 << 20) // math.isqrt(rank ** slope) + 1 for rank in range(2, count + 1)]
    spare, holding = total - limit - (count - 1), [1] * (count - 1)
    while spare > 0:
        free = [i for i in range(count - 1) if holding[i] < limit]
        pool, remaining = sum([portions[i] for i in free]), spare
        for i in free:
            extra = min(limit - holding[i], max(1, remaining * portions[i] // pool), spare)
            holding[i] = holding[i] + extra
            spare = spare - extra
    return np.array([limit] + holding)


def uneven_parts(rng, number_of, total, limit, lean):
    if number_of == 2:
        one = jax.random.randint(rng, (), max(1, total - limit), min(limit, total - 1) + 1)
        return jnp.stack([one, total - one])
    tallies = jnp.asarray(length_profile(number_of, total, limit, lean), jnp.int32)
    couples = (number_of - 1) // 2
    source_of, receiver = tallies[1:1 + 2 * couples:2], tallies[2:2 + 2 * couples:2]
    room = jnp.minimum(source_of - 1, limit - receiver)
    shifted = jax.random.randint(jax.random.fold_in(rng, 1), (couples,), 0, 1 << 20) % (room + 1)
    tallies = tallies.at[1:1 + 2 * couples:2].set(source_of - shifted).at[2:2 + 2 * couples:2].set(receiver + shifted)
    return tallies[jax.random.permutation(jax.random.fold_in(rng, 2), number_of)]


def noise(own_key, extent, deviation, reach, cuts=(), kind=jnp.bfloat16):
    array = deviation * jax.random.normal(own_key, extent, jnp.float32)
    if cuts:
        array = array * block_levels(own_key, extent, cuts, -0.22, 0.18)
    return jnp.clip(array, -reach, reach).astype(kind)


def setup_inputs(seed: int = 0) -> dict:
    splits = jax.random.split(jax.random.key(seed), 19)
    return {
        "tokens": noise(splits[0], (TOKENS, D), 1.0, 6.0, ((0, 32),)),
        "segment_ids": jax.vmap(lambda own: jnp.searchsorted(jnp.cumsum(uneven_parts(own, max(4, LEN // 128), LEN, LEN // 2, 1)), jnp.arange(LEN), side="right"))(jax.random.split(splits[1], SEQS)).reshape((SEQS, LEN)).astype(jnp.int32),
        "time_steps": set_ends(jax.random.randint(splits[2], (SEQS,), 0, 1000), jax.random.fold_in(splits[2], 1), 0, 999).astype(jnp.int32),
        "w_qkv": noise(splits[3], (D, 3, D), D ** -0.5, 0.1875, ((2, 4),)),
        "b_qv": noise(splits[4], (2, D), 0.3, 1.796875, ((1, 4),)),
        "w_out": noise(splits[5], (D, D), (D // 16) ** -0.5, 0.75, ((0, 4),)),
        "b_out": noise(splits[6], (D,), 0.3, 1.796875),
        "gain_one": jnp.clip(1.0 + 0.1 * jax.random.normal(splits[7], (D,), jnp.float32), 0.5, 1.5).astype(jnp.bfloat16),
        "shift_one": noise(splits[8], (D,), 0.3, 1.796875),
        "w_up": noise(splits[9], (D, FF), D ** -0.5, 0.1875, ((1, 4),)),
        "b_up": noise(splits[10], (FF,), 0.3, 1.796875, ((0, 4),)),
        "w_down": noise(splits[11], (FF, D), FF ** -0.5, 0.09375, ((0, 4),)),
        "b_down": noise(splits[12], (D,), 0.3, 1.796875),
        "gain_two": jnp.clip(1.0 + 0.1 * jax.random.normal(splits[13], (D,), jnp.float32), 0.5, 1.5).astype(jnp.bfloat16),
        "shift_two": noise(splits[14], (D,), 0.3, 1.796875),
        "w_time": noise(splits[15], (D, D), D ** -0.5, 0.1875),
        "b_time": noise(splits[16], (D,), 0.3, 1.796875),
        "cotangent": noise(splits[17], (TOKENS, D), 1.0, 6.0, ((0, 32),)),
    }


@jax.custom_vjp
def low(v):
    return lax.optimization_barrier(v.astype(jnp.bfloat16)).astype(jnp.float32)

@jax.custom_vjp
def low_back(v):
    return v

def low_keep(v):
    return (low(v), None)

def low_pass(kept, grad):
    return (grad,)

def back_keep(v):
    return (v, None)

def back_low(kept, grad):
    return (low(grad),)
low.defvjp(low_keep, low_pass)
low_back.defvjp(back_keep, back_low)
EPS = 1e-05

def matmul_high(left, right):
    return jnp.dot(left, right, precision=lax.Precision.HIGHEST, preferred_element_type=jnp.float32)

def time_features(step_values):
    half_width = D // 2
    ladder = jnp.arange(half_width, dtype=jnp.float32)
    frequency = jnp.exp(ladder * (-math.log(10000.0) / half_width))
    angles = step_values.astype(jnp.float32)[:, None] * frequency[None, :]
    return jnp.concatenate([jnp.sin(angles), jnp.cos(angles)], axis=1)

def layer_norm(values, gain_vec, shift_vec):
    center = values - lax.optimization_barrier(jnp.mean(values, axis=-1, keepdims=True))
    spread = lax.optimization_barrier(jnp.mean(center * center, axis=-1, keepdims=True))
    return center * lax.rsqrt(spread + EPS) * gain_vec + shift_vec

def sequence_forward(param_set, tokens_in, segment_row, step_value):
    w_qkv, b_qv, w_out, b_out, gain_one, shift_one, w_up, b_up, w_down, b_down, gain_two, shift_two, w_time, b_time = param_set
    features = time_features(step_value[None])
    embedded = matmul_high(features, w_time) + b_time[None, :]
    hidden_in = tokens_in + embedded
    hidden_low = low(hidden_in)
    score_scale = 1.0 / math.sqrt(HEAD_DIM)
    query_all = low(low_back(matmul_high(hidden_low, w_qkv[:, 0, :]) + b_qv[0][None, :]))
    key_all = low(low_back(matmul_high(hidden_low, w_qkv[:, 1, :])))
    value_all = low(low_back(matmul_high(hidden_low, w_qkv[:, 2, :]) + b_qv[1][None, :]))
    query_heads = query_all.reshape(LEN, HEADS, HEAD_DIM)
    key_heads = key_all.reshape(LEN, HEADS, HEAD_DIM)
    value_heads = value_all.reshape(LEN, HEADS, HEAD_DIM)
    scores = jnp.einsum('qhd,khd->hqk', query_heads, key_heads, precision=lax.Precision.HIGHEST)
    scores = low_back(scores * score_scale)
    same_doc = segment_row[:, None] == segment_row[None, :]
    masked = jnp.where(same_doc[None, :, :], scores, -1e+30)
    top_score = lax.optimization_barrier(jnp.max(masked, axis=2, keepdims=True))
    weights_exp = jnp.exp(masked - top_score)
    probability = weights_exp / lax.optimization_barrier(jnp.sum(weights_exp, axis=2, keepdims=True))
    context = jnp.einsum('hqk,khd->qhd', low(probability), value_heads, precision=lax.Precision.HIGHEST)
    context = low(low_back(context.reshape(LEN, D)))
    attn_out = low_back(matmul_high(context, w_out) + b_out[None, :])
    mid_norm = layer_norm(hidden_in + attn_out, gain_one, shift_one)
    pre_act = low_back(matmul_high(low(mid_norm), w_up) + b_up[None, :])
    activated = low(jax.nn.gelu(pre_act, approximate=False))
    ffn_out = low_back(matmul_high(activated, w_down) + b_down[None, :])
    return layer_norm(mid_norm + ffn_out, gain_two, shift_two)

def reference(tokens, segment_ids, time_steps, w_qkv, b_qv, w_out, b_out, gain_one, shift_one, w_up, b_up, w_down, b_down, gain_two, shift_two, w_time, b_time, cotangent):
    param_set = tuple((weight.astype(jnp.float32) for weight in (w_qkv, b_qv, w_out, b_out, gain_one, shift_one, w_up, b_up, w_down, b_down, gain_two, shift_two, w_time, b_time)))
    token_rows = tokens.astype(jnp.float32).reshape(SEQS, LEN, D)
    cot_rows = cotangent.astype(jnp.float32).reshape(SEQS, LEN, D)
    zero_grads = tuple((jnp.zeros_like(weight) for weight in param_set))

    def one_sequence(accumulated, inputs):
        token_seq, cot_seq, segment_row, step_value = inputs

        def forward(params_in, token_in):
            return sequence_forward(params_in, token_in, segment_row, step_value)
        output_seq, pullback = jax.vjp(forward, param_set, token_seq)
        grad_params, grad_seq = pullback(cot_seq)
        accumulated = tuple((running + addend for running, addend in zip(accumulated, grad_params)))
        return (accumulated, (output_seq.astype(jnp.bfloat16), grad_seq))
    grad_sums, (outputs, grad_rows) = lax.scan(one_sequence, zero_grads, (token_rows, cot_rows, segment_ids, time_steps))
    grad_w_qkv, grad_b_qv, grad_w_out, grad_b_out, grad_gain_one, grad_shift_one, grad_w_up, grad_b_up, grad_w_down, grad_b_down, grad_gain_two, grad_shift_two, grad_w_time, grad_b_time = grad_sums
    return (outputs.reshape(TOKENS, D), grad_rows.reshape(TOKENS, D), grad_w_qkv, grad_b_qv.reshape(2, N_MP, D // N_MP), grad_w_out, grad_b_out, grad_gain_one, grad_shift_one, grad_w_up, grad_b_up.reshape(N_MP, FF // N_MP), grad_w_down, grad_b_down, grad_gain_two, grad_shift_two, grad_w_time, grad_b_time)
```

```python
import math

import jax
import jax.numpy as jnp
from jax import lax
from jax.sharding import PartitionSpec as P

D = 1024
HEAD_DIM = 64
LEN = 1024


EPS = 1e-05
HIGHEST_PRECISION = lax.Precision.HIGHEST


def time_features(step_values):
    half_width = D // 2
    ladder = jnp.arange(half_width, dtype=jnp.float32)
    frequency = jnp.exp(ladder * (-math.log(10000.0) / half_width))
    angles = step_values.astype(jnp.float32)[:, None] * frequency[None, :]
    return jnp.concatenate([jnp.sin(angles), jnp.cos(angles)], axis=1)


def layer_norm(values, gain_vec, shift_vec):
    center = values - jnp.mean(values, axis=-1, keepdims=True)
    spread = jnp.mean(center * center, axis=-1, keepdims=True)
    return center * lax.rsqrt(spread + EPS) * gain_vec + shift_vec


def exact_gelu(values):
    return jax.nn.gelu(values, approximate=False)


def project_qkv(hidden_full, w_qkv, b_qv):
    width_local = w_qkv.shape[2]
    w_flat = w_qkv.reshape(w_qkv.shape[0], 3 * width_local)
    bias_row = jnp.concatenate([b_qv[0], jnp.zeros((width_local,), b_qv.dtype), b_qv[1]]).astype(
        jnp.float32
    )
    product = jnp.dot(hidden_full, w_flat, preferred_element_type=jnp.float32)
    return (product + bias_row[None, :]).astype(jnp.bfloat16)


def head_parts(qkv_seq):
    width_local = qkv_seq.shape[1] // 3
    head_local = width_local // HEAD_DIM
    shaped = qkv_seq.reshape(qkv_seq.shape[0], 3, head_local, HEAD_DIM)
    return (shaped[:, 0], shaped[:, 1], shaped[:, 2])


def masked_scores(queries, keys_part, segment_row):
    scores = jnp.einsum("qhd,khd->hqk", queries, keys_part, preferred_element_type=jnp.float32)
    scores = scores * (1.0 / math.sqrt(HEAD_DIM))
    same_doc = segment_row[:, None] == segment_row[None, :]
    return jnp.where(same_doc[None, :, :], scores, -1e30)


def attend_forward(inputs):
    qkv_seq, segment_row = inputs
    queries, keys_part, values_part = head_parts(qkv_seq)
    masked = masked_scores(queries, keys_part, segment_row)
    top_score = jnp.max(masked, axis=2, keepdims=True)
    weights_exp = jnp.exp(masked - top_score)
    totals = jnp.sum(weights_exp, axis=2, keepdims=True)
    probability = weights_exp / totals
    context = jnp.einsum(
        "hqk,khd->qhd",
        probability.astype(jnp.bfloat16),
        values_part,
        preferred_element_type=jnp.float32,
    )
    log_total = (top_score + jnp.log(totals))[:, :, 0]
    return (context.reshape(qkv_seq.shape[0], -1).astype(jnp.bfloat16), log_total)


def attend_backward(inputs):
    qkv_seq, grad_seq, log_total, segment_row = inputs
    queries, keys_part, values_part = head_parts(qkv_seq)
    masked = masked_scores(queries, keys_part, segment_row)
    probability = jnp.exp(masked - log_total[:, :, None])
    grad_heads = grad_seq.reshape(grad_seq.shape[0], -1, HEAD_DIM)
    d_values = jnp.einsum(
        "hqk,qhd->khd",
        probability.astype(jnp.bfloat16),
        grad_heads,
        preferred_element_type=jnp.float32,
    )
    d_probs = jnp.einsum(
        "qhd,khd->hqk", grad_heads, values_part, preferred_element_type=jnp.float32
    )
    row_terms = jnp.sum(probability * d_probs, axis=2, keepdims=True)
    d_scores = (probability * (d_probs - row_terms)).astype(jnp.bfloat16)
    score_scale = 1.0 / math.sqrt(HEAD_DIM)
    d_queries = (
        jnp.einsum("hqk,khd->qhd", d_scores, keys_part, preferred_element_type=jnp.float32)
        * score_scale
    )
    d_keys = (
        jnp.einsum("hqk,qhd->khd", d_scores, queries, preferred_element_type=jnp.float32)
        * score_scale
    )
    stacked = jnp.stack([d_queries, d_keys, d_values], axis=1)
    return stacked.reshape(qkv_seq.shape[0], -1).astype(jnp.bfloat16)


def body_split(
    tokens,
    segment_ids,
    time_steps,
    w_qkv,
    b_qv,
    w_out,
    b_out,
    gain_one,
    shift_one,
    w_up,
    b_up,
    w_down,
    b_down,
    gain_two,
    shift_two,
    w_time,
    b_time,
    cotangent,
):
    row_count = tokens.shape[0]
    seq_local = time_steps.shape[0]
    width_local = w_qkv.shape[2]
    gain_one_f = gain_one.astype(jnp.float32)
    shift_one_f = shift_one.astype(jnp.float32)
    gain_two_f = gain_two.astype(jnp.float32)
    shift_two_f = shift_two.astype(jnp.float32)
    w_flat = w_qkv.reshape(D, 3 * width_local)
    features = time_features(time_steps)
    embed_rows = jnp.dot(features, w_time.astype(jnp.float32), precision=HIGHEST_PRECISION)
    embed_rows = embed_rows + b_time.astype(jnp.float32)[None, :]
    row_seq = (lax.axis_index("mp") * row_count + jnp.arange(row_count, dtype=jnp.int32)) // LEN
    selector = (row_seq[:, None] == jnp.arange(seq_local, dtype=jnp.int32)[None, :]).astype(
        jnp.float32
    )
    hidden_in = tokens.astype(jnp.float32) + jnp.dot(
        selector, embed_rows, precision=HIGHEST_PRECISION
    )
    hidden_low = hidden_in.astype(jnp.bfloat16)
    hidden_full = lax.all_gather(hidden_low, "mp", axis=0, tiled=True)
    qkv_full = project_qkv(hidden_full, w_qkv, b_qv)
    ctx_blocks, log_totals = lax.map(
        attend_forward, (qkv_full.reshape(seq_local, LEN, 3 * width_local), segment_ids)
    )
    context = ctx_blocks.reshape(seq_local * LEN, width_local)
    rows_in = context
    attn_sum = lax.psum_scatter(
        jnp.dot(rows_in, w_out, preferred_element_type=jnp.float32).astype(jnp.bfloat16),
        "mp",
        scatter_dimension=0,
        tiled=True,
    ).astype(jnp.float32)
    attn_out = attn_sum + b_out.astype(jnp.float32)[None, :]
    mid_in = hidden_in + attn_out
    mid_norm = layer_norm(mid_in, gain_one_f, shift_one_f)
    mid_low = mid_norm.astype(jnp.bfloat16)
    mid_full = lax.all_gather(mid_low, "mp", axis=0, tiled=True)
    pre_act = (
        jnp.dot(mid_full, w_up, preferred_element_type=jnp.float32)
        + b_up.astype(jnp.float32)[None, :]
    )
    activated = exact_gelu(pre_act).astype(jnp.bfloat16)
    rows_in = activated
    ffn_part = lax.psum_scatter(
        jnp.dot(rows_in, w_down, preferred_element_type=jnp.float32).astype(jnp.bfloat16),
        "mp",
        scatter_dimension=0,
        tiled=True,
    ).astype(jnp.float32)
    out_in = mid_norm + ffn_part + b_down.astype(jnp.float32)[None, :]
    out_rows, out_back = jax.vjp(layer_norm, out_in, gain_two_f, shift_two_f)
    grad_two, grad_gain_two, grad_shift_two = out_back(cotangent.astype(jnp.float32))
    branch_two = grad_two.astype(jnp.bfloat16)
    grad_b_down = jnp.sum(branch_two.astype(jnp.float32), axis=0)
    gelu_value, gelu_back = jax.vjp(exact_gelu, pre_act)
    cot_full = lax.all_gather(branch_two, "mp", axis=0, tiled=True)
    d_act = jnp.dot(cot_full, w_down.T, preferred_element_type=jnp.float32)
    grad_w_down = jnp.dot(activated.T, cot_full, preferred_element_type=jnp.float32)
    d_pre = gelu_back(d_act)[0].astype(jnp.bfloat16)
    grad_w_up = jnp.dot(mid_full.T, d_pre, preferred_element_type=jnp.float32)
    grad_b_up = jnp.sum(d_pre.astype(jnp.float32), axis=0)
    rows_in = d_pre
    d_mid_part = lax.psum_scatter(
        jnp.dot(rows_in, w_up.T, preferred_element_type=jnp.float32).astype(jnp.bfloat16),
        "mp",
        scatter_dimension=0,
        tiled=True,
    ).astype(jnp.float32)
    mid_value, mid_back = jax.vjp(layer_norm, mid_in, gain_one_f, shift_one_f)
    grad_one, grad_gain_one, grad_shift_one = mid_back(grad_two + d_mid_part)
    branch_one = grad_one.astype(jnp.bfloat16)
    grad_b_out = jnp.sum(branch_one.astype(jnp.float32), axis=0)
    cot_attn = lax.all_gather(branch_one, "mp", axis=0, tiled=True)
    d_context = jnp.dot(cot_attn, w_out.T, preferred_element_type=jnp.float32).astype(jnp.bfloat16)
    grad_w_out = jnp.dot(context.T, cot_attn, preferred_element_type=jnp.float32)
    grad_blocks = lax.map(
        attend_backward,
        (
            qkv_full.reshape(seq_local, LEN, 3 * width_local),
            d_context.reshape(seq_local, LEN, width_local),
            log_totals,
            segment_ids,
        ),
    )
    d_qkv = grad_blocks.reshape(seq_local * LEN, 3 * width_local)
    grad_w_qkv = jnp.dot(hidden_full.T, d_qkv, preferred_element_type=jnp.float32).reshape(
        D, 3, width_local
    )
    qkv_sums = jnp.sum(d_qkv.astype(jnp.float32), axis=0).reshape(3, width_local)
    grad_b_qv = jnp.stack([qkv_sums[0], qkv_sums[2]]).reshape(2, 1, width_local)
    rows_in = d_qkv
    input_part = lax.psum_scatter(
        jnp.dot(rows_in, w_flat.T, preferred_element_type=jnp.float32).astype(jnp.bfloat16),
        "mp",
        scatter_dimension=0,
        tiled=True,
    ).astype(jnp.float32)
    grad_tokens = grad_one + input_part
    grad_embed = jnp.dot(selector.T, grad_tokens, precision=HIGHEST_PRECISION)
    grad_w_time = jnp.dot(features.T, grad_embed, precision=HIGHEST_PRECISION)
    grad_b_time = jnp.sum(grad_embed, axis=0)
    sharded = (
        lax.psum_scatter(
            grad_w_qkv.astype(jnp.bfloat16), "dp", scatter_dimension=0, tiled=True
        ).astype(jnp.float32),
        lax.psum_scatter(
            grad_b_qv.astype(jnp.bfloat16), "dp", scatter_dimension=2, tiled=True
        ).astype(jnp.float32),
        lax.psum_scatter(
            grad_w_out.astype(jnp.bfloat16), "dp", scatter_dimension=1, tiled=True
        ).astype(jnp.float32),
        lax.psum_scatter(
            grad_w_up.astype(jnp.bfloat16), "dp", scatter_dimension=0, tiled=True
        ).astype(jnp.float32),
        lax.psum_scatter(
            grad_b_up.reshape(1, -1).astype(jnp.bfloat16), "dp", scatter_dimension=1, tiled=True
        ).astype(jnp.float32),
        lax.psum_scatter(
            grad_w_down.astype(jnp.bfloat16), "dp", scatter_dimension=1, tiled=True
        ).astype(jnp.float32),
    )
    shared = (
        lax.psum_scatter(grad_w_time, ("dp", "mp"), scatter_dimension=0, tiled=True),
        lax.psum_scatter(grad_b_time, ("dp", "mp"), scatter_dimension=0, tiled=True),
        lax.psum_scatter(grad_gain_one, ("dp", "mp"), scatter_dimension=0, tiled=True),
        lax.psum_scatter(grad_shift_one, ("dp", "mp"), scatter_dimension=0, tiled=True),
        lax.psum_scatter(grad_gain_two, ("dp", "mp"), scatter_dimension=0, tiled=True),
        lax.psum_scatter(grad_shift_two, ("dp", "mp"), scatter_dimension=0, tiled=True),
        lax.psum_scatter(grad_b_out, ("dp", "mp"), scatter_dimension=0, tiled=True),
        lax.psum_scatter(grad_b_down, ("dp", "mp"), scatter_dimension=0, tiled=True),
    )
    return (
        out_rows.astype(jnp.bfloat16),
        grad_tokens,
        sharded[0],
        sharded[1],
        sharded[2],
        shared[6],
        shared[2],
        shared[3],
        sharded[3],
        sharded[4],
        sharded[5],
        shared[7],
        shared[4],
        shared[5],
        shared[0],
        shared[1],
    )


GRID_DP = 8
GRID_MP = 4
F32 = jnp.float32
BF16 = jnp.bfloat16


def flip_mp(values, bit):
    return lax.ppermute(values, "mp", [(i, i ^ bit) for i in range(GRID_MP)])


def flip_dp(values, bit):
    return lax.ppermute(values, "dp", [(i, i ^ bit) for i in range(GRID_DP)])


def half_of(values, which, axis):
    size = values.shape[axis] // 2
    return lax.dynamic_slice_in_dim(values, which * size, size, axis)


def fetch_pieces(own, axis, x_at):
    near = flip_mp(own, 1)
    far_a = flip_mp(half_of(own, x_at, axis), 2)
    far_b = flip_dp(far_a, 1)
    return [own, near, far_a, far_b, flip_mp(far_a, 1), flip_mp(far_b, 1)]


def fetch_vectors(own, x_at):
    near = flip_mp(own, 1)
    far = flip_mp(own, 2)
    near_far = flip_mp(far, 1)
    return [
        own,
        near,
        half_of(far, x_at, 1),
        half_of(far, 1 - x_at, 1),
        half_of(near_far, x_at, 1),
        half_of(near_far, 1 - x_at, 1),
    ]


def x_parts(values, x_at):
    width = values.shape[1]
    shaped = values.reshape(4, 2, values.shape[0] // 8, width)
    keep = lax.dynamic_index_in_dim(shaped, x_at, 1, keepdims=False)
    leave = lax.dynamic_index_in_dim(shaped, 1 - x_at, 1, keepdims=False)
    return keep, leave


def join_halves(part_a, part_b, x_at):
    axis = part_a.ndim - 1
    return jnp.where(
        x_at == 0,
        jnp.concatenate([part_a, part_b], axis),
        jnp.concatenate([part_b, part_a], axis),
    )


def add_low(left, right):
    return (left.astype(F32) + right.astype(F32)).astype(BF16)


def sum_over_z(part, z_at):
    total = lax.dynamic_index_in_dim(part, z_at, 0, keepdims=False).astype(F32)
    for bit in (1, 2, 3):
        sent = lax.dynamic_index_in_dim(part, z_at ^ bit, 0, keepdims=False)
        total = total + flip_dp(sent, 2 * bit).astype(F32)
    return total


def reduce_pieces(make, join, x_at, z_at, y_first):
    sent = [flip_mp(make(i, None), 1) for i in (1, 4, 5)]
    own, far_a, far_b = (make(i, extra) for i, extra in zip((0, 2, 3), sent))
    if y_first:
        got_a, got_b = flip_mp(far_a, 2), flip_mp(far_b, 2)
        block = add_low(own, join(got_a, got_b, x_at))
        keep, leave = x_parts(block, x_at)
        part = add_low(keep, flip_dp(leave, 1))
    else:
        own_keep, own_leave = x_parts(own, x_at)
        a_keep, a_leave = x_parts(far_a, x_at)
        b_keep, b_leave = x_parts(far_b, x_at)
        got_b, got_a = flip_dp(a_leave, 1), flip_dp(b_leave, 1)
        got_own = flip_dp(own_leave, 1)
        far_a, far_b = add_low(a_keep, got_a), add_low(b_keep, got_b)
        far_a, far_b = flip_mp(far_a, 2), flip_mp(far_b, 2)
        part = add_low(add_low(own_keep, got_own), join(far_a, far_b, x_at))
    return sum_over_z(part, z_at)


def sum_vectors(rows, place):
    for flip, bit, at in place:
        size = rows.shape[0] // 2
        keep = lax.dynamic_slice_in_dim(rows, at * size, size, 0)
        leave = lax.dynamic_slice_in_dim(rows, (1 - at) * size, size, 0)
        rows = keep + flip(leave, bit)
    return rows[0]


def by_device(parts):
    shaped = parts.reshape(2, 2, 2, 2, 2, -1)
    return shaped.transpose(4, 3, 2, 0, 1, 5).reshape(32, -1)


def gather_all(row, order):
    index = lax.axis_index("dp") * GRID_MP + lax.axis_index("mp")
    full = jnp.zeros((GRID_DP * GRID_MP, row.shape[1]), row.dtype)
    rows = row
    for flip, bit, shift in order:
        other = flip(rows, bit)
        low = (index >> shift) & 1
        rows = jnp.where(low == 0, jnp.concatenate([rows, other]), jnp.concatenate([other, rows]))
    return rows


def norm_stats(values):
    center = values - jnp.mean(values, axis=-1, keepdims=True)
    spread = jnp.mean(center * center, axis=-1, keepdims=True)
    scale = lax.rsqrt(spread + EPS)
    return center * scale, scale


def norm_back(normal, scale, grad, gain_vec):
    scaled = grad * gain_vec
    mean_e = jnp.mean(scaled, axis=-1, keepdims=True)
    mean_en = jnp.mean(scaled * normal, axis=-1, keepdims=True)
    return scale * (scaled - mean_e - normal * mean_en)


def dot_f32(left, right, dims):
    return lax.dot_general(left, right, (dims, ((), ())), preferred_element_type=F32)


def body_rows(
    tokens,
    segment_ids,
    time_steps,
    w_qkv,
    b_qv,
    w_out,
    b_out,
    gain_one,
    shift_one,
    w_up,
    b_up,
    w_down,
    b_down,
    gain_two,
    shift_two,
    w_time,
    b_time,
    cotangent,
):
    dp_at, mp_at = lax.axis_index("dp"), lax.axis_index("mp")
    x_at, z_at = dp_at % 2, dp_at // 2
    y_at, c_at = mp_at // 2, mp_at % 2
    width_local = w_qkv.shape[2]
    row = lambda v: v.astype(F32)[None, :]

    qkv_w = fetch_pieces(w_qkv, 2, x_at)
    qkv_w = [w.reshape(D, -1) for w in qkv_w]
    vectors = fetch_vectors(b_qv, x_at)
    vec_qkv = [
        jnp.concatenate([v[0], jnp.zeros_like(v[0]), v[1]]).astype(F32)[None, :] for v in vectors
    ]
    out_w = fetch_pieces(w_out, 0, x_at)
    up_w = fetch_pieces(w_up, 1, x_at)
    vec_up = [v.astype(F32) for v in fetch_vectors(b_up[None, :], x_at)]
    down_w = fetch_pieces(w_down, 0, x_at)
    pieces = range(len(qkv_w))

    own_step = lax.dynamic_slice_in_dim(time_steps, mp_at, 1, 0)
    segment_row = lax.dynamic_index_in_dim(segment_ids, mp_at, 0, keepdims=False)
    features = time_features(own_step)
    embed_row = jnp.dot(features, w_time.astype(F32), precision=HIGHEST_PRECISION)
    embed_row = embed_row + b_time.astype(F32)[None, :]
    hidden_in = tokens.astype(F32) + embed_row
    hidden_low = hidden_in.astype(BF16)

    qkv, context, log_total = [], [], []
    for i in pieces:
        product = dot_f32(hidden_low, qkv_w[i], ((1,), (0,)))
        qkv.append((product + vec_qkv[i]).astype(BF16))
        ctx, lse = attend_forward((qkv[i], segment_row))
        context.append(ctx)
        log_total.append(lse)
    attn_out = row(b_out)
    for i in pieces:
        attn_out = attn_out + dot_f32(context[i], out_w[i], ((1,), (0,)))
    normal_one, scale_one = norm_stats(hidden_in + attn_out)
    mid_norm = normal_one * row(gain_one) + row(shift_one)
    mid_low = mid_norm.astype(BF16)

    act, slope = [], []
    for i in pieces:
        pre = dot_f32(mid_low, up_w[i], ((1,), (0,))) + vec_up[i]
        phi = 0.5 * (1.0 + lax.erf(pre * math.sqrt(0.5)))
        act.append((pre * phi).astype(BF16))
        slope.append((phi + pre * jnp.exp(-0.5 * pre * pre) * (1.0 / math.sqrt(2.0 * math.pi))).astype(BF16))
    ffn = row(b_down)
    for i in pieces:
        ffn = ffn + dot_f32(act[i], down_w[i], ((1,), (0,)))
    normal_two, scale_two = norm_stats(mid_norm + ffn)
    out_rows = (normal_two * row(gain_two) + row(shift_two)).astype(BF16)

    cot = cotangent.astype(F32)
    grad_two = norm_back(normal_two, scale_two, cot, row(gain_two))
    branch_two = grad_two.astype(BF16)
    d_pre = []
    for i in pieces:
        d_act = dot_f32(branch_two, down_w[i], ((1,), (1,)))
        d_pre.append((d_act * slope[i].astype(F32)).astype(BF16))

    def grad_maker(left, rights):
        def make(i, extra):
            total = dot_f32(left, rights[i], ((0,), (0,)))
            if extra is not None:
                total = total + extra.astype(F32)
            return total.astype(BF16)

        return make

    g_w_down = reduce_pieces(grad_maker(branch_two, act), join_halves, x_at, z_at, True)
    g_w_up = reduce_pieces(grad_maker(mid_low, d_pre), join_halves, x_at, z_at, False)
    d_mid = grad_two
    for i in pieces:
        d_mid = d_mid + dot_f32(d_pre[i], up_w[i], ((1,), (1,)))
    grad_one = norm_back(normal_one, scale_one, d_mid, row(gain_one))
    branch_one = grad_one.astype(BF16)
    d_context = [
        dot_f32(branch_one, out_w[i], ((1,), (1,))).astype(BF16) for i in pieces
    ]
    g_w_out = reduce_pieces(grad_maker(branch_one, context), join_halves, x_at, z_at, True)
    d_qkv = [
        attend_backward((qkv[i], d_context[i], log_total[i], segment_row)) for i in pieces
    ]

    def join_qkv(part_a, part_b, at):
        lead = part_a.shape[:-1]
        joined = join_halves(part_a.reshape(lead + (3, -1)), part_b.reshape(lead + (3, -1)), at)
        return joined.reshape(lead + (3 * width_local,))

    g_w_qkv = reduce_pieces(grad_maker(hidden_low, d_qkv), join_qkv, x_at, z_at, False)
    grad_tokens = grad_one
    for i in pieces:
        grad_tokens = grad_tokens + dot_f32(d_qkv[i], qkv_w[i], ((1,), (1,)))

    place = (
        (flip_mp, 1, c_at),
        (flip_mp, 2, y_at),
        (flip_dp, 1, x_at),
        (flip_dp, 4, z_at // 2),
        (flip_dp, 2, z_at % 2),
    )
    sum_rows = lambda v: jnp.sum(v.astype(F32), axis=0)

    def natural(parts):
        far = join_halves(parts[2], parts[3], x_at)
        near_far = join_halves(parts[4], parts[5], x_at)
        stacked = jnp.stack([parts[0], parts[1], far, near_far])
        return jnp.stack([stacked[i ^ mp_at] for i in range(4)])

    def spread(vector):
        return vector.reshape(8, 4, -1)

    def spread_blocks(blocks):
        return blocks.reshape(4, 8, -1).transpose(1, 0, 2)

    rows_two = jnp.concatenate(
        [
            spread(sum_rows(branch_two)),
            spread(sum_rows(cot * normal_two)),
            spread(sum_rows(cot)),
            spread_blocks(natural([sum_rows(v) for v in d_pre])),
        ],
        axis=2,
    )
    rows_two = sum_vectors(by_device(rows_two), place)
    rows_one = jnp.concatenate(
        [
            spread(sum_rows(branch_one)),
            spread(sum_rows(d_mid * normal_one)),
            spread(sum_rows(d_mid)),
        ],
        axis=2,
    )
    rows_one = sum_vectors(by_device(rows_one), place)
    qkv_sums = [sum_rows(v).reshape(3, -1) for v in d_qkv]
    rows_qkv = jnp.concatenate(
        [spread_blocks(natural([v[i] for v in qkv_sums])) for i in (0, 2)], axis=2
    )
    rows_qkv = sum_vectors(by_device(rows_qkv), place)

    grad_embed = jnp.sum(grad_tokens, axis=0, keepdims=True)
    tail_row = jnp.concatenate(
        [grad_embed, jnp.broadcast_to(own_step.astype(F32)[None, :], (1, 128))], axis=1
    )
    order = (
        (flip_mp, 1, 0),
        (flip_mp, 2, 1),
        (flip_dp, 1, 2),
        (flip_dp, 2, 3),
        (flip_dp, 4, 4),
    )
    all_rows = gather_all(tail_row, order)
    device_at = dp_at * GRID_MP + mp_at
    span = D // (GRID_DP * GRID_MP)
    all_grads = all_rows[:, :D]
    all_features = time_features(all_rows[:, D])
    own_features = lax.dynamic_slice_in_dim(all_features, device_at * span, span, 1)
    g_w_time = jnp.dot(own_features.T, all_grads, precision=HIGHEST_PRECISION)
    g_b_time = lax.dynamic_slice_in_dim(jnp.sum(all_grads, axis=0), device_at * span, span, 0)

    return (
        out_rows,
        grad_tokens,
        g_w_qkv.reshape(-1, 3, width_local),
        rows_qkv.reshape(2, 1, -1),
        g_w_out.T,
        rows_one[:span],
        rows_one[span : 2 * span],
        rows_one[2 * span :],
        g_w_up,
        rows_two[None, 3 * span :],
        g_w_down.T,
        rows_two[:span],
        rows_two[span : 2 * span],
        rows_two[2 * span : 3 * span],
        g_w_time,
        g_b_time,
    )


def solution(mesh):
    placed = (
        P(("dp", "mp"), None),
        P("dp", None),
        P("dp"),
        P(None, None, "mp"),
        P(None, "mp"),
        P("mp", None),
        P(),
        P(),
        P(),
        P(None, "mp"),
        P("mp"),
        P("mp", None),
        P(),
        P(),
        P(),
        P(),
        P(),
        P(("dp", "mp"), None),
    )
    def body(*args):
        whole_rows = args[0].shape[0] == LEN and mesh.shape["dp"] == GRID_DP and mesh.shape["mp"] == GRID_MP
        return (body_rows if whole_rows else body_split)(*args)

    return jax.shard_map(
        body,
        mesh=mesh,
        in_specs=placed,
        out_specs=(
            P(("dp", "mp"), None),
            P(("dp", "mp"), None),
            P("dp", None, "mp"),
            P(None, "mp", "dp"),
            P("mp", "dp"),
            P(("dp", "mp")),
            P(("dp", "mp")),
            P(("dp", "mp")),
            P("dp", "mp"),
            P("mp", "dp"),
            P("mp", "dp"),
            P(("dp", "mp")),
            P(("dp", "mp")),
            P(("dp", "mp")),
            P(("dp", "mp"), None),
            P(("dp", "mp")),
        ),
        check_vma=False,
    )
```

```python
import functools
import math

import jax
import jax.numpy as jnp
from jax import lax
from jax.experimental import pallas as pl
from jax.experimental.pallas import tpu as pltpu
from jax.sharding import PartitionSpec as P

D = 1024
HEAD_DIM = 64
LEN = 1024


EPS = 1e-05
HIGHEST_PRECISION = lax.Precision.HIGHEST


def time_features(step_values):
    half_width = D // 2
    ladder = jnp.arange(half_width, dtype=jnp.float32)
    frequency = jnp.exp(ladder * (-math.log(10000.0) / half_width))
    angles = step_values.astype(jnp.float32)[:, None] * frequency[None, :]
    return jnp.concatenate([jnp.sin(angles), jnp.cos(angles)], axis=1)


def layer_norm(values, gain_vec, shift_vec):
    center = values - jnp.mean(values, axis=-1, keepdims=True)
    spread = jnp.mean(center * center, axis=-1, keepdims=True)
    return center * lax.rsqrt(spread + EPS) * gain_vec + shift_vec


def exact_gelu(values):
    return jax.nn.gelu(values, approximate=False)


def project_qkv(hidden_full, w_qkv, b_qv):
    width_local = w_qkv.shape[2]
    w_flat = w_qkv.reshape(w_qkv.shape[0], 3 * width_local)
    bias_row = jnp.concatenate([b_qv[0], jnp.zeros((width_local,), b_qv.dtype), b_qv[1]]).astype(
        jnp.float32
    )
    product = jnp.dot(hidden_full, w_flat, preferred_element_type=jnp.float32)
    return (product + bias_row[None, :]).astype(jnp.bfloat16)


def head_parts(qkv_seq):
    width_local = qkv_seq.shape[1] // 3
    head_local = width_local // HEAD_DIM
    shaped = qkv_seq.reshape(qkv_seq.shape[0], 3, head_local, HEAD_DIM)
    return (shaped[:, 0], shaped[:, 1], shaped[:, 2])


def masked_scores(queries, keys_part, segment_row):
    scores = jnp.einsum("qhd,khd->hqk", queries, keys_part, preferred_element_type=jnp.float32)
    scores = scores * (1.0 / math.sqrt(HEAD_DIM))
    same_doc = segment_row[:, None] == segment_row[None, :]
    return jnp.where(same_doc[None, :, :], scores, -1e30)


def attend_forward(inputs):
    qkv_seq, segment_row = inputs
    queries, keys_part, values_part = head_parts(qkv_seq)
    masked = masked_scores(queries, keys_part, segment_row)
    top_score = jnp.max(masked, axis=2, keepdims=True)
    weights_exp = jnp.exp(masked - top_score)
    totals = jnp.sum(weights_exp, axis=2, keepdims=True)
    probability = weights_exp / totals
    context = jnp.einsum(
        "hqk,khd->qhd",
        probability.astype(jnp.bfloat16),
        values_part,
        preferred_element_type=jnp.float32,
    )
    log_total = (top_score + jnp.log(totals))[:, :, 0]
    return (context.reshape(qkv_seq.shape[0], -1).astype(jnp.bfloat16), log_total)


def attend_backward(inputs):
    qkv_seq, grad_seq, log_total, segment_row = inputs
    queries, keys_part, values_part = head_parts(qkv_seq)
    masked = masked_scores(queries, keys_part, segment_row)
    probability = jnp.exp(masked - log_total[:, :, None])
    grad_heads = grad_seq.reshape(grad_seq.shape[0], -1, HEAD_DIM)
    d_values = jnp.einsum(
        "hqk,qhd->khd",
        probability.astype(jnp.bfloat16),
        grad_heads,
        preferred_element_type=jnp.float32,
    )
    d_probs = jnp.einsum(
        "qhd,khd->hqk", grad_heads, values_part, preferred_element_type=jnp.float32
    )
    row_terms = jnp.sum(probability * d_probs, axis=2, keepdims=True)
    d_scores = (probability * (d_probs - row_terms)).astype(jnp.bfloat16)
    score_scale = 1.0 / math.sqrt(HEAD_DIM)
    d_queries = (
        jnp.einsum("hqk,khd->qhd", d_scores, keys_part, preferred_element_type=jnp.float32)
        * score_scale
    )
    d_keys = (
        jnp.einsum("hqk,qhd->khd", d_scores, queries, preferred_element_type=jnp.float32)
        * score_scale
    )
    stacked = jnp.stack([d_queries, d_keys, d_values], axis=1)
    return stacked.reshape(qkv_seq.shape[0], -1).astype(jnp.bfloat16)


def body_split(
    tokens,
    segment_ids,
    time_steps,
    w_qkv,
    b_qv,
    w_out,
    b_out,
    gain_one,
    shift_one,
    w_up,
    b_up,
    w_down,
    b_down,
    gain_two,
    shift_two,
    w_time,
    b_time,
    cotangent,
):
    row_count = tokens.shape[0]
    seq_local = time_steps.shape[0]
    width_local = w_qkv.shape[2]
    gain_one_f = gain_one.astype(jnp.float32)
    shift_one_f = shift_one.astype(jnp.float32)
    gain_two_f = gain_two.astype(jnp.float32)
    shift_two_f = shift_two.astype(jnp.float32)
    w_flat = w_qkv.reshape(D, 3 * width_local)
    features = time_features(time_steps)
    embed_rows = jnp.dot(features, w_time.astype(jnp.float32), precision=HIGHEST_PRECISION)
    embed_rows = embed_rows + b_time.astype(jnp.float32)[None, :]
    row_seq = (lax.axis_index("mp") * row_count + jnp.arange(row_count, dtype=jnp.int32)) // LEN
    selector = (row_seq[:, None] == jnp.arange(seq_local, dtype=jnp.int32)[None, :]).astype(
        jnp.float32
    )
    hidden_in = tokens.astype(jnp.float32) + jnp.dot(
        selector, embed_rows, precision=HIGHEST_PRECISION
    )
    hidden_low = hidden_in.astype(jnp.bfloat16)
    hidden_full = lax.all_gather(hidden_low, "mp", axis=0, tiled=True)
    qkv_full = project_qkv(hidden_full, w_qkv, b_qv)
    ctx_blocks, log_totals = lax.map(
        attend_forward, (qkv_full.reshape(seq_local, LEN, 3 * width_local), segment_ids)
    )
    context = ctx_blocks.reshape(seq_local * LEN, width_local)
    rows_in = context
    attn_sum = lax.psum_scatter(
        jnp.dot(rows_in, w_out, preferred_element_type=jnp.float32).astype(jnp.bfloat16),
        "mp",
        scatter_dimension=0,
        tiled=True,
    ).astype(jnp.float32)
    attn_out = attn_sum + b_out.astype(jnp.float32)[None, :]
    mid_in = hidden_in + attn_out
    mid_norm = layer_norm(mid_in, gain_one_f, shift_one_f)
    mid_low = mid_norm.astype(jnp.bfloat16)
    mid_full = lax.all_gather(mid_low, "mp", axis=0, tiled=True)
    pre_act = (
        jnp.dot(mid_full, w_up, preferred_element_type=jnp.float32)
        + b_up.astype(jnp.float32)[None, :]
    )
    activated = exact_gelu(pre_act).astype(jnp.bfloat16)
    rows_in = activated
    ffn_part = lax.psum_scatter(
        jnp.dot(rows_in, w_down, preferred_element_type=jnp.float32).astype(jnp.bfloat16),
        "mp",
        scatter_dimension=0,
        tiled=True,
    ).astype(jnp.float32)
    out_in = mid_norm + ffn_part + b_down.astype(jnp.float32)[None, :]
    out_rows, out_back = jax.vjp(layer_norm, out_in, gain_two_f, shift_two_f)
    grad_two, grad_gain_two, grad_shift_two = out_back(cotangent.astype(jnp.float32))
    branch_two = grad_two.astype(jnp.bfloat16)
    grad_b_down = jnp.sum(branch_two.astype(jnp.float32), axis=0)
    gelu_value, gelu_back = jax.vjp(exact_gelu, pre_act)
    cot_full = lax.all_gather(branch_two, "mp", axis=0, tiled=True)
    d_act = jnp.dot(cot_full, w_down.T, preferred_element_type=jnp.float32)
    grad_w_down = jnp.dot(activated.T, cot_full, preferred_element_type=jnp.float32)
    d_pre = gelu_back(d_act)[0].astype(jnp.bfloat16)
    grad_w_up = jnp.dot(mid_full.T, d_pre, preferred_element_type=jnp.float32)
    grad_b_up = jnp.sum(d_pre.astype(jnp.float32), axis=0)
    rows_in = d_pre
    d_mid_part = lax.psum_scatter(
        jnp.dot(rows_in, w_up.T, preferred_element_type=jnp.float32).astype(jnp.bfloat16),
        "mp",
        scatter_dimension=0,
        tiled=True,
    ).astype(jnp.float32)
    mid_value, mid_back = jax.vjp(layer_norm, mid_in, gain_one_f, shift_one_f)
    grad_one, grad_gain_one, grad_shift_one = mid_back(grad_two + d_mid_part)
    branch_one = grad_one.astype(jnp.bfloat16)
    grad_b_out = jnp.sum(branch_one.astype(jnp.float32), axis=0)
    cot_attn = lax.all_gather(branch_one, "mp", axis=0, tiled=True)
    d_context = jnp.dot(cot_attn, w_out.T, preferred_element_type=jnp.float32).astype(jnp.bfloat16)
    grad_w_out = jnp.dot(context.T, cot_attn, preferred_element_type=jnp.float32)
    grad_blocks = lax.map(
        attend_backward,
        (
            qkv_full.reshape(seq_local, LEN, 3 * width_local),
            d_context.reshape(seq_local, LEN, width_local),
            log_totals,
            segment_ids,
        ),
    )
    d_qkv = grad_blocks.reshape(seq_local * LEN, 3 * width_local)
    grad_w_qkv = jnp.dot(hidden_full.T, d_qkv, preferred_element_type=jnp.float32).reshape(
        D, 3, width_local
    )
    qkv_sums = jnp.sum(d_qkv.astype(jnp.float32), axis=0).reshape(3, width_local)
    grad_b_qv = jnp.stack([qkv_sums[0], qkv_sums[2]]).reshape(2, 1, width_local)
    rows_in = d_qkv
    input_part = lax.psum_scatter(
        jnp.dot(rows_in, w_flat.T, preferred_element_type=jnp.float32).astype(jnp.bfloat16),
        "mp",
        scatter_dimension=0,
        tiled=True,
    ).astype(jnp.float32)
    grad_tokens = grad_one + input_part
    grad_embed = jnp.dot(selector.T, grad_tokens, precision=HIGHEST_PRECISION)
    grad_w_time = jnp.dot(features.T, grad_embed, precision=HIGHEST_PRECISION)
    grad_b_time = jnp.sum(grad_embed, axis=0)
    sharded = (
        lax.psum_scatter(
            grad_w_qkv.astype(jnp.bfloat16), "dp", scatter_dimension=0, tiled=True
        ).astype(jnp.float32),
        lax.psum_scatter(
            grad_b_qv.astype(jnp.bfloat16), "dp", scatter_dimension=2, tiled=True
        ).astype(jnp.float32),
        lax.psum_scatter(
            grad_w_out.astype(jnp.bfloat16), "dp", scatter_dimension=1, tiled=True
        ).astype(jnp.float32),
        lax.psum_scatter(
            grad_w_up.astype(jnp.bfloat16), "dp", scatter_dimension=0, tiled=True
        ).astype(jnp.float32),
        lax.psum_scatter(
            grad_b_up.reshape(1, -1).astype(jnp.bfloat16), "dp", scatter_dimension=1, tiled=True
        ).astype(jnp.float32),
        lax.psum_scatter(
            grad_w_down.astype(jnp.bfloat16), "dp", scatter_dimension=1, tiled=True
        ).astype(jnp.float32),
    )
    shared = (
        lax.psum_scatter(grad_w_time, ("dp", "mp"), scatter_dimension=0, tiled=True),
        lax.psum_scatter(grad_b_time, ("dp", "mp"), scatter_dimension=0, tiled=True),
        lax.psum_scatter(grad_gain_one, ("dp", "mp"), scatter_dimension=0, tiled=True),
        lax.psum_scatter(grad_shift_one, ("dp", "mp"), scatter_dimension=0, tiled=True),
        lax.psum_scatter(grad_gain_two, ("dp", "mp"), scatter_dimension=0, tiled=True),
        lax.psum_scatter(grad_shift_two, ("dp", "mp"), scatter_dimension=0, tiled=True),
        lax.psum_scatter(grad_b_out, ("dp", "mp"), scatter_dimension=0, tiled=True),
        lax.psum_scatter(grad_b_down, ("dp", "mp"), scatter_dimension=0, tiled=True),
    )
    return (
        out_rows.astype(jnp.bfloat16),
        grad_tokens,
        sharded[0],
        sharded[1],
        sharded[2],
        shared[6],
        shared[2],
        shared[3],
        sharded[3],
        sharded[4],
        sharded[5],
        shared[7],
        shared[4],
        shared[5],
        shared[0],
        shared[1],
    )


GRID_DP = 8
GRID_MP = 4
HALF = 2
UNIT = 128
F32 = jnp.float32
BF16 = jnp.bfloat16
TILE_F = 512
TILE_B = 256
ROWS = 256
GRAIN = 256
STEP = 128
FAR = -(2.0**100)
NN = (((1,), (0,)), ((), ()))
NT = (((1,), (1,)), ((), ()))


def dot(left, right, dims=NN):
    return lax.dot_general(left, right, dims, preferred_element_type=F32)


def flip_mp(values, bit):
    return lax.ppermute(values, "mp", [(i, i ^ bit) for i in range(GRID_MP)])


def flip_dp(values, bit):
    return lax.ppermute(values, "dp", [(i, i ^ bit) for i in range(GRID_DP)])


def after(values, others):
    return lax.optimization_barrier((values, others))[0]


def half_of(values, which, axis):
    size = values.shape[axis] // 2
    return lax.dynamic_slice_in_dim(values, which * size, size, axis)


def whole(shape):
    return pl.BlockSpec(shape, lambda *_: (0,) * len(shape))


def struct(shape, kind=BF16):
    return jax.ShapeDtypeStruct(shape, kind)


def cost(flops, moved):
    return pl.CostEstimate(flops=int(flops), bytes_accessed=int(moved), transcendentals=0)


def fetch(own, axis, x_at, wait_for):
    half = half_of(own, x_at, axis)
    if wait_for is not None:
        half = after(half, wait_for)
    far_a = flip_mp(half, 2)
    far_b = flip_dp(far_a, 1)
    near = flip_mp(own, 1)
    return [own, near, far_a, flip_mp(far_a, 1), far_b, flip_mp(far_b, 1)]


def fetch_rows(own, x_at):
    near, far = flip_mp(own, 1), flip_mp(own, 2)
    near_far = flip_mp(far, 1)
    cut = lambda v, at: half_of(v, at, 1)
    order = ((own, near), (far, near_far))
    first = [cut(v, at) for v in order[0] for at in (x_at, 1 - x_at)]
    return first + [cut(v, at) for at in (x_at, 1 - x_at) for v in order[1]]


def piece_specs(shape, column, skip):
    def spec(which):
        def index(*args):
            at = 0 if which is None else args[skip][which]
            return (0, at) if column else (at, 0)

        return pl.BlockSpec(shape, index)

    return [spec(w) for w in (0, 1, 0, 1, None, None, None, None)]


def eight(pieces):
    own, near, far_a, near_a, far_b, near_b = pieces
    return [own, own, near, near, far_a, near_a, far_b, near_b]


def mark_segments(segment_row):
    lane = jnp.arange(UNIT, dtype=jnp.int32)[None, :]
    hot = segment_row[:, None] == (lane % HEAD_DIM)
    used = (lane % HEAD_DIM) < 8
    return (
        jnp.where(hot & used, 1.0, 0.0).astype(BF16),
        jnp.where(used & ~hot, FAR, 0.0).astype(BF16),
    )


def windows(segment_row, tile):
    first, last = segment_row[::tile], segment_row[tile - 1 :: tile]
    low = jnp.sum(segment_row[None, :] < first[:, None], axis=1) // STEP * STEP
    high = jnp.sum(segment_row[None, :] <= last[:, None], axis=1)
    count = jnp.maximum((high - low + GRAIN - 1) // GRAIN, tile // GRAIN)
    low = jnp.minimum(low, LEN - count * GRAIN)
    return jnp.stack([low, count]).astype(jnp.int32)


def variants(count, tile, run):
    for n in range(tile // GRAIN, LEN // GRAIN + 1):

        @pl.when(count == n)
        def _(n=n):
            run(n * GRAIN)


def lanes_at(at, base=0):
    return pl.ds(pl.multiple_of(base + at * UNIT, UNIT), UNIT)


def attend_kernel(
    win_ref, info_ref, x_ref, *refs
):
    weights, (bias_ref, hotq_ref, hotk_ref, qkv_ref, ctx_ref, lse_ref, w_ref, kx) = refs[:6], refs[6:]
    unit, step = pl.program_id(0), pl.program_id(1)

    @pl.when((unit == 0) & (step == 0))
    def _():
        for j in range(3):
            for u in range(HALF):
                at = (2 * j + u) * UNIT
                w_ref[:, at : at + UNIT] = weights[3 * u + j][...]
        for r in range(LEN // ROWS):
            rows = slice(r * ROWS, (r + 1) * ROWS)
            qkv_ref[rows, :] = (dot(x_ref[rows, :], w_ref[...]) + bias_ref[...]).astype(BF16)

    @pl.when(step == 0)
    def _():
        lane = lax.broadcasted_iota(jnp.int32, (LEN, UNIT), 1)
        keys = qkv_ref[:, lanes_at(unit, 2 * UNIT)]
        for h in range(HALF):
            kx[h] = jnp.where((lane // HEAD_DIM) == h, keys, hotk_ref[...])

    lane = lax.broadcasted_iota(jnp.int32, (TILE_F, UNIT), 1)
    rows = pl.ds(pl.multiple_of(step * TILE_F, TILE_F), TILE_F)
    queries = qkv_ref[rows, lanes_at(unit)] * jnp.asarray(1.0 / math.sqrt(HEAD_DIM), BF16)
    start = pl.multiple_of(win_ref[0, step], STEP)

    def run(width):
        window = pl.ds(start, width)
        values = qkv_ref[window, lanes_at(unit, 4 * UNIT)]
        scores = [
            dot(
                jnp.where((lane // HEAD_DIM) == h, queries, hotq_ref[...]), kx[h, window, :], NT
            )
            for h in range(HALF)
        ]
        outs = []
        for h in range(HALF):
            top = jnp.max(scores[h], axis=1, keepdims=True)
            weight = jnp.exp(scores[h] - top)
            total = jnp.sum(weight, axis=1, keepdims=True)
            outs.append(dot(weight.astype(BF16), values) * (1.0 / total))
            lse_ref[0, h : h + 1, :] = (top + jnp.log(total)).T
        ctx_ref[...] = jnp.where(lane < HEAD_DIM, outs[0], outs[1]).astype(BF16)

    variants(win_ref[1, step], TILE_F, run)


def attend_pair(win, info, hidden_low, pair, far, bias, hotq, hotk):
    def w_spec(j, u):
        if far:
            return pl.BlockSpec((D, UNIT), lambda n, i, win, info: (0, j))
        return pl.BlockSpec((D, UNIT), lambda n, i, win, info: (0, 2 * j + info[u]))

    return pl.pallas_call(
        attend_kernel,
        out_shape=(
            struct((LEN, 6 * UNIT)),
            struct((LEN, 2 * UNIT)),
            struct((HALF, 8, LEN), F32),
            struct((D, 6 * UNIT)),
        ),
        grid_spec=pltpu.PrefetchScalarGridSpec(
            num_scalar_prefetch=2,
            grid=(HALF, LEN // TILE_F),
            in_specs=[whole((LEN, D))]
            + [w_spec(j, u) for u in range(HALF) for j in range(3)]
            + [
                whole((1, 6 * UNIT)),
                pl.BlockSpec((TILE_F, UNIT), lambda n, i, win, info: (i, 0)),
                whole((LEN, UNIT)),
            ],
            out_specs=[
                whole((LEN, 6 * UNIT)),
                pl.BlockSpec((TILE_F, UNIT), lambda n, i, win, info: (i, n)),
                pl.BlockSpec((1, 8, TILE_F), lambda n, i, win, info: (n, 0, i)),
                whole((D, 6 * UNIT)),
            ],
            scratch_shapes=[pltpu.VMEM((HALF, LEN, UNIT), BF16)],
        ),
        cost_estimate=cost(6e9, 8e6),
        name="attend",
    )(win, info, hidden_low, *[pair[u] for u in range(HALF) for _ in range(3)], bias, hotq, hotk)


def attend_back_kernel(
    win_ref,
    qkv_ref,
    hotq_ref,
    hotk_ref,
    branch_ref,
    wout_ref,
    ctx_ref,
    lse_ref,
    out_ref,
    sum_ref,
    kx,
    kt,
    grads,
    dk,
    dv,
):
    unit, step = pl.program_id(0), pl.program_id(1)
    scale = jnp.asarray(1.0 / math.sqrt(HEAD_DIM), BF16)

    @pl.when((unit == 0) & (step == 0))
    def _():
        for r in range(LEN // ROWS):
            rows = slice(r * ROWS, (r + 1) * ROWS)
            grads[rows, :] = dot(branch_ref[rows, :], wout_ref[...], NT).astype(BF16)

    @pl.when(step == 0)
    def _():
        lane = lax.broadcasted_iota(jnp.int32, (LEN, UNIT), 1)
        keys = qkv_ref[:, lanes_at(unit, 2 * UNIT)]
        for h in range(HALF):
            kx[h] = jnp.where((lane // HEAD_DIM) == h, keys, hotk_ref[...])
        kt[...] = (keys * scale).T
        dk[...] = jnp.zeros_like(dk)
        dv[...] = jnp.zeros_like(dv)

    lane = lax.broadcasted_iota(jnp.int32, (TILE_B, UNIT), 1)
    rows = pl.ds(pl.multiple_of(step * TILE_B, TILE_B), TILE_B)
    queries = qkv_ref[rows, lanes_at(unit)] * scale
    grad = grads[rows, lanes_at(unit)]
    product = (grad.astype(F32) * ctx_ref[...].astype(F32)).T
    start = pl.multiple_of(win_ref[0, step], STEP)

    def run(width):
        window = pl.ds(start, width)
        values = qkv_ref[window, lanes_at(unit, 4 * UNIT)]
        d_queries, d_keys, d_values = [], [], []
        for h in range(HALF):
            mine = (lane // HEAD_DIM) == h
            q_mine = jnp.where(mine, queries, jnp.zeros_like(queries))
            g_mine = jnp.where(mine, grad, jnp.zeros_like(grad))
            scores = dot(kx[h, window, :], jnp.where(mine, queries, hotq_ref[...]), NT)
            weight = jnp.exp(scores - lse_ref[0, h : h + 1, :])
            d_weight = dot(values, g_mine, NT)
            row_term = jnp.sum(
                product[h * HEAD_DIM : (h + 1) * HEAD_DIM], axis=0, keepdims=True
            )
            d_scores = (weight * (d_weight - row_term)).astype(BF16)
            d_values.append(dot(weight.astype(BF16), g_mine))
            d_keys.append(dot(d_scores, q_mine))
            d_queries.append(dot(kt[h * HEAD_DIM : (h + 1) * HEAD_DIM, window], d_scores))
        dv[window, :] += d_values[0] + d_values[1]
        dk[window, :] += d_keys[0] + d_keys[1]
        out_ref[rows, lanes_at(unit)] = jnp.concatenate(d_queries, 0).T.astype(BF16)

    variants(win_ref[1, step], TILE_B, run)

    @pl.when(step == LEN // TILE_B - 1)
    def _():
        out_ref[:, lanes_at(unit, 2 * UNIT)] = dk[...].astype(BF16)
        out_ref[:, lanes_at(unit, 4 * UNIT)] = dv[...].astype(BF16)

    @pl.when((unit == HALF - 1) & (step == LEN // TILE_B - 1))
    def _():
        total = jnp.sum(out_ref[...].astype(F32), axis=0, keepdims=True)
        sum_ref[...] = jnp.broadcast_to(total, sum_ref.shape)


def attend_back_pair(win, qkv, hotq, hotk, branch_one, wout_all, pair, ctx, lse):
    return pl.pallas_call(
        attend_back_kernel,
        out_shape=(struct((LEN, 6 * UNIT)), struct((8, 6 * UNIT), F32)),
        grid_spec=pltpu.PrefetchScalarGridSpec(
            num_scalar_prefetch=1,
            grid=(HALF, LEN // TILE_B),
            in_specs=[
                whole((LEN, 6 * UNIT)),
                pl.BlockSpec((TILE_B, UNIT), lambda n, i, win: (i, 0)),
                whole((LEN, UNIT)),
                whole((LEN, D)),
                pl.BlockSpec((2 * UNIT, D), lambda n, i, win: (pair, 0)),
                pl.BlockSpec((TILE_B, UNIT), lambda n, i, win: (i, n)),
                pl.BlockSpec((1, 8, TILE_B), lambda n, i, win: (n, 0, i)),
            ],
            out_specs=[whole((LEN, 6 * UNIT)), whole((8, 6 * UNIT))],
            scratch_shapes=[
                pltpu.VMEM((HALF, LEN, UNIT), BF16),
                pltpu.VMEM((UNIT, LEN), BF16),
                pltpu.VMEM((LEN, 2 * UNIT), BF16),
                pltpu.VMEM((LEN, UNIT), F32),
                pltpu.VMEM((LEN, UNIT), F32),
            ],
        ),
        cost_estimate=cost(8e9, 8e6),
        name="attend_back",
    )(win, qkv, hotq, hotk, branch_one, wout_all, ctx, lse)


def norm_of(values):
    center = values - jnp.mean(values, axis=-1, keepdims=True)
    spread = jnp.mean(center * center, axis=-1, keepdims=True)
    scale = lax.rsqrt(spread + EPS)
    return center * scale, scale


def norm_back(normal, scale, grad, gain_row):
    scaled = grad * gain_row
    mean_e = jnp.mean(scaled, axis=-1, keepdims=True)
    mean_en = jnp.mean(scaled * normal, axis=-1, keepdims=True)
    return scale * (scaled - mean_e - normal * mean_en)


def first_norm_kernel(info_ref, tok_ref, *refs):
    ctx_refs, weights, refs = refs[:4], refs[4:12], refs[12:]
    embed_ref, bout_ref, gain_ref, shift_ref, normal_ref, scale_ref, mid_ref, mid_t, hid_t, wout_ref = refs

    @pl.when(pl.program_id(0) == 0)
    def _():
        for j in range(8):
            wout_ref[j * UNIT : (j + 1) * UNIT, :] = weights[j][...]

    hidden = tok_ref[...].astype(F32) + embed_ref[...]
    hid_t[...] = hidden.astype(BF16).T
    total = bout_ref[...]
    for p in range(4):
        total = total + dot(ctx_refs[p][...], wout_ref[2 * p * UNIT : 2 * (p + 1) * UNIT, :])
    normal, scale = norm_of(hidden + total)
    normal_ref[...] = normal
    scale_ref[...] = scale
    mid = (normal * gain_ref[...] + shift_ref[...]).astype(BF16)
    mid_ref[...] = mid
    mid_t[...] = mid.T


def first_norm(info, tokens, contexts, w_out, embed_row, b_out, gain, shift):
    tile = pl.BlockSpec((ROWS, D), lambda i, info: (i, 0))
    column = pl.BlockSpec((D, ROWS), lambda i, info: (0, i))
    return pl.pallas_call(
        first_norm_kernel,
        out_shape=(
            struct((LEN, D), F32),
            struct((LEN, 1), F32),
            struct((LEN, D)),
            struct((D, LEN)),
            struct((D, LEN)),
            struct((D, D)),
        ),
        grid_spec=pltpu.PrefetchScalarGridSpec(
            num_scalar_prefetch=1,
            grid=(LEN // ROWS,),
            in_specs=[tile]
            + [pl.BlockSpec((ROWS, 2 * UNIT), lambda i, info: (i, 0))] * 4
            + piece_specs((UNIT, D), False, 1)
            + [whole((1, D))] * 4,
            out_specs=[
                tile,
                pl.BlockSpec((ROWS, 1), lambda i, info: (i, 0)),
                tile,
                column,
                column,
                whole((D, D)),
            ],
        ),
        cost_estimate=cost(2.2e9, 20e6),
        name="first_norm",
    )(info, tokens, *contexts, *eight(w_out), embed_row, b_out, gain, shift)


def second_norm_kernel(
    ffn_ref, one_ref, cot_ref, gain1, shift1, gain2, shift2, out_ref, grad_ref, low_ref, low_t, sum_ref
):
    @pl.when(pl.program_id(0) == 0)
    def _():
        sum_ref[...] = jnp.zeros_like(sum_ref)

    mid = one_ref[...] * gain1[...] + shift1[...]
    normal, scale = norm_of(mid + ffn_ref[...])
    out_ref[...] = (normal * gain2[...] + shift2[...]).astype(BF16)
    cot = cot_ref[...].astype(F32)
    grad = norm_back(normal, scale, cot, gain2[...])
    grad_ref[...] = grad
    low = grad.astype(BF16)
    low_ref[...] = low
    low_t[...] = low.T
    sums = [jnp.sum(v, axis=0, keepdims=True) for v in (low.astype(F32), cot * normal, cot)]
    for j in range(3):
        sum_ref[j : j + 1, :] += sums[j]


def second_norm(ffn, normal_one, cot, *rows):
    tile = pl.BlockSpec((ROWS, D), lambda i: (i, 0))
    return pl.pallas_call(
        second_norm_kernel,
        out_shape=(
            struct((LEN, D)),
            struct((LEN, D), F32),
            struct((LEN, D)),
            struct((D, LEN)),
            struct((8, D), F32),
        ),
        grid=(LEN // ROWS,),
        in_specs=[tile] * 3 + [whole((1, D))] * 4,
        out_specs=[tile] * 3 + [pl.BlockSpec((D, ROWS), lambda i: (0, i)), whole((8, D))],
        cost_estimate=cost(1e8, 20e6),
        name="second_norm",
    )(ffn, normal_one, cot, *rows)


def first_back_kernel(
    part_ref, grad_ref, one_ref, scale_ref, gain_ref, out_ref, low_ref, low_t, sum_ref
):
    @pl.when(pl.program_id(0) == 0)
    def _():
        sum_ref[...] = jnp.zeros_like(sum_ref)

    d_mid = part_ref[...] + grad_ref[...]
    normal = one_ref[...]
    grad = norm_back(normal, scale_ref[...], d_mid, gain_ref[...])
    out_ref[...] = grad
    low = grad.astype(BF16)
    low_ref[...] = low
    low_t[...] = low.T
    sums = [jnp.sum(v, axis=0, keepdims=True) for v in (low.astype(F32), d_mid * normal, d_mid)]
    for j in range(3):
        sum_ref[j : j + 1, :] += sums[j]


def first_back(part, grad_two, normal_one, scale_one, gain):
    tile = pl.BlockSpec((ROWS, D), lambda i: (i, 0))
    return pl.pallas_call(
        first_back_kernel,
        out_shape=(struct((LEN, D), F32), struct((LEN, D)), struct((D, LEN)), struct((8, D), F32)),
        grid=(LEN // ROWS,),
        in_specs=[tile] * 3 + [pl.BlockSpec((ROWS, 1), lambda i: (i, 0)), whole((1, D))],
        out_specs=[tile, tile, pl.BlockSpec((D, ROWS), lambda i: (0, i)), whole((8, D))],
        cost_estimate=cost(1e8, 20e6),
        name="first_back",
    )(part, grad_two, normal_one, scale_one, gain)


def ffn_kernel(info_ref, mid_ref, *refs):
    up_refs, down_refs, bias_refs = refs[0:2], refs[2:4], refs[4:6]
    into_ref, act_ref, slope_ref, total_ref = refs[6:]
    size = up_refs[0].shape[1]
    for u in range(HALF):
        columns = slice(u * size, (u + 1) * size)
        for r in range(LEN // ROWS):
            rows = slice(r * ROWS, (r + 1) * ROWS)
            pre = dot(mid_ref[rows, :], up_refs[u][...]) + bias_refs[u][...]
            phi = 0.5 * (1.0 + lax.erf(pre * math.sqrt(0.5)))
            bell = jnp.exp(-0.5 * pre * pre) * (1.0 / math.sqrt(2.0 * math.pi))
            act = (pre * phi).astype(BF16)
            act_ref[rows, columns] = act
            slope_ref[rows, columns] = (phi + pre * bell).astype(BF16)
            before = into_ref[rows, :] if u == 0 else total_ref[rows, :]
            total_ref[rows, :] = before + dot(act, down_refs[u][...])


def ffn_pair(info, mid_low, up, down, bias, into, far):
    def spec(shape, u, column):
        if far:
            return whole(shape)
        return pl.BlockSpec(shape, lambda i, info: (0, info[u]) if column else (info[u], 0))

    size = up[0].shape[1] if far else up[0].shape[1] // 2
    return pl.pallas_call(
        ffn_kernel,
        out_shape=(
            struct((LEN, 2 * size)),
            struct((LEN, 2 * size)),
            struct((LEN, D), F32),
        ),
        grid_spec=pltpu.PrefetchScalarGridSpec(
            num_scalar_prefetch=1,
            grid=(1,),
            in_specs=[whole((LEN, D))]
            + [spec((D, size), u, True) for u in range(HALF)]
            + [spec((size, D), u, False) for u in range(HALF)]
            + [whole((1, size))] * 2
            + [whole((LEN, D))],
            out_specs=[whole((LEN, 2 * size)), whole((LEN, 2 * size)), whole((LEN, D))],
        ),
        cost_estimate=cost(4.3e9, 18e6),
        name="ffn",
    )(info, mid_low, *up, *down, *bias, into)


def ffn_back_kernel(info_ref, branch_hbm, *refs):
    down_hbm, up_hbm, slope_hbm, refs = refs[0:6], refs[6:12], refs[12:16], refs[16:]
    pre_refs, total_ref, sum_ref, refs = refs[0:4], refs[4], refs[5], refs[6:]
    branch, down, up, slope, sems = refs
    size = up.shape[2]
    plan = ((0, 0), (0, 1), (1, 0), (1, 1), (2, None), (3, None), (4, None), (5, None))
    first = pltpu.make_async_copy(branch_hbm, branch, sems.at[0])
    first.start()
    copies = []
    for j, (piece, which) in enumerate(plan):
        if which is None:
            down_part, up_part = down_hbm[piece], up_hbm[piece]
        else:
            part = pl.ds(pl.multiple_of(info_ref[which] * size, size), size)
            down_part, up_part = down_hbm[piece].at[part, :], up_hbm[piece].at[:, part]
        group = [
            pltpu.make_async_copy(down_part, down.at[j], sems.at[1 + 3 * j]),
            pltpu.make_async_copy(
                slope_hbm[j // 2].at[:, (j % 2) * size : (j % 2 + 1) * size],
                slope.at[j],
                sems.at[2 + 3 * j],
            ),
            pltpu.make_async_copy(up_part, up.at[j], sems.at[3 + 3 * j]),
        ]
        for copy in group:
            copy.start()
        copies.append(group)
    first.wait()
    for j in range(len(plan)):
        for copy in copies[j]:
            copy.wait()
        columns = slice((j % 2) * size, (j % 2 + 1) * size)
        sums = 0.0
        for r in range(LEN // ROWS):
            rows = slice(r * ROWS, (r + 1) * ROWS)
            d_act = dot(branch[rows, :], down[j], NT)
            d_pre = (d_act * slope[j, rows, :].astype(F32)).astype(BF16)
            pre_refs[j // 2][rows, columns] = d_pre
            sums = sums + jnp.sum(d_pre.astype(F32), axis=0, keepdims=True)
            part = dot(d_pre, up[j], NT)
            if j == 0:
                total_ref[rows, :] = part
            else:
                total_ref[rows, :] += part
        sum_ref[j : j + 1, :] = sums


def ffn_back(info, branch_two, down, up, slopes):
    size = down[2].shape[0]
    hbm = pl.BlockSpec(memory_space=pl.ANY)
    return pl.pallas_call(
        ffn_back_kernel,
        out_shape=(struct((LEN, 2 * size)),) * 4 + (struct((LEN, D), F32), struct((8, size), F32)),
        grid_spec=pltpu.PrefetchScalarGridSpec(
            num_scalar_prefetch=1,
            grid=(1,),
            in_specs=[hbm] * 17,
            out_specs=[whole((LEN, 2 * size))] * 4 + [whole((LEN, D)), whole((8, size))],
            scratch_shapes=[
                pltpu.VMEM((LEN, D), BF16),
                pltpu.VMEM((8, size, D), BF16),
                pltpu.VMEM((8, D, size), BF16),
                pltpu.VMEM((8, LEN, size), BF16),
                pltpu.SemaphoreType.DMA((25,)),
            ],
        ),
        cost_estimate=cost(17e9, 40e6),
        name="ffn_back",
    )(info, branch_two, *down, *up, *slopes)


def grad_columns(refs, group, size, which):
    full, part_a, part_b = refs
    for at in range(0, size, 2 * group):
        yield full, at, at, 2 * group
    for at in range(0, size, 2 * group):
        yield part_a, at + which * group, size + at, group
        yield part_b, at + which * group, size + at + group, group


def grad_send_kernel(group, info_ref, left_ref, *refs):
    *rights, out_ref = refs
    size = rights[0].shape[1]
    left = left_ref[...].reshape(D // 2, LEN)
    for right, source, target, width in grad_columns(rights, group, size, 1):
        out_ref[0, :, target : target + width] = dot(left, right[:, source : source + width]).astype(
            BF16
        )


def left_spec():
    return pl.BlockSpec((4, 1, D // 8, LEN), lambda i, info: (0, i ^ info[0], 0, 0))


def grad_send(info, left_t, near, part_a, part_b, group):
    size = near.shape[1]
    return pl.pallas_call(
        functools.partial(grad_send_kernel, group),
        out_shape=struct((2, D // 2, 2 * size)),
        grid_spec=pltpu.PrefetchScalarGridSpec(
            num_scalar_prefetch=1,
            grid=(2,),
            in_specs=[left_spec()] + [whole((LEN, size))] * 3,
            out_specs=pl.BlockSpec((1, D // 2, 2 * size), lambda i, info: (i, 0, 0)),
        ),
        cost_estimate=cost(4 * D * LEN * size, 10e6),
        name="grad_send",
    )(info, left_t.reshape(4, 2, D // 8, LEN), near, part_a, part_b)


def grad_keep_kernel(group, info_ref, left_ref, *refs):
    rights, got_ref, outs = refs[:3], refs[3], refs[4:]
    size = rights[0].shape[1]
    left = left_ref[...].reshape(D // 2, LEN)
    for side in range(2):

        @pl.when(pl.program_id(0) == side)
        def _():
            for right, source, target, width in grad_columns(rights, group, size, 0):
                total = dot(left, right[:, source : source + width])
                total = total + got_ref[0, :, target : target + width].astype(F32)
                out_ref = outs[side + 2 * (target // size)]
                at = target % size
                out_ref[:, at : at + width] = total.astype(BF16)


def grad_keep(info, left_t, own, part_a, part_b, got, group):
    size = own.shape[1]
    return pl.pallas_call(
        functools.partial(grad_keep_kernel, group),
        out_shape=(struct((D // 2, size)),) * 4,
        grid_spec=pltpu.PrefetchScalarGridSpec(
            num_scalar_prefetch=1,
            grid=(2,),
            in_specs=[left_spec()]
            + [whole((LEN, size))] * 3
            + [pl.BlockSpec((1, D // 2, 2 * size), lambda i, info: (i, 0, 0))],
            out_specs=[whole((D // 2, size))] * 4,
        ),
        cost_estimate=cost(4 * D * LEN * size, 14e6),
        name="grad_keep",
    )(info, left_t.reshape(4, 2, D // 8, LEN), own, part_a, part_b, got)


def swapped(ref, group, rows=slice(None)):
    size = ref.shape[-1]
    return [(at, ref[rows, at ^ group : (at ^ group) + group]) for at in range(0, size, group)]


def add_kernel(group, swap, mine_ref, got_ref, out_ref):
    for at in range(0, mine_ref.shape[1], group):
        source = at ^ group if swap else at
        total = mine_ref[:, at : at + group].astype(F32) + got_ref[:, source : source + group].astype(F32)
        out_ref[:, at : at + group] = total.astype(BF16)


def add_parts(mine, got, group, swap):
    return pl.pallas_call(
        functools.partial(add_kernel, group, swap),
        out_shape=struct(mine.shape),
        cost_estimate=cost(1e6, 3e6),
        name="add_parts",
    )(mine, got)


def split_kernel(group, info_ref, mine_ref, x_ref, y_ref, *out_refs):
    span = mine_ref.shape[0] // 4
    for k in range(4):
        rows = pl.ds(pl.multiple_of((info_ref[2] ^ k) * span, span), span)
        for at in range(0, mine_ref.shape[1], group):
            swap = at ^ group
            total = mine_ref[rows, at : at + group].astype(F32)
            total = total + x_ref[rows, swap : swap + group].astype(F32)
            total = total + y_ref[rows, at : at + group].astype(F32)
            out_refs[k][:, at : at + group] = total.astype(BF16)


def split_z(info, mine, from_x, from_y, group):
    rows, size = mine.shape
    return pl.pallas_call(
        functools.partial(split_kernel, group),
        out_shape=(struct((rows // 4, size)),) * 4,
        grid_spec=pltpu.PrefetchScalarGridSpec(
            num_scalar_prefetch=1,
            grid=(1,),
            in_specs=[whole((rows, size))] * 3,
            out_specs=[whole((rows // 4, size))] * 4,
        ),
        cost_estimate=cost(1e6, 4e6),
        name="split_z",
    )(info, mine, from_x, from_y)


def reduce_parts(info, parts, group, y_first):
    own_keep, own_leave, far_keep, far_leave = parts
    if y_first:
        from_y_leave = flip_mp(far_leave, 2)
        from_y = flip_mp(after(far_keep, from_y_leave), 2)
        from_x = flip_dp(add_parts(own_leave, from_y_leave, group, False), 1)
    else:
        from_x_far = flip_dp(far_leave, 1)
        from_x = flip_dp(after(own_leave, from_x_far), 1)
        from_y = flip_mp(add_parts(far_keep, from_x_far, group, True), 2)
    mine, *others = split_z(info, own_keep, from_x, from_y, group)
    total = mine.astype(F32)
    for k, other in enumerate(others):
        total = total + flip_dp(other, 2 * (k + 1)).astype(F32)
    return total


def natural_columns(values, group, x_at):
    rows = values.shape[0]
    shaped = values.reshape(rows, -1, 2, group)
    return jnp.where(x_at == 0, shaped, shaped[:, :, ::-1]).reshape(rows, -1)


def input_grad_kernel(one_ref, *refs):
    grads, weights, out_ref, sum_ref = refs[:4], refs[4:8], refs[8], refs[9]

    @pl.when(pl.program_id(0) == 0)
    def _():
        sum_ref[...] = jnp.zeros_like(sum_ref)

    total = one_ref[...]
    for p in range(4):
        total = total + dot(grads[p][...], weights[p][...], NT)
    out_ref[...] = total
    sum_ref[0:1, :] += jnp.sum(total, axis=0, keepdims=True)


def input_grad(grad_one, d_qkv, weights):
    tile = pl.BlockSpec((ROWS, D), lambda i: (i, 0))
    width = d_qkv[0].shape[1]
    return pl.pallas_call(
        input_grad_kernel,
        out_shape=(struct((LEN, D), F32), struct((8, D), F32)),
        grid=(LEN // ROWS,),
        in_specs=[tile]
        + [pl.BlockSpec((ROWS, width), lambda i: (i, 0))] * 4
        + [whole((D, width))] * 4,
        out_specs=[tile, whole((8, D))],
        cost_estimate=cost(6.4e9, 20e6),
        name="input_grad",
    )(grad_one, *d_qkv, *weights)


def sum_vectors(rows, place):
    for flip, bit, at in place:
        size = rows.shape[0] // 2
        keep = lax.dynamic_slice_in_dim(rows, at * size, size, 0)
        leave = lax.dynamic_slice_in_dim(rows, (1 - at) * size, size, 0)
        rows = keep + flip(leave, bit)
    return rows[0]


def by_device(parts):
    shaped = parts.reshape(2, 2, 2, 2, 2, -1)
    return shaped.transpose(4, 3, 2, 0, 1, 5).reshape(32, -1)


def gather_rows(rows, order, index):
    for flip, bit, shift in order:
        other = flip(rows, bit)
        low = (index >> shift) & 1
        rows = jnp.where(low == 0, jnp.concatenate([rows, other]), jnp.concatenate([other, rows]))
    return rows


def natural_blocks(halves, x_at, mp_at):
    join = lambda a, b: jnp.where(x_at == 0, jnp.concatenate([a, b]), jnp.concatenate([b, a]))
    stacked = jnp.stack(
        [
            join(halves[0], halves[1]),
            join(halves[2], halves[3]),
            join(halves[4], halves[6]),
            join(halves[5], halves[7]),
        ]
    )
    return jnp.stack([stacked[i ^ mp_at] for i in range(4)])


def body_rows(
    tokens,
    segment_ids,
    time_steps,
    w_qkv,
    b_qv,
    w_out,
    b_out,
    gain_one,
    shift_one,
    w_up,
    b_up,
    w_down,
    b_down,
    gain_two,
    shift_two,
    w_time,
    b_time,
    cotangent,
):
    dp_at, mp_at = lax.axis_index("dp"), lax.axis_index("mp")
    x_at, z_at = dp_at % 2, dp_at // 2
    y_at, c_at = mp_at // 2, mp_at % 2
    info = jnp.stack([x_at, 1 - x_at, z_at, mp_at]).astype(jnp.int32)
    row = lambda v: v.astype(F32)[None, :]
    width = w_qkv.shape[2]
    flat = lambda w: w.reshape(D, -1)

    w_all = fetch(w_qkv, 2, x_at, None)
    qkv_w = [flat(w) for w in w_all]
    out_w = fetch(w_out, 0, x_at, w_all[2])
    up_w = fetch(w_up, 1, x_at, out_w[2])
    down_w = fetch(w_down, 0, x_at, up_w[2])
    qv_rows = [v.astype(F32) for v in fetch_rows(b_qv, x_at)]
    up_rows = [v.astype(F32) for v in fetch_rows(b_up[None, :], x_at)]
    zero = jnp.zeros((1, width // 2), F32)

    own_step = lax.dynamic_slice_in_dim(time_steps, mp_at, 1, 0)
    segment_row = lax.dynamic_index_in_dim(segment_ids, mp_at, 0, keepdims=False)
    features = time_features(own_step)
    embed_row = jnp.dot(features, w_time.astype(F32), precision=HIGHEST_PRECISION)
    embed_row = embed_row + row(b_time)
    hidden_low = (tokens.astype(F32) + embed_row).astype(BF16)
    hotq, hotk = mark_segments(segment_row)
    win_f, win_b = windows(segment_row, TILE_F), windows(segment_row, TILE_B)

    qkv, ctx, lse, qkv_cat = [], [], [], []
    pairs = [(qkv_w[0],) * 2, (qkv_w[1],) * 2, qkv_w[2:4], qkv_w[4:6]]
    for p in range(4):
        first, second = qv_rows[2 * p : 2 * p + 2]
        bias = jnp.concatenate(
            [first[0:1], second[0:1], zero, zero, first[1:2], second[1:2]], axis=1
        )
        parts = attend_pair(win_f, info, hidden_low, pairs[p], p >= 2, bias, hotq, hotk)
        for kept, part in zip((qkv, ctx, lse, qkv_cat), parts):
            kept.append(part)
    normal_one, scale_one, mid_low, mid_t, hidden_t, out_cat = first_norm(
        info, tokens, ctx, out_w, embed_row, row(b_out), row(gain_one), row(shift_one)
    )

    up_pairs = [(up_w[0],) * 2, (up_w[1],) * 2, up_w[2:4], up_w[4:6]]
    down_pairs = [(down_w[0],) * 2, (down_w[1],) * 2, down_w[2:4], down_w[4:6]]
    act, slope = [], []
    ffn = jnp.broadcast_to(row(b_down), (LEN, D))
    for p in range(4):
        act_p, slope_p, ffn = ffn_pair(
            info, mid_low, up_pairs[p], down_pairs[p], up_rows[2 * p : 2 * p + 2], ffn, p >= 2
        )
        act.append(act_p)
        slope.append(slope_p)
    out_rows, grad_two, branch_two, branch_two_t, sums_two = second_norm(
        ffn, normal_one, cotangent, row(gain_one), row(shift_one), row(gain_two), row(shift_two)
    )

    ff_group = act[0].shape[1] // 2
    sent_down = flip_mp(grad_send(info, branch_two_t, act[1], act[2], act[3], ff_group), 1)
    *d_pre, d_mid, sums_up = ffn_back(info, branch_two, down_w, up_w, slope)
    parts_down = grad_keep(info, branch_two_t, act[0], act[2], act[3], sent_down, ff_group)
    g_w_down = reduce_parts(info, parts_down, ff_group, True)
    sent_up = flip_mp(grad_send(info, mid_t, d_pre[1], d_pre[2], d_pre[3], ff_group), 1)
    grad_one, branch_one, branch_one_t, sums_one = first_back(
        d_mid, grad_two, normal_one, scale_one, row(gain_one)
    )
    parts_up = grad_keep(info, mid_t, d_pre[0], d_pre[2], d_pre[3], sent_up, ff_group)
    g_w_up = reduce_parts(info, parts_up, ff_group, False)
    sent_out = flip_mp(grad_send(info, branch_one_t, ctx[1], ctx[2], ctx[3], UNIT), 1)
    d_qkv, qkv_sums = [None] * 4, [None] * 4
    for p in (1, 2, 3, 0):
        d_qkv[p], qkv_sums[p] = attend_back_pair(
            win_b, qkv[p], hotq, hotk, branch_one, out_cat, p, ctx[p], lse[p]
        )
        if p == 1:
            parts_out = grad_keep(info, branch_one_t, ctx[0], ctx[2], ctx[3], sent_out, UNIT)
            g_w_out = reduce_parts(info, parts_out, UNIT, True)
        if p == 3:
            sent_qkv = flip_mp(grad_send(info, hidden_t, d_qkv[1], d_qkv[2], d_qkv[3], UNIT), 1)
    parts_qkv = grad_keep(info, hidden_t, d_qkv[0], d_qkv[2], d_qkv[3], sent_qkv, UNIT)
    g_w_qkv = reduce_parts(info, parts_qkv, UNIT, False)
    grad_tokens, sums_in = input_grad(grad_one, d_qkv, qkv_cat)

    place = (
        (flip_mp, 1, c_at),
        (flip_mp, 2, y_at),
        (flip_dp, 1, x_at),
        (flip_dp, 4, z_at // 2),
        (flip_dp, 2, z_at % 2),
    )
    spread = lambda v: v.reshape(8, 4, -1)
    spread_blocks = lambda b: b.reshape(4, 8, -1).transpose(1, 0, 2)
    rows_two = jnp.concatenate(
        [spread(sums_two[j]) for j in range(3)]
        + [spread_blocks(natural_blocks([sums_up[j] for j in range(8)], x_at, mp_at))],
        axis=2,
    )
    rows_two = sum_vectors(by_device(rows_two), place)
    rows_one = jnp.concatenate([spread(sums_one[j]) for j in range(3)], axis=2)
    rows_one = sum_vectors(by_device(rows_one), place)
    rows_qkv = []
    for j in (0, 2):
        halves = [
            qkv_sums[p][0, (2 * j + u) * UNIT : (2 * j + u + 1) * UNIT]
            for p in range(4)
            for u in range(HALF)
        ]
        rows_qkv.append(spread_blocks(natural_blocks(halves, x_at, mp_at)))
    rows_qkv = sum_vectors(by_device(jnp.concatenate(rows_qkv, axis=2)), place)

    tail_row = jnp.concatenate(
        [sums_in[0:1], jnp.broadcast_to(own_step.astype(F32)[None, :], (1, UNIT))], axis=1
    )
    order = (
        (flip_mp, 1, 0),
        (flip_mp, 2, 1),
        (flip_dp, 1, 2),
        (flip_dp, 2, 3),
        (flip_dp, 4, 4),
    )
    device_at = dp_at * GRID_MP + mp_at
    all_rows = gather_rows(tail_row, order, device_at)
    span = D // (GRID_DP * GRID_MP)
    all_grads = all_rows[:, :D]
    own_features = lax.dynamic_slice_in_dim(
        time_features(all_rows[:, D]), device_at * span, span, 1
    )
    g_w_time = jnp.dot(own_features.T, all_grads, precision=HIGHEST_PRECISION)
    g_b_time = lax.dynamic_slice_in_dim(jnp.sum(all_grads, axis=0), device_at * span, span, 0)

    return (
        out_rows,
        grad_tokens,
        natural_columns(g_w_qkv, UNIT, x_at).reshape(-1, 3, width),
        rows_qkv.reshape(2, 1, -1),
        natural_columns(g_w_out, UNIT, x_at).T,
        rows_one[:span],
        rows_one[span : 2 * span],
        rows_one[2 * span :],
        natural_columns(g_w_up, ff_group, x_at),
        rows_two[None, 3 * span :],
        natural_columns(g_w_down, ff_group, x_at).T,
        rows_two[:span],
        rows_two[span : 2 * span],
        rows_two[2 * span : 3 * span],
        g_w_time,
        g_b_time,
    )


def solution(mesh):
    placed = (
        P(("dp", "mp"), None),
        P("dp", None),
        P("dp"),
        P(None, None, "mp"),
        P(None, "mp"),
        P("mp", None),
        P(),
        P(),
        P(),
        P(None, "mp"),
        P("mp"),
        P("mp", None),
        P(),
        P(),
        P(),
        P(),
        P(),
        P(("dp", "mp"), None),
    )
    def body(*args):
        whole_rows = args[0].shape[0] == LEN and (mesh.shape["dp"], mesh.shape["mp"]) == (GRID_DP, GRID_MP)
        return (body_rows if whole_rows else body_split)(*args)

    return jax.shard_map(
        body,
        mesh=mesh,
        in_specs=placed,
        out_specs=(
            P(("dp", "mp"), None),
            P(("dp", "mp"), None),
            P("dp", None, "mp"),
            P(None, "mp", "dp"),
            P("mp", "dp"),
            P(("dp", "mp")),
            P(("dp", "mp")),
            P(("dp", "mp")),
            P("dp", "mp"),
            P("mp", "dp"),
            P("mp", "dp"),
            P(("dp", "mp")),
            P(("dp", "mp")),
            P(("dp", "mp")),
            P(("dp", "mp"), None),
            P(("dp", "mp")),
        ),
        check_vma=False,
    )
```

```python
import functools
import math
from typing import NamedTuple

import jax
import jax.numpy as jnp
from jax import lax
from jax.experimental import pallas as pl
from jax.experimental.pallas import tpu as pltpu
from jax.sharding import PartitionSpec as P


D = 1024
HEAD_DIM = 64
LEN = 1024


EPS = 1e-05
HIGHEST_PRECISION = lax.Precision.HIGHEST


def time_features(step_values):
    half_width = D // 2
    ladder = jnp.arange(half_width, dtype=jnp.float32)
    frequency = jnp.exp(ladder * (-math.log(10000.0) / half_width))
    angles = step_values.astype(jnp.float32)[:, None] * frequency[None, :]
    return jnp.concatenate([jnp.sin(angles), jnp.cos(angles)], axis=1)


def layer_norm(values, gain_vec, shift_vec):
    center = values - jnp.mean(values, axis=-1, keepdims=True)
    spread = jnp.mean(center * center, axis=-1, keepdims=True)
    return center * lax.rsqrt(spread + EPS) * gain_vec + shift_vec


def exact_gelu(values):
    return jax.nn.gelu(values, approximate=False)


def project_qkv(hidden_full, w_qkv, b_qv):
    width_local = w_qkv.shape[2]
    w_flat = w_qkv.reshape(w_qkv.shape[0], 3 * width_local)
    bias_row = jnp.concatenate([b_qv[0], jnp.zeros((width_local,), b_qv.dtype), b_qv[1]]).astype(
        jnp.float32
    )
    product = jnp.dot(hidden_full, w_flat, preferred_element_type=jnp.float32)
    return (product + bias_row[None, :]).astype(jnp.bfloat16)


def head_parts(qkv_seq):
    width_local = qkv_seq.shape[1] // 3
    head_local = width_local // HEAD_DIM
    shaped = qkv_seq.reshape(qkv_seq.shape[0], 3, head_local, HEAD_DIM)
    return (shaped[:, 0], shaped[:, 1], shaped[:, 2])


def masked_scores(queries, keys_part, segment_row):
    scores = jnp.einsum("qhd,khd->hqk", queries, keys_part, preferred_element_type=jnp.float32)
    scores = scores * (1.0 / math.sqrt(HEAD_DIM))
    same_doc = segment_row[:, None] == segment_row[None, :]
    return jnp.where(same_doc[None, :, :], scores, -1e30)


def attend_forward(inputs):
    qkv_seq, segment_row = inputs
    queries, keys_part, values_part = head_parts(qkv_seq)
    masked = masked_scores(queries, keys_part, segment_row)
    top_score = jnp.max(masked, axis=2, keepdims=True)
    weights_exp = jnp.exp(masked - top_score)
    totals = jnp.sum(weights_exp, axis=2, keepdims=True)
    probability = weights_exp / totals
    context = jnp.einsum(
        "hqk,khd->qhd",
        probability.astype(jnp.bfloat16),
        values_part,
        preferred_element_type=jnp.float32,
    )
    log_total = (top_score + jnp.log(totals))[:, :, 0]
    return (context.reshape(qkv_seq.shape[0], -1).astype(jnp.bfloat16), log_total)


def attend_backward(inputs):
    qkv_seq, grad_seq, log_total, segment_row = inputs
    queries, keys_part, values_part = head_parts(qkv_seq)
    masked = masked_scores(queries, keys_part, segment_row)
    probability = jnp.exp(masked - log_total[:, :, None])
    grad_heads = grad_seq.reshape(grad_seq.shape[0], -1, HEAD_DIM)
    d_values = jnp.einsum(
        "hqk,qhd->khd",
        probability.astype(jnp.bfloat16),
        grad_heads,
        preferred_element_type=jnp.float32,
    )
    d_probs = jnp.einsum(
        "qhd,khd->hqk", grad_heads, values_part, preferred_element_type=jnp.float32
    )
    row_terms = jnp.sum(probability * d_probs, axis=2, keepdims=True)
    d_scores = (probability * (d_probs - row_terms)).astype(jnp.bfloat16)
    score_scale = 1.0 / math.sqrt(HEAD_DIM)
    d_queries = (
        jnp.einsum("hqk,khd->qhd", d_scores, keys_part, preferred_element_type=jnp.float32)
        * score_scale
    )
    d_keys = (
        jnp.einsum("hqk,qhd->khd", d_scores, queries, preferred_element_type=jnp.float32)
        * score_scale
    )
    stacked = jnp.stack([d_queries, d_keys, d_values], axis=1)
    return stacked.reshape(qkv_seq.shape[0], -1).astype(jnp.bfloat16)


def body_split(
    tokens,
    segment_ids,
    time_steps,
    w_qkv,
    b_qv,
    w_out,
    b_out,
    gain_one,
    shift_one,
    w_up,
    b_up,
    w_down,
    b_down,
    gain_two,
    shift_two,
    w_time,
    b_time,
    cotangent,
):
    row_count = tokens.shape[0]
    seq_local = time_steps.shape[0]
    width_local = w_qkv.shape[2]
    gain_one_f = gain_one.astype(jnp.float32)
    shift_one_f = shift_one.astype(jnp.float32)
    gain_two_f = gain_two.astype(jnp.float32)
    shift_two_f = shift_two.astype(jnp.float32)
    w_flat = w_qkv.reshape(D, 3 * width_local)
    features = time_features(time_steps)
    embed_rows = jnp.dot(features, w_time.astype(jnp.float32), precision=HIGHEST_PRECISION)
    embed_rows = embed_rows + b_time.astype(jnp.float32)[None, :]
    row_seq = (lax.axis_index("mp") * row_count + jnp.arange(row_count, dtype=jnp.int32)) // LEN
    selector = (row_seq[:, None] == jnp.arange(seq_local, dtype=jnp.int32)[None, :]).astype(
        jnp.float32
    )
    hidden_in = tokens.astype(jnp.float32) + jnp.dot(
        selector, embed_rows, precision=HIGHEST_PRECISION
    )
    hidden_low = hidden_in.astype(jnp.bfloat16)
    hidden_full = lax.all_gather(hidden_low, "mp", axis=0, tiled=True)
    qkv_full = project_qkv(hidden_full, w_qkv, b_qv)
    ctx_blocks, log_totals = lax.map(
        attend_forward, (qkv_full.reshape(seq_local, LEN, 3 * width_local), segment_ids)
    )
    context = ctx_blocks.reshape(seq_local * LEN, width_local)
    rows_in = context
    attn_sum = lax.psum_scatter(
        jnp.dot(rows_in, w_out, preferred_element_type=jnp.float32).astype(jnp.bfloat16),
        "mp",
        scatter_dimension=0,
        tiled=True,
    ).astype(jnp.float32)
    attn_out = attn_sum + b_out.astype(jnp.float32)[None, :]
    mid_in = hidden_in + attn_out
    mid_norm = layer_norm(mid_in, gain_one_f, shift_one_f)
    mid_low = mid_norm.astype(jnp.bfloat16)
    mid_full = lax.all_gather(mid_low, "mp", axis=0, tiled=True)
    pre_act = (
        jnp.dot(mid_full, w_up, preferred_element_type=jnp.float32)
        + b_up.astype(jnp.float32)[None, :]
    )
    activated = exact_gelu(pre_act).astype(jnp.bfloat16)
    rows_in = activated
    ffn_part = lax.psum_scatter(
        jnp.dot(rows_in, w_down, preferred_element_type=jnp.float32).astype(jnp.bfloat16),
        "mp",
        scatter_dimension=0,
        tiled=True,
    ).astype(jnp.float32)
    out_in = mid_norm + ffn_part + b_down.astype(jnp.float32)[None, :]
    out_rows, out_back = jax.vjp(layer_norm, out_in, gain_two_f, shift_two_f)
    grad_two, grad_gain_two, grad_shift_two = out_back(cotangent.astype(jnp.float32))
    branch_two = grad_two.astype(jnp.bfloat16)
    grad_b_down = jnp.sum(branch_two.astype(jnp.float32), axis=0)
    _, gelu_back = jax.vjp(exact_gelu, pre_act)
    cot_full = lax.all_gather(branch_two, "mp", axis=0, tiled=True)
    d_act = jnp.dot(cot_full, w_down.T, preferred_element_type=jnp.float32)
    grad_w_down = jnp.dot(activated.T, cot_full, preferred_element_type=jnp.float32)
    d_pre = gelu_back(d_act)[0].astype(jnp.bfloat16)
    grad_w_up = jnp.dot(mid_full.T, d_pre, preferred_element_type=jnp.float32)
    grad_b_up = jnp.sum(d_pre.astype(jnp.float32), axis=0)
    rows_in = d_pre
    d_mid_part = lax.psum_scatter(
        jnp.dot(rows_in, w_up.T, preferred_element_type=jnp.float32).astype(jnp.bfloat16),
        "mp",
        scatter_dimension=0,
        tiled=True,
    ).astype(jnp.float32)
    _, mid_back = jax.vjp(layer_norm, mid_in, gain_one_f, shift_one_f)
    grad_one, grad_gain_one, grad_shift_one = mid_back(grad_two + d_mid_part)
    branch_one = grad_one.astype(jnp.bfloat16)
    grad_b_out = jnp.sum(branch_one.astype(jnp.float32), axis=0)
    cot_attn = lax.all_gather(branch_one, "mp", axis=0, tiled=True)
    d_context = jnp.dot(cot_attn, w_out.T, preferred_element_type=jnp.float32).astype(jnp.bfloat16)
    grad_w_out = jnp.dot(context.T, cot_attn, preferred_element_type=jnp.float32)
    grad_blocks = lax.map(
        attend_backward,
        (
            qkv_full.reshape(seq_local, LEN, 3 * width_local),
            d_context.reshape(seq_local, LEN, width_local),
            log_totals,
            segment_ids,
        ),
    )
    d_qkv = grad_blocks.reshape(seq_local * LEN, 3 * width_local)
    grad_w_qkv = jnp.dot(hidden_full.T, d_qkv, preferred_element_type=jnp.float32).reshape(
        D, 3, width_local
    )
    qkv_sums = jnp.sum(d_qkv.astype(jnp.float32), axis=0).reshape(3, width_local)
    grad_b_qv = jnp.stack([qkv_sums[0], qkv_sums[2]]).reshape(2, 1, width_local)
    rows_in = d_qkv
    input_part = lax.psum_scatter(
        jnp.dot(rows_in, w_flat.T, preferred_element_type=jnp.float32).astype(jnp.bfloat16),
        "mp",
        scatter_dimension=0,
        tiled=True,
    ).astype(jnp.float32)
    grad_tokens = grad_one + input_part
    grad_embed = jnp.dot(selector.T, grad_tokens, precision=HIGHEST_PRECISION)
    grad_w_time = jnp.dot(features.T, grad_embed, precision=HIGHEST_PRECISION)
    grad_b_time = jnp.sum(grad_embed, axis=0)
    sharded = (
        lax.psum_scatter(
            grad_w_qkv.astype(jnp.bfloat16), "dp", scatter_dimension=0, tiled=True
        ).astype(jnp.float32),
        lax.psum_scatter(
            grad_b_qv.astype(jnp.bfloat16), "dp", scatter_dimension=2, tiled=True
        ).astype(jnp.float32),
        lax.psum_scatter(
            grad_w_out.astype(jnp.bfloat16), "dp", scatter_dimension=1, tiled=True
        ).astype(jnp.float32),
        lax.psum_scatter(
            grad_w_up.astype(jnp.bfloat16), "dp", scatter_dimension=0, tiled=True
        ).astype(jnp.float32),
        lax.psum_scatter(
            grad_b_up.reshape(1, -1).astype(jnp.bfloat16), "dp", scatter_dimension=1, tiled=True
        ).astype(jnp.float32),
        lax.psum_scatter(
            grad_w_down.astype(jnp.bfloat16), "dp", scatter_dimension=1, tiled=True
        ).astype(jnp.float32),
    )
    shared = (
        lax.psum_scatter(grad_w_time, ("dp", "mp"), scatter_dimension=0, tiled=True),
        lax.psum_scatter(grad_b_time, ("dp", "mp"), scatter_dimension=0, tiled=True),
        lax.psum_scatter(grad_gain_one, ("dp", "mp"), scatter_dimension=0, tiled=True),
        lax.psum_scatter(grad_shift_one, ("dp", "mp"), scatter_dimension=0, tiled=True),
        lax.psum_scatter(grad_gain_two, ("dp", "mp"), scatter_dimension=0, tiled=True),
        lax.psum_scatter(grad_shift_two, ("dp", "mp"), scatter_dimension=0, tiled=True),
        lax.psum_scatter(grad_b_out, ("dp", "mp"), scatter_dimension=0, tiled=True),
        lax.psum_scatter(grad_b_down, ("dp", "mp"), scatter_dimension=0, tiled=True),
    )
    return (
        out_rows.astype(jnp.bfloat16),
        grad_tokens,
        sharded[0],
        sharded[1],
        sharded[2],
        shared[6],
        shared[2],
        shared[3],
        sharded[3],
        sharded[4],
        sharded[5],
        shared[7],
        shared[4],
        shared[5],
        shared[0],
        shared[1],
    )


GRID_DP = 8
GRID_MP = 4
HALF = 2
UNIT = 128
F32 = jnp.float32
BF16 = jnp.bfloat16
TILE_F = 512
TILE_B = 256
ROWS = 256
GRAIN = 256
STEP = 128
FAR = -(2.0**100)
NN = (((1,), (0,)), ((), ()))
NT = (((1,), (1,)), ((), ()))


def dot(left, right, dims=NN):
    return lax.dot_general(left, right, dims, preferred_element_type=F32)


def half_of(values, which, axis):
    size = values.shape[axis] // 2
    return lax.dynamic_slice_in_dim(values, which * size, size, axis)


def whole(shape):
    return pl.BlockSpec(shape, lambda *_: (0,) * len(shape))


def struct(shape, kind=BF16):
    return jax.ShapeDtypeStruct(shape, kind)


def cost(flops, moved):
    return pl.CostEstimate(flops=int(flops), bytes_accessed=int(moved), transcendentals=0)


def send_mp(values, bit):
    return lax.ppermute(values, "mp", [(i, i ^ bit) for i in range(GRID_MP)])


def send_dp(values, bit):
    return lax.ppermute(values, "dp", [(i, i ^ bit) for i in range(GRID_DP)])


def fetch(own, first_half):
    near = send_mp(own, 1)
    far_a = send_mp(first_half, 2)
    near_a = send_mp(far_a, 1)
    far_b = send_dp(far_a, 1)
    near_b = send_mp(far_b, 1)
    return [own, near, far_a, near_a, far_b, near_b]


def pack_heads_kernel(info_ref, qkv_ref, out_ref, both_ref, first_ref):
    for u in range(HALF):
        for j in range(3):
            at = pl.ds(pl.multiple_of(info_ref[u] * UNIT, UNIT), UNIT)
            both_ref[u, j * UNIT : (j + 1) * UNIT, :] = qkv_ref[j, :, at].T
        at = pl.ds(pl.multiple_of(info_ref[u] * UNIT, UNIT), UNIT)
        both_ref[u, 3 * UNIT :, :] = out_ref[at, :]
    first_ref[...] = both_ref[0]


def pack_heads(info, w_qkv, w_out):
    return pl.pallas_call(
        pack_heads_kernel,
        out_shape=(struct((HALF, 4 * UNIT, D)), struct((4 * UNIT, D))),
        grid_spec=pltpu.PrefetchScalarGridSpec(
            num_scalar_prefetch=1,
            grid=(1,),
            in_specs=[whole((3, D, 2 * UNIT)), whole((2 * UNIT, D))],
            out_specs=[whole((HALF, 4 * UNIT, D)), whole((4 * UNIT, D))],
        ),
        cost_estimate=cost(1e6, 5e6),
    )(info, w_qkv.transpose(1, 0, 2), w_out)


def pack_units_kernel(info_ref, up_ref, down_ref, up_both, up_first, down_both, down_first):
    step = pl.program_id(0)
    up = up_ref[...].T
    up_both[0] = up
    down_both[0] = down_ref[...]

    @pl.when(step == 0)
    def _():
        up_first[...] = up
        down_first[...] = down_ref[...]


def pack_units(info, w_up, w_down):
    size = w_down.shape[0] // 2
    return pl.pallas_call(
        pack_units_kernel,
        out_shape=(struct((HALF, size, D)), struct((size, D))) * 2,
        grid_spec=pltpu.PrefetchScalarGridSpec(
            num_scalar_prefetch=1,
            grid=(HALF,),
            in_specs=[
                pl.BlockSpec((D, size), lambda i, info: (0, info[i])),
                pl.BlockSpec((size, D), lambda i, info: (info[i], 0)),
            ],
            out_specs=[pl.BlockSpec((1, size, D), lambda i, info: (i, 0, 0)), whole((size, D))] * 2,
        ),
        cost_estimate=cost(1e6, 10e6),
    )(info, w_up, w_down)


def fetch_bias(own, x_at):
    packed = jnp.concatenate(own, axis=1)
    near, far = send_mp(packed, 1), send_mp(packed, 2)
    near_far = send_mp(far, 1)
    order = [(packed, x_at), (packed, 1 - x_at), (near, x_at), (near, 1 - x_at)]
    order += [(v, at) for at in (x_at, 1 - x_at) for v in (far, near_far)]
    pieces, start = [], 0
    for row in own:
        size = row.shape[1]
        pieces.append(
            [half_of(v[:, start : start + size], at, 1).astype(F32) for v, at in order]
        )
        start += size
    return pieces


def half_specs(rows, block):
    both = [pl.BlockSpec((1, rows, D), lambda *_, u=u: (u, block, 0)) for u in range(HALF)]
    return both * 2 + [pl.BlockSpec((rows, D), lambda *_: (block, 0))] * 4


def eight(pieces):
    own, near, far_a, near_a, far_b, near_b = pieces
    return [own, own, near, near, far_a, near_a, far_b, near_b]


def pair_specs(rows, block, pair):
    return half_specs(rows, block)[2 * pair : 2 * pair + 2]


def pair_of(pieces, pair):
    return eight(pieces)[2 * pair : 2 * pair + 2]


def rows_of(ref):
    return ref[...].reshape(-1, D)


def mark_segments(segment_row):
    lane = jnp.arange(UNIT, dtype=jnp.int32)[None, :]
    hot = segment_row[:, None] == (lane % HEAD_DIM)
    used = (lane % HEAD_DIM) < 8
    return (
        jnp.where(hot & used, 1.0, 0.0).astype(BF16),
        jnp.where(used & ~hot, FAR, 0.0).astype(BF16),
    )


def windows(segment_row, tile):
    first, last = segment_row[::tile], segment_row[tile - 1 :: tile]
    low = jnp.sum(segment_row[None, :] < first[:, None], axis=1) // STEP * STEP
    high = jnp.sum(segment_row[None, :] <= last[:, None], axis=1)
    count = jnp.maximum((high - low + GRAIN - 1) // GRAIN, tile // GRAIN)
    low = jnp.minimum(low, LEN - count * GRAIN)
    return jnp.stack([low, count]).astype(jnp.int32)


def variants(count, tile, run):
    for n in range(tile // GRAIN, LEN // GRAIN + 1):

        @pl.when(count == n)
        def _(n=n):
            run(n * GRAIN)


def lanes_at(at, base=0):
    return pl.ds(pl.multiple_of(base + at * UNIT, UNIT), UNIT)


def attend_kernel(
    win_ref, x_ref, *refs
):
    weights, (bias_ref, hotq_ref, hotk_ref, qkv_ref, ctx_ref, lse_ref, w_ref, kx) = refs[:2], refs[2:]
    unit, step = pl.program_id(0), pl.program_id(1)

    @pl.when((unit == 0) & (step == 0))
    def _():
        for u in range(HALF):
            part = rows_of(weights[u])
            for j in range(3):
                at = (2 * j + u) * UNIT
                w_ref[at : at + UNIT, :] = part[j * UNIT : (j + 1) * UNIT]
        for r in range(LEN // ROWS):
            rows = slice(r * ROWS, (r + 1) * ROWS)
            qkv_ref[rows, :] = (dot(x_ref[rows, :], w_ref[...], NT) + bias_ref[...]).astype(BF16)

    @pl.when(step == 0)
    def _():
        lane = lax.broadcasted_iota(jnp.int32, (LEN, UNIT), 1)
        keys = qkv_ref[:, lanes_at(unit, 2 * UNIT)]
        for h in range(HALF):
            kx[h] = jnp.where((lane // HEAD_DIM) == h, keys, hotk_ref[...])

    lane = lax.broadcasted_iota(jnp.int32, (TILE_F, UNIT), 1)
    rows = pl.ds(pl.multiple_of(step * TILE_F, TILE_F), TILE_F)
    queries = qkv_ref[rows, lanes_at(unit)] * jnp.asarray(1.0 / math.sqrt(HEAD_DIM), BF16)
    start = pl.multiple_of(win_ref[0, step], STEP)

    def run(width):
        window = pl.ds(start, width)
        values = qkv_ref[window, lanes_at(unit, 4 * UNIT)]
        scores = [
            dot(
                jnp.where((lane // HEAD_DIM) == h, queries, hotq_ref[...]), kx[h, window, :], NT
            )
            for h in range(HALF)
        ]
        outs = []
        for h in range(HALF):
            top = jnp.max(scores[h], axis=1, keepdims=True)
            weight = jnp.exp(scores[h] - top)
            total = jnp.sum(weight, axis=1, keepdims=True)
            outs.append(dot(weight.astype(BF16), values) * (1.0 / total))
            lse_ref[0, h : h + 1, :] = (top + jnp.log(total)).T
        ctx_ref[...] = jnp.where(lane < HEAD_DIM, outs[0], outs[1]).astype(BF16)

    variants(win_ref[1, step], TILE_F, run)


def attend_pair(win, hidden_low, heads, pair, bias, hotq, hotk):
    return pl.pallas_call(
        attend_kernel,
        out_shape=(
            struct((LEN, 6 * UNIT)),
            struct((LEN, 2 * UNIT)),
            struct((HALF, 8, LEN), F32),
            struct((6 * UNIT, D)),
        ),
        grid_spec=pltpu.PrefetchScalarGridSpec(
            num_scalar_prefetch=1,
            grid=(HALF, LEN // TILE_F),
            in_specs=[whole((LEN, D))]
            + pair_specs(4 * UNIT, 0, pair)
            + [
                whole((1, 6 * UNIT)),
                pl.BlockSpec((TILE_F, UNIT), lambda n, i, win: (i, 0)),
                whole((LEN, UNIT)),
            ],
            out_specs=[
                whole((LEN, 6 * UNIT)),
                pl.BlockSpec((TILE_F, UNIT), lambda n, i, win: (i, n)),
                pl.BlockSpec((1, 8, TILE_F), lambda n, i, win: (n, 0, i)),
                whole((6 * UNIT, D)),
            ],
            scratch_shapes=[pltpu.VMEM((HALF, LEN, UNIT), BF16)],
        ),
        cost_estimate=cost(6e9, 8e6),
    )(win, hidden_low, *pair_of(heads, pair), bias, hotq, hotk)


def attend_back_kernel(
    win_ref,
    qkv_ref,
    hotq_ref,
    hotk_ref,
    branch_ref,
    wout_ref,
    ctx_ref,
    lse_ref,
    out_ref,
    sum_ref,
    kx,
    kt,
    grads,
    dk,
    dv,
):
    unit, step = pl.program_id(0), pl.program_id(1)
    scale = jnp.asarray(1.0 / math.sqrt(HEAD_DIM), BF16)

    @pl.when((unit == 0) & (step == 0))
    def _():
        for r in range(LEN // ROWS):
            rows = slice(r * ROWS, (r + 1) * ROWS)
            grads[rows, :] = dot(branch_ref[rows, :], wout_ref[...], NT).astype(BF16)

    @pl.when(step == 0)
    def _():
        lane = lax.broadcasted_iota(jnp.int32, (LEN, UNIT), 1)
        keys = qkv_ref[:, lanes_at(unit, 2 * UNIT)]
        for h in range(HALF):
            kx[h] = jnp.where((lane // HEAD_DIM) == h, keys, hotk_ref[...])
        kt[...] = (keys * scale).T
        dk[...] = jnp.zeros_like(dk)
        dv[...] = jnp.zeros_like(dv)

    lane = lax.broadcasted_iota(jnp.int32, (TILE_B, UNIT), 1)
    rows = pl.ds(pl.multiple_of(step * TILE_B, TILE_B), TILE_B)
    queries = qkv_ref[rows, lanes_at(unit)] * scale
    grad = grads[rows, lanes_at(unit)]
    product = (grad.astype(F32) * ctx_ref[...].astype(F32)).T
    start = pl.multiple_of(win_ref[0, step], STEP)

    def run(width):
        window = pl.ds(start, width)
        values = qkv_ref[window, lanes_at(unit, 4 * UNIT)]
        d_queries, d_keys, d_values = [], [], []
        for h in range(HALF):
            mine = (lane // HEAD_DIM) == h
            q_mine = jnp.where(mine, queries, jnp.zeros_like(queries))
            g_mine = jnp.where(mine, grad, jnp.zeros_like(grad))
            scores = dot(kx[h, window, :], jnp.where(mine, queries, hotq_ref[...]), NT)
            weight = jnp.exp(scores - lse_ref[0, h : h + 1, :])
            d_weight = dot(values, g_mine, NT)
            row_term = jnp.sum(
                product[h * HEAD_DIM : (h + 1) * HEAD_DIM], axis=0, keepdims=True
            )
            d_scores = (weight * (d_weight - row_term)).astype(BF16)
            d_values.append(dot(weight.astype(BF16), g_mine))
            d_keys.append(dot(d_scores, q_mine))
            d_queries.append(dot(kt[h * HEAD_DIM : (h + 1) * HEAD_DIM, window], d_scores))
        dv[window, :] += d_values[0] + d_values[1]
        dk[window, :] += d_keys[0] + d_keys[1]
        out_ref[rows, lanes_at(unit)] = jnp.concatenate(d_queries, 0).T.astype(BF16)

    variants(win_ref[1, step], TILE_B, run)

    @pl.when(step == LEN // TILE_B - 1)
    def _():
        out_ref[:, lanes_at(unit, 2 * UNIT)] = dk[...].astype(BF16)
        out_ref[:, lanes_at(unit, 4 * UNIT)] = dv[...].astype(BF16)

    @pl.when((unit == HALF - 1) & (step == LEN // TILE_B - 1))
    def _():
        total = jnp.sum(out_ref[...].astype(F32), axis=0, keepdims=True)
        sum_ref[...] = jnp.broadcast_to(total, sum_ref.shape)


def attend_back_pair(win, qkv, hotq, hotk, branch_one, wout_all, pair, ctx, lse):
    return pl.pallas_call(
        attend_back_kernel,
        out_shape=(struct((LEN, 6 * UNIT)), struct((8, 6 * UNIT), F32)),
        grid_spec=pltpu.PrefetchScalarGridSpec(
            num_scalar_prefetch=1,
            grid=(HALF, LEN // TILE_B),
            in_specs=[
                whole((LEN, 6 * UNIT)),
                pl.BlockSpec((TILE_B, UNIT), lambda n, i, win: (i, 0)),
                whole((LEN, UNIT)),
                whole((LEN, D)),
                pl.BlockSpec((2 * UNIT, D), lambda n, i, win: (pair, 0)),
                pl.BlockSpec((TILE_B, UNIT), lambda n, i, win: (i, n)),
                pl.BlockSpec((1, 8, TILE_B), lambda n, i, win: (n, 0, i)),
            ],
            out_specs=[whole((LEN, 6 * UNIT)), whole((8, 6 * UNIT))],
            scratch_shapes=[
                pltpu.VMEM((HALF, LEN, UNIT), BF16),
                pltpu.VMEM((UNIT, LEN), BF16),
                pltpu.VMEM((LEN, 2 * UNIT), BF16),
                pltpu.VMEM((LEN, UNIT), F32),
                pltpu.VMEM((LEN, UNIT), F32),
            ],
        ),
        cost_estimate=cost(8e9, 8e6),
    )(win, qkv, hotq, hotk, branch_one, wout_all, ctx, lse)


def norm_of(values):
    center = values - jnp.mean(values, axis=-1, keepdims=True)
    spread = jnp.mean(center * center, axis=-1, keepdims=True)
    scale = lax.rsqrt(spread + EPS)
    return center * scale, scale


def norm_back(normal, scale, grad, gain_row):
    scaled = grad * gain_row
    mean_e = jnp.mean(scaled, axis=-1, keepdims=True)
    mean_en = jnp.mean(scaled * normal, axis=-1, keepdims=True)
    return scale * (scaled - mean_e - normal * mean_en)


def first_norm_kernel(tok_ref, *refs):
    ctx_refs, weights, refs = refs[:4], refs[4:12], refs[12:]
    embed_ref, bout_ref, gain_ref, shift_ref, normal_ref, scale_ref, mid_ref, mid_t, hid_t, wout_ref = refs

    @pl.when(pl.program_id(0) == 0)
    def _():
        for j in range(8):
            wout_ref[j * UNIT : (j + 1) * UNIT, :] = rows_of(weights[j])

    hidden = tok_ref[...].astype(F32) + embed_ref[...]
    hid_t[...] = hidden.astype(BF16).T
    total = bout_ref[...]
    for p in range(4):
        total = total + dot(ctx_refs[p][...], wout_ref[2 * p * UNIT : 2 * (p + 1) * UNIT, :])
    normal, scale = norm_of(hidden + total)
    normal_ref[...] = normal
    scale_ref[...] = scale
    mid = (normal * gain_ref[...] + shift_ref[...]).astype(BF16)
    mid_ref[...] = mid
    mid_t[...] = mid.T


def first_norm(tokens, contexts, heads, embed_row, b_out, gain, shift):
    tile = pl.BlockSpec((ROWS, D), lambda i: (i, 0))
    column = pl.BlockSpec((D, ROWS), lambda i: (0, i))
    return pl.pallas_call(
        first_norm_kernel,
        out_shape=(
            struct((LEN, D), F32),
            struct((LEN, 1), F32),
            struct((LEN, D)),
            struct((D, LEN)),
            struct((D, LEN)),
            struct((D, D)),
        ),
        grid=(LEN // ROWS,),
        in_specs=[tile]
        + [pl.BlockSpec((ROWS, 2 * UNIT), lambda i: (i, 0))] * 4
        + half_specs(UNIT, 3)
        + [whole((1, D))] * 4,
        out_specs=[
            tile,
            pl.BlockSpec((ROWS, 1), lambda i: (i, 0)),
            tile,
            column,
            column,
            whole((D, D)),
        ],
        cost_estimate=cost(2.2e9, 20e6),
    )(tokens, *contexts, *eight(heads), embed_row, b_out, gain, shift)


def second_norm_kernel(
    ffn_ref, one_ref, cot_ref, gain1, shift1, gain2, shift2, out_ref, grad_ref, low_ref, low_t, sum_ref
):
    @pl.when(pl.program_id(0) == 0)
    def _():
        sum_ref[...] = jnp.zeros_like(sum_ref)

    mid = one_ref[...] * gain1[...] + shift1[...]
    normal, scale = norm_of(mid + ffn_ref[...])
    out_ref[...] = (normal * gain2[...] + shift2[...]).astype(BF16)
    cot = cot_ref[...].astype(F32)
    grad = norm_back(normal, scale, cot, gain2[...])
    grad_ref[...] = grad
    low = grad.astype(BF16)
    low_ref[...] = low
    low_t[...] = low.T
    sums = [jnp.sum(v, axis=0, keepdims=True) for v in (low.astype(F32), cot * normal, cot)]
    for j in range(3):
        sum_ref[j : j + 1, :] += sums[j]


def second_norm(ffn, normal_one, cot, *rows):
    tile = pl.BlockSpec((ROWS, D), lambda i: (i, 0))
    return pl.pallas_call(
        second_norm_kernel,
        out_shape=(
            struct((LEN, D)),
            struct((LEN, D), F32),
            struct((LEN, D)),
            struct((D, LEN)),
            struct((8, D), F32),
        ),
        grid=(LEN // ROWS,),
        in_specs=[tile] * 3 + [whole((1, D))] * 4,
        out_specs=[tile] * 3 + [pl.BlockSpec((D, ROWS), lambda i: (0, i)), whole((8, D))],
        cost_estimate=cost(1e8, 20e6),
    )(ffn, normal_one, cot, *rows)


def first_back_kernel(
    part_ref, grad_ref, one_ref, scale_ref, gain_ref, out_ref, low_ref, low_t, sum_ref
):
    @pl.when(pl.program_id(0) == 0)
    def _():
        sum_ref[...] = jnp.zeros_like(sum_ref)

    d_mid = part_ref[...] + grad_ref[...]
    normal = one_ref[...]
    grad = norm_back(normal, scale_ref[...], d_mid, gain_ref[...])
    out_ref[...] = grad
    low = grad.astype(BF16)
    low_ref[...] = low
    low_t[...] = low.T
    sums = [jnp.sum(v, axis=0, keepdims=True) for v in (low.astype(F32), d_mid * normal, d_mid)]
    for j in range(3):
        sum_ref[j : j + 1, :] += sums[j]


def first_back(part, grad_two, normal_one, scale_one, gain):
    tile = pl.BlockSpec((ROWS, D), lambda i: (i, 0))
    return pl.pallas_call(
        first_back_kernel,
        out_shape=(struct((LEN, D), F32), struct((LEN, D)), struct((D, LEN)), struct((8, D), F32)),
        grid=(LEN // ROWS,),
        in_specs=[tile] * 3 + [pl.BlockSpec((ROWS, 1), lambda i: (i, 0)), whole((1, D))],
        out_specs=[tile, tile, pl.BlockSpec((D, ROWS), lambda i: (0, i)), whole((8, D))],
        cost_estimate=cost(1e8, 20e6),
    )(part, grad_two, normal_one, scale_one, gain)


def ffn_kernel(mid_ref, *refs):
    up_refs, down_refs, bias_refs = refs[0:2], refs[2:4], refs[4:6]
    into_ref, act_ref, slope_ref, total_ref = refs[6:]
    size = bias_refs[0].shape[1]
    for u in range(HALF):
        up, down = rows_of(up_refs[u]), rows_of(down_refs[u])
        columns = slice(u * size, (u + 1) * size)
        for r in range(LEN // ROWS):
            rows = slice(r * ROWS, (r + 1) * ROWS)
            pre = dot(mid_ref[rows, :], up, NT) + bias_refs[u][...]
            phi = 0.5 * (1.0 + lax.erf(pre * math.sqrt(0.5)))
            bell = jnp.exp(-0.5 * pre * pre) * (1.0 / math.sqrt(2.0 * math.pi))
            act = (pre * phi).astype(BF16)
            act_ref[rows, columns] = act
            slope_ref[rows, columns] = (phi + pre * bell).astype(BF16)
            before = into_ref[rows, :] if u == 0 else total_ref[rows, :]
            total_ref[rows, :] = before + dot(act, down)


def ffn_pair(mid_low, up, down, pair, bias, into):
    size = bias[0].shape[1]
    return pl.pallas_call(
        ffn_kernel,
        out_shape=(
            struct((LEN, 2 * size)),
            struct((LEN, 2 * size)),
            struct((LEN, D), F32),
        ),
        in_specs=[whole((LEN, D))]
        + pair_specs(size, 0, pair) * 2
        + [whole((1, size))] * 2
        + [whole((LEN, D))],
        out_specs=[whole((LEN, 2 * size)), whole((LEN, 2 * size)), whole((LEN, D))],
        grid=(1,),
        cost_estimate=cost(4.3e9, 18e6),
    )(mid_low, *pair_of(up, pair), *pair_of(down, pair), *bias, into)


def ffn_back_kernel(branch_hbm, *refs):
    down_hbm, up_hbm, slope_hbm, refs = refs[0:6], refs[6:12], refs[12:16], refs[16:]
    pre_refs, total_ref, sum_ref, refs = refs[0:4], refs[4], refs[5], refs[6:]
    branch, down, up, slope, sems = refs
    size = up.shape[1]
    plan = ((0, 0), (0, 1), (1, 0), (1, 1), (2, None), (3, None), (4, None), (5, None))
    first = pltpu.make_async_copy(branch_hbm, branch, sems.at[0])
    first.start()
    copies = []
    for j, (piece, which) in enumerate(plan):
        if which is None:
            down_part, up_part = down_hbm[piece], up_hbm[piece]
        else:
            down_part, up_part = down_hbm[piece].at[which], up_hbm[piece].at[which]
        group = [
            pltpu.make_async_copy(down_part, down.at[j], sems.at[1 + 3 * j]),
            pltpu.make_async_copy(
                slope_hbm[j // 2].at[:, (j % 2) * size : (j % 2 + 1) * size],
                slope.at[j],
                sems.at[2 + 3 * j],
            ),
            pltpu.make_async_copy(up_part, up.at[j], sems.at[3 + 3 * j]),
        ]
        for copy in group:
            copy.start()
        copies.append(group)
    first.wait()
    for j in range(len(plan)):
        for copy in copies[j]:
            copy.wait()
        columns = slice((j % 2) * size, (j % 2 + 1) * size)
        sums = 0.0
        for r in range(LEN // ROWS):
            rows = slice(r * ROWS, (r + 1) * ROWS)
            d_act = dot(branch[rows, :], down[j], NT)
            d_pre = (d_act * slope[j, rows, :].astype(F32)).astype(BF16)
            pre_refs[j // 2][rows, columns] = d_pre
            sums = sums + jnp.sum(d_pre.astype(F32), axis=0, keepdims=True)
            part = dot(d_pre, up[j])
            if j == 0:
                total_ref[rows, :] = part
            else:
                total_ref[rows, :] += part
        sum_ref[j : j + 1, :] = sums


def ffn_back(branch_two, down, up, slopes):
    size = down[2].shape[0]
    hbm = pl.BlockSpec(memory_space=pl.ANY)
    return pl.pallas_call(
        ffn_back_kernel,
        out_shape=(struct((LEN, 2 * size)),) * 4 + (struct((LEN, D), F32), struct((8, size), F32)),
        grid=(1,),
        in_specs=[hbm] * 17,
        out_specs=[whole((LEN, 2 * size))] * 4 + [whole((LEN, D)), whole((8, size))],
        scratch_shapes=[
            pltpu.VMEM((LEN, D), BF16),
            pltpu.VMEM((8, size, D), BF16),
            pltpu.VMEM((8, size, D), BF16),
            pltpu.VMEM((8, LEN, size), BF16),
            pltpu.SemaphoreType.DMA((25,)),
        ],
        cost_estimate=cost(17e9, 40e6),
    )(branch_two, *down, *up, *slopes)


class Run(NamedTuple):
    which: int
    first: int
    second: int
    size: int
    base: int
    stride: int


def unit_runs(count, size):
    half = size // 2
    return [Run(0, r * half // count, half + r * half // count, half // count, r * half // count, half) for r in range(count)]


def head_runs(which, count):
    return [Run(which, 2 * j * UNIT, (2 * j + 1) * UNIT, UNIT, 2 * j * UNIT, UNIT) for j in range(count)]


def part_width(part):
    return sum(2 * run.size for run in part)


def grad_kernel(blocks, side_from, outputs, lefts, got_from, left_at, *refs):
    n_right = 3 * lefts
    left_hbm, right_hbm, refs = refs[:lefts], refs[lefts : lefts + n_right], refs[lefts + n_right :]
    got_hbm, refs = (None, refs) if got_from is None else (refs[0], refs[1:])
    out_hbm, (left, right, got, out, sems) = refs[: len(outputs)], refs[len(outputs) :]
    count = [0]

    def copy_of(source, target):
        copy = pltpu.make_async_copy(source, target, sems.at[count[0]])
        copy.start()
        count[0] += 1
        return copy

    first = [
        copy_of(left_hbm[k].at[:, left_at[side]], left.at[k, side])
        for k in range(lefts)
        for side in range(2)
    ]
    chunks, at = [], 0
    for part, far in blocks:
        for run in part:
            copies = []
            for h in range(2):
                if far:
                    piece, source = 1 + h, run.second if side_from else run.first
                else:
                    piece, source = 0, run.second if h else run.first
                copies.append(
                    copy_of(
                        right_hbm[3 * run.which + piece].at[:, source : source + run.size],
                        right.at[:, at + h * run.size : at + (h + 1) * run.size],
                    )
                )
            chunks.append((run.which, at, 2 * run.size, copies))
            at += 2 * run.size
    if got_from is not None:
        first.append(copy_of(got_hbm.at[:, :, got_from : got_from + at], got))
    for copy in first:
        copy.wait()
    stores = []
    for which, at, size, copies in chunks:
        for copy in copies:
            copy.wait()
        columns = slice(at, at + size)
        for side in range(2):
            total = dot(left[which, side].reshape(D // 2, LEN), right[:, columns])
            if got_from is not None:
                total = total + got[side, :, columns].astype(F32)
            out[side, :, columns] = total.astype(BF16)
        for (start, end, side), target in zip(outputs, out_hbm):
            if start <= at < end:
                place = slice(at - start, at - start + size)
                if side is None:
                    stores.append(copy_of(out.at[:, :, columns], target.at[:, :, place]))
                else:
                    stores.append(copy_of(out.at[side, :, columns], target.at[:, place]))
    for copy in stores:
        copy.wait()


def grad_call(info, left_t, rights, blocks, side, outputs, got=None, got_from=None):
    width = sum(part_width(part) for part, _ in blocks)
    hbm = pl.BlockSpec(memory_space=pl.ANY)
    lefts = len(left_t)
    operands = [v.reshape(4, 2, D // 8, LEN) for v in left_t] + [v for r in rights for v in r]
    operands += [] if got is None else [got]
    shapes = [
        (2, D // 2, end - start) if at is None else (D // 2, end - start) for start, end, at in outputs
    ]
    return pl.pallas_call(
        functools.partial(grad_kernel, blocks, side, outputs, lefts, got_from),
        out_shape=tuple(struct(shape) for shape in shapes),
        grid_spec=pltpu.PrefetchScalarGridSpec(
            num_scalar_prefetch=1,
            grid=(1,),
            in_specs=[hbm] * len(operands),
            out_specs=[hbm] * len(shapes),
            scratch_shapes=[
                pltpu.VMEM((lefts, 2, 4, D // 8, LEN), BF16),
                pltpu.VMEM((LEN, width), BF16),
                pltpu.VMEM((2, D // 2, 128 if got is None else width), BF16),
                pltpu.VMEM((2, D // 2, width), BF16),
                pltpu.SemaphoreType.DMA((48,)),
            ],
        ),
        cost_estimate=cost(2 * D * LEN * width, 10e6),
    )(info, *operands)


def column_runs(part, swap):
    at = 0
    for run in part:
        for h in range(2):
            source = at + (1 - h if swap else h) * run.size
            yield at + h * run.size, source, run.size
        at += 2 * run.size


def add_kernel(part, swap, mine_ref, got_ref, out_ref):
    rows = out_ref.shape[0]
    mine, got = mine_ref[...].reshape(rows, -1), got_ref[...].reshape(rows, -1)
    for at, source, size in column_runs(part, swap):
        total = mine[:, at : at + size].astype(F32) + got[:, source : source + size].astype(F32)
        out_ref[:, at : at + size] = total.astype(BF16)


def block_spec(array, where, width):
    side, column = where
    if len(array.shape) == 3:
        return pl.BlockSpec((1, D // 2, width), lambda *_: (side, 0, column))
    return pl.BlockSpec((D // 2, width), lambda *_: (0, column))


def add_parts(mine, got, part, swap):
    width = part_width(part)
    return pl.pallas_call(
        functools.partial(add_kernel, part, swap),
        out_shape=struct((D // 2, width)),
        grid=(1,),
        in_specs=[block_spec(*v, width) for v in (mine, got)],
        out_specs=whole((D // 2, width)),
        cost_estimate=cost(1e6, 3e6),
    )(mine[0], got[0])


def split_kernel(parts, info_ref, *refs):
    ins, out_refs = refs[: 3 * len(parts)], refs[3 * len(parts) :]
    span = D // 8
    for k in range(4):
        rows = pl.ds(pl.multiple_of((info_ref[2] ^ k) * span, span), span)
        first = 0
        for p, part in enumerate(parts):
            mine, from_x, from_y = [
                (ref[0, rows, :] if len(ref.shape) == 3 else ref[rows, :]).astype(F32)
                for ref in ins[3 * p : 3 * p + 3]
            ]
            for at, source, size in column_runs(part, True):
                total = mine[:, at : at + size] + from_y[:, at : at + size]
                total = total + from_x[:, source : source + size]
                out_refs[k][:, first + at : first + at + size] = total.astype(BF16)
            first += part_width(part)


def split_z(info, parts, sources):
    width = sum(part_width(part) for part in parts)
    specs = [
        block_spec(*v, part_width(part)) for part, triple in zip(parts, sources) for v in triple
    ]
    out = pl.pallas_call(
        functools.partial(split_kernel, parts),
        out_shape=(struct((D // 8, width)),) * 4,
        grid_spec=pltpu.PrefetchScalarGridSpec(
            num_scalar_prefetch=1,
            grid=(1,),
            in_specs=specs,
            out_specs=[whole((D // 8, width))] * 4,
        ),
        cost_estimate=cost(1e6, 4e6),
    )(info, *[v[0] for triple in sources for v in triple])
    return [out[0]] + [send_dp(out[k], 2 * k) for k in (1, 2, 3)]


def finish_kernel(runs, turned, info_ref, *refs):
    parts, outs = refs[:4], refs[4:]
    at = 0
    for run in runs:
        for h in range(2):
            columns = slice(at, at + run.size)
            total = parts[0][:, columns].astype(F32)
            for part in parts[1:]:
                total = total + part[:, columns].astype(F32)
            spot = pl.ds(pl.multiple_of(run.base + info_ref[h] * run.stride, UNIT), run.size)
            if turned[run.which]:
                outs[run.which][spot, :] = total.T
            else:
                outs[run.which][:, spot] = total
            at += run.size


def finish(info, values, parts, turned):
    rows = D // 8
    runs = tuple(run for part in parts for run in part)
    sizes = [sum(2 * r.size for r in runs if r.which == k) for k in range(len(turned))]
    shapes = [(size, rows) if t else (rows, size) for size, t in zip(sizes, turned)]
    return pl.pallas_call(
        functools.partial(finish_kernel, runs, turned),
        out_shape=tuple(struct(shape, F32) for shape in shapes),
        grid_spec=pltpu.PrefetchScalarGridSpec(
            num_scalar_prefetch=1,
            grid=(1,),
            in_specs=[whole((rows, sum(sizes)))] * 4,
            out_specs=[whole(shape) for shape in shapes],
        ),
        cost_estimate=cost(1e6, 4e6),
    )(info, *values)


def input_grad_kernel(one_ref, *refs):
    grads, weights, out_ref, sum_ref = refs[:4], refs[4:8], refs[8], refs[9]

    @pl.when(pl.program_id(0) == 0)
    def _():
        sum_ref[...] = jnp.zeros_like(sum_ref)

    total = one_ref[...]
    for p in range(4):
        total = total + dot(grads[p][...], weights[p][...])
    out_ref[...] = total
    sum_ref[0:1, :] += jnp.sum(total, axis=0, keepdims=True)


def input_grad(grad_one, d_qkv, weights):
    tile = pl.BlockSpec((ROWS, D), lambda i: (i, 0))
    width = d_qkv[0].shape[1]
    return pl.pallas_call(
        input_grad_kernel,
        out_shape=(struct((LEN, D), F32), struct((8, D), F32)),
        grid=(LEN // ROWS,),
        in_specs=[tile]
        + [pl.BlockSpec((ROWS, width), lambda i: (i, 0))] * 4
        + [whole((width, D))] * 4,
        out_specs=[tile, whole((8, D))],
        cost_estimate=cost(6.4e9, 20e6),
    )(grad_one, *d_qkv, *weights)


def exchange_kernel(sum_ref, row_ref, total_ref, rows_ref, got, sems_a, sems_b):
    devices = GRID_DP * GRID_MP
    me = lax.axis_index("dp") * GRID_MP + lax.axis_index("mp")

    def place(index):
        return {"dp": index // GRID_MP, "mp": index % GRID_MP}

    barrier = pltpu.get_barrier_semaphore()

    def greet(k, carry):
        target = (me + k) % devices
        pl.semaphore_signal(
            barrier, inc=1, device_id=place(target), device_id_type=pl.DeviceIdType.MESH
        )
        return carry

    lax.fori_loop(1, devices, greet, 0)
    pl.semaphore_wait(barrier, devices - 1)

    def copies(k):
        target = (me + k) % devices
        first = pltpu.make_async_remote_copy(
            src_ref=sum_ref.at[target],
            dst_ref=got.at[k],
            send_sem=sems_a.at[0, k],
            recv_sem=sems_a.at[1, k],
            device_id=place(target),
            device_id_type=pl.DeviceIdType.MESH,
        )
        second = pltpu.make_async_remote_copy(
            src_ref=row_ref,
            dst_ref=rows_ref.at[k],
            send_sem=sems_b.at[0, k],
            recv_sem=sems_b.at[1, k],
            device_id=place(target),
            device_id_type=pl.DeviceIdType.MESH,
        )
        return first, second

    def start(k, carry):
        for copy in copies(k):
            copy.start()
        return carry

    lax.fori_loop(1, devices, start, 0)
    rows_ref[0] = row_ref[...]

    def finish_copy(k, carry):
        for copy in copies(k):
            copy.wait()
        return carry

    lax.fori_loop(1, devices, finish_copy, 0)
    total_ref[...] = sum_ref[me] + jnp.sum(got[1:], axis=0)


def exchange(sums, row):
    devices = GRID_DP * GRID_MP
    vmem = pl.BlockSpec(memory_space=pltpu.VMEM)
    return pl.pallas_call(
        exchange_kernel,
        out_shape=(struct(sums.shape[1:], F32), struct((devices,) + row.shape, F32)),
        in_specs=[vmem, vmem],
        out_specs=[vmem, vmem],
        scratch_shapes=[
            pltpu.VMEM(sums.shape, F32),
            pltpu.SemaphoreType.DMA((2, devices)),
            pltpu.SemaphoreType.DMA((2, devices)),
        ],
        compiler_params=pltpu.CompilerParams(collective_id=0, has_side_effects=True),
        cost_estimate=cost(1e6, 1e6),
    )(sums, row)


def natural_blocks(halves, x_at, mp_at):
    join = lambda a, b: jnp.where(x_at == 0, jnp.concatenate([a, b]), jnp.concatenate([b, a]))
    stacked = jnp.stack(
        [
            join(halves[0], halves[1]),
            join(halves[2], halves[3]),
            join(halves[4], halves[6]),
            join(halves[5], halves[7]),
        ]
    )
    return jnp.stack([stacked[i ^ mp_at] for i in range(4)])


def body_rows(
    tokens,
    segment_ids,
    time_steps,
    w_qkv,
    b_qv,
    w_out,
    b_out,
    gain_one,
    shift_one,
    w_up,
    b_up,
    w_down,
    b_down,
    gain_two,
    shift_two,
    w_time,
    b_time,
    cotangent,
):
    dp_at, mp_at = lax.axis_index("dp"), lax.axis_index("mp")
    x_at, z_at = dp_at % 2, dp_at // 2
    info = jnp.stack([x_at, 1 - x_at, z_at, mp_at]).astype(jnp.int32)
    row = lambda v: v.astype(F32)[None, :]
    width = w_qkv.shape[2]

    heads_own, heads_first = pack_heads(info, w_qkv, w_out)
    heads = fetch(heads_own, heads_first)
    up_own, up_first, down_own, down_first = pack_units(info, w_up, w_down)
    up = fetch(up_own, up_first)
    down = fetch(down_own, down_first)
    q_rows, v_rows, up_rows = fetch_bias([b_qv[0:1], b_qv[1:2], b_up[None, :]], x_at)
    zero = jnp.zeros((1, width // 2), F32)

    own_step = lax.dynamic_slice_in_dim(time_steps, mp_at, 1, 0)
    segment_row = lax.dynamic_index_in_dim(segment_ids, mp_at, 0, keepdims=False)
    features = time_features(own_step)
    embed_row = jnp.dot(features, w_time.astype(F32), precision=HIGHEST_PRECISION)
    embed_row = embed_row + row(b_time)
    hidden_low = (tokens.astype(F32) + embed_row).astype(BF16)
    hotq, hotk = mark_segments(segment_row)
    win_f, win_b = windows(segment_row, TILE_F), windows(segment_row, TILE_B)

    qkv, ctx, lse, qkv_cat = [], [], [], []
    for p in range(4):
        first, second = 2 * p, 2 * p + 1
        bias = jnp.concatenate(
            [q_rows[first], q_rows[second], zero, zero, v_rows[first], v_rows[second]], axis=1
        )
        parts = attend_pair(win_f, hidden_low, heads, p, bias, hotq, hotk)
        for kept, part in zip((qkv, ctx, lse, qkv_cat), parts):
            kept.append(part)
    normal_one, scale_one, mid_low, mid_t, hidden_t, out_cat = first_norm(
        tokens, ctx, heads, embed_row, row(b_out), row(gain_one), row(shift_one)
    )

    act, slope = [], []
    ffn = jnp.broadcast_to(row(b_down), (LEN, D))
    for p in range(4):
        act_p, slope_p, ffn = ffn_pair(
            mid_low, up, down, p, up_rows[2 * p : 2 * p + 2], ffn
        )
        act.append(act_p)
        slope.append(slope_p)
    out_rows, grad_two, branch_two, branch_two_t, sums_two = second_norm(
        ffn, normal_one, cotangent, row(gain_one), row(shift_one), row(gain_two), row(shift_two)
    )

    units = act[0].shape[1]
    down_parts = [(run,) for run in unit_runs(2, units)]
    up_parts = [down_parts[0], (down_parts[1][0], *head_runs(1, 1))]
    qkv_part = tuple(head_runs(0, 3))

    def two_way(left_t, rights, parts, cover):
        blocks = tuple((part, far) for part in parts for far in (False, True))
        one, two = (part_width(part) for part in parts)
        every = 2 * (one + two)
        (sent,) = grad_call(info, left_t, [r[1:] for r in rights], blocks, 1, ((0, every, None),))
        got = send_mp(sent, 1)
        covered = cover()
        outputs = (
            (0, one, None),
            (one, 2 * one, None),
            (2 * one, every, 0),
            (2 * one, every, 1),
        )
        result = grad_call(
            info, left_t, [r[:1] + r[2:] for r in rights], blocks, 0, outputs, got, 0
        )
        return covered, result

    def first_sends(blocks):
        own, far, keep, leave = blocks
        return own, keep, send_mp(far, 2), send_dp(leave, 1)

    def second_sends(sums, parts):
        own, keep, from_y, from_x = sums
        low = add_parts((own, (1, 0)), (from_y, (1, 0)), parts[0], False)
        x_two = send_dp(low, 1)
        low = add_parts((keep, (0, 1)), (from_x, (0, 1)), parts[1], True)
        y_two = send_mp(low, 2)
        here = (0, 0)
        return (
            ((own, here), (x_two, here), (from_y, here)),
            ((keep, here), (from_x, here), (y_two, here)),
        )

    def ffn_part():
        return ffn_back(branch_two, down, up, slope)

    (*d_pre, d_mid, sums_up), down_blocks = two_way([branch_two_t], [act], down_parts, ffn_part)
    down_sums = first_sends(down_blocks)
    grad_one, branch_one, branch_one_t, sums_one = first_back(
        d_mid, grad_two, normal_one, scale_one, row(gain_one)
    )
    d_qkv, qkv_sums = [None] * 4, [None] * 4

    def back(p):
        d_qkv[p], qkv_sums[p] = attend_back_pair(
            win_b, qkv[p], hotq, hotk, branch_one, out_cat, p, ctx[p], lse[p]
        )

    _, up_blocks = two_way([mid_t, branch_one_t], [d_pre, ctx], up_parts, lambda: back(1))
    up_sums = first_sends(up_blocks)
    down_last = second_sends(down_sums, down_parts)
    back(2)
    down_values = split_z(info, down_parts, down_last)
    back(3)
    up_last = second_sends(up_sums, up_parts)
    wide = part_width(qkv_part)
    far_only, own_only = ((qkv_part, True),), ((qkv_part, False),)
    (sent,) = grad_call(
        info, [hidden_t], [d_qkv[1:]], own_only + far_only, 1, ((0, 2 * wide, None),)
    )
    got = send_mp(sent, 1)
    up_values = split_z(info, up_parts, up_last)
    sides = ((0, wide, 0), (0, wide, 1))
    far_keep, far_leave = grad_call(
        info, [hidden_t], [[d_qkv[1]] + d_qkv[2:]], far_only, 0, sides, got, wide
    )
    far_x = send_dp(far_leave, 1)
    back(0)
    own_keep, own_leave = grad_call(
        info, [hidden_t], [d_qkv[:1] + d_qkv[2:]], own_only, 0, sides, got, 0
    )
    own_x = send_dp(own_leave, 1)
    here = (0, 0)
    far_low = add_parts((far_keep, here), (far_x, here), qkv_part, True)
    far_y = send_mp(far_low, 2)
    grad_tokens, sums_in = input_grad(grad_one, d_qkv, qkv_cat)
    qkv_values = split_z(info, (qkv_part,), (((own_keep, here), (own_x, here), (far_y, here)),))

    spread = lambda v: v.reshape(GRID_DP * GRID_MP, -1)
    spread_blocks = lambda b: b.reshape(GRID_MP, GRID_DP, -1).transpose(1, 0, 2).reshape(GRID_DP * GRID_MP, -1)
    rows = [spread(sums[j]) for sums in (sums_two, sums_one) for j in range(3)]
    rows.append(spread_blocks(natural_blocks([sums_up[j] for j in range(8)], x_at, mp_at)))
    for j in (0, 2):
        halves = [
            qkv_sums[p][0, (2 * j + u) * UNIT : (2 * j + u + 1) * UNIT]
            for p in range(4)
            for u in range(HALF)
        ]
        rows.append(spread_blocks(natural_blocks(halves, x_at, mp_at)))
    tail_row = jnp.concatenate(
        [sums_in[0:1], jnp.broadcast_to(own_step.astype(F32)[None, :], (1, UNIT))], axis=1
    )
    totals, all_rows = exchange(jnp.concatenate(rows, axis=1)[:, None, :], tail_row)
    all_rows = all_rows[:, 0]
    span = D // (GRID_DP * GRID_MP)
    own = [totals[0, j * span : (j + 1) * span] for j in range(6)]
    device_at = dp_at * GRID_MP + mp_at
    all_grads = all_rows[:, :D]
    dims = device_at * span + jnp.arange(span, dtype=jnp.int32)
    ladder = (dims % (D // 2)).astype(F32)
    frequency = jnp.exp(ladder * (-math.log(10000.0) / (D // 2)))
    angles = all_rows[:, D : D + 1] * frequency[None, :]
    own_features = jnp.where((dims < D // 2)[None, :], jnp.sin(angles), jnp.cos(angles))
    g_w_time = jnp.dot(own_features.T, all_grads, precision=HIGHEST_PRECISION)
    g_b_time = lax.dynamic_slice_in_dim(jnp.sum(all_grads, axis=0), device_at * span, span, 0)

    (g_w_qkv,) = finish(info, qkv_values, (qkv_part,), (False,))
    (g_w_down,) = finish(info, down_values, down_parts, (True,))
    g_w_up, g_w_out = finish(info, up_values, up_parts, (False, True))
    up_end = totals.shape[1] - 2 * span
    return (
        out_rows,
        grad_tokens,
        g_w_qkv.reshape(D // 8, 3, width),
        totals[0, up_end:].reshape(2, 1, -1),
        g_w_out,
        own[3],
        own[4],
        own[5],
        g_w_up,
        totals[:, 6 * span : up_end],
        g_w_down,
        own[0],
        own[1],
        own[2],
        g_w_time,
        g_b_time,
    )


def solution(mesh):
    placed = (
        P(("dp", "mp"), None),
        P("dp", None),
        P("dp"),
        P(None, None, "mp"),
        P(None, "mp"),
        P("mp", None),
        P(),
        P(),
        P(),
        P(None, "mp"),
        P("mp"),
        P("mp", None),
        P(),
        P(),
        P(),
        P(),
        P(),
        P(("dp", "mp"), None),
    )
    rows = mesh.shape["dp"], mesh.shape["mp"]

    def body(*args):
        if args[0].shape[0] != LEN or rows != (GRID_DP, GRID_MP):
            return body_split(*args)
        return body_rows(*args)

    return jax.shard_map(
        body,
        mesh=mesh,
        in_specs=placed,
        out_specs=(
            P(("dp", "mp"), None),
            P(("dp", "mp"), None),
            P("dp", None, "mp"),
            P(None, "mp", "dp"),
            P("mp", "dp"),
            P(("dp", "mp")),
            P(("dp", "mp")),
            P(("dp", "mp")),
            P("dp", "mp"),
            P("mp", "dp"),
            P("mp", "dp"),
            P(("dp", "mp")),
            P(("dp", "mp")),
            P(("dp", "mp")),
            P(("dp", "mp"), None),
            P(("dp", "mp")),
        ),
        check_vma=False,
    )
```

```python
import functools
import math
from typing import NamedTuple

import jax
import jax.numpy as jnp
from jax import lax
from jax.experimental import pallas as pl
from jax.experimental.pallas import tpu as pltpu
from jax.sharding import PartitionSpec as P


D = 1024
HEAD_DIM = 64
LEN = 1024


EPS = 1e-05
HIGHEST_PRECISION = lax.Precision.HIGHEST


def time_features(step_values):
    half_width = D // 2
    ladder = jnp.arange(half_width, dtype=jnp.float32)
    frequency = jnp.exp(ladder * (-math.log(10000.0) / half_width))
    angles = step_values.astype(jnp.float32)[:, None] * frequency[None, :]
    return jnp.concatenate([jnp.sin(angles), jnp.cos(angles)], axis=1)


def layer_norm(values, gain_vec, shift_vec):
    center = values - jnp.mean(values, axis=-1, keepdims=True)
    spread = jnp.mean(center * center, axis=-1, keepdims=True)
    return center * lax.rsqrt(spread + EPS) * gain_vec + shift_vec


def exact_gelu(values):
    return jax.nn.gelu(values, approximate=False)


def project_qkv(hidden_full, w_qkv, b_qv):
    width_local = w_qkv.shape[2]
    w_flat = w_qkv.reshape(w_qkv.shape[0], 3 * width_local)
    bias_row = jnp.concatenate([b_qv[0], jnp.zeros((width_local,), b_qv.dtype), b_qv[1]]).astype(
        jnp.float32
    )
    product = jnp.dot(hidden_full, w_flat, preferred_element_type=jnp.float32)
    return (product + bias_row[None, :]).astype(jnp.bfloat16)


def head_parts(qkv_seq):
    width_local = qkv_seq.shape[1] // 3
    head_local = width_local // HEAD_DIM
    shaped = qkv_seq.reshape(qkv_seq.shape[0], 3, head_local, HEAD_DIM)
    return (shaped[:, 0], shaped[:, 1], shaped[:, 2])


def masked_scores(queries, keys_part, segment_row):
    scores = jnp.einsum("qhd,khd->hqk", queries, keys_part, preferred_element_type=jnp.float32)
    scores = scores * (1.0 / math.sqrt(HEAD_DIM))
    same_doc = segment_row[:, None] == segment_row[None, :]
    return jnp.where(same_doc[None, :, :], scores, -1e30)


def attend_forward(inputs):
    qkv_seq, segment_row = inputs
    queries, keys_part, values_part = head_parts(qkv_seq)
    masked = masked_scores(queries, keys_part, segment_row)
    top_score = jnp.max(masked, axis=2, keepdims=True)
    weights_exp = jnp.exp(masked - top_score)
    totals = jnp.sum(weights_exp, axis=2, keepdims=True)
    probability = weights_exp / totals
    context = jnp.einsum(
        "hqk,khd->qhd",
        probability.astype(jnp.bfloat16),
        values_part,
        preferred_element_type=jnp.float32,
    )
    log_total = (top_score + jnp.log(totals))[:, :, 0]
    return (context.reshape(qkv_seq.shape[0], -1).astype(jnp.bfloat16), log_total)


def attend_backward(inputs):
    qkv_seq, grad_seq, log_total, segment_row = inputs
    queries, keys_part, values_part = head_parts(qkv_seq)
    masked = masked_scores(queries, keys_part, segment_row)
    probability = jnp.exp(masked - log_total[:, :, None])
    grad_heads = grad_seq.reshape(grad_seq.shape[0], -1, HEAD_DIM)
    d_values = jnp.einsum(
        "hqk,qhd->khd",
        probability.astype(jnp.bfloat16),
        grad_heads,
        preferred_element_type=jnp.float32,
    )
    d_probs = jnp.einsum(
        "qhd,khd->hqk", grad_heads, values_part, preferred_element_type=jnp.float32
    )
    row_terms = jnp.sum(probability * d_probs, axis=2, keepdims=True)
    d_scores = (probability * (d_probs - row_terms)).astype(jnp.bfloat16)
    score_scale = 1.0 / math.sqrt(HEAD_DIM)
    d_queries = (
        jnp.einsum("hqk,khd->qhd", d_scores, keys_part, preferred_element_type=jnp.float32)
        * score_scale
    )
    d_keys = (
        jnp.einsum("hqk,qhd->khd", d_scores, queries, preferred_element_type=jnp.float32)
        * score_scale
    )
    stacked = jnp.stack([d_queries, d_keys, d_values], axis=1)
    return stacked.reshape(qkv_seq.shape[0], -1).astype(jnp.bfloat16)


def body_split(
    tokens,
    segment_ids,
    time_steps,
    w_qkv,
    b_qv,
    w_out,
    b_out,
    gain_one,
    shift_one,
    w_up,
    b_up,
    w_down,
    b_down,
    gain_two,
    shift_two,
    w_time,
    b_time,
    cotangent,
):
    row_count = tokens.shape[0]
    seq_local = time_steps.shape[0]
    width_local = w_qkv.shape[2]
    gain_one_f = gain_one.astype(jnp.float32)
    shift_one_f = shift_one.astype(jnp.float32)
    gain_two_f = gain_two.astype(jnp.float32)
    shift_two_f = shift_two.astype(jnp.float32)
    w_flat = w_qkv.reshape(D, 3 * width_local)
    features = time_features(time_steps)
    embed_rows = jnp.dot(features, w_time.astype(jnp.float32), precision=HIGHEST_PRECISION)
    embed_rows = embed_rows + b_time.astype(jnp.float32)[None, :]
    row_seq = (lax.axis_index("mp") * row_count + jnp.arange(row_count, dtype=jnp.int32)) // LEN
    selector = (row_seq[:, None] == jnp.arange(seq_local, dtype=jnp.int32)[None, :]).astype(
        jnp.float32
    )
    hidden_in = tokens.astype(jnp.float32) + jnp.dot(
        selector, embed_rows, precision=HIGHEST_PRECISION
    )
    hidden_low = hidden_in.astype(jnp.bfloat16)
    hidden_full = lax.all_gather(hidden_low, "mp", axis=0, tiled=True)
    qkv_full = project_qkv(hidden_full, w_qkv, b_qv)
    ctx_blocks, log_totals = lax.map(
        attend_forward, (qkv_full.reshape(seq_local, LEN, 3 * width_local), segment_ids)
    )
    context = ctx_blocks.reshape(seq_local * LEN, width_local)
    rows_in = context
    attn_sum = lax.psum_scatter(
        jnp.dot(rows_in, w_out, preferred_element_type=jnp.float32).astype(jnp.bfloat16),
        "mp",
        scatter_dimension=0,
        tiled=True,
    ).astype(jnp.float32)
    attn_out = attn_sum + b_out.astype(jnp.float32)[None, :]
    mid_in = hidden_in + attn_out
    mid_norm = layer_norm(mid_in, gain_one_f, shift_one_f)
    mid_low = mid_norm.astype(jnp.bfloat16)
    mid_full = lax.all_gather(mid_low, "mp", axis=0, tiled=True)
    pre_act = (
        jnp.dot(mid_full, w_up, preferred_element_type=jnp.float32)
        + b_up.astype(jnp.float32)[None, :]
    )
    activated = exact_gelu(pre_act).astype(jnp.bfloat16)
    rows_in = activated
    ffn_part = lax.psum_scatter(
        jnp.dot(rows_in, w_down, preferred_element_type=jnp.float32).astype(jnp.bfloat16),
        "mp",
        scatter_dimension=0,
        tiled=True,
    ).astype(jnp.float32)
    out_in = mid_norm + ffn_part + b_down.astype(jnp.float32)[None, :]
    out_rows, out_back = jax.vjp(layer_norm, out_in, gain_two_f, shift_two_f)
    grad_two, grad_gain_two, grad_shift_two = out_back(cotangent.astype(jnp.float32))
    branch_two = grad_two.astype(jnp.bfloat16)
    grad_b_down = jnp.sum(branch_two.astype(jnp.float32), axis=0)
    _, gelu_back = jax.vjp(exact_gelu, pre_act)
    cot_full = lax.all_gather(branch_two, "mp", axis=0, tiled=True)
    d_act = jnp.dot(cot_full, w_down.T, preferred_element_type=jnp.float32)
    grad_w_down = jnp.dot(activated.T, cot_full, preferred_element_type=jnp.float32)
    d_pre = gelu_back(d_act)[0].astype(jnp.bfloat16)
    grad_w_up = jnp.dot(mid_full.T, d_pre, preferred_element_type=jnp.float32)
    grad_b_up = jnp.sum(d_pre.astype(jnp.float32), axis=0)
    rows_in = d_pre
    d_mid_part = lax.psum_scatter(
        jnp.dot(rows_in, w_up.T, preferred_element_type=jnp.float32).astype(jnp.bfloat16),
        "mp",
        scatter_dimension=0,
        tiled=True,
    ).astype(jnp.float32)
    _, mid_back = jax.vjp(layer_norm, mid_in, gain_one_f, shift_one_f)
    grad_one, grad_gain_one, grad_shift_one = mid_back(grad_two + d_mid_part)
    branch_one = grad_one.astype(jnp.bfloat16)
    grad_b_out = jnp.sum(branch_one.astype(jnp.float32), axis=0)
    cot_attn = lax.all_gather(branch_one, "mp", axis=0, tiled=True)
    d_context = jnp.dot(cot_attn, w_out.T, preferred_element_type=jnp.float32).astype(jnp.bfloat16)
    grad_w_out = jnp.dot(context.T, cot_attn, preferred_element_type=jnp.float32)
    grad_blocks = lax.map(
        attend_backward,
        (
            qkv_full.reshape(seq_local, LEN, 3 * width_local),
            d_context.reshape(seq_local, LEN, width_local),
            log_totals,
            segment_ids,
        ),
    )
    d_qkv = grad_blocks.reshape(seq_local * LEN, 3 * width_local)
    grad_w_qkv = jnp.dot(hidden_full.T, d_qkv, preferred_element_type=jnp.float32).reshape(
        D, 3, width_local
    )
    qkv_sums = jnp.sum(d_qkv.astype(jnp.float32), axis=0).reshape(3, width_local)
    grad_b_qv = jnp.stack([qkv_sums[0], qkv_sums[2]]).reshape(2, 1, width_local)
    rows_in = d_qkv
    input_part = lax.psum_scatter(
        jnp.dot(rows_in, w_flat.T, preferred_element_type=jnp.float32).astype(jnp.bfloat16),
        "mp",
        scatter_dimension=0,
        tiled=True,
    ).astype(jnp.float32)
    grad_tokens = grad_one + input_part
    grad_embed = jnp.dot(selector.T, grad_tokens, precision=HIGHEST_PRECISION)
    grad_w_time = jnp.dot(features.T, grad_embed, precision=HIGHEST_PRECISION)
    grad_b_time = jnp.sum(grad_embed, axis=0)
    sharded = (
        lax.psum_scatter(
            grad_w_qkv.astype(jnp.bfloat16), "dp", scatter_dimension=0, tiled=True
        ).astype(jnp.float32),
        lax.psum_scatter(
            grad_b_qv.astype(jnp.bfloat16), "dp", scatter_dimension=2, tiled=True
        ).astype(jnp.float32),
        lax.psum_scatter(
            grad_w_out.astype(jnp.bfloat16), "dp", scatter_dimension=1, tiled=True
        ).astype(jnp.float32),
        lax.psum_scatter(
            grad_w_up.astype(jnp.bfloat16), "dp", scatter_dimension=0, tiled=True
        ).astype(jnp.float32),
        lax.psum_scatter(
            grad_b_up.reshape(1, -1).astype(jnp.bfloat16), "dp", scatter_dimension=1, tiled=True
        ).astype(jnp.float32),
        lax.psum_scatter(
            grad_w_down.astype(jnp.bfloat16), "dp", scatter_dimension=1, tiled=True
        ).astype(jnp.float32),
    )
    shared = (
        lax.psum_scatter(grad_w_time, ("dp", "mp"), scatter_dimension=0, tiled=True),
        lax.psum_scatter(grad_b_time, ("dp", "mp"), scatter_dimension=0, tiled=True),
        lax.psum_scatter(grad_gain_one, ("dp", "mp"), scatter_dimension=0, tiled=True),
        lax.psum_scatter(grad_shift_one, ("dp", "mp"), scatter_dimension=0, tiled=True),
        lax.psum_scatter(grad_gain_two, ("dp", "mp"), scatter_dimension=0, tiled=True),
        lax.psum_scatter(grad_shift_two, ("dp", "mp"), scatter_dimension=0, tiled=True),
        lax.psum_scatter(grad_b_out, ("dp", "mp"), scatter_dimension=0, tiled=True),
        lax.psum_scatter(grad_b_down, ("dp", "mp"), scatter_dimension=0, tiled=True),
    )
    return (
        out_rows.astype(jnp.bfloat16),
        grad_tokens,
        sharded[0],
        sharded[1],
        sharded[2],
        shared[6],
        shared[2],
        shared[3],
        sharded[3],
        sharded[4],
        sharded[5],
        shared[7],
        shared[4],
        shared[5],
        shared[0],
        shared[1],
    )


GRID_DP = 8
GRID_MP = 4
HALF = 2
UNIT = 128
F32 = jnp.float32
BF16 = jnp.bfloat16
TILE_F = 512
TILE_B = 256
TILE_U = 256
ROWS = 256
GRAIN = 256
STEP = 128
FAR = -(2.0**100)
NN = (((1,), (0,)), ((), ()))
NT = (((1,), (1,)), ((), ()))


def dot(left, right, dims=NN):
    return lax.dot_general(left, right, dims, preferred_element_type=F32)


def half_of(values, which, axis):
    size = values.shape[axis] // 2
    return lax.dynamic_slice_in_dim(values, which * size, size, axis)


def whole(shape):
    return pl.BlockSpec(shape, lambda *_: (0,) * len(shape))


def struct(shape, kind=BF16):
    return jax.ShapeDtypeStruct(shape, kind)


def far(shape, kind=BF16):
    return pltpu.HBM(shape, kind)


def room(mib):
    return pltpu.CompilerParams(vmem_limit_bytes=mib * 2**20)


def cost(flops, moved):
    return pl.CostEstimate(flops=int(flops), bytes_accessed=int(moved), transcendentals=0)


def send_mp(values, bit):
    return lax.ppermute(values, "mp", [(i, i ^ bit) for i in range(GRID_MP)])


def send_dp(values, bit):
    return lax.ppermute(values, "dp", [(i, i ^ bit) for i in range(GRID_DP)])


def fetch(own, first_half):
    near = send_mp(own, 1)
    far_a = send_mp(first_half, 2)
    near_a = send_mp(far_a, 1)
    far_b = send_dp(far_a, 1)
    near_b = send_mp(far_b, 1)
    return [own, near, far_a, near_a, far_b, near_b]


def pack_heads_kernel(info_ref, qkv_ref, out_ref, both_ref, first_ref):
    for u in range(HALF):
        for j in range(3):
            at = pl.ds(pl.multiple_of(info_ref[u] * UNIT, UNIT), UNIT)
            both_ref[u, j * UNIT : (j + 1) * UNIT, :] = qkv_ref[j, :, at].T
        at = pl.ds(pl.multiple_of(info_ref[u] * UNIT, UNIT), UNIT)
        both_ref[u, 3 * UNIT :, :] = out_ref[at, :]
    first_ref[...] = both_ref[0]


def pack_heads(info, w_qkv, w_out):
    return pl.pallas_call(
        pack_heads_kernel,
        out_shape=(struct((HALF, 4 * UNIT, D)), struct((4 * UNIT, D))),
        grid_spec=pltpu.PrefetchScalarGridSpec(
            num_scalar_prefetch=1,
            grid=(1,),
            in_specs=[whole((3, D, 2 * UNIT)), whole((2 * UNIT, D))],
            out_specs=[whole((HALF, 4 * UNIT, D)), whole((4 * UNIT, D))],
        ),
        compiler_params=room(24),
        cost_estimate=cost(1e6, 5e6),
    )(info, w_qkv.transpose(1, 0, 2), w_out)


def pack_units_kernel(info_ref, up_ref, down_ref, up_both, up_first, down_both, down_first):
    step = pl.program_id(0)
    up = up_ref[...].T
    up_both[0] = up
    down_both[0] = down_ref[...]

    @pl.when(step == 0)
    def _():
        up_first[...] = up
        down_first[...] = down_ref[...]


def pack_units(info, w_up, w_down):
    size = w_down.shape[0] // 2
    return pl.pallas_call(
        pack_units_kernel,
        out_shape=(struct((HALF, size, D)), struct((size, D))) * 2,
        grid_spec=pltpu.PrefetchScalarGridSpec(
            num_scalar_prefetch=1,
            grid=(HALF,),
            in_specs=[
                pl.BlockSpec((D, size), lambda i, info: (0, info[i])),
                pl.BlockSpec((size, D), lambda i, info: (info[i], 0)),
            ],
            out_specs=[pl.BlockSpec((1, size, D), lambda i, info: (i, 0, 0)), whole((size, D))] * 2,
        ),
        compiler_params=room(24),
        cost_estimate=cost(1e6, 10e6),
    )(info, w_up, w_down)


def fetch_bias(own, x_at):
    packed = jnp.concatenate(own, axis=1)
    near, far = send_mp(packed, 1), send_mp(packed, 2)
    near_far = send_mp(far, 1)
    order = [(packed, x_at), (packed, 1 - x_at), (near, x_at), (near, 1 - x_at)]
    order += [(v, at) for at in (x_at, 1 - x_at) for v in (far, near_far)]
    pieces, start = [], 0
    for row in own:
        size = row.shape[1]
        pieces.append(
            [half_of(v[:, start : start + size], at, 1).astype(F32) for v, at in order]
        )
        start += size
    return pieces


def half_specs(rows, block):
    both = [pl.BlockSpec((1, rows, D), lambda *_, u=u: (u, block, 0)) for u in range(HALF)]
    return both * 2 + [pl.BlockSpec((rows, D), lambda *_: (block, 0))] * 4


def eight(pieces):
    own, near, far_a, near_a, far_b, near_b = pieces
    return [own, own, near, near, far_a, near_a, far_b, near_b]


def pair_specs(rows, block, pair):
    return half_specs(rows, block)[2 * pair : 2 * pair + 2]


def pair_of(pieces, pair):
    return eight(pieces)[2 * pair : 2 * pair + 2]


def rows_of(ref):
    return ref[...].reshape(-1, D)


def mark_segments(segment_row):
    lane = jnp.arange(UNIT, dtype=jnp.int32)[None, :]
    hot = segment_row[:, None] == (lane % HEAD_DIM)
    used = (lane % HEAD_DIM) < 8
    return (
        jnp.where(hot & used, 1.0, 0.0).astype(BF16),
        jnp.where(used & ~hot, FAR, 0.0).astype(BF16),
    )


def windows(segment_row, tile):
    first, last = segment_row[::tile], segment_row[tile - 1 :: tile]
    low = jnp.sum(segment_row[None, :] < first[:, None], axis=1) // STEP * STEP
    high = jnp.sum(segment_row[None, :] <= last[:, None], axis=1)
    count = jnp.maximum((high - low + GRAIN - 1) // GRAIN, tile // GRAIN)
    low = jnp.minimum(low, LEN - count * GRAIN)
    return jnp.stack([low, count]).astype(jnp.int32)


def variants(count, tile, run):
    for n in range(tile // GRAIN, LEN // GRAIN + 1):

        @pl.when(count == n)
        def _(n=n):
            run(n * GRAIN)


def lanes_at(at, base=0):
    return pl.ds(pl.multiple_of(base + at * UNIT, UNIT), UNIT)


def attend_kernel(
    win_ref, x_ref, *refs
):
    weights, (bias_ref, hotq_ref, hotk_ref, qkv_ref, ctx_ref, lse_ref, w_ref, kx) = refs[:2], refs[2:]
    unit, step = pl.program_id(0), pl.program_id(1)

    @pl.when((unit == 0) & (step == 0))
    def _():
        for u in range(HALF):
            part = rows_of(weights[u])
            for j in range(3):
                at = (2 * j + u) * UNIT
                w_ref[at : at + UNIT, :] = part[j * UNIT : (j + 1) * UNIT]
        for r in range(LEN // ROWS):
            rows = slice(r * ROWS, (r + 1) * ROWS)
            qkv_ref[rows, :] = (dot(x_ref[rows, :], w_ref[...], NT) + bias_ref[...]).astype(BF16)

    @pl.when(step == 0)
    def _():
        lane = lax.broadcasted_iota(jnp.int32, (LEN, UNIT), 1)
        keys = qkv_ref[:, lanes_at(unit, 2 * UNIT)]
        for h in range(HALF):
            kx[h] = jnp.where((lane // HEAD_DIM) == h, keys, hotk_ref[...])

    lane = lax.broadcasted_iota(jnp.int32, (TILE_F, UNIT), 1)
    rows = pl.ds(pl.multiple_of(step * TILE_F, TILE_F), TILE_F)
    queries = qkv_ref[rows, lanes_at(unit)] * jnp.asarray(1.0 / math.sqrt(HEAD_DIM), BF16)
    start = pl.multiple_of(win_ref[0, step], STEP)

    def run(width):
        window = pl.ds(start, width)
        values = qkv_ref[window, lanes_at(unit, 4 * UNIT)]
        scores = [
            dot(
                jnp.where((lane // HEAD_DIM) == h, queries, hotq_ref[...]), kx[h, window, :], NT
            )
            for h in range(HALF)
        ]
        outs = []
        for h in range(HALF):
            top = jnp.max(scores[h], axis=1, keepdims=True)
            weight = jnp.exp(scores[h] - top)
            total = jnp.sum(weight, axis=1, keepdims=True)
            outs.append(dot(weight.astype(BF16), values) * (1.0 / total))
            lse_ref[0, h : h + 1, :] = (top + jnp.log(total)).T
        ctx_ref[...] = jnp.where(lane < HEAD_DIM, outs[0], outs[1]).astype(BF16)

    variants(win_ref[1, step], TILE_F, run)


def attend_pair(win, hidden_low, heads, pair, bias, hotq, hotk):
    return pl.pallas_call(
        attend_kernel,
        out_shape=(
            far((LEN, 6 * UNIT)),
            far((LEN, 2 * UNIT)),
            far((HALF, 8, LEN), F32),
        ),
        grid_spec=pltpu.PrefetchScalarGridSpec(
            num_scalar_prefetch=1,
            grid=(HALF, LEN // TILE_F),
            in_specs=[whole((LEN, D))]
            + pair_specs(4 * UNIT, 0, pair)
            + [
                whole((1, 6 * UNIT)),
                pl.BlockSpec((TILE_F, UNIT), lambda n, i, win: (i, 0)),
                whole((LEN, UNIT)),
            ],
            out_specs=[
                whole((LEN, 6 * UNIT)),
                pl.BlockSpec((TILE_F, UNIT), lambda n, i, win: (i, n)),
                pl.BlockSpec((1, 8, TILE_F), lambda n, i, win: (n, 0, i)),
            ],
            scratch_shapes=[pltpu.VMEM((6 * UNIT, D), BF16), pltpu.VMEM((HALF, LEN, UNIT), BF16)],
        ),
        compiler_params=room(32),
        cost_estimate=cost(6e9, 8e6),
    )(win, hidden_low, *pair_of(heads, pair), bias, hotq, hotk)


def attend_back_kernel(
    win_ref,
    qkv_ref,
    hotq_ref,
    hotk_ref,
    branch_ref,
    wa_ref,
    wb_ref,
    ctx_ref,
    lse_ref,
    out_ref,
    sum_ref,
    kx,
    kt,
    grads,
    dk,
    dv,
):
    unit, step = pl.program_id(0), pl.program_id(1)
    scale = jnp.asarray(1.0 / math.sqrt(HEAD_DIM), BF16)

    @pl.when((unit == 0) & (step == 0))
    def _():
        for r in range(LEN // ROWS):
            rows = slice(r * ROWS, (r + 1) * ROWS)
            for u, ref in enumerate((wa_ref, wb_ref)):
                part = dot(branch_ref[rows, :], rows_of(ref), NT)
                grads[rows, u * UNIT : (u + 1) * UNIT] = part.astype(BF16)

    @pl.when(step == 0)
    def _():
        lane = lax.broadcasted_iota(jnp.int32, (LEN, UNIT), 1)
        keys = qkv_ref[:, lanes_at(unit, 2 * UNIT)]
        for h in range(HALF):
            kx[h] = jnp.where((lane // HEAD_DIM) == h, keys, hotk_ref[...])
        kt[...] = (keys * scale).T
        dk[...] = jnp.zeros_like(dk)
        dv[...] = jnp.zeros_like(dv)

    lane = lax.broadcasted_iota(jnp.int32, (TILE_B, UNIT), 1)
    rows = pl.ds(pl.multiple_of(step * TILE_B, TILE_B), TILE_B)
    queries = qkv_ref[rows, lanes_at(unit)] * scale
    grad = grads[rows, lanes_at(unit)]
    product = (grad.astype(F32) * ctx_ref[...].astype(F32)).T
    start = pl.multiple_of(win_ref[0, step], STEP)

    def run(width):
        window = pl.ds(start, width)
        values = qkv_ref[window, lanes_at(unit, 4 * UNIT)]
        d_queries, d_keys, d_values = [], [], []
        for h in range(HALF):
            mine = (lane // HEAD_DIM) == h
            q_mine = jnp.where(mine, queries, jnp.zeros_like(queries))
            g_mine = jnp.where(mine, grad, jnp.zeros_like(grad))
            scores = dot(kx[h, window, :], jnp.where(mine, queries, hotq_ref[...]), NT)
            weight = jnp.exp(scores - lse_ref[0, h : h + 1, :])
            d_weight = dot(values, g_mine, NT)
            row_term = jnp.sum(
                product[h * HEAD_DIM : (h + 1) * HEAD_DIM], axis=0, keepdims=True
            )
            d_scores = (weight * (d_weight - row_term)).astype(BF16)
            d_values.append(dot(weight.astype(BF16), g_mine))
            d_keys.append(dot(d_scores, q_mine))
            d_queries.append(dot(kt[h * HEAD_DIM : (h + 1) * HEAD_DIM, window], d_scores))
        dv[window, :] += d_values[0] + d_values[1]
        dk[window, :] += d_keys[0] + d_keys[1]
        out_ref[rows, lanes_at(unit)] = jnp.concatenate(d_queries, 0).T.astype(BF16)

    variants(win_ref[1, step], TILE_B, run)

    @pl.when(step == LEN // TILE_B - 1)
    def _():
        out_ref[:, lanes_at(unit, 2 * UNIT)] = dk[...].astype(BF16)
        out_ref[:, lanes_at(unit, 4 * UNIT)] = dv[...].astype(BF16)

    @pl.when((unit == HALF - 1) & (step == LEN // TILE_B - 1))
    def _():
        total = jnp.sum(out_ref[...].astype(F32), axis=0, keepdims=True)
        sum_ref[...] = jnp.broadcast_to(total, sum_ref.shape)


def attend_back_pair(win, qkv, hotq, hotk, branch_one, heads, pair, ctx, lse):
    return pl.pallas_call(
        attend_back_kernel,
        out_shape=(far((LEN, 6 * UNIT)), struct((8, 6 * UNIT), F32)),
        grid_spec=pltpu.PrefetchScalarGridSpec(
            num_scalar_prefetch=1,
            grid=(HALF, LEN // TILE_B),
            in_specs=[
                whole((LEN, 6 * UNIT)),
                pl.BlockSpec((TILE_B, UNIT), lambda n, i, win: (i, 0)),
                whole((LEN, UNIT)),
                whole((LEN, D)),
                *pair_specs(UNIT, 3, pair),
                pl.BlockSpec((TILE_B, UNIT), lambda n, i, win: (i, n)),
                pl.BlockSpec((1, 8, TILE_B), lambda n, i, win: (n, 0, i)),
            ],
            out_specs=[whole((LEN, 6 * UNIT)), whole((8, 6 * UNIT))],
            scratch_shapes=[
                pltpu.VMEM((HALF, LEN, UNIT), BF16),
                pltpu.VMEM((UNIT, LEN), BF16),
                pltpu.VMEM((LEN, 2 * UNIT), BF16),
                pltpu.VMEM((LEN, UNIT), F32),
                pltpu.VMEM((LEN, UNIT), F32),
            ],
        ),
        compiler_params=room(32),
        cost_estimate=cost(8e9, 8e6),
    )(win, qkv, hotq, hotk, branch_one, *pair_of(heads, pair), ctx, lse)


def norm_of(values):
    center = values - jnp.mean(values, axis=-1, keepdims=True)
    spread = jnp.mean(center * center, axis=-1, keepdims=True)
    scale = lax.rsqrt(spread + EPS)
    return center * scale, scale


def norm_back(normal, scale, grad, gain_row):
    scaled = grad * gain_row
    mean_e = jnp.mean(scaled, axis=-1, keepdims=True)
    mean_en = jnp.mean(scaled * normal, axis=-1, keepdims=True)
    return scale * (scaled - mean_e - normal * mean_en)


def first_norm_kernel(tok_ref, *refs):
    ctx_refs, weights, refs = refs[:4], refs[4:12], refs[12:]
    embed_ref, bout_ref, gain_ref, shift_ref, normal_ref, scale_ref, mid_ref, mid_t, hid_t, wout_ref = refs

    @pl.when(pl.program_id(0) == 0)
    def _():
        for j in range(8):
            wout_ref[j * UNIT : (j + 1) * UNIT, :] = rows_of(weights[j])

    hidden = tok_ref[...].astype(F32) + embed_ref[...]
    hid_t[...] = hidden.astype(BF16).T
    total = bout_ref[...]
    for p in range(4):
        total = total + dot(ctx_refs[p][...], wout_ref[2 * p * UNIT : 2 * (p + 1) * UNIT, :])
    normal, scale = norm_of(hidden + total)
    normal_ref[...] = normal.astype(BF16)
    scale_ref[...] = scale
    mid = (normal * gain_ref[...] + shift_ref[...]).astype(BF16)
    mid_ref[...] = mid
    mid_t[...] = mid.T


def first_norm(tokens, contexts, heads, embed_row, b_out, gain, shift):
    tile = pl.BlockSpec((ROWS, D), lambda i: (i, 0))
    column = pl.BlockSpec((D, ROWS), lambda i: (0, i))
    return pl.pallas_call(
        first_norm_kernel,
        out_shape=(
        far((LEN, D)),
        far((LEN, 1), F32),
        struct((LEN, D)),
        far((D, LEN)),
        far((D, LEN)),
        ),
        grid=(LEN // ROWS,),
        in_specs=[tile]
        + [pl.BlockSpec((ROWS, 2 * UNIT), lambda i: (i, 0))] * 4
        + half_specs(UNIT, 3)
        + [whole((1, D))] * 4,
        out_specs=[
            tile,
            pl.BlockSpec((ROWS, 1), lambda i: (i, 0)),
            tile,
            column,
            column,
        ],
        scratch_shapes=[pltpu.VMEM((D, D), BF16)],
        compiler_params=room(24),
        cost_estimate=cost(2.2e9, 20e6),
    )(tokens, *contexts, *eight(heads), embed_row, b_out, gain, shift)


def ffn_tile(mid_ref, up_refs, down_refs, bias_refs, act_ref, slope_ref):
    size = bias_refs[0].shape[1]
    pres = [
        dot(mid_ref[...], rows_of(up), NT) + bias[...] for up, bias in zip(up_refs, bias_refs)
    ]
    total = 0.0
    for u in range(HALF):
        columns = slice(u * size, (u + 1) * size)
        pre = pres[u]
        phi = 0.5 * (1.0 + lax.erf(pre * math.sqrt(0.5)))
        bell = jnp.exp(-0.5 * pre * pre) * (1.0 / math.sqrt(2.0 * math.pi))
        act = (pre * phi).astype(BF16)
        act_ref[:, columns] = act
        slope_ref[:, columns] = (phi + pre * bell).astype(BF16)
        total = total + dot(act, rows_of(down_refs[u]))
    return total


def ffn_kernel(mid_ref, *refs):
    *into, act_ref, slope_ref, total_ref = refs[6:]
    total = ffn_tile(mid_ref, refs[0:2], refs[2:4], refs[4:6], act_ref, slope_ref)
    for ref in into:
        total = total + ref[...]
    total_ref[...] = total


def ffn_specs(size, pair):
    return (
        [pl.BlockSpec((TILE_U, D), lambda i: (i, 0))]
        + pair_specs(size, 0, pair) * 2
        + [whole((1, size))] * 2
    )


def ffn_pair(mid_low, up, down, pair, bias, into):
    size = bias[0].shape[1]
    tile = lambda n: pl.BlockSpec((TILE_U, n), lambda i: (i, 0))
    return pl.pallas_call(
        ffn_kernel,
        out_shape=(
            far((LEN, 2 * size)),
            far((LEN, 2 * size)),
            struct((LEN, D), F32),
        ),
        in_specs=ffn_specs(size, pair) + [tile(D)] * len(into),
        out_specs=[tile(2 * size), tile(2 * size), tile(D)],
        grid=(LEN // TILE_U,),
        compiler_params=room(24),
        cost_estimate=cost(4.3e9, 18e6),
    )(mid_low, *pair_of(up, pair), *pair_of(down, pair), *bias, *into)


def ffn_last_kernel(mid_ref, *refs):
    into_ref, cot_ref, bias_ref, gain_ref, shift_ref = refs[6:11]
    act_ref, slope_ref, out_ref, low_ref, low_t, sum_ref = refs[11:]

    @pl.when(pl.program_id(0) == 0)
    def _():
        sum_ref[...] = jnp.zeros_like(sum_ref)

    total = ffn_tile(mid_ref, refs[0:2], refs[2:4], refs[4:6], act_ref, slope_ref)
    total = total + into_ref[...] + bias_ref[...]
    normal, scale = norm_of(mid_ref[...].astype(F32) + total)
    out_ref[...] = (normal * gain_ref[...] + shift_ref[...]).astype(BF16)
    cot = cot_ref[...].astype(F32)
    low = norm_back(normal, scale, cot, gain_ref[...]).astype(BF16)
    low_ref[...] = low
    low_t[...] = low.T
    sums = [jnp.sum(v, axis=0, keepdims=True) for v in (low.astype(F32), cot * normal, cot)]
    for j in range(3):
        sum_ref[j : j + 1, :] += sums[j]


def ffn_last(mid_low, up, down, pair, bias, into, cot, *rows):
    size = bias[0].shape[1]
    tile = lambda n: pl.BlockSpec((TILE_U, n), lambda i: (i, 0))
    return pl.pallas_call(
        ffn_last_kernel,
        out_shape=(
            far((LEN, 2 * size)),
            far((LEN, 2 * size)),
            far((LEN, D)),
            struct((LEN, D)),
            struct((D, LEN)),
            struct((8, D), F32),
        ),
        in_specs=ffn_specs(size, pair) + [tile(D)] * 2 + [whole((1, D))] * 3,
        out_specs=[tile(2 * size), tile(2 * size), tile(D), tile(D)]
        + [pl.BlockSpec((D, TILE_U), lambda i: (0, i)), whole((8, D))],
        grid=(LEN // TILE_U,),
        compiler_params=room(30),
        cost_estimate=cost(4.3e9, 30e6),
    )(
        mid_low, *pair_of(up, pair), *pair_of(down, pair), *bias, into, cot, *rows
    )


def ffn_back_kernel(branch_hbm, *refs):
    down_hbm, up_hbm, slope_hbm, refs = refs[0:6], refs[6:12], refs[12:16], refs[16:]
    one_hbm, scale_ref, gain_ref, refs = refs[0], refs[1], refs[2], refs[3:]
    pre_hbm, sum_ref, low_ref, low_t, norm_sum_ref, refs = (
        refs[0:4],
        refs[4],
        refs[5],
        refs[6],
        refs[7],
        refs[8:],
    )
    branch, down, up, slope, total, one, sems = refs
    size = up.shape[1]
    plan = ((0, 0), (0, 1), (1, 0), (1, 1), (2, None), (3, None), (4, None), (5, None))
    first = pltpu.make_async_copy(branch_hbm, branch, sems.at[0])
    first.start()
    copies = []
    for j, (piece, which) in enumerate(plan):
        if which is None:
            down_part, up_part = down_hbm[piece], up_hbm[piece]
        else:
            down_part, up_part = down_hbm[piece].at[which], up_hbm[piece].at[which]
        columns = slice((j % 2) * size, (j % 2 + 1) * size)
        group = [
            pltpu.make_async_copy(down_part, down.at[j], sems.at[1 + 3 * j]),
            pltpu.make_async_copy(
                slope_hbm[j // 2].at[:, columns], slope.at[j], sems.at[2 + 3 * j]
            ),
            pltpu.make_async_copy(up_part, up.at[j], sems.at[3 + 3 * j]),
        ]
        for copy in group:
            copy.start()
        copies.append(group)
    last = pltpu.make_async_copy(one_hbm, one, sems.at[25])
    last.start()
    first.wait()
    stores = []
    norm_sums = [0.0] * 3
    for j in range(len(plan)):
        for copy in copies[j]:
            copy.wait()
        if j == len(plan) - 1:
            last.wait()
        columns = slice((j % 2) * size, (j % 2 + 1) * size)
        sums = 0.0
        for r in range(LEN // ROWS):
            rows = slice(r * ROWS, (r + 1) * ROWS)
            d_act = dot(branch[rows, :], down[j], NT)
            d_pre = (d_act * slope[j, rows, :].astype(F32)).astype(BF16)
            slope[j, rows, :] = d_pre
            sums = sums + jnp.sum(d_pre.astype(F32), axis=0, keepdims=True)
            part = dot(d_pre, up[j])
            if j == 0:
                total[rows, :] = part
            elif j < len(plan) - 1:
                total[rows, :] += part
            else:
                d_mid = total[rows, :] + part + branch[rows, :].astype(F32)
                normal = one[rows, :].astype(F32)
                low = norm_back(normal, scale_ref[rows, :], d_mid, gain_ref[...]).astype(BF16)
                low_ref[rows, :] = low
                low_t[:, rows] = low.T
                for k, v in enumerate((low.astype(F32), d_mid * normal, d_mid)):
                    norm_sums[k] = norm_sums[k] + jnp.sum(v, axis=0, keepdims=True)
        sum_ref[j : j + 1, :] = sums
        store = pltpu.make_async_copy(slope.at[j], pre_hbm[j // 2].at[:, columns], sems.at[26 + j])
        store.start()
        stores.append(store)
    for k in range(3):
        norm_sum_ref[k : k + 1, :] = norm_sums[k]
    for store in stores:
        store.wait()


def ffn_back(branch_two, down, up, slopes, normal_one, scale_one, gain):
    size = down[2].shape[0]
    hbm = pl.BlockSpec(memory_space=pl.ANY)
    return pl.pallas_call(
        ffn_back_kernel,
        out_shape=(far((LEN, 2 * size)),) * 4
        + (struct((8, size), F32), struct((LEN, D)), struct((D, LEN)), struct((8, D), F32)),
        grid=(1,),
        in_specs=[hbm] * 18 + [whole((LEN, 1)), whole((1, D))],
        out_specs=[hbm] * 4 + [whole((8, size)), whole((LEN, D)), whole((D, LEN)), whole((8, D))],
        scratch_shapes=[
            pltpu.VMEM((LEN, D), BF16),
            pltpu.VMEM((8, size, D), BF16),
            pltpu.VMEM((8, size, D), BF16),
            pltpu.VMEM((8, LEN, size), BF16),
            pltpu.VMEM((LEN, D), F32),
            pltpu.VMEM((LEN, D), BF16),
            pltpu.SemaphoreType.DMA((34,)),
        ],
        compiler_params=room(52),
        cost_estimate=cost(17e9, 40e6),
    )(branch_two, *down, *up, *slopes, normal_one, scale_one, gain)


class Run(NamedTuple):
    which: int
    first: int
    second: int
    size: int
    base: int
    stride: int


def unit_runs(count, size):
    half = size // 2
    return [Run(0, r * half // count, half + r * half // count, half // count, r * half // count, half) for r in range(count)]


def head_runs(which, count):
    return [Run(which, 2 * j * UNIT, (2 * j + 1) * UNIT, UNIT, 2 * j * UNIT, UNIT) for j in range(count)]


def part_width(part):
    return sum(2 * run.size for run in part)


def grad_kernel(blocks, side_from, outputs, lefts, got_from, left_at, *refs):
    n_right = 3 * lefts
    left_hbm, right_hbm, refs = refs[:lefts], refs[lefts : lefts + n_right], refs[lefts + n_right :]
    got_hbm, refs = (None, refs) if got_from is None else (refs[0], refs[1:])
    out_hbm, (left, right, got, out, sems) = refs[: len(outputs)], refs[len(outputs) :]
    count = [0]

    def copy_of(source, target):
        copy = pltpu.make_async_copy(source, target, sems.at[count[0]])
        copy.start()
        count[0] += 1
        return copy

    first = [
        copy_of(left_hbm[k].at[:, left_at[side]], left.at[k, side])
        for k in range(lefts)
        for side in range(2)
    ]
    chunks, at = [], 0
    for part, far in blocks:
        for run in part:
            copies = []
            for h in range(2):
                if far:
                    piece, source = 1 + h, run.second if side_from else run.first
                else:
                    piece, source = 0, run.second if h else run.first
                copies.append(
                    copy_of(
                        right_hbm[3 * run.which + piece].at[:, source : source + run.size],
                        right.at[:, at + h * run.size : at + (h + 1) * run.size],
                    )
                )
            chunks.append((run.which, at, 2 * run.size, copies))
            at += 2 * run.size
    if got_from is not None:
        first.append(copy_of(got_hbm.at[:, :, got_from : got_from + at], got))
    for copy in first:
        copy.wait()
    stores = []
    for which, at, size, copies in chunks:
        for copy in copies:
            copy.wait()
        columns = slice(at, at + size)
        for side in range(2):
            total = dot(left[which, side].reshape(D // 2, LEN), right[:, columns])
            if got_from is not None:
                total = total + got[side, :, columns].astype(F32)
            out[side, :, columns] = total.astype(BF16)
        for (start, end, side), target in zip(outputs, out_hbm):
            if start <= at < end:
                place = slice(at - start, at - start + size)
                if side is None:
                    stores.append(copy_of(out.at[:, :, columns], target.at[:, :, place]))
                else:
                    stores.append(copy_of(out.at[side, :, columns], target.at[:, place]))
    for copy in stores:
        copy.wait()


def grad_call(info, left_t, rights, blocks, side, outputs, got=None, got_from=None):
    width = sum(part_width(part) for part, _ in blocks)
    hbm = pl.BlockSpec(memory_space=pl.ANY)
    lefts = len(left_t)
    operands = [v.reshape(4, 2, D // 8, LEN) for v in left_t] + [v for r in rights for v in r]
    operands += [] if got is None else [got]
    shapes = [
        (2, D // 2, end - start) if at is None else (D // 2, end - start) for start, end, at in outputs
    ]
    return pl.pallas_call(
        functools.partial(grad_kernel, blocks, side, outputs, lefts, got_from),
        out_shape=tuple(far(shape) for shape in shapes),
        grid_spec=pltpu.PrefetchScalarGridSpec(
            num_scalar_prefetch=1,
            grid=(1,),
            in_specs=[hbm] * len(operands),
            out_specs=[hbm] * len(shapes),
            scratch_shapes=[
                pltpu.VMEM((lefts, 2, 4, D // 8, LEN), BF16),
                pltpu.VMEM((LEN, width), BF16),
                pltpu.VMEM((2, D // 2, 128 if got is None else width), BF16),
                pltpu.VMEM((2, D // 2, width), BF16),
                pltpu.SemaphoreType.DMA((48,)),
            ],
        ),
        compiler_params=room(32),
        cost_estimate=cost(2 * D * LEN * width, 10e6),
    )(info, *operands)


def column_runs(part, swap):
    at = 0
    for run in part:
        for h in range(2):
            source = at + (1 - h if swap else h) * run.size
            yield at + h * run.size, source, run.size
        at += 2 * run.size


def add_kernel(part, swap, mine_ref, got_ref, out_ref):
    rows = out_ref.shape[0]
    mine, got = mine_ref[...].reshape(rows, -1), got_ref[...].reshape(rows, -1)
    for at, source, size in column_runs(part, swap):
        total = mine[:, at : at + size].astype(F32) + got[:, source : source + size].astype(F32)
        out_ref[:, at : at + size] = total.astype(BF16)


def block_spec(array, where, width):
    side, column = where
    if len(array.shape) == 3:
        return pl.BlockSpec((1, D // 2, width), lambda *_: (side, 0, column))
    return pl.BlockSpec((D // 2, width), lambda *_: (0, column))


def add_parts(mine, got, part, swap):
    width = part_width(part)
    return pl.pallas_call(
        functools.partial(add_kernel, part, swap),
        out_shape=struct((D // 2, width)),
        grid=(1,),
        in_specs=[block_spec(*v, width) for v in (mine, got)],
        out_specs=whole((D // 2, width)),
        compiler_params=room(24),
        cost_estimate=cost(1e6, 3e6),
    )(mine[0], got[0])


def split_kernel(parts, info_ref, *refs):
    ins, out_refs = refs[: 3 * len(parts)], refs[3 * len(parts) :]
    span = D // 8
    for k in range(4):
        rows = pl.ds(pl.multiple_of((info_ref[2] ^ k) * span, span), span)
        first = 0
        for p, part in enumerate(parts):
            mine, from_x, from_y = [
                (ref[0, rows, :] if len(ref.shape) == 3 else ref[rows, :]).astype(F32)
                for ref in ins[3 * p : 3 * p + 3]
            ]
            for at, source, size in column_runs(part, True):
                total = mine[:, at : at + size] + from_y[:, at : at + size]
                total = total + from_x[:, source : source + size]
                out_refs[k][:, first + at : first + at + size] = total.astype(BF16)
            first += part_width(part)


def split_z(info, parts, sources):
    width = sum(part_width(part) for part in parts)
    specs = [
        block_spec(*v, part_width(part)) for part, triple in zip(parts, sources) for v in triple
    ]
    out = pl.pallas_call(
        functools.partial(split_kernel, parts),
        out_shape=(struct((D // 8, width)),) * 4,
        grid_spec=pltpu.PrefetchScalarGridSpec(
            num_scalar_prefetch=1,
            grid=(1,),
            in_specs=specs,
            out_specs=[whole((D // 8, width))] * 4,
        ),
        compiler_params=room(24),
        cost_estimate=cost(1e6, 4e6),
    )(info, *[v[0] for triple in sources for v in triple])
    return [out[0]] + [send_dp(out[k], 2 * k) for k in (1, 2, 3)]


def finish_kernel(runs, turned, info_ref, *refs):
    parts, outs = refs[:4], refs[4:]
    at = 0
    for run in runs:
        for h in range(2):
            columns = slice(at, at + run.size)
            total = parts[0][:, columns].astype(F32)
            for part in parts[1:]:
                total = total + part[:, columns].astype(F32)
            spot = pl.ds(pl.multiple_of(run.base + info_ref[h] * run.stride, UNIT), run.size)
            if turned[run.which]:
                outs[run.which][spot, :] = total.T
            else:
                outs[run.which][:, spot] = total
            at += run.size


def finish(info, values, parts, turned):
    rows = D // 8
    runs = tuple(run for part in parts for run in part)
    sizes = [sum(2 * r.size for r in runs if r.which == k) for k in range(len(turned))]
    shapes = [(size, rows) if t else (rows, size) for size, t in zip(sizes, turned)]
    return pl.pallas_call(
        functools.partial(finish_kernel, runs, turned),
        out_shape=tuple(struct(shape, F32) for shape in shapes),
        grid_spec=pltpu.PrefetchScalarGridSpec(
            num_scalar_prefetch=1,
            grid=(1,),
            in_specs=[whole((rows, sum(sizes)))] * 4,
            out_specs=[whole(shape) for shape in shapes],
        ),
        compiler_params=room(24),
        cost_estimate=cost(1e6, 4e6),
    )(info, *values)


def input_grad_kernel(branch_ref, *refs):
    grads, heads, (out_ref, sum_ref, weight, sems) = refs[:4], refs[4:10], refs[10:]
    step = pl.program_id(0)
    plan = ((0, 0), (0, 1), (1, 0), (1, 1), (2, None), (3, None), (4, None), (5, None))
    copies = []
    for j, (piece, which) in enumerate(plan):
        source = heads[piece] if which is None else heads[piece].at[which]
        for k in range(3):
            at = ((j // 2) * 6 + 2 * k + j % 2) * UNIT
            copies.append(
                pltpu.make_async_copy(
                    source.at[k * UNIT : (k + 1) * UNIT, :],
                    weight.at[at : at + UNIT, :],
                    sems.at[3 * j + k],
                )
            )

    @pl.when(step == 0)
    def _():
        for copy in copies:
            copy.start()
        sum_ref[...] = jnp.zeros_like(sum_ref)

    total = branch_ref[...].astype(F32)
    for p in range(4):

        @pl.when(step == 0)
        def _():
            for copy in copies[6 * p : 6 * p + 6]:
                copy.wait()

        total = total + dot(grads[p][...], weight[6 * p * UNIT : 6 * (p + 1) * UNIT, :])
    out_ref[...] = total
    sum_ref[0:1, :] += jnp.sum(total, axis=0, keepdims=True)


def input_grad(branch_one, d_qkv, heads):
    tile = pl.BlockSpec((ROWS, D), lambda i: (i, 0))
    width = d_qkv[0].shape[1]
    return pl.pallas_call(
        input_grad_kernel,
        out_shape=(far((LEN, D), F32), struct((8, D), F32)),
        grid=(LEN // ROWS,),
        in_specs=[tile]
        + [pl.BlockSpec((ROWS, width), lambda i: (i, 0))] * 4
        + [pl.BlockSpec(memory_space=pl.ANY)] * 6,
        out_specs=[tile, whole((8, D))],
        scratch_shapes=[pltpu.VMEM((4 * width, D), BF16), pltpu.SemaphoreType.DMA((24,))],
        compiler_params=room(26),
        cost_estimate=cost(6.4e9, 20e6),
    )(branch_one, *d_qkv, *heads)


def exchange_kernel(sum_ref, row_ref, total_ref, rows_ref, got, sems_a, sems_b):
    devices = GRID_DP * GRID_MP
    me = lax.axis_index("dp") * GRID_MP + lax.axis_index("mp")

    def place(index):
        return {"dp": index // GRID_MP, "mp": index % GRID_MP}

    barrier = pltpu.get_barrier_semaphore()

    def greet(k, carry):
        target = (me + k) % devices
        pl.semaphore_signal(
            barrier, inc=1, device_id=place(target), device_id_type=pl.DeviceIdType.MESH
        )
        return carry

    lax.fori_loop(1, devices, greet, 0)
    pl.semaphore_wait(barrier, devices - 1)

    def copies(k):
        target = (me + k) % devices
        first = pltpu.make_async_remote_copy(
            src_ref=sum_ref.at[target],
            dst_ref=got.at[k],
            send_sem=sems_a.at[0, k],
            recv_sem=sems_a.at[1, k],
            device_id=place(target),
            device_id_type=pl.DeviceIdType.MESH,
        )
        second = pltpu.make_async_remote_copy(
            src_ref=row_ref,
            dst_ref=rows_ref.at[k],
            send_sem=sems_b.at[0, k],
            recv_sem=sems_b.at[1, k],
            device_id=place(target),
            device_id_type=pl.DeviceIdType.MESH,
        )
        return first, second

    def start(k, carry):
        for copy in copies(k):
            copy.start()
        return carry

    lax.fori_loop(1, devices, start, 0)
    rows_ref[0] = row_ref[...]

    def finish_copy(k, carry):
        for copy in copies(k):
            copy.wait()
        return carry

    lax.fori_loop(1, devices, finish_copy, 0)
    total_ref[...] = sum_ref[me] + jnp.sum(got[1:], axis=0)


def exchange(sums, row):
    devices = GRID_DP * GRID_MP
    vmem = pl.BlockSpec(memory_space=pltpu.VMEM)
    return pl.pallas_call(
        exchange_kernel,
        out_shape=(struct(sums.shape[1:], F32), struct((devices,) + row.shape, F32)),
        in_specs=[vmem, vmem],
        out_specs=[vmem, vmem],
        scratch_shapes=[
            pltpu.VMEM(sums.shape, F32),
            pltpu.SemaphoreType.DMA((2, devices)),
            pltpu.SemaphoreType.DMA((2, devices)),
        ],
        compiler_params=pltpu.CompilerParams(collective_id=0, has_side_effects=True),
        cost_estimate=cost(1e6, 1e6),
    )(sums, row)


def natural_blocks(halves, x_at, mp_at):
    join = lambda a, b: jnp.where(x_at == 0, jnp.concatenate([a, b]), jnp.concatenate([b, a]))
    stacked = jnp.stack(
        [
            join(halves[0], halves[1]),
            join(halves[2], halves[3]),
            join(halves[4], halves[6]),
            join(halves[5], halves[7]),
        ]
    )
    return jnp.stack([stacked[i ^ mp_at] for i in range(4)])


def body_rows(
    tokens,
    segment_ids,
    time_steps,
    w_qkv,
    b_qv,
    w_out,
    b_out,
    gain_one,
    shift_one,
    w_up,
    b_up,
    w_down,
    b_down,
    gain_two,
    shift_two,
    w_time,
    b_time,
    cotangent,
):
    dp_at, mp_at = lax.axis_index("dp"), lax.axis_index("mp")
    x_at, z_at = dp_at % 2, dp_at // 2
    info = jnp.stack([x_at, 1 - x_at, z_at, mp_at]).astype(jnp.int32)
    row = lambda v: v.astype(F32)[None, :]
    width = w_qkv.shape[2]

    heads_own, heads_first = pack_heads(info, w_qkv, w_out)
    heads = fetch(heads_own, heads_first)
    up_own, up_first, down_own, down_first = pack_units(info, w_up, w_down)
    up = fetch(up_own, up_first)
    down = fetch(down_own, down_first)
    q_rows, v_rows, up_rows = fetch_bias([b_qv[0:1], b_qv[1:2], b_up[None, :]], x_at)
    zero = jnp.zeros((1, width // 2), F32)

    own_step = lax.dynamic_slice_in_dim(time_steps, mp_at, 1, 0)
    segment_row = lax.dynamic_index_in_dim(segment_ids, mp_at, 0, keepdims=False)
    features = time_features(own_step)
    embed_row = jnp.dot(features, w_time.astype(F32), precision=HIGHEST_PRECISION)
    embed_row = embed_row + row(b_time)
    hidden_low = (tokens.astype(F32) + embed_row).astype(BF16)
    hotq, hotk = mark_segments(segment_row)
    win_f, win_b = windows(segment_row, TILE_F), windows(segment_row, TILE_B)

    qkv, ctx, lse = [], [], []
    for p in range(4):
        first, second = 2 * p, 2 * p + 1
        bias = jnp.concatenate(
            [q_rows[first], q_rows[second], zero, zero, v_rows[first], v_rows[second]], axis=1
        )
        parts = attend_pair(win_f, hidden_low, heads, p, bias, hotq, hotk)
        for kept, part in zip((qkv, ctx, lse), parts):
            kept.append(part)
    normal_one, scale_one, mid_low, mid_t, hidden_t = first_norm(
        tokens, ctx, heads, embed_row, row(b_out), row(gain_one), row(shift_one)
    )

    act, slope, ffn = [], [], ()
    for p in range(3):
        act_p, slope_p, *ffn = ffn_pair(mid_low, up, down, p, up_rows[2 * p : 2 * p + 2], ffn)
        act.append(act_p)
        slope.append(slope_p)
    act_p, slope_p, out_rows, branch_two, branch_two_t, sums_two = ffn_last(
        mid_low,
        up,
        down,
        3,
        up_rows[6:8],
        *ffn,
        cotangent,
        *[row(v) for v in (b_down, gain_two, shift_two)],
    )
    act.append(act_p)
    slope.append(slope_p)

    units = act[0].shape[1]
    down_parts = [(run,) for run in unit_runs(2, units)]
    up_parts = [down_parts[0], (down_parts[1][0], *head_runs(1, 1))]
    qkv_part = tuple(head_runs(0, 3))

    def two_way(left_t, rights, parts, cover):
        blocks = tuple((part, far) for part in parts for far in (False, True))
        one, two = (part_width(part) for part in parts)
        every = 2 * (one + two)
        (sent,) = grad_call(info, left_t, [r[1:] for r in rights], blocks, 1, ((0, every, None),))
        got = send_mp(sent, 1)
        covered = cover()
        outputs = (
            (0, one, None),
            (one, 2 * one, None),
            (2 * one, every, 0),
            (2 * one, every, 1),
        )
        result = grad_call(
            info, left_t, [r[:1] + r[2:] for r in rights], blocks, 0, outputs, got, 0
        )
        return covered, result

    def first_sends(blocks):
        own, far, keep, leave = blocks
        return own, keep, send_mp(far, 2), send_dp(leave, 1)

    def second_sends(sums, parts):
        own, keep, from_y, from_x = sums
        low = add_parts((own, (1, 0)), (from_y, (1, 0)), parts[0], False)
        x_two = send_dp(low, 1)
        low = add_parts((keep, (0, 1)), (from_x, (0, 1)), parts[1], True)
        y_two = send_mp(low, 2)
        here = (0, 0)
        return (
            ((own, here), (x_two, here), (from_y, here)),
            ((keep, here), (from_x, here), (y_two, here)),
        )

    def ffn_part():
        return ffn_back(
            branch_two, down, up, slope, normal_one, scale_one, row(gain_one)
        )

    (*d_pre, sums_up, branch_one, branch_one_t, sums_one), down_blocks = two_way(
        [branch_two_t], [act], down_parts, ffn_part
    )
    down_sums = first_sends(down_blocks)
    d_qkv, qkv_sums = [None] * 4, [None] * 4

    def back(p):
        d_qkv[p], qkv_sums[p] = attend_back_pair(
            win_b, qkv[p], hotq, hotk, branch_one, heads, p, ctx[p], lse[p]
        )

    _, up_blocks = two_way([mid_t, branch_one_t], [d_pre, ctx], up_parts, lambda: back(1))
    down_last = second_sends(down_sums, down_parts)
    up_sums = first_sends(up_blocks)
    back(2)
    down_values = split_z(info, down_parts, down_last)
    back(3)
    up_last = second_sends(up_sums, up_parts)
    wide = part_width(qkv_part)
    far_only, own_only = ((qkv_part, True),), ((qkv_part, False),)
    (sent,) = grad_call(
        info, [hidden_t], [d_qkv[1:]], own_only + far_only, 1, ((0, 2 * wide, None),)
    )
    got = send_mp(sent, 1)
    up_values = split_z(info, up_parts, up_last)
    sides = ((0, wide, 0), (0, wide, 1))
    far_keep, far_leave = grad_call(
        info, [hidden_t], [[d_qkv[1]] + d_qkv[2:]], far_only, 0, sides, got, wide
    )
    far_x = send_dp(far_leave, 1)
    back(0)
    here = (0, 0)
    far_low = add_parts((far_keep, here), (far_x, here), qkv_part, True)
    far_y = send_mp(far_low, 2)
    own_keep, own_leave = grad_call(
        info, [hidden_t], [d_qkv[:1] + d_qkv[2:]], own_only, 0, sides, got, 0
    )
    own_x = send_dp(own_leave, 1)
    grad_tokens, sums_in = input_grad(branch_one, d_qkv, heads)
    qkv_values = split_z(info, (qkv_part,), (((own_keep, here), (own_x, here), (far_y, here)),))

    spread = lambda v: v.reshape(GRID_DP * GRID_MP, -1)
    spread_blocks = lambda b: b.reshape(GRID_MP, GRID_DP, -1).transpose(1, 0, 2).reshape(GRID_DP * GRID_MP, -1)
    rows = [spread(sums[j]) for sums in (sums_two, sums_one) for j in range(3)]
    rows.append(spread_blocks(natural_blocks([sums_up[j] for j in range(8)], x_at, mp_at)))
    for j in (0, 2):
        halves = [
            qkv_sums[p][0, (2 * j + u) * UNIT : (2 * j + u + 1) * UNIT]
            for p in range(4)
            for u in range(HALF)
        ]
        rows.append(spread_blocks(natural_blocks(halves, x_at, mp_at)))
    tail_row = jnp.concatenate(
        [sums_in[0:1], jnp.broadcast_to(own_step.astype(F32)[None, :], (1, UNIT))], axis=1
    )
    totals, all_rows = exchange(jnp.concatenate(rows, axis=1)[:, None, :], tail_row)
    all_rows = all_rows[:, 0]
    span = D // (GRID_DP * GRID_MP)
    own = [totals[0, j * span : (j + 1) * span] for j in range(6)]
    device_at = dp_at * GRID_MP + mp_at
    all_grads = all_rows[:, :D]
    dims = device_at * span + jnp.arange(span, dtype=jnp.int32)
    ladder = (dims % (D // 2)).astype(F32)
    frequency = jnp.exp(ladder * (-math.log(10000.0) / (D // 2)))
    angles = all_rows[:, D : D + 1] * frequency[None, :]
    own_features = jnp.where((dims < D // 2)[None, :], jnp.sin(angles), jnp.cos(angles))
    g_w_time = jnp.dot(own_features.T, all_grads, precision=HIGHEST_PRECISION)
    g_b_time = lax.dynamic_slice_in_dim(jnp.sum(all_grads, axis=0), device_at * span, span, 0)

    (g_w_qkv,) = finish(info, qkv_values, (qkv_part,), (False,))
    (g_w_down,) = finish(info, down_values, down_parts, (True,))
    g_w_up, g_w_out = finish(info, up_values, up_parts, (False, True))
    up_end = totals.shape[1] - 2 * span
    return (
        out_rows,
        grad_tokens,
        g_w_qkv.reshape(D // 8, 3, width),
        totals[0, up_end:].reshape(2, 1, -1),
        g_w_out,
        own[3],
        own[4],
        own[5],
        g_w_up,
        totals[:, 6 * span : up_end],
        g_w_down,
        own[0],
        own[1],
        own[2],
        g_w_time,
        g_b_time,
    )


def solution(mesh):
    placed = (
        P(("dp", "mp"), None),
        P("dp", None),
        P("dp"),
        P(None, None, "mp"),
        P(None, "mp"),
        P("mp", None),
        P(),
        P(),
        P(),
        P(None, "mp"),
        P("mp"),
        P("mp", None),
        P(),
        P(),
        P(),
        P(),
        P(),
        P(("dp", "mp"), None),
    )
    rows = mesh.shape["dp"], mesh.shape["mp"]

    def body(*args):
        if args[0].shape[0] != LEN or rows != (GRID_DP, GRID_MP):
            return body_split(*args)
        return body_rows(*args)

    return jax.shard_map(
        body,
        mesh=mesh,
        in_specs=placed,
        out_specs=(
            P(("dp", "mp"), None),
            P(("dp", "mp"), None),
            P("dp", None, "mp"),
            P(None, "mp", "dp"),
            P("mp", "dp"),
            P(("dp", "mp")),
            P(("dp", "mp")),
            P(("dp", "mp")),
            P("dp", "mp"),
            P("mp", "dp"),
            P("mp", "dp"),
            P(("dp", "mp")),
            P(("dp", "mp")),
            P(("dp", "mp")),
            P(("dp", "mp"), None),
            P(("dp", "mp")),
        ),
        check_vma=False,
    )
```

```python
import functools
import math
from typing import NamedTuple

import jax
import jax.numpy as jnp
from jax import lax
from jax.experimental import pallas as pl
from jax.experimental.pallas import tpu as pltpu
from jax.sharding import PartitionSpec as P


D = 1024
HEAD_DIM = 64
LEN = 1024


EPS = 1e-05
HIGHEST_PRECISION = lax.Precision.HIGHEST


def time_features(step_values):
    half_width = D // 2
    ladder = jnp.arange(half_width, dtype=jnp.float32)
    frequency = jnp.exp(ladder * (-math.log(10000.0) / half_width))
    angles = step_values.astype(jnp.float32)[:, None] * frequency[None, :]
    return jnp.concatenate([jnp.sin(angles), jnp.cos(angles)], axis=1)


def layer_norm(values, gain_vec, shift_vec):
    center = values - jnp.mean(values, axis=-1, keepdims=True)
    spread = jnp.mean(center * center, axis=-1, keepdims=True)
    return center * lax.rsqrt(spread + EPS) * gain_vec + shift_vec


def exact_gelu(values):
    return jax.nn.gelu(values, approximate=False)


def project_qkv(hidden_full, w_qkv, b_qv):
    width_local = w_qkv.shape[2]
    w_flat = w_qkv.reshape(w_qkv.shape[0], 3 * width_local)
    bias_row = jnp.concatenate([b_qv[0], jnp.zeros((width_local,), b_qv.dtype), b_qv[1]]).astype(
        jnp.float32
    )
    product = jnp.dot(hidden_full, w_flat, preferred_element_type=jnp.float32)
    return (product + bias_row[None, :]).astype(jnp.bfloat16)


def head_parts(qkv_seq):
    width_local = qkv_seq.shape[1] // 3
    head_local = width_local // HEAD_DIM
    shaped = qkv_seq.reshape(qkv_seq.shape[0], 3, head_local, HEAD_DIM)
    return (shaped[:, 0], shaped[:, 1], shaped[:, 2])


def masked_scores(queries, keys_part, segment_row):
    scores = jnp.einsum("qhd,khd->hqk", queries, keys_part, preferred_element_type=jnp.float32)
    scores = scores * (1.0 / math.sqrt(HEAD_DIM))
    same_doc = segment_row[:, None] == segment_row[None, :]
    return jnp.where(same_doc[None, :, :], scores, -1e30)


def attend_forward(inputs):
    qkv_seq, segment_row = inputs
    queries, keys_part, values_part = head_parts(qkv_seq)
    masked = masked_scores(queries, keys_part, segment_row)
    top_score = jnp.max(masked, axis=2, keepdims=True)
    weights_exp = jnp.exp(masked - top_score)
    totals = jnp.sum(weights_exp, axis=2, keepdims=True)
    probability = weights_exp / totals
    context = jnp.einsum(
        "hqk,khd->qhd",
        probability.astype(jnp.bfloat16),
        values_part,
        preferred_element_type=jnp.float32,
    )
    log_total = (top_score + jnp.log(totals))[:, :, 0]
    return (context.reshape(qkv_seq.shape[0], -1).astype(jnp.bfloat16), log_total)


def attend_backward(inputs):
    qkv_seq, grad_seq, log_total, segment_row = inputs
    queries, keys_part, values_part = head_parts(qkv_seq)
    masked = masked_scores(queries, keys_part, segment_row)
    probability = jnp.exp(masked - log_total[:, :, None])
    grad_heads = grad_seq.reshape(grad_seq.shape[0], -1, HEAD_DIM)
    d_values = jnp.einsum(
        "hqk,qhd->khd",
        probability.astype(jnp.bfloat16),
        grad_heads,
        preferred_element_type=jnp.float32,
    )
    d_probs = jnp.einsum(
        "qhd,khd->hqk", grad_heads, values_part, preferred_element_type=jnp.float32
    )
    row_terms = jnp.sum(probability * d_probs, axis=2, keepdims=True)
    d_scores = (probability * (d_probs - row_terms)).astype(jnp.bfloat16)
    score_scale = 1.0 / math.sqrt(HEAD_DIM)
    d_queries = (
        jnp.einsum("hqk,khd->qhd", d_scores, keys_part, preferred_element_type=jnp.float32)
        * score_scale
    )
    d_keys = (
        jnp.einsum("hqk,qhd->khd", d_scores, queries, preferred_element_type=jnp.float32)
        * score_scale
    )
    stacked = jnp.stack([d_queries, d_keys, d_values], axis=1)
    return stacked.reshape(qkv_seq.shape[0], -1).astype(jnp.bfloat16)


def body_split(
    tokens,
    segment_ids,
    time_steps,
    w_qkv,
    b_qv,
    w_out,
    b_out,
    gain_one,
    shift_one,
    w_up,
    b_up,
    w_down,
    b_down,
    gain_two,
    shift_two,
    w_time,
    b_time,
    cotangent,
):
    row_count = tokens.shape[0]
    seq_local = time_steps.shape[0]
    width_local = w_qkv.shape[2]
    gain_one_f = gain_one.astype(jnp.float32)
    shift_one_f = shift_one.astype(jnp.float32)
    gain_two_f = gain_two.astype(jnp.float32)
    shift_two_f = shift_two.astype(jnp.float32)
    w_flat = w_qkv.reshape(D, 3 * width_local)
    features = time_features(time_steps)
    embed_rows = jnp.dot(features, w_time.astype(jnp.float32), precision=HIGHEST_PRECISION)
    embed_rows = embed_rows + b_time.astype(jnp.float32)[None, :]
    row_seq = (lax.axis_index("mp") * row_count + jnp.arange(row_count, dtype=jnp.int32)) // LEN
    selector = (row_seq[:, None] == jnp.arange(seq_local, dtype=jnp.int32)[None, :]).astype(
        jnp.float32
    )
    hidden_in = tokens.astype(jnp.float32) + jnp.dot(
        selector, embed_rows, precision=HIGHEST_PRECISION
    )
    hidden_low = hidden_in.astype(jnp.bfloat16)
    hidden_full = lax.all_gather(hidden_low, "mp", axis=0, tiled=True)
    qkv_full = project_qkv(hidden_full, w_qkv, b_qv)
    ctx_blocks, log_totals = lax.map(
        attend_forward, (qkv_full.reshape(seq_local, LEN, 3 * width_local), segment_ids)
    )
    context = ctx_blocks.reshape(seq_local * LEN, width_local)
    rows_in = context
    attn_sum = lax.psum_scatter(
        jnp.dot(rows_in, w_out, preferred_element_type=jnp.float32).astype(jnp.bfloat16),
        "mp",
        scatter_dimension=0,
        tiled=True,
    ).astype(jnp.float32)
    attn_out = attn_sum + b_out.astype(jnp.float32)[None, :]
    mid_in = hidden_in + attn_out
    mid_norm = layer_norm(mid_in, gain_one_f, shift_one_f)
    mid_low = mid_norm.astype(jnp.bfloat16)
    mid_full = lax.all_gather(mid_low, "mp", axis=0, tiled=True)
    pre_act = (
        jnp.dot(mid_full, w_up, preferred_element_type=jnp.float32)
        + b_up.astype(jnp.float32)[None, :]
    )
    activated = exact_gelu(pre_act).astype(jnp.bfloat16)
    rows_in = activated
    ffn_part = lax.psum_scatter(
        jnp.dot(rows_in, w_down, preferred_element_type=jnp.float32).astype(jnp.bfloat16),
        "mp",
        scatter_dimension=0,
        tiled=True,
    ).astype(jnp.float32)
    out_in = mid_norm + ffn_part + b_down.astype(jnp.float32)[None, :]
    out_rows, out_back = jax.vjp(layer_norm, out_in, gain_two_f, shift_two_f)
    grad_two, grad_gain_two, grad_shift_two = out_back(cotangent.astype(jnp.float32))
    branch_two = grad_two.astype(jnp.bfloat16)
    grad_b_down = jnp.sum(branch_two.astype(jnp.float32), axis=0)
    _, gelu_back = jax.vjp(exact_gelu, pre_act)
    cot_full = lax.all_gather(branch_two, "mp", axis=0, tiled=True)
    d_act = jnp.dot(cot_full, w_down.T, preferred_element_type=jnp.float32)
    grad_w_down = jnp.dot(activated.T, cot_full, preferred_element_type=jnp.float32)
    d_pre = gelu_back(d_act)[0].astype(jnp.bfloat16)
    grad_w_up = jnp.dot(mid_full.T, d_pre, preferred_element_type=jnp.float32)
    grad_b_up = jnp.sum(d_pre.astype(jnp.float32), axis=0)
    rows_in = d_pre
    d_mid_part = lax.psum_scatter(
        jnp.dot(rows_in, w_up.T, preferred_element_type=jnp.float32).astype(jnp.bfloat16),
        "mp",
        scatter_dimension=0,
        tiled=True,
    ).astype(jnp.float32)
    _, mid_back = jax.vjp(layer_norm, mid_in, gain_one_f, shift_one_f)
    grad_one, grad_gain_one, grad_shift_one = mid_back(grad_two + d_mid_part)
    branch_one = grad_one.astype(jnp.bfloat16)
    grad_b_out = jnp.sum(branch_one.astype(jnp.float32), axis=0)
    cot_attn = lax.all_gather(branch_one, "mp", axis=0, tiled=True)
    d_context = jnp.dot(cot_attn, w_out.T, preferred_element_type=jnp.float32).astype(jnp.bfloat16)
    grad_w_out = jnp.dot(context.T, cot_attn, preferred_element_type=jnp.float32)
    grad_blocks = lax.map(
        attend_backward,
        (
            qkv_full.reshape(seq_local, LEN, 3 * width_local),
            d_context.reshape(seq_local, LEN, width_local),
            log_totals,
            segment_ids,
        ),
    )
    d_qkv = grad_blocks.reshape(seq_local * LEN, 3 * width_local)
    grad_w_qkv = jnp.dot(hidden_full.T, d_qkv, preferred_element_type=jnp.float32).reshape(
        D, 3, width_local
    )
    qkv_sums = jnp.sum(d_qkv.astype(jnp.float32), axis=0).reshape(3, width_local)
    grad_b_qv = jnp.stack([qkv_sums[0], qkv_sums[2]]).reshape(2, 1, width_local)
    rows_in = d_qkv
    input_part = lax.psum_scatter(
        jnp.dot(rows_in, w_flat.T, preferred_element_type=jnp.float32).astype(jnp.bfloat16),
        "mp",
        scatter_dimension=0,
        tiled=True,
    ).astype(jnp.float32)
    grad_tokens = grad_one + input_part
    grad_embed = jnp.dot(selector.T, grad_tokens, precision=HIGHEST_PRECISION)
    grad_w_time = jnp.dot(features.T, grad_embed, precision=HIGHEST_PRECISION)
    grad_b_time = jnp.sum(grad_embed, axis=0)
    sharded = (
        lax.psum_scatter(
            grad_w_qkv.astype(jnp.bfloat16), "dp", scatter_dimension=0, tiled=True
        ).astype(jnp.float32),
        lax.psum_scatter(
            grad_b_qv.astype(jnp.bfloat16), "dp", scatter_dimension=2, tiled=True
        ).astype(jnp.float32),
        lax.psum_scatter(
            grad_w_out.astype(jnp.bfloat16), "dp", scatter_dimension=1, tiled=True
        ).astype(jnp.float32),
        lax.psum_scatter(
            grad_w_up.astype(jnp.bfloat16), "dp", scatter_dimension=0, tiled=True
        ).astype(jnp.float32),
        lax.psum_scatter(
            grad_b_up.reshape(1, -1).astype(jnp.bfloat16), "dp", scatter_dimension=1, tiled=True
        ).astype(jnp.float32),
        lax.psum_scatter(
            grad_w_down.astype(jnp.bfloat16), "dp", scatter_dimension=1, tiled=True
        ).astype(jnp.float32),
    )
    shared = (
        lax.psum_scatter(grad_w_time, ("dp", "mp"), scatter_dimension=0, tiled=True),
        lax.psum_scatter(grad_b_time, ("dp", "mp"), scatter_dimension=0, tiled=True),
        lax.psum_scatter(grad_gain_one, ("dp", "mp"), scatter_dimension=0, tiled=True),
        lax.psum_scatter(grad_shift_one, ("dp", "mp"), scatter_dimension=0, tiled=True),
        lax.psum_scatter(grad_gain_two, ("dp", "mp"), scatter_dimension=0, tiled=True),
        lax.psum_scatter(grad_shift_two, ("dp", "mp"), scatter_dimension=0, tiled=True),
        lax.psum_scatter(grad_b_out, ("dp", "mp"), scatter_dimension=0, tiled=True),
        lax.psum_scatter(grad_b_down, ("dp", "mp"), scatter_dimension=0, tiled=True),
    )
    return (
        out_rows.astype(jnp.bfloat16),
        grad_tokens,
        sharded[0],
        sharded[1],
        sharded[2],
        shared[6],
        shared[2],
        shared[3],
        sharded[3],
        sharded[4],
        sharded[5],
        shared[7],
        shared[4],
        shared[5],
        shared[0],
        shared[1],
    )


GRID_DP = 8
GRID_MP = 4
HALF = 2
UNIT = 128
F32 = jnp.float32
BF16 = jnp.bfloat16
TILE_F = 512
TILE_B = 256
TILE_U = 256
ROWS = 256
GRAIN = 256
STEP = 128
FAR = -(2.0**100)
NN = (((1,), (0,)), ((), ()))
NT = (((1,), (1,)), ((), ()))


def dot(left, right, dims=NN):
    return lax.dot_general(left, right, dims, preferred_element_type=F32)


def after(values, others):
    return lax.optimization_barrier((values, others))[0]


def half_of(values, which, axis):
    size = values.shape[axis] // 2
    return lax.dynamic_slice_in_dim(values, which * size, size, axis)


def whole(shape):
    return pl.BlockSpec(shape, lambda *_: (0,) * len(shape))


def struct(shape, kind=BF16):
    return jax.ShapeDtypeStruct(shape, kind)


def far(shape, kind=BF16):
    return pltpu.HBM(shape, kind)


def room(mib):
    return pltpu.CompilerParams(vmem_limit_bytes=mib * 2**20)


def cost(flops, moved):
    return pl.CostEstimate(flops=int(flops), bytes_accessed=int(moved), transcendentals=0)


def send_mp(values, bit):
    return lax.ppermute(values, "mp", [(i, i ^ bit) for i in range(GRID_MP)])


def send_dp(values, bit):
    return lax.ppermute(values, "dp", [(i, i ^ bit) for i in range(GRID_DP)])


def fetch(own, first_half):
    near = send_mp(own, 1)
    far_a = send_mp(first_half, 2)
    near_a = send_mp(far_a, 1)
    far_b = send_dp(far_a, 1)
    near_b = send_mp(far_b, 1)
    return [own, near, far_a, near_a, far_b, near_b]


def pack_heads_kernel(info_ref, qkv_ref, out_ref, both_ref, first_ref):
    for u in range(HALF):
        for j in range(3):
            at = pl.ds(pl.multiple_of(info_ref[u] * UNIT, UNIT), UNIT)
            both_ref[u, j * UNIT : (j + 1) * UNIT, :] = qkv_ref[j, :, at].T
        at = pl.ds(pl.multiple_of(info_ref[u] * UNIT, UNIT), UNIT)
        both_ref[u, 3 * UNIT :, :] = out_ref[at, :]
    first_ref[...] = both_ref[0]


def pack_heads(info, w_qkv, w_out):
    return pl.pallas_call(
        pack_heads_kernel,
        out_shape=(far((HALF, 4 * UNIT, D)), far((4 * UNIT, D))),
        grid_spec=pltpu.PrefetchScalarGridSpec(
            num_scalar_prefetch=1,
            grid=(1,),
            in_specs=[whole((3, D, 2 * UNIT)), whole((2 * UNIT, D))],
            out_specs=[whole((HALF, 4 * UNIT, D)), whole((4 * UNIT, D))],
        ),
        compiler_params=room(60),
        cost_estimate=cost(1e6, 5e6),
    )(info, w_qkv.transpose(1, 0, 2), w_out)


def pack_units_kernel(info_ref, up_ref, down_ref, up_both, up_first, down_both, down_first):
    step = pl.program_id(0)
    up = up_ref[...].T
    up_both[0] = up
    down_both[0] = down_ref[...]

    @pl.when(step == 0)
    def _():
        up_first[...] = up
        down_first[...] = down_ref[...]


def pack_units(info, w_up, w_down):
    size = w_down.shape[0] // 2
    return pl.pallas_call(
        pack_units_kernel,
        out_shape=(far((HALF, size, D)), far((size, D))) * 2,
        grid_spec=pltpu.PrefetchScalarGridSpec(
            num_scalar_prefetch=1,
            grid=(HALF,),
            in_specs=[
                pl.BlockSpec((D, size), lambda i, info: (0, info[i])),
                pl.BlockSpec((size, D), lambda i, info: (info[i], 0)),
            ],
            out_specs=[pl.BlockSpec((1, size, D), lambda i, info: (i, 0, 0)), whole((size, D))] * 2,
        ),
        compiler_params=room(24),
        cost_estimate=cost(1e6, 10e6),
    )(info, w_up, w_down)


def fetch_bias(own, x_at):
    packed = jnp.concatenate(own, axis=1)
    near, far = send_mp(packed, 1), send_mp(packed, 2)
    near_far = send_mp(far, 1)
    order = [(packed, x_at), (packed, 1 - x_at), (near, x_at), (near, 1 - x_at)]
    order += [(v, at) for at in (x_at, 1 - x_at) for v in (far, near_far)]
    pieces, start = [], 0
    for row in own:
        size = row.shape[1]
        pieces.append(
            [half_of(v[:, start : start + size], at, 1).astype(F32) for v, at in order]
        )
        start += size
    return pieces


def half_specs(rows, block):
    both = [pl.BlockSpec((1, rows, D), lambda *_, u=u: (u, block, 0)) for u in range(HALF)]
    return both * 2 + [pl.BlockSpec((rows, D), lambda *_: (block, 0))] * 4


def eight(pieces):
    own, near, far_a, near_a, far_b, near_b = pieces
    return [own, own, near, near, far_a, near_a, far_b, near_b]


def pair_specs(rows, block, pair):
    return half_specs(rows, block)[2 * pair : 2 * pair + 2]


def pair_of(pieces, pair):
    return eight(pieces)[2 * pair : 2 * pair + 2]


def rows_of(ref):
    return ref[...].reshape(-1, D)


def mark_segments(segment_row):
    lane = jnp.arange(UNIT, dtype=jnp.int32)[None, :]
    hot = segment_row[:, None] == (lane % HEAD_DIM)
    used = (lane % HEAD_DIM) < 8
    return (
        jnp.where(hot & used, 1.0, 0.0).astype(BF16),
        jnp.where(used & ~hot, FAR, 0.0).astype(BF16),
    )


def windows(segment_row, tile):
    first, last = segment_row[::tile], segment_row[tile - 1 :: tile]
    low = jnp.sum(segment_row[None, :] < first[:, None], axis=1) // STEP * STEP
    high = jnp.sum(segment_row[None, :] <= last[:, None], axis=1)
    count = jnp.maximum((high - low + GRAIN - 1) // GRAIN, tile // GRAIN)
    low = jnp.minimum(low, LEN - count * GRAIN)
    return jnp.stack([low, count]).astype(jnp.int32)


def variants(count, tile, run):
    for n in range(tile // GRAIN, LEN // GRAIN + 1):

        @pl.when(count == n)
        def _(n=n):
            run(n * GRAIN)


def lanes_at(at, base=0):
    return pl.ds(pl.multiple_of(base + at * UNIT, UNIT), UNIT)


def attend_kernel(
    win_ref, x_ref, *refs
):
    weights, (bias_ref, hotq_ref, hotk_ref, qkv_ref, ctx_ref, lse_ref, w_ref, kx) = refs[:2], refs[2:]
    unit, step = pl.program_id(0), pl.program_id(1)

    @pl.when((unit == 0) & (step == 0))
    def _():
        for u in range(HALF):
            part = rows_of(weights[u])
            for j in range(3):
                at = (2 * j + u) * UNIT
                w_ref[at : at + UNIT, :] = part[j * UNIT : (j + 1) * UNIT]
        for r in range(LEN // ROWS):
            rows = slice(r * ROWS, (r + 1) * ROWS)
            qkv_ref[rows, :] = (dot(x_ref[rows, :], w_ref[...], NT) + bias_ref[...]).astype(BF16)

    @pl.when(step == 0)
    def _():
        lane = lax.broadcasted_iota(jnp.int32, (LEN, UNIT), 1)
        keys = qkv_ref[:, lanes_at(unit, 2 * UNIT)]
        for h in range(HALF):
            kx[h] = jnp.where((lane // HEAD_DIM) == h, keys, hotk_ref[...])

    lane = lax.broadcasted_iota(jnp.int32, (TILE_F, UNIT), 1)
    rows = pl.ds(pl.multiple_of(step * TILE_F, TILE_F), TILE_F)
    queries = qkv_ref[rows, lanes_at(unit)] * jnp.asarray(1.0 / math.sqrt(HEAD_DIM), BF16)
    start = pl.multiple_of(win_ref[0, step], STEP)

    def run(width):
        window = pl.ds(start, width)
        values = qkv_ref[window, lanes_at(unit, 4 * UNIT)]
        scores = [
            dot(
                jnp.where((lane // HEAD_DIM) == h, queries, hotq_ref[...]), kx[h, window, :], NT
            )
            for h in range(HALF)
        ]
        outs = []
        for h in range(HALF):
            top = jnp.max(scores[h], axis=1, keepdims=True)
            weight = jnp.exp(scores[h] - top)
            total = jnp.sum(weight, axis=1, keepdims=True)
            outs.append(dot(weight.astype(BF16), values) * (1.0 / total))
            lse_ref[0, h : h + 1, :] = (top + jnp.log(total)).T
        ctx_ref[...] = jnp.where(lane < HEAD_DIM, outs[0], outs[1]).astype(BF16)

    variants(win_ref[1, step], TILE_F, run)


def attend_pair(win, hidden_low, heads, pair, bias, hotq, hotk):
    return pl.pallas_call(
        attend_kernel,
        out_shape=(
            far((LEN, 6 * UNIT)),
            far((LEN, 2 * UNIT)),
            far((HALF, 8, LEN), F32),
        ),
        grid_spec=pltpu.PrefetchScalarGridSpec(
            num_scalar_prefetch=1,
            grid=(HALF, LEN // TILE_F),
            in_specs=[whole((LEN, D))]
            + pair_specs(4 * UNIT, 0, pair)
            + [
                whole((1, 6 * UNIT)),
                pl.BlockSpec((TILE_F, UNIT), lambda n, i, win: (i, 0)),
                whole((LEN, UNIT)),
            ],
            out_specs=[
                whole((LEN, 6 * UNIT)),
                pl.BlockSpec((TILE_F, UNIT), lambda n, i, win: (i, n)),
                pl.BlockSpec((1, 8, TILE_F), lambda n, i, win: (n, 0, i)),
            ],
            scratch_shapes=[pltpu.VMEM((6 * UNIT, D), BF16), pltpu.VMEM((HALF, LEN, UNIT), BF16)],
        ),
        compiler_params=room(32),
        cost_estimate=cost(6e9, 8e6),
    )(win, hidden_low, *pair_of(heads, pair), bias, hotq, hotk)


def attend_back_kernel(
    win_ref,
    qkv_ref,
    hotq_ref,
    hotk_ref,
    branch_ref,
    wa_ref,
    wb_ref,
    ctx_ref,
    lse_ref,
    out_ref,
    sum_ref,
    kx,
    kt,
    grads,
    dk,
    dv,
):
    unit, step = pl.program_id(0), pl.program_id(1)
    scale = jnp.asarray(1.0 / math.sqrt(HEAD_DIM), BF16)

    @pl.when((unit == 0) & (step == 0))
    def _():
        weight = jnp.concatenate([rows_of(wa_ref), rows_of(wb_ref)], axis=0)
        for r in range(LEN // ROWS):
            rows = slice(r * ROWS, (r + 1) * ROWS)
            grads[rows, :] = dot(branch_ref[rows, :], weight, NT).astype(BF16)

    @pl.when(step == 0)
    def _():
        lane = lax.broadcasted_iota(jnp.int32, (LEN, UNIT), 1)
        keys = qkv_ref[:, lanes_at(unit, 2 * UNIT)]
        for h in range(HALF):
            kx[h] = jnp.where((lane // HEAD_DIM) == h, keys, hotk_ref[...])
        kt[...] = (keys * scale).T
        dk[...] = jnp.zeros_like(dk)
        dv[...] = jnp.zeros_like(dv)

    lane = lax.broadcasted_iota(jnp.int32, (TILE_B, UNIT), 1)
    rows = pl.ds(pl.multiple_of(step * TILE_B, TILE_B), TILE_B)
    queries = qkv_ref[rows, lanes_at(unit)] * scale
    grad = grads[rows, lanes_at(unit)]
    product = (grad.astype(F32) * ctx_ref[...].astype(F32)).T
    start = pl.multiple_of(win_ref[0, step], STEP)

    def run(width):
        window = pl.ds(start, width)
        values = qkv_ref[window, lanes_at(unit, 4 * UNIT)]
        d_queries, d_keys, d_values = [], [], []
        for h in range(HALF):
            mine = (lane // HEAD_DIM) == h
            q_mine = jnp.where(mine, queries, jnp.zeros_like(queries))
            g_mine = jnp.where(mine, grad, jnp.zeros_like(grad))
            scores = dot(kx[h, window, :], jnp.where(mine, queries, hotq_ref[...]), NT)
            weight = jnp.exp(scores - lse_ref[0, h : h + 1, :])
            d_weight = dot(values, g_mine, NT)
            row_term = jnp.sum(
                product[h * HEAD_DIM : (h + 1) * HEAD_DIM], axis=0, keepdims=True
            )
            d_scores = (weight * (d_weight - row_term)).astype(BF16)
            d_values.append(dot(weight.astype(BF16), g_mine))
            d_keys.append(dot(d_scores, q_mine))
            d_queries.append(dot(kt[h * HEAD_DIM : (h + 1) * HEAD_DIM, window], d_scores))
        dv[window, :] += d_values[0] + d_values[1]
        dk[window, :] += d_keys[0] + d_keys[1]
        out_ref[rows, lanes_at(unit)] = jnp.concatenate(d_queries, 0).T.astype(BF16)

    variants(win_ref[1, step], TILE_B, run)

    @pl.when(step == LEN // TILE_B - 1)
    def _():
        out_ref[:, lanes_at(unit, 2 * UNIT)] = dk[...].astype(BF16)
        out_ref[:, lanes_at(unit, 4 * UNIT)] = dv[...].astype(BF16)

    @pl.when((unit == HALF - 1) & (step == LEN // TILE_B - 1))
    def _():
        total = jnp.sum(out_ref[...].astype(F32), axis=0, keepdims=True)
        sum_ref[...] = jnp.broadcast_to(total, sum_ref.shape)


def attend_back_pair(win, qkv, hotq, hotk, branch_one, heads, pair, ctx, lse):
    return pl.pallas_call(
        attend_back_kernel,
        out_shape=(far((LEN, 6 * UNIT)), struct((8, 6 * UNIT), F32)),
        grid_spec=pltpu.PrefetchScalarGridSpec(
            num_scalar_prefetch=1,
            grid=(HALF, LEN // TILE_B),
            in_specs=[
                whole((LEN, 6 * UNIT)),
                pl.BlockSpec((TILE_B, UNIT), lambda n, i, win: (i, 0)),
                whole((LEN, UNIT)),
                whole((LEN, D)),
                *pair_specs(UNIT, 3, pair),
                pl.BlockSpec((TILE_B, UNIT), lambda n, i, win: (i, n)),
                pl.BlockSpec((1, 8, TILE_B), lambda n, i, win: (n, 0, i)),
            ],
            out_specs=[whole((LEN, 6 * UNIT)), whole((8, 6 * UNIT))],
            scratch_shapes=[
                pltpu.VMEM((HALF, LEN, UNIT), BF16),
                pltpu.VMEM((UNIT, LEN), BF16),
                pltpu.VMEM((LEN, 2 * UNIT), BF16),
                pltpu.VMEM((LEN, UNIT), F32),
                pltpu.VMEM((LEN, UNIT), F32),
            ],
        ),
        compiler_params=room(32),
        cost_estimate=cost(8e9, 8e6),
    )(win, qkv, hotq, hotk, branch_one, *pair_of(heads, pair), ctx, lse)


def norm_of(values):
    center = values - jnp.mean(values, axis=-1, keepdims=True)
    spread = jnp.mean(center * center, axis=-1, keepdims=True)
    scale = lax.rsqrt(spread + EPS)
    return center * scale, scale


def norm_back(normal, scale, grad, gain_row):
    scaled = grad * gain_row
    mean_e = jnp.mean(scaled, axis=-1, keepdims=True)
    mean_en = jnp.mean(scaled * normal, axis=-1, keepdims=True)
    return scale * (scaled - mean_e - normal * mean_en)


def first_norm_kernel(tok_ref, *refs):
    ctx_refs, weights, refs = refs[:4], refs[4:12], refs[12:]
    embed_ref, bout_ref, gain_ref, shift_ref, normal_ref, scale_ref, mid_ref, mid_t, hid_t, wout_ref = refs

    @pl.when(pl.program_id(0) == 0)
    def _():
        for j in range(8):
            wout_ref[j * UNIT : (j + 1) * UNIT, :] = rows_of(weights[j])

    hidden = tok_ref[...].astype(F32) + embed_ref[...]
    hid_t[...] = hidden.astype(BF16).T
    total = bout_ref[...]
    for p in range(4):
        total = total + dot(ctx_refs[p][...], wout_ref[2 * p * UNIT : 2 * (p + 1) * UNIT, :])
    normal, scale = norm_of(hidden + total)
    normal_ref[...] = normal.astype(BF16)
    scale_ref[...] = scale
    mid = (normal * gain_ref[...] + shift_ref[...]).astype(BF16)
    mid_ref[...] = mid
    mid_t[...] = mid.T


def first_norm(tokens, contexts, heads, embed_row, b_out, gain, shift):
    tile = pl.BlockSpec((ROWS, D), lambda i: (i, 0))
    column = pl.BlockSpec((D, ROWS), lambda i: (0, i))
    return pl.pallas_call(
        first_norm_kernel,
        out_shape=(
        far((LEN, D)),
        far((LEN, 1), F32),
        struct((LEN, D)),
        far((D, LEN)),
        far((D, LEN)),
        ),
        grid=(LEN // ROWS,),
        in_specs=[tile]
        + [pl.BlockSpec((ROWS, 2 * UNIT), lambda i: (i, 0))] * 4
        + half_specs(UNIT, 3)
        + [whole((1, D))] * 4,
        out_specs=[
            tile,
            pl.BlockSpec((ROWS, 1), lambda i: (i, 0)),
            tile,
            column,
            column,
        ],
        scratch_shapes=[pltpu.VMEM((D, D), BF16)],
        compiler_params=room(24),
        cost_estimate=cost(2.2e9, 20e6),
    )(tokens, *contexts, *eight(heads), embed_row, b_out, gain, shift)


def ffn_tile(mid_ref, up_refs, down_refs, bias_refs, act_ref, slope_ref):
    size = bias_refs[0].shape[1]
    pres = [
        dot(mid_ref[...], rows_of(up), NT) + bias[...] for up, bias in zip(up_refs, bias_refs)
    ]
    total = 0.0
    for u in range(HALF):
        columns = slice(u * size, (u + 1) * size)
        pre = pres[u]
        phi = 0.5 * (1.0 + lax.erf(pre * math.sqrt(0.5)))
        bell = jnp.exp(-0.5 * pre * pre) * (1.0 / math.sqrt(2.0 * math.pi))
        act = (pre * phi).astype(BF16)
        act_ref[:, columns] = act
        slope_ref[:, columns] = (phi + pre * bell).astype(BF16)
        total = total + dot(act, rows_of(down_refs[u]))
    return total


def ffn_kernel(mid_ref, *refs):
    *into, act_ref, slope_ref, total_ref = refs[6:]
    total = ffn_tile(mid_ref, refs[0:2], refs[2:4], refs[4:6], act_ref, slope_ref)
    for ref in into:
        total = total + ref[...]
    total_ref[...] = total


def ffn_specs(size, pair):
    return (
        [pl.BlockSpec((TILE_U, D), lambda i: (i, 0))]
        + pair_specs(size, 0, pair) * 2
        + [whole((1, size))] * 2
    )


def ffn_pair(mid_low, up, down, pair, bias, into):
    size = bias[0].shape[1]
    tile = lambda n: pl.BlockSpec((TILE_U, n), lambda i: (i, 0))
    return pl.pallas_call(
        ffn_kernel,
        out_shape=(
            far((LEN, 2 * size)),
            far((LEN, 2 * size)),
            struct((LEN, D), F32),
        ),
        in_specs=ffn_specs(size, pair) + [tile(D)] * len(into),
        out_specs=[tile(2 * size), tile(2 * size), tile(D)],
        grid=(LEN // TILE_U,),
        compiler_params=room(24),
        cost_estimate=cost(4.3e9, 18e6),
    )(mid_low, *pair_of(up, pair), *pair_of(down, pair), *bias, *into)


def ffn_last_kernel(mid_ref, *refs):
    into_ref, cot_ref, bias_ref, gain_ref, shift_ref = refs[6:11]
    act_ref, slope_ref, out_ref, low_ref, low_t, sum_ref = refs[11:]

    @pl.when(pl.program_id(0) == 0)
    def _():
        sum_ref[...] = jnp.zeros_like(sum_ref)

    total = ffn_tile(mid_ref, refs[0:2], refs[2:4], refs[4:6], act_ref, slope_ref)
    total = total + into_ref[...] + bias_ref[...]
    normal, scale = norm_of(mid_ref[...].astype(F32) + total)
    out_ref[...] = (normal * gain_ref[...] + shift_ref[...]).astype(BF16)
    cot = cot_ref[...].astype(F32)
    low = norm_back(normal, scale, cot, gain_ref[...]).astype(BF16)
    low_ref[...] = low
    low_t[...] = low.T
    sums = [jnp.sum(v, axis=0, keepdims=True) for v in (low.astype(F32), cot * normal, cot)]
    for j in range(3):
        sum_ref[j : j + 1, :] += sums[j]


def ffn_last(mid_low, up, down, pair, bias, into, cot, *rows):
    size = bias[0].shape[1]
    tile = lambda n: pl.BlockSpec((TILE_U, n), lambda i: (i, 0))
    return pl.pallas_call(
        ffn_last_kernel,
        out_shape=(
            far((LEN, 2 * size)),
            far((LEN, 2 * size)),
            far((LEN, D)),
            far((LEN, D)),
            far((D, LEN)),
            struct((8, D), F32),
        ),
        in_specs=ffn_specs(size, pair) + [tile(D)] * 2 + [whole((1, D))] * 3,
        out_specs=[tile(2 * size), tile(2 * size), tile(D), tile(D)]
        + [pl.BlockSpec((D, TILE_U), lambda i: (0, i)), whole((8, D))],
        grid=(LEN // TILE_U,),
        compiler_params=room(30),
        cost_estimate=cost(4.3e9, 30e6),
    )(
        mid_low, *pair_of(up, pair), *pair_of(down, pair), *bias, into, cot, *rows
    )


def ffn_back_kernel(branch_hbm, *refs):
    down_hbm, up_hbm, slope_hbm, refs = refs[0:6], refs[6:12], refs[12:16], refs[16:]
    one_hbm, scale_ref, gain_ref, refs = refs[0], refs[1], refs[2], refs[3:]
    pre_hbm, sum_ref, low_ref, low_t, norm_sum_ref, refs = (
        refs[0:4],
        refs[4],
        refs[5],
        refs[6],
        refs[7],
        refs[8:],
    )
    branch, down, up, slope, total, one, low, low_turned, sems = refs
    size = up.shape[1]
    plan = ((0, 0), (0, 1), (1, 0), (1, 1), (2, None), (3, None), (4, None), (5, None))
    first = pltpu.make_async_copy(branch_hbm, branch, sems.at[0])
    first.start()
    copies = []
    for j, (piece, which) in enumerate(plan):
        if which is None:
            down_part, up_part = down_hbm[piece], up_hbm[piece]
        else:
            down_part, up_part = down_hbm[piece].at[which], up_hbm[piece].at[which]
        columns = slice((j % 2) * size, (j % 2 + 1) * size)
        group = [
            pltpu.make_async_copy(down_part, down.at[j], sems.at[1 + 3 * j]),
            pltpu.make_async_copy(
                slope_hbm[j // 2].at[:, columns], slope.at[j], sems.at[2 + 3 * j]
            ),
            pltpu.make_async_copy(up_part, up.at[j], sems.at[3 + 3 * j]),
        ]
        for copy in group:
            copy.start()
        copies.append(group)
    last = pltpu.make_async_copy(one_hbm, one, sems.at[25])
    last.start()
    first.wait()
    stores = []
    norm_sums = [0.0] * 3
    for j in range(len(plan)):
        for copy in copies[j]:
            copy.wait()
        if j == len(plan) - 1:
            last.wait()
        columns = slice((j % 2) * size, (j % 2 + 1) * size)
        sums = 0.0
        for r in range(LEN // ROWS):
            rows = slice(r * ROWS, (r + 1) * ROWS)
            d_act = dot(branch[rows, :], down[j], NT)
            d_pre = (d_act * slope[j, rows, :].astype(F32)).astype(BF16)
            slope[j, rows, :] = d_pre
            sums = sums + jnp.sum(d_pre.astype(F32), axis=0, keepdims=True)
            part = dot(d_pre, up[j])
            if j == 0:
                total[rows, :] = part
            elif j < len(plan) - 1:
                total[rows, :] += part
            else:
                d_mid = total[rows, :] + part + branch[rows, :].astype(F32)
                normal = one[rows, :].astype(F32)
                part = norm_back(normal, scale_ref[rows, :], d_mid, gain_ref[...]).astype(BF16)
                low[rows, :] = part
                low_turned[:, rows] = part.T
                for k, (source, target) in enumerate(
                    (
                        (low.at[rows, :], low_ref.at[rows, :]),
                        (low_turned.at[:, rows], low_t.at[:, rows]),
                    )
                ):
                    store = pltpu.make_async_copy(source, target, sems.at[34 + 2 * r + k])
                    store.start()
                    stores.append(store)
                for k, v in enumerate((part.astype(F32), d_mid * normal, d_mid)):
                    norm_sums[k] = norm_sums[k] + jnp.sum(v, axis=0, keepdims=True)
        sum_ref[j : j + 1, :] = sums
        store = pltpu.make_async_copy(slope.at[j], pre_hbm[j // 2].at[:, columns], sems.at[26 + j])
        store.start()
        stores.append(store)
    for k in range(3):
        norm_sum_ref[k : k + 1, :] = norm_sums[k]
    for store in stores:
        store.wait()


def ffn_back(branch_two, down, up, slopes, normal_one, scale_one, gain):
    size = down[2].shape[0]
    hbm = pl.BlockSpec(memory_space=pltpu.HBM)
    return pl.pallas_call(
        ffn_back_kernel,
        out_shape=(far((LEN, 2 * size)),) * 4
        + (struct((8, size), F32), far((LEN, D)), far((D, LEN)), struct((8, D), F32)),
        grid=(1,),
        in_specs=[hbm] * 18 + [whole((LEN, 1)), whole((1, D))],
        out_specs=[hbm] * 4 + [whole((8, size)), hbm, hbm, whole((8, D))],
        scratch_shapes=[
            pltpu.VMEM((LEN, D), BF16),
            pltpu.VMEM((8, size, D), BF16),
            pltpu.VMEM((8, size, D), BF16),
            pltpu.VMEM((8, LEN, size), BF16),
            pltpu.VMEM((LEN, D), F32),
            pltpu.VMEM((LEN, D), BF16),
            pltpu.VMEM((LEN, D), BF16),
            pltpu.VMEM((D, LEN), BF16),
            pltpu.SemaphoreType.DMA((42,)),
        ],
        compiler_params=room(52),
        cost_estimate=cost(17e9, 40e6),
    )(branch_two, *down, *up, *slopes, normal_one, scale_one, gain)


class Run(NamedTuple):
    which: int
    first: int
    second: int
    size: int
    base: int
    stride: int


def unit_runs(count, size):
    half = size // 2
    return [Run(0, r * half // count, half + r * half // count, half // count, r * half // count, half) for r in range(count)]


def head_runs(which, count):
    return [Run(which, 2 * j * UNIT, (2 * j + 1) * UNIT, UNIT, 2 * j * UNIT, UNIT) for j in range(count)]


def part_width(part):
    return sum(2 * run.size for run in part)


def grad_kernel(blocks, side_from, outputs, lefts, got_from, left_at, *refs):
    n_right = 3 * lefts
    left_hbm, right_hbm, refs = refs[:lefts], refs[lefts : lefts + n_right], refs[lefts + n_right :]
    got_hbm, refs = (None, refs) if got_from is None else (refs[0], refs[1:])
    out_hbm, (left, right, got, out, sems) = refs[: len(outputs)], refs[len(outputs) :]
    count = [0]

    def copy_of(source, target):
        copy = pltpu.make_async_copy(source, target, sems.at[count[0]])
        copy.start()
        count[0] += 1
        return copy

    ready = {}
    chunks, at = [], 0
    for part, far in blocks:
        for run in part:
            copies = []
            if (run.which, 0) not in ready:
                source = left_hbm[run.which]
                ready[run.which, 0] = copy_of(source.at[:, left_at[0]], left.at[run.which, 0])
            for h in range(2):
                if far:
                    piece, source = 1 + h, run.second if side_from else run.first
                else:
                    piece, source = 0, run.second if h else run.first
                copies.append(
                    copy_of(
                        right_hbm[3 * run.which + piece].at[:, source : source + run.size],
                        right.at[:, at + h * run.size : at + (h + 1) * run.size],
                    )
                )
            columns = slice(at, at + 2 * run.size)
            if got_from is not None:
                source = got_hbm.at[:, :, got_from + at : got_from + at + 2 * run.size]
                copies.append(copy_of(source, got.at[:, :, columns]))
            if (run.which, 1) not in ready:
                source = left_hbm[run.which]
                ready[run.which, 1] = copy_of(source.at[:, left_at[1]], left.at[run.which, 1])
            chunks.append((run.which, at, 2 * run.size, copies))
            at += 2 * run.size
    stores = []
    for which, at, size, copies in chunks:
        for copy in copies:
            copy.wait()
        columns = slice(at, at + size)
        for side in range(2):
            if (which, side) in ready:
                ready.pop((which, side)).wait()
            total = dot(left[which, side].reshape(D // 2, LEN), right[:, columns])
            if got_from is not None:
                total = total + got[side, :, columns].astype(F32)
            out[side, :, columns] = total.astype(BF16)
        for (start, end, side), target in zip(outputs, out_hbm):
            if start <= at < end:
                place = slice(at - start, at - start + size)
                if side is None:
                    stores.append(copy_of(out.at[:, :, columns], target.at[:, :, place]))
                else:
                    stores.append(copy_of(out.at[side, :, columns], target.at[:, place]))
    for copy in stores:
        copy.wait()


def grad_call(info, left_t, rights, blocks, side, outputs, got=None, got_from=None):
    width = sum(part_width(part) for part, _ in blocks)
    hbm = pl.BlockSpec(memory_space=pltpu.HBM)
    lefts = len(left_t)
    operands = [v.reshape(4, 2, D // 8, LEN) for v in left_t] + [v for r in rights for v in r]
    operands += [] if got is None else [got]
    shapes = [
        (2, D // 2, end - start) if at is None else (D // 2, end - start) for start, end, at in outputs
    ]
    return pl.pallas_call(
        functools.partial(grad_kernel, blocks, side, outputs, lefts, got_from),
        out_shape=tuple(far(shape) for shape in shapes),
        grid_spec=pltpu.PrefetchScalarGridSpec(
            num_scalar_prefetch=1,
            grid=(1,),
            in_specs=[hbm] * len(operands),
            out_specs=[hbm] * len(shapes),
            scratch_shapes=[
                pltpu.VMEM((lefts, 2, 4, D // 8, LEN), BF16),
                pltpu.VMEM((LEN, width), BF16),
                pltpu.VMEM((2, D // 2, 128 if got is None else width), BF16),
                pltpu.VMEM((2, D // 2, width), BF16),
                pltpu.SemaphoreType.DMA((48,)),
            ],
        ),
        compiler_params=room(60),
        cost_estimate=cost(2 * D * LEN * width, 10e6),
    )(info, *operands)


def column_runs(part, swap):
    at = 0
    for run in part:
        for h in range(2):
            source = at + (1 - h if swap else h) * run.size
            yield at + h * run.size, source, run.size
        at += 2 * run.size


def add_kernel(part, swap, mine_ref, got_ref, out_ref):
    rows = out_ref.shape[0]
    mine, got = mine_ref[...].reshape(rows, -1), got_ref[...].reshape(rows, -1)
    for at, source, size in column_runs(part, swap):
        total = mine[:, at : at + size].astype(F32) + got[:, source : source + size].astype(F32)
        out_ref[:, at : at + size] = total.astype(BF16)


def block_spec(array, where, width):
    side, column = where
    if len(array.shape) == 3:
        return pl.BlockSpec((1, D // 2, width), lambda *_: (side, 0, column))
    return pl.BlockSpec((D // 2, width), lambda *_: (0, column))


def add_parts(mine, got, part, swap):
    width = part_width(part)
    return pl.pallas_call(
        functools.partial(add_kernel, part, swap),
        out_shape=struct((D // 2, width)),
        grid=(1,),
        in_specs=[block_spec(*v, width) for v in (mine, got)],
        out_specs=whole((D // 2, width)),
        compiler_params=room(24),
        cost_estimate=cost(1e6, 3e6),
    )(mine[0], got[0])


def split_kernel(parts, info_ref, *refs):
    ins, out_refs = refs[: 3 * len(parts)], refs[3 * len(parts) :]
    span = D // 8
    for k in range(4):
        rows = pl.ds(pl.multiple_of((info_ref[2] ^ k) * span, span), span)
        first = 0
        for p, part in enumerate(parts):
            mine, from_x, from_y = [
                (ref[0, rows, :] if len(ref.shape) == 3 else ref[rows, :]).astype(F32)
                for ref in ins[3 * p : 3 * p + 3]
            ]
            for at, source, size in column_runs(part, True):
                total = mine[:, at : at + size] + from_y[:, at : at + size]
                total = total + from_x[:, source : source + size]
                out_refs[k][:, first + at : first + at + size] = total.astype(BF16)
            first += part_width(part)


def split_z(info, parts, sources):
    width = sum(part_width(part) for part in parts)
    specs = [
        block_spec(*v, part_width(part)) for part, triple in zip(parts, sources) for v in triple
    ]
    out = pl.pallas_call(
        functools.partial(split_kernel, parts),
        out_shape=(struct((D // 8, width)),) * 4,
        grid_spec=pltpu.PrefetchScalarGridSpec(
            num_scalar_prefetch=1,
            grid=(1,),
            in_specs=specs,
            out_specs=[whole((D // 8, width))] * 4,
        ),
        compiler_params=room(60),
        cost_estimate=cost(1e6, 4e6),
    )(info, *[v[0] for triple in sources for v in triple])
    return [out[0]] + [send_dp(out[k], 2 * k) for k in (1, 2, 3)]


def finish_kernel(runs, turned, info_ref, *refs):
    parts, outs = refs[:4], refs[4:]
    at = 0
    for run in runs:
        for h in range(2):
            columns = slice(at, at + run.size)
            total = parts[0][:, columns].astype(F32)
            for part in parts[1:]:
                total = total + part[:, columns].astype(F32)
            spot = pl.ds(pl.multiple_of(run.base + info_ref[h] * run.stride, UNIT), run.size)
            if turned[run.which]:
                outs[run.which][spot, :] = total.T
            else:
                outs[run.which][:, spot] = total
            at += run.size


def finish(info, values, parts, turned):
    rows = D // 8
    runs = tuple(run for part in parts for run in part)
    sizes = [sum(2 * r.size for r in runs if r.which == k) for k in range(len(turned))]
    shapes = [(size, rows) if t else (rows, size) for size, t in zip(sizes, turned)]
    return pl.pallas_call(
        functools.partial(finish_kernel, runs, turned),
        out_shape=tuple(struct(shape, F32) for shape in shapes),
        grid_spec=pltpu.PrefetchScalarGridSpec(
            num_scalar_prefetch=1,
            grid=(1,),
            in_specs=[whole((rows, sum(sizes)))] * 4,
            out_specs=[whole(shape) for shape in shapes],
        ),
        compiler_params=room(24),
        cost_estimate=cost(1e6, 4e6),
    )(info, *values)


def input_grad_kernel(branch_ref, *refs):
    grads, heads, (out_ref, sum_ref, weight, sems) = refs[:4], refs[4:10], refs[10:]
    step = pl.program_id(0)
    plan = ((0, 0), (0, 1), (1, 0), (1, 1), (2, None), (3, None), (4, None), (5, None))
    copies = []
    for j, (piece, which) in enumerate(plan):
        source = heads[piece] if which is None else heads[piece].at[which]
        for k in range(3):
            at = ((j // 2) * 6 + 2 * k + j % 2) * UNIT
            copies.append(
                pltpu.make_async_copy(
                    source.at[k * UNIT : (k + 1) * UNIT, :],
                    weight.at[at : at + UNIT, :],
                    sems.at[3 * j + k],
                )
            )

    @pl.when(step == 0)
    def _():
        for copy in copies:
            copy.start()
        sum_ref[...] = jnp.zeros_like(sum_ref)

    total = branch_ref[...].astype(F32)
    for p in range(4):

        @pl.when(step == 0)
        def _():
            for copy in copies[6 * p : 6 * p + 6]:
                copy.wait()

        total = total + dot(grads[p][...], weight[6 * p * UNIT : 6 * (p + 1) * UNIT, :])
    out_ref[...] = total
    sum_ref[0:1, :] += jnp.sum(total, axis=0, keepdims=True)


def input_grad(branch_one, d_qkv, heads):
    tile = pl.BlockSpec((ROWS, D), lambda i: (i, 0))
    width = d_qkv[0].shape[1]
    return pl.pallas_call(
        input_grad_kernel,
        out_shape=(far((LEN, D), F32), struct((8, D), F32)),
        grid=(LEN // ROWS,),
        in_specs=[tile]
        + [pl.BlockSpec((ROWS, width), lambda i: (i, 0))] * 4
        + [pl.BlockSpec(memory_space=pltpu.HBM)] * 6,
        out_specs=[tile, whole((8, D))],
        scratch_shapes=[pltpu.VMEM((4 * width, D), BF16), pltpu.SemaphoreType.DMA((24,))],
        compiler_params=room(60),
        cost_estimate=cost(6.4e9, 20e6),
    )(branch_one, *d_qkv, *heads)


def exchange_kernel(sum_ref, row_ref, total_ref, rows_ref, got, sems_a, sems_b):
    devices = GRID_DP * GRID_MP
    me = lax.axis_index("dp") * GRID_MP + lax.axis_index("mp")

    def place(index):
        return {"dp": index // GRID_MP, "mp": index % GRID_MP}

    barrier = pltpu.get_barrier_semaphore()

    def greet(k, carry):
        target = (me + k) % devices
        pl.semaphore_signal(
            barrier, inc=1, device_id=place(target), device_id_type=pl.DeviceIdType.MESH
        )
        return carry

    lax.fori_loop(1, devices, greet, 0)
    pl.semaphore_wait(barrier, devices - 1)

    def copies(k):
        target = (me + k) % devices
        first = pltpu.make_async_remote_copy(
            src_ref=sum_ref.at[target],
            dst_ref=got.at[k],
            send_sem=sems_a.at[0, k],
            recv_sem=sems_a.at[1, k],
            device_id=place(target),
            device_id_type=pl.DeviceIdType.MESH,
        )
        second = pltpu.make_async_remote_copy(
            src_ref=row_ref,
            dst_ref=rows_ref.at[k],
            send_sem=sems_b.at[0, k],
            recv_sem=sems_b.at[1, k],
            device_id=place(target),
            device_id_type=pl.DeviceIdType.MESH,
        )
        return first, second

    def start(k, carry):
        for copy in copies(k):
            copy.start()
        return carry

    lax.fori_loop(1, devices, start, 0)
    rows_ref[0] = row_ref[...]

    def finish_copy(k, carry):
        for copy in copies(k):
            copy.wait()
        return carry

    lax.fori_loop(1, devices, finish_copy, 0)
    total_ref[...] = sum_ref[me] + jnp.sum(got[1:], axis=0)


def exchange(sums, row):
    devices = GRID_DP * GRID_MP
    vmem = pl.BlockSpec(memory_space=pltpu.VMEM)
    return pl.pallas_call(
        exchange_kernel,
        out_shape=(struct(sums.shape[1:], F32), struct((devices,) + row.shape, F32)),
        in_specs=[vmem, vmem],
        out_specs=[vmem, vmem],
        scratch_shapes=[
            pltpu.VMEM(sums.shape, F32),
            pltpu.SemaphoreType.DMA((2, devices)),
            pltpu.SemaphoreType.DMA((2, devices)),
        ],
        compiler_params=pltpu.CompilerParams(collective_id=0, has_side_effects=True),
        cost_estimate=cost(1e6, 1e6),
    )(sums, row)


def natural_order(x_at, mp_at):
    block, half = jnp.arange(8, dtype=jnp.int32) // 2, jnp.arange(8, dtype=jnp.int32) % 2
    away, at = block ^ mp_at, half ^ x_at
    source = jnp.where(away < 2, 2 * away + at, 2 + away + 2 * at)
    return (source[:, None] == jnp.arange(8, dtype=jnp.int32)[None, :]).astype(F32)


def body_rows(
    tokens,
    segment_ids,
    time_steps,
    w_qkv,
    b_qv,
    w_out,
    b_out,
    gain_one,
    shift_one,
    w_up,
    b_up,
    w_down,
    b_down,
    gain_two,
    shift_two,
    w_time,
    b_time,
    cotangent,
):
    dp_at, mp_at = lax.axis_index("dp"), lax.axis_index("mp")
    x_at, z_at = dp_at % 2, dp_at // 2
    info = jnp.stack([x_at, 1 - x_at, z_at, mp_at]).astype(jnp.int32)
    row = lambda v: v.astype(F32)[None, :]
    width = w_qkv.shape[2]

    heads_own, heads_first = pack_heads(info, w_qkv, w_out)
    heads = fetch(heads_own, heads_first)
    up_own, up_first, down_own, down_first = pack_units(info, w_up, w_down)
    up = fetch(up_own, up_first)
    down = fetch(down_own, down_first)
    q_rows, v_rows, up_rows = fetch_bias([b_qv[0:1], b_qv[1:2], b_up[None, :]], x_at)
    zero = jnp.zeros((1, width // 2), F32)

    own_step = lax.dynamic_slice_in_dim(time_steps, mp_at, 1, 0)
    segment_row = lax.dynamic_index_in_dim(segment_ids, mp_at, 0, keepdims=False)
    features = time_features(own_step)
    embed_row = jnp.dot(features, w_time.astype(F32), precision=HIGHEST_PRECISION)
    embed_row = embed_row + row(b_time)
    hidden_low = (tokens.astype(F32) + embed_row).astype(BF16)
    hotq, hotk = mark_segments(segment_row)
    win_f, win_b = windows(segment_row, TILE_F), windows(segment_row, TILE_B)

    qkv, ctx, lse = [], [], []
    for p in range(4):
        first, second = 2 * p, 2 * p + 1
        bias = jnp.concatenate(
            [q_rows[first], q_rows[second], zero, zero, v_rows[first], v_rows[second]], axis=1
        )
        parts = attend_pair(win_f, hidden_low, heads, p, bias, hotq, hotk)
        for kept, part in zip((qkv, ctx, lse), parts):
            kept.append(part)
    normal_one, scale_one, mid_low, mid_t, hidden_t = first_norm(
        tokens, ctx, heads, embed_row, row(b_out), row(gain_one), row(shift_one)
    )

    act, slope, ffn = [], [], ()
    for p in range(3):
        act_p, slope_p, *ffn = ffn_pair(mid_low, up, down, p, up_rows[2 * p : 2 * p + 2], ffn)
        act.append(act_p)
        slope.append(slope_p)
    act_p, slope_p, out_rows, branch_two, branch_two_t, sums_two = ffn_last(
        mid_low,
        up,
        down,
        3,
        up_rows[6:8],
        *ffn,
        cotangent,
        *[row(v) for v in (b_down, gain_two, shift_two)],
    )
    act.append(act_p)
    slope.append(slope_p)

    units = act[0].shape[1]
    down_parts = [(run,) for run in unit_runs(2, units)]
    up_parts = [down_parts[0], (down_parts[1][0], *head_runs(1, 1))]
    qkv_part = tuple(head_runs(0, 3))

    def two_way(left_t, rights, parts, cover):
        blocks = tuple((part, far) for part in parts for far in (False, True))
        one, two = (part_width(part) for part in parts)
        every = 2 * (one + two)
        (sent,) = grad_call(info, left_t, [r[1:] for r in rights], blocks, 1, ((0, every, None),))
        got = send_mp(sent, 1)
        covered = cover()
        outputs = (
            (0, one, None),
            (one, 2 * one, None),
            (2 * one, every, 0),
            (2 * one, every, 1),
        )
        result = grad_call(
            info, left_t, [r[:1] + r[2:] for r in rights], blocks, 0, outputs, got, 0
        )
        return covered, result

    def first_sends(blocks):
        own, far, keep, leave = blocks
        return own, keep, send_mp(far, 2), send_dp(leave, 1)

    def second_sends(sums, parts):
        own, keep, from_y, from_x = sums
        low = add_parts((own, (1, 0)), (from_y, (1, 0)), parts[0], False)
        x_two = send_dp(low, 1)
        low = add_parts((keep, (0, 1)), (from_x, (0, 1)), parts[1], True)
        y_two = send_mp(low, 2)
        here = (0, 0)
        return (
            ((own, here), (x_two, here), (from_y, here)),
            ((keep, here), (from_x, here), (y_two, here)),
        )

    def ffn_part():
        return ffn_back(
            branch_two, down, up, slope, normal_one, scale_one, row(gain_one)
        )

    (*d_pre, sums_up, branch_one, branch_one_t, sums_one), down_blocks = two_way(
        [branch_two_t], [act], down_parts, ffn_part
    )
    down_sums = first_sends(down_blocks)
    d_qkv, qkv_sums = [None] * 4, [None] * 4

    def back(p):
        d_qkv[p], qkv_sums[p] = attend_back_pair(
            win_b, qkv[p], hotq, hotk, branch_one, heads, p, ctx[p], lse[p]
        )

    _, up_blocks = two_way([mid_t, branch_one_t], [d_pre, ctx], up_parts, lambda: back(1))
    down_last = second_sends(down_sums, down_parts)
    up_sums = first_sends(up_blocks)
    back(2)
    down_values = split_z(info, down_parts, down_last)
    back(3)
    wide = part_width(qkv_part)
    far_only, own_only = ((qkv_part, True),), ((qkv_part, False),)
    (sent,) = grad_call(
        info, [hidden_t], [d_qkv[1:]], own_only + far_only, 1, ((0, 2 * wide, None),)
    )
    got = send_mp(sent, 1)
    up_last = second_sends(after(up_sums, sent), up_parts)
    sides = ((0, wide, 0), (0, wide, 1))
    far_keep, far_leave = grad_call(
        info, [hidden_t], [[d_qkv[1]] + d_qkv[2:]], far_only, 0, sides, got, wide
    )
    far_x = send_dp(far_leave, 1)
    back(0)
    up_values = split_z(info, up_parts, up_last)
    here = (0, 0)
    far_low = add_parts((far_keep, here), (far_x, here), qkv_part, True)
    far_y = send_mp(far_low, 2)
    own_keep, own_leave = grad_call(
        info, [hidden_t], [d_qkv[:1] + d_qkv[2:]], own_only, 0, sides, got, 0
    )
    own_x = send_dp(own_leave, 1)
    grad_tokens, sums_in = input_grad(branch_one, d_qkv, heads)
    qkv_values = split_z(info, (qkv_part,), (((own_keep, here), (own_x, here), (far_y, here)),))

    devices = GRID_DP * GRID_MP
    heads_sum = jnp.concatenate([v[0:1] for v in qkv_sums]).reshape(4, 3, HALF, UNIT)
    heads_sum = heads_sum.transpose(0, 2, 1, 3).reshape(8, -1)
    blocks = jnp.dot(
        natural_order(x_at, mp_at),
        jnp.concatenate([sums_up, heads_sum], axis=1),
        precision=HIGHEST_PRECISION,
    )

    def spread(v):
        return v.reshape(GRID_MP, GRID_DP, -1).transpose(1, 0, 2).reshape(devices, -1)

    ends = (0, units // 2, units // 2 + UNIT, units // 2 + 3 * UNIT)
    full = jnp.concatenate([sums_two[:3], sums_one[:3]]).reshape(6, devices, -1)
    rows = [full.transpose(1, 0, 2).reshape(devices, -1), spread(blocks[:, : ends[1]])]
    rows += [spread(blocks[:, at : at + UNIT]) for at in (ends[1], ends[3] - UNIT)]
    tail_row = jnp.concatenate(
        [sums_in[0:1], jnp.broadcast_to(own_step.astype(F32)[None, :], (1, UNIT))], axis=1
    )
    totals, all_rows = exchange(jnp.concatenate(rows, axis=1)[:, None, :], tail_row)
    totals, all_rows, down_values, up_values = after(
        (totals, all_rows, down_values, up_values), qkv_values[0]
    )
    all_rows = all_rows[:, 0]
    span = D // (GRID_DP * GRID_MP)
    own = [totals[0, j * span : (j + 1) * span] for j in range(6)]
    device_at = dp_at * GRID_MP + mp_at
    all_grads = all_rows[:, :D]
    dims = device_at * span + jnp.arange(span, dtype=jnp.int32)
    ladder = (dims % (D // 2)).astype(F32)
    frequency = jnp.exp(ladder * (-math.log(10000.0) / (D // 2)))
    angles = all_rows[:, D : D + 1] * frequency[None, :]
    own_features = jnp.where((dims < D // 2)[None, :], jnp.sin(angles), jnp.cos(angles))
    g_w_time = jnp.dot(own_features.T, all_grads, precision=HIGHEST_PRECISION)
    g_b_time = lax.dynamic_slice_in_dim(jnp.sum(all_grads, axis=0), device_at * span, span, 0)

    (g_w_qkv,) = finish(info, qkv_values, (qkv_part,), (False,))
    (g_w_down,) = finish(info, down_values, down_parts, (True,))
    g_w_up, g_w_out = finish(info, up_values, up_parts, (False, True))
    up_end = totals.shape[1] - 2 * span
    return (
        out_rows,
        grad_tokens,
        g_w_qkv.reshape(D // 8, 3, width),
        totals[0, up_end:].reshape(2, 1, -1),
        g_w_out,
        own[3],
        own[4],
        own[5],
        g_w_up,
        totals[:, 6 * span : up_end],
        g_w_down,
        own[0],
        own[1],
        own[2],
        g_w_time,
        g_b_time,
    )


def solution(mesh):
    placed = (
        P(("dp", "mp"), None),
        P("dp", None),
        P("dp"),
        P(None, None, "mp"),
        P(None, "mp"),
        P("mp", None),
        P(),
        P(),
        P(),
        P(None, "mp"),
        P("mp"),
        P("mp", None),
        P(),
        P(),
        P(),
        P(),
        P(),
        P(("dp", "mp"), None),
    )
    rows = mesh.shape["dp"], mesh.shape["mp"]

    def body(*args):
        if args[0].shape[0] != LEN or rows != (GRID_DP, GRID_MP):
            return body_split(*args)
        return body_rows(*args)

    return jax.shard_map(
        body,
        mesh=mesh,
        in_specs=placed,
        out_specs=(
            P(("dp", "mp"), None),
            P(("dp", "mp"), None),
            P("dp", None, "mp"),
            P(None, "mp", "dp"),
            P("mp", "dp"),
            P(("dp", "mp")),
            P(("dp", "mp")),
            P(("dp", "mp")),
            P("dp", "mp"),
            P("mp", "dp"),
            P("mp", "dp"),
            P(("dp", "mp")),
            P(("dp", "mp")),
            P(("dp", "mp")),
            P(("dp", "mp"), None),
            P(("dp", "mp")),
        ),
        check_vma=False,
    )
```

```python
import functools
import math
from typing import NamedTuple

import jax
import jax.numpy as jnp
from jax import lax
from jax.experimental import pallas as pl
from jax.experimental.pallas import tpu as pltpu
from jax.sharding import PartitionSpec as P


D = 1024
HEAD_DIM = 64
LEN = 1024


EPS = 1e-05
HIGHEST_PRECISION = lax.Precision.HIGHEST


def time_features(step_values):
    half_width = D // 2
    ladder = jnp.arange(half_width, dtype=jnp.float32)
    frequency = jnp.exp(ladder * (-math.log(10000.0) / half_width))
    angles = step_values.astype(jnp.float32)[:, None] * frequency[None, :]
    return jnp.concatenate([jnp.sin(angles), jnp.cos(angles)], axis=1)


def layer_norm(values, gain_vec, shift_vec):
    center = values - jnp.mean(values, axis=-1, keepdims=True)
    spread = jnp.mean(center * center, axis=-1, keepdims=True)
    return center * lax.rsqrt(spread + EPS) * gain_vec + shift_vec


def exact_gelu(values):
    return jax.nn.gelu(values, approximate=False)


def project_qkv(hidden_full, w_qkv, b_qv):
    width_local = w_qkv.shape[2]
    w_flat = w_qkv.reshape(w_qkv.shape[0], 3 * width_local)
    bias_row = jnp.concatenate([b_qv[0], jnp.zeros((width_local,), b_qv.dtype), b_qv[1]]).astype(
        jnp.float32
    )
    product = jnp.dot(hidden_full, w_flat, preferred_element_type=jnp.float32)
    return (product + bias_row[None, :]).astype(jnp.bfloat16)


def head_parts(qkv_seq):
    width_local = qkv_seq.shape[1] // 3
    head_local = width_local // HEAD_DIM
    shaped = qkv_seq.reshape(qkv_seq.shape[0], 3, head_local, HEAD_DIM)
    return (shaped[:, 0], shaped[:, 1], shaped[:, 2])


def masked_scores(queries, keys_part, segment_row):
    scores = jnp.einsum("qhd,khd->hqk", queries, keys_part, preferred_element_type=jnp.float32)
    scores = scores * (1.0 / math.sqrt(HEAD_DIM))
    same_doc = segment_row[:, None] == segment_row[None, :]
    return jnp.where(same_doc[None, :, :], scores, -1e30)


def attend_forward(inputs):
    qkv_seq, segment_row = inputs
    queries, keys_part, values_part = head_parts(qkv_seq)
    masked = masked_scores(queries, keys_part, segment_row)
    top_score = jnp.max(masked, axis=2, keepdims=True)
    weights_exp = jnp.exp(masked - top_score)
    totals = jnp.sum(weights_exp, axis=2, keepdims=True)
    probability = weights_exp / totals
    context = jnp.einsum(
        "hqk,khd->qhd",
        probability.astype(jnp.bfloat16),
        values_part,
        preferred_element_type=jnp.float32,
    )
    log_total = (top_score + jnp.log(totals))[:, :, 0]
    return (context.reshape(qkv_seq.shape[0], -1).astype(jnp.bfloat16), log_total)


def attend_backward(inputs):
    qkv_seq, grad_seq, log_total, segment_row = inputs
    queries, keys_part, values_part = head_parts(qkv_seq)
    masked = masked_scores(queries, keys_part, segment_row)
    probability = jnp.exp(masked - log_total[:, :, None])
    grad_heads = grad_seq.reshape(grad_seq.shape[0], -1, HEAD_DIM)
    d_values = jnp.einsum(
        "hqk,qhd->khd",
        probability.astype(jnp.bfloat16),
        grad_heads,
        preferred_element_type=jnp.float32,
    )
    d_probs = jnp.einsum(
        "qhd,khd->hqk", grad_heads, values_part, preferred_element_type=jnp.float32
    )
    row_terms = jnp.sum(probability * d_probs, axis=2, keepdims=True)
    d_scores = (probability * (d_probs - row_terms)).astype(jnp.bfloat16)
    score_scale = 1.0 / math.sqrt(HEAD_DIM)
    d_queries = (
        jnp.einsum("hqk,khd->qhd", d_scores, keys_part, preferred_element_type=jnp.float32)
        * score_scale
    )
    d_keys = (
        jnp.einsum("hqk,qhd->khd", d_scores, queries, preferred_element_type=jnp.float32)
        * score_scale
    )
    stacked = jnp.stack([d_queries, d_keys, d_values], axis=1)
    return stacked.reshape(qkv_seq.shape[0], -1).astype(jnp.bfloat16)


def body_split(
    tokens,
    segment_ids,
    time_steps,
    w_qkv,
    b_qv,
    w_out,
    b_out,
    gain_one,
    shift_one,
    w_up,
    b_up,
    w_down,
    b_down,
    gain_two,
    shift_two,
    w_time,
    b_time,
    cotangent,
):
    row_count = tokens.shape[0]
    seq_local = time_steps.shape[0]
    width_local = w_qkv.shape[2]
    gain_one_f = gain_one.astype(jnp.float32)
    shift_one_f = shift_one.astype(jnp.float32)
    gain_two_f = gain_two.astype(jnp.float32)
    shift_two_f = shift_two.astype(jnp.float32)
    w_flat = w_qkv.reshape(D, 3 * width_local)
    features = time_features(time_steps)
    embed_rows = jnp.dot(features, w_time.astype(jnp.float32), precision=HIGHEST_PRECISION)
    embed_rows = embed_rows + b_time.astype(jnp.float32)[None, :]
    row_seq = (lax.axis_index("mp") * row_count + jnp.arange(row_count, dtype=jnp.int32)) // LEN
    selector = (row_seq[:, None] == jnp.arange(seq_local, dtype=jnp.int32)[None, :]).astype(
        jnp.float32
    )
    hidden_in = tokens.astype(jnp.float32) + jnp.dot(
        selector, embed_rows, precision=HIGHEST_PRECISION
    )
    hidden_low = hidden_in.astype(jnp.bfloat16)
    hidden_full = lax.all_gather(hidden_low, "mp", axis=0, tiled=True)
    qkv_full = project_qkv(hidden_full, w_qkv, b_qv)
    ctx_blocks, log_totals = lax.map(
        attend_forward, (qkv_full.reshape(seq_local, LEN, 3 * width_local), segment_ids)
    )
    context = ctx_blocks.reshape(seq_local * LEN, width_local)
    rows_in = context
    attn_sum = lax.psum_scatter(
        jnp.dot(rows_in, w_out, preferred_element_type=jnp.float32).astype(jnp.bfloat16),
        "mp",
        scatter_dimension=0,
        tiled=True,
    ).astype(jnp.float32)
    attn_out = attn_sum + b_out.astype(jnp.float32)[None, :]
    mid_in = hidden_in + attn_out
    mid_norm = layer_norm(mid_in, gain_one_f, shift_one_f)
    mid_low = mid_norm.astype(jnp.bfloat16)
    mid_full = lax.all_gather(mid_low, "mp", axis=0, tiled=True)
    pre_act = (
        jnp.dot(mid_full, w_up, preferred_element_type=jnp.float32)
        + b_up.astype(jnp.float32)[None, :]
    )
    activated = exact_gelu(pre_act).astype(jnp.bfloat16)
    rows_in = activated
    ffn_part = lax.psum_scatter(
        jnp.dot(rows_in, w_down, preferred_element_type=jnp.float32).astype(jnp.bfloat16),
        "mp",
        scatter_dimension=0,
        tiled=True,
    ).astype(jnp.float32)
    out_in = mid_norm + ffn_part + b_down.astype(jnp.float32)[None, :]
    out_rows, out_back = jax.vjp(layer_norm, out_in, gain_two_f, shift_two_f)
    grad_two, grad_gain_two, grad_shift_two = out_back(cotangent.astype(jnp.float32))
    branch_two = grad_two.astype(jnp.bfloat16)
    grad_b_down = jnp.sum(branch_two.astype(jnp.float32), axis=0)
    _, gelu_back = jax.vjp(exact_gelu, pre_act)
    cot_full = lax.all_gather(branch_two, "mp", axis=0, tiled=True)
    d_act = jnp.dot(cot_full, w_down.T, preferred_element_type=jnp.float32)
    grad_w_down = jnp.dot(activated.T, cot_full, preferred_element_type=jnp.float32)
    d_pre = gelu_back(d_act)[0].astype(jnp.bfloat16)
    grad_w_up = jnp.dot(mid_full.T, d_pre, preferred_element_type=jnp.float32)
    grad_b_up = jnp.sum(d_pre.astype(jnp.float32), axis=0)
    rows_in = d_pre
    d_mid_part = lax.psum_scatter(
        jnp.dot(rows_in, w_up.T, preferred_element_type=jnp.float32).astype(jnp.bfloat16),
        "mp",
        scatter_dimension=0,
        tiled=True,
    ).astype(jnp.float32)
    _, mid_back = jax.vjp(layer_norm, mid_in, gain_one_f, shift_one_f)
    grad_one, grad_gain_one, grad_shift_one = mid_back(grad_two + d_mid_part)
    branch_one = grad_one.astype(jnp.bfloat16)
    grad_b_out = jnp.sum(branch_one.astype(jnp.float32), axis=0)
    cot_attn = lax.all_gather(branch_one, "mp", axis=0, tiled=True)
    d_context = jnp.dot(cot_attn, w_out.T, preferred_element_type=jnp.float32).astype(jnp.bfloat16)
    grad_w_out = jnp.dot(context.T, cot_attn, preferred_element_type=jnp.float32)
    grad_blocks = lax.map(
        attend_backward,
        (
            qkv_full.reshape(seq_local, LEN, 3 * width_local),
            d_context.reshape(seq_local, LEN, width_local),
            log_totals,
            segment_ids,
        ),
    )
    d_qkv = grad_blocks.reshape(seq_local * LEN, 3 * width_local)
    grad_w_qkv = jnp.dot(hidden_full.T, d_qkv, preferred_element_type=jnp.float32).reshape(
        D, 3, width_local
    )
    qkv_sums = jnp.sum(d_qkv.astype(jnp.float32), axis=0).reshape(3, width_local)
    grad_b_qv = jnp.stack([qkv_sums[0], qkv_sums[2]]).reshape(2, 1, width_local)
    rows_in = d_qkv
    input_part = lax.psum_scatter(
        jnp.dot(rows_in, w_flat.T, preferred_element_type=jnp.float32).astype(jnp.bfloat16),
        "mp",
        scatter_dimension=0,
        tiled=True,
    ).astype(jnp.float32)
    grad_tokens = grad_one + input_part
    grad_embed = jnp.dot(selector.T, grad_tokens, precision=HIGHEST_PRECISION)
    grad_w_time = jnp.dot(features.T, grad_embed, precision=HIGHEST_PRECISION)
    grad_b_time = jnp.sum(grad_embed, axis=0)
    sharded = (
        lax.psum_scatter(
            grad_w_qkv.astype(jnp.bfloat16), "dp", scatter_dimension=0, tiled=True
        ).astype(jnp.float32),
        lax.psum_scatter(
            grad_b_qv.astype(jnp.bfloat16), "dp", scatter_dimension=2, tiled=True
        ).astype(jnp.float32),
        lax.psum_scatter(
            grad_w_out.astype(jnp.bfloat16), "dp", scatter_dimension=1, tiled=True
        ).astype(jnp.float32),
        lax.psum_scatter(
            grad_w_up.astype(jnp.bfloat16), "dp", scatter_dimension=0, tiled=True
        ).astype(jnp.float32),
        lax.psum_scatter(
            grad_b_up.reshape(1, -1).astype(jnp.bfloat16), "dp", scatter_dimension=1, tiled=True
        ).astype(jnp.float32),
        lax.psum_scatter(
            grad_w_down.astype(jnp.bfloat16), "dp", scatter_dimension=1, tiled=True
        ).astype(jnp.float32),
    )
    shared = (
        lax.psum_scatter(grad_w_time, ("dp", "mp"), scatter_dimension=0, tiled=True),
        lax.psum_scatter(grad_b_time, ("dp", "mp"), scatter_dimension=0, tiled=True),
        lax.psum_scatter(grad_gain_one, ("dp", "mp"), scatter_dimension=0, tiled=True),
        lax.psum_scatter(grad_shift_one, ("dp", "mp"), scatter_dimension=0, tiled=True),
        lax.psum_scatter(grad_gain_two, ("dp", "mp"), scatter_dimension=0, tiled=True),
        lax.psum_scatter(grad_shift_two, ("dp", "mp"), scatter_dimension=0, tiled=True),
        lax.psum_scatter(grad_b_out, ("dp", "mp"), scatter_dimension=0, tiled=True),
        lax.psum_scatter(grad_b_down, ("dp", "mp"), scatter_dimension=0, tiled=True),
    )
    return (
        out_rows.astype(jnp.bfloat16),
        grad_tokens,
        sharded[0],
        sharded[1],
        sharded[2],
        shared[6],
        shared[2],
        shared[3],
        sharded[3],
        sharded[4],
        sharded[5],
        shared[7],
        shared[4],
        shared[5],
        shared[0],
        shared[1],
    )


GRID_DP = 8
GRID_MP = 4
HALF = 2
UNIT = 128
F32 = jnp.float32
BF16 = jnp.bfloat16
TILE_F = 512
TILE_B = 256
TILE_U = 256
ROWS = 256
GRAIN = 256
STEP = 128
EXTRA = 16
FAR = -(2.0**100)
NN = (((1,), (0,)), ((), ()))
NT = (((1,), (1,)), ((), ()))


def dot(left, right, dims=NN):
    return lax.dot_general(left, right, dims, preferred_element_type=F32)


def after(values, others):
    return lax.optimization_barrier((values, others))[0]


def whole(shape):
    return pl.BlockSpec(shape, lambda *_: (0,) * len(shape))


def struct(shape, kind=BF16):
    return jax.ShapeDtypeStruct(shape, kind)


def far(shape, kind=BF16):
    return pltpu.HBM(shape, kind)


def room(mib):
    return pltpu.CompilerParams(vmem_limit_bytes=mib * 2**20)


def cost(flops, moved):
    return pl.CostEstimate(flops=int(flops), bytes_accessed=int(moved), transcendentals=0)


def send_mp(values, bit):
    return lax.ppermute(values, "mp", [(i, i ^ bit) for i in range(GRID_MP)])


def send_dp(values, bit):
    return lax.ppermute(values, "dp", [(i, i ^ bit) for i in range(GRID_DP)])


def fetch(own, first_half):
    near = send_mp(own, 1)
    far_a = send_mp(first_half, 2)
    near_a = send_mp(far_a, 1)
    far_b = send_dp(far_a, 1)
    near_b = send_mp(far_b, 1)
    return [own, near, far_a, near_a, far_b, near_b]


def pack_heads_kernel(info_ref, qkv_ref, out_ref, qv_ref, up_ref, both_ref, first_ref):
    size = up_ref.shape[1] // 2
    for u in range(HALF):
        at = pl.ds(pl.multiple_of(info_ref[u] * UNIT, UNIT), UNIT)
        for j in range(3):
            both_ref[u, j * UNIT : (j + 1) * UNIT, :] = qkv_ref[j, :, at].T
        both_ref[u, 3 * UNIT : 4 * UNIT, :] = out_ref[at, :]
        hidden = pl.ds(pl.multiple_of(info_ref[u] * size, UNIT), size)
        rest = jnp.zeros((1, D - 2 * UNIT - size), F32)
        qv = qv_ref[:, at].astype(F32)
        parts = [qv[0:1], qv[1:2], up_ref[0:1, hidden], rest]
        bias = jnp.broadcast_to(jnp.concatenate(parts, axis=1), (EXTRA, D))
        both_ref[u, 4 * UNIT :, :] = bias.astype(BF16)
    first_ref[...] = both_ref[0]


def pack_heads(info, w_qkv, w_out, b_qv, b_up):
    rows = 4 * UNIT + EXTRA
    return pl.pallas_call(
        pack_heads_kernel,
        out_shape=(far((HALF, rows, D)), far((rows, D))),
        grid_spec=pltpu.PrefetchScalarGridSpec(
            num_scalar_prefetch=1,
            grid=(1,),
            in_specs=[
                whole((3, D, 2 * UNIT)),
                whole((2 * UNIT, D)),
                whole((2, 2 * UNIT)),
                whole((1, b_up.shape[0])),
            ],
            out_specs=[whole((HALF, rows, D)), whole((rows, D))],
        ),
        compiler_params=room(60),
        cost_estimate=cost(1e6, 5e6),
    )(info, w_qkv.transpose(1, 0, 2), w_out, b_qv, b_up.astype(F32)[None, :])


def pack_units_kernel(info_ref, up_ref, down_ref, up_both, up_first, down_both, down_first):
    step = pl.program_id(0)
    up = up_ref[...].T
    up_both[0] = up
    down_both[0] = down_ref[...]

    @pl.when(step == 0)
    def _():
        up_first[...] = up
        down_first[...] = down_ref[...]


def pack_units(info, w_up, w_down):
    size = w_down.shape[0] // 2
    return pl.pallas_call(
        pack_units_kernel,
        out_shape=(far((HALF, size, D)), far((size, D))) * 2,
        grid_spec=pltpu.PrefetchScalarGridSpec(
            num_scalar_prefetch=1,
            grid=(HALF,),
            in_specs=[
                pl.BlockSpec((D, size), lambda i, info: (0, info[i])),
                pl.BlockSpec((size, D), lambda i, info: (info[i], 0)),
            ],
            out_specs=[pl.BlockSpec((1, size, D), lambda i, info: (i, 0, 0)), whole((size, D))] * 2,
        ),
        compiler_params=room(60),
        cost_estimate=cost(1e6, 10e6),
    )(info, w_up, w_down)


def half_specs(rows, block):
    both = [pl.BlockSpec((1, rows, D), lambda *_, u=u: (u, block, 0)) for u in range(HALF)]
    return both * 2 + [pl.BlockSpec((rows, D), lambda *_: (block, 0))] * 4


def eight(pieces):
    own, near, far_a, near_a, far_b, near_b = pieces
    return [own, own, near, near, far_a, near_a, far_b, near_b]


def pair_specs(rows, block, pair):
    return half_specs(rows, block)[2 * pair : 2 * pair + 2]


def pair_of(pieces, pair):
    return eight(pieces)[2 * pair : 2 * pair + 2]


def rows_of(ref):
    return ref[...].reshape(-1, D)


def mark_segments(segment_row):
    lane = jnp.arange(UNIT, dtype=jnp.int32)[None, :]
    hot = segment_row[:, None] == (lane % HEAD_DIM)
    used = (lane % HEAD_DIM) < 8
    return (
        jnp.where(hot & used, 1.0, 0.0).astype(BF16),
        jnp.where(used & ~hot, FAR, 0.0).astype(BF16),
    )


def windows(segment_row, tile):
    first, last = segment_row[::tile], segment_row[tile - 1 :: tile]
    low = jnp.sum(segment_row[None, :] < first[:, None], axis=1) // STEP * STEP
    high = jnp.sum(segment_row[None, :] <= last[:, None], axis=1)
    count = jnp.maximum((high - low + GRAIN - 1) // GRAIN, tile // GRAIN)
    low = jnp.minimum(low, LEN - count * GRAIN)
    return jnp.stack([low, count]).astype(jnp.int32)


def variants(count, tile, run):
    for n in range(tile // GRAIN, LEN // GRAIN + 1):

        @pl.when(count == n)
        def _(n=n):
            run(n * GRAIN)


def lanes_at(at, base=0):
    return pl.ds(pl.multiple_of(base + at * UNIT, UNIT), UNIT)


def attend_kernel(
    win_ref, x_ref, *refs
):
    weights, biases, (hotq_ref, hotk_ref, qkv_ref, ctx_ref, lse_ref, w_ref, kx) = refs[:2], refs[2:4], refs[4:]
    unit, step = pl.program_id(0), pl.program_id(1)

    @pl.when((unit == 0) & (step == 0))
    def _():
        for u in range(HALF):
            part = rows_of(weights[u])
            for j in range(3):
                at = (2 * j + u) * UNIT
                w_ref[at : at + UNIT, :] = part[j * UNIT : (j + 1) * UNIT]
        first, second = [rows_of(ref)[0:1].astype(F32) for ref in biases]
        none = jnp.zeros((1, 2 * UNIT), F32)
        bias = [first[:, :UNIT], second[:, :UNIT], none]
        bias += [first[:, UNIT : 2 * UNIT], second[:, UNIT : 2 * UNIT]]
        bias = jnp.concatenate(bias, axis=1)
        for r in range(LEN // ROWS):
            rows = slice(r * ROWS, (r + 1) * ROWS)
            qkv_ref[rows, :] = (dot(x_ref[rows, :], w_ref[...], NT) + bias).astype(BF16)

    @pl.when(step == 0)
    def _():
        lane = lax.broadcasted_iota(jnp.int32, (LEN, UNIT), 1)
        keys = qkv_ref[:, lanes_at(unit, 2 * UNIT)]
        for h in range(HALF):
            kx[h] = jnp.where((lane // HEAD_DIM) == h, keys, hotk_ref[...])

    lane = lax.broadcasted_iota(jnp.int32, (TILE_F, UNIT), 1)
    rows = pl.ds(pl.multiple_of(step * TILE_F, TILE_F), TILE_F)
    queries = qkv_ref[rows, lanes_at(unit)] * jnp.asarray(1.0 / math.sqrt(HEAD_DIM), BF16)
    start = pl.multiple_of(win_ref[0, step], STEP)

    def run(width):
        window = pl.ds(start, width)
        values = qkv_ref[window, lanes_at(unit, 4 * UNIT)]
        scores = [
            dot(
                jnp.where((lane // HEAD_DIM) == h, queries, hotq_ref[...]), kx[h, window, :], NT
            )
            for h in range(HALF)
        ]
        outs = []
        for h in range(HALF):
            top = jnp.max(scores[h], axis=1, keepdims=True)
            weight = jnp.exp(scores[h] - top)
            total = jnp.sum(weight, axis=1, keepdims=True)
            outs.append(dot(weight.astype(BF16), values) * (1.0 / total))
            lse_ref[0, h : h + 1, :] = (top + jnp.log(total)).T
        ctx_ref[...] = jnp.where(lane < HEAD_DIM, outs[0], outs[1]).astype(BF16)

    variants(win_ref[1, step], TILE_F, run)


def attend_pair(win, hidden_low, heads, pair, hotq, hotk):
    return pl.pallas_call(
        attend_kernel,
        out_shape=(
            far((LEN, 6 * UNIT)),
            far((LEN, 2 * UNIT)),
            far((HALF, 8, LEN), F32),
        ),
        grid_spec=pltpu.PrefetchScalarGridSpec(
            num_scalar_prefetch=1,
            grid=(HALF, LEN // TILE_F),
            in_specs=[whole((LEN, D))]
            + pair_specs(4 * UNIT, 0, pair)
            + pair_specs(EXTRA, 4 * UNIT // EXTRA, pair)
            + [
                pl.BlockSpec((TILE_F, UNIT), lambda n, i, win: (i, 0)),
                whole((LEN, UNIT)),
            ],
            out_specs=[
                whole((LEN, 6 * UNIT)),
                pl.BlockSpec((TILE_F, UNIT), lambda n, i, win: (i, n)),
                pl.BlockSpec((1, 8, TILE_F), lambda n, i, win: (n, 0, i)),
            ],
            scratch_shapes=[pltpu.VMEM((6 * UNIT, D), BF16), pltpu.VMEM((HALF, LEN, UNIT), BF16)],
        ),
        compiler_params=room(32),
        cost_estimate=cost(6e9, 8e6),
    )(win, hidden_low, *pair_of(heads, pair) * 2, hotq, hotk)


def attend_back_kernel(
    win_ref,
    qkv_ref,
    hotq_ref,
    hotk_ref,
    branch_ref,
    wa_ref,
    wb_ref,
    ctx_ref,
    lse_ref,
    out_ref,
    sum_ref,
    kx,
    kt,
    grads,
    dk,
    dv,
):
    unit, step = pl.program_id(0), pl.program_id(1)
    scale = jnp.asarray(1.0 / math.sqrt(HEAD_DIM), BF16)

    @pl.when(step == 0)
    def _():
        lane = lax.broadcasted_iota(jnp.int32, (LEN, UNIT), 1)
        keys = qkv_ref[:, lanes_at(unit, 2 * UNIT)]
        for h in range(HALF):
            kx[h] = jnp.where((lane // HEAD_DIM) == h, keys, hotk_ref[...])
        kt[...] = (keys * scale).T
        dk[...] = jnp.zeros_like(dk)
        dv[...] = jnp.zeros_like(dv)

    lane = lax.broadcasted_iota(jnp.int32, (TILE_B, UNIT), 1)
    rows = pl.ds(pl.multiple_of(step * TILE_B, TILE_B), TILE_B)

    @pl.when(unit == 0)
    def _():
        weight = jnp.concatenate([rows_of(wa_ref), rows_of(wb_ref)], axis=0)
        grads[rows, :] = dot(branch_ref[...], weight, NT).astype(BF16)

    queries = qkv_ref[rows, lanes_at(unit)] * scale
    grad = grads[rows, lanes_at(unit)]
    product = (grad.astype(F32) * ctx_ref[...].astype(F32)).T
    start = pl.multiple_of(win_ref[0, step], STEP)

    def run(width):
        window = pl.ds(start, width)
        values = qkv_ref[window, lanes_at(unit, 4 * UNIT)]
        d_queries, d_keys, d_values = [], [], []
        for h in range(HALF):
            mine = (lane // HEAD_DIM) == h
            q_mine = jnp.where(mine, queries, jnp.zeros_like(queries))
            g_mine = jnp.where(mine, grad, jnp.zeros_like(grad))
            scores = dot(kx[h, window, :], jnp.where(mine, queries, hotq_ref[...]), NT)
            weight = jnp.exp(scores - lse_ref[0, h : h + 1, :])
            d_weight = dot(values, g_mine, NT)
            row_term = jnp.sum(
                product[h * HEAD_DIM : (h + 1) * HEAD_DIM], axis=0, keepdims=True
            )
            d_scores = (weight * (d_weight - row_term)).astype(BF16)
            d_values.append(dot(weight.astype(BF16), g_mine))
            d_keys.append(dot(d_scores, q_mine))
            d_queries.append(dot(kt[h * HEAD_DIM : (h + 1) * HEAD_DIM, window], d_scores))
        dv[window, :] += d_values[0] + d_values[1]
        dk[window, :] += d_keys[0] + d_keys[1]
        out_ref[rows, lanes_at(unit)] = jnp.concatenate(d_queries, 0).T.astype(BF16)

    variants(win_ref[1, step], TILE_B, run)

    @pl.when(step == LEN // TILE_B - 1)
    def _():
        out_ref[:, lanes_at(unit, 2 * UNIT)] = dk[...].astype(BF16)
        out_ref[:, lanes_at(unit, 4 * UNIT)] = dv[...].astype(BF16)

    @pl.when((unit == HALF - 1) & (step == LEN // TILE_B - 1))
    def _():
        total = jnp.sum(out_ref[...].astype(F32), axis=0, keepdims=True)
        sum_ref[...] = jnp.broadcast_to(total, sum_ref.shape)


def attend_back_pair(win, qkv, hotq, hotk, branch_one, heads, pair, ctx, lse):
    return pl.pallas_call(
        attend_back_kernel,
        out_shape=(far((LEN, 6 * UNIT)), struct((8, 6 * UNIT), F32)),
        grid_spec=pltpu.PrefetchScalarGridSpec(
            num_scalar_prefetch=1,
            grid=(HALF, LEN // TILE_B),
            in_specs=[
                whole((LEN, 6 * UNIT)),
                pl.BlockSpec((TILE_B, UNIT), lambda n, i, win: (i, 0)),
                whole((LEN, UNIT)),
                pl.BlockSpec((TILE_B, D), lambda n, i, win: (jnp.where(n == 0, i, LEN // TILE_B - 1), 0)),
                *pair_specs(UNIT, 3, pair),
                pl.BlockSpec((TILE_B, UNIT), lambda n, i, win: (i, n)),
                pl.BlockSpec((1, 8, TILE_B), lambda n, i, win: (n, 0, i)),
            ],
            out_specs=[whole((LEN, 6 * UNIT)), whole((8, 6 * UNIT))],
            scratch_shapes=[
                pltpu.VMEM((HALF, LEN, UNIT), BF16),
                pltpu.VMEM((UNIT, LEN), BF16),
                pltpu.VMEM((LEN, 2 * UNIT), BF16),
                pltpu.VMEM((LEN, UNIT), F32),
                pltpu.VMEM((LEN, UNIT), F32),
            ],
        ),
        compiler_params=room(32),
        cost_estimate=cost(8e9, 8e6),
    )(win, qkv, hotq, hotk, branch_one, *pair_of(heads, pair), ctx, lse)


def norm_of(values):
    center = values - jnp.mean(values, axis=-1, keepdims=True)
    spread = jnp.mean(center * center, axis=-1, keepdims=True)
    scale = lax.rsqrt(spread + EPS)
    return center * scale, scale


def norm_back(normal, scale, grad, gain_row):
    scaled = grad * gain_row
    mean_e = jnp.mean(scaled, axis=-1, keepdims=True)
    mean_en = jnp.mean(scaled * normal, axis=-1, keepdims=True)
    return scale * (scaled - mean_e - normal * mean_en)


def first_norm_kernel(tok_ref, *refs):
    ctx_refs, weights, refs = refs[:4], refs[4:12], refs[12:]
    embed_ref, bout_ref, gain_ref, shift_ref, normal_ref, scale_ref, mid_ref, mid_t, hid_t, wout_ref = refs

    @pl.when(pl.program_id(0) == 0)
    def _():
        for j in range(8):
            wout_ref[j * UNIT : (j + 1) * UNIT, :] = rows_of(weights[j])

    hidden = tok_ref[...].astype(F32) + embed_ref[...]
    hid_t[...] = hidden.astype(BF16).T
    total = bout_ref[...]
    for p in range(4):
        total = total + dot(ctx_refs[p][...], wout_ref[2 * p * UNIT : 2 * (p + 1) * UNIT, :])
    normal, scale = norm_of(hidden + total)
    normal_ref[...] = normal.astype(BF16)
    scale_ref[...] = scale
    mid = (normal * gain_ref[...] + shift_ref[...]).astype(BF16)
    mid_ref[...] = mid
    mid_t[...] = mid.T


def first_norm(tokens, contexts, heads, embed_row, b_out, gain, shift):
    tile = pl.BlockSpec((ROWS, D), lambda i: (i, 0))
    column = pl.BlockSpec((D, ROWS), lambda i: (0, i))
    return pl.pallas_call(
        first_norm_kernel,
        out_shape=(
        far((LEN, D)),
        far((LEN, 1), F32),
        struct((LEN, D)),
        far((D, LEN)),
        far((D, LEN)),
        ),
        grid=(LEN // ROWS,),
        in_specs=[tile]
        + [pl.BlockSpec((ROWS, 2 * UNIT), lambda i: (i, 0))] * 4
        + half_specs(UNIT, 3)
        + [whole((1, D))] * 4,
        out_specs=[
            tile,
            pl.BlockSpec((ROWS, 1), lambda i: (i, 0)),
            tile,
            column,
            column,
        ],
        scratch_shapes=[pltpu.VMEM((D, D), BF16)],
        compiler_params=room(24),
        cost_estimate=cost(2.2e9, 20e6),
    )(tokens, *contexts, *eight(heads), embed_row, b_out, gain, shift)


def ffn_tile(mid_ref, up_refs, down_refs, bias_refs, act_ref, slope_ref):
    size = act_ref.shape[1] // 2
    pres = []
    for up, ref in zip(up_refs, bias_refs):
        bias = rows_of(ref)[0:1, 2 * UNIT : 2 * UNIT + size].astype(F32)
        pres.append(dot(mid_ref[...], rows_of(up), NT) + bias)
    total = 0.0
    for u in range(HALF):
        columns = slice(u * size, (u + 1) * size)
        pre = pres[u]
        phi = 0.5 * (1.0 + lax.erf(pre * math.sqrt(0.5)))
        bell = jnp.exp(-0.5 * pre * pre) * (1.0 / math.sqrt(2.0 * math.pi))
        act = (pre * phi).astype(BF16)
        act_ref[:, columns] = act
        slope_ref[:, columns] = (phi + pre * bell).astype(BF16)
        total = total + dot(act, rows_of(down_refs[u]))
    return total


def ffn_kernel(mid_ref, *refs):
    *into, act_ref, slope_ref, total_ref = refs[6:]
    total = ffn_tile(mid_ref, refs[0:2], refs[2:4], refs[4:6], act_ref, slope_ref)
    for ref in into:
        total = total + ref[...]
    total_ref[...] = total


def ffn_specs(size, pair):
    return (
        [pl.BlockSpec((TILE_U, D), lambda i: (i, 0))]
        + pair_specs(size, 0, pair) * 2
        + pair_specs(EXTRA, 4 * UNIT // EXTRA, pair)
    )


def ffn_pair(mid_low, up, down, pair, heads, into):
    size = up[2].shape[0]
    tile = lambda n: pl.BlockSpec((TILE_U, n), lambda i: (i, 0))
    return pl.pallas_call(
        ffn_kernel,
        out_shape=(
            far((LEN, 2 * size)),
            far((LEN, 2 * size)),
            struct((LEN, D), F32),
        ),
        in_specs=ffn_specs(size, pair) + [tile(D)] * len(into),
        out_specs=[tile(2 * size), tile(2 * size), tile(D)],
        grid=(LEN // TILE_U,),
        compiler_params=room(24),
        cost_estimate=cost(4.3e9, 18e6),
    )(mid_low, *pair_of(up, pair), *pair_of(down, pair), *pair_of(heads, pair), *into)


def ffn_last_kernel(mid_ref, *refs):
    into_ref, cot_ref, bias_ref, gain_ref, shift_ref = refs[6:11]
    act_ref, slope_ref, out_ref, low_ref, low_t, sum_ref = refs[11:]

    @pl.when(pl.program_id(0) == 0)
    def _():
        sum_ref[...] = jnp.zeros_like(sum_ref)

    total = ffn_tile(mid_ref, refs[0:2], refs[2:4], refs[4:6], act_ref, slope_ref)
    total = total + into_ref[...] + bias_ref[...]
    normal, scale = norm_of(mid_ref[...].astype(F32) + total)
    out_ref[...] = (normal * gain_ref[...] + shift_ref[...]).astype(BF16)
    cot = cot_ref[...].astype(F32)
    low = norm_back(normal, scale, cot, gain_ref[...]).astype(BF16)
    low_ref[...] = low
    low_t[...] = low.T
    sums = [jnp.sum(v, axis=0, keepdims=True) for v in (low.astype(F32), cot * normal, cot)]
    for j in range(3):
        sum_ref[j : j + 1, :] += sums[j]


def ffn_last(mid_low, up, down, pair, heads, into, cot, *rows):
    size = up[2].shape[0]
    tile = lambda n: pl.BlockSpec((TILE_U, n), lambda i: (i, 0))
    return pl.pallas_call(
        ffn_last_kernel,
        out_shape=(
            far((LEN, 2 * size)),
            far((LEN, 2 * size)),
            far((LEN, D)),
            far((LEN, D)),
            far((D, LEN)),
            struct((8, D), F32),
        ),
        in_specs=ffn_specs(size, pair) + [tile(D)] * 2 + [whole((1, D))] * 3,
        out_specs=[tile(2 * size), tile(2 * size), tile(D), tile(D)]
        + [pl.BlockSpec((D, TILE_U), lambda i: (0, i)), whole((8, D))],
        grid=(LEN // TILE_U,),
        compiler_params=room(30),
        cost_estimate=cost(4.3e9, 30e6),
    )(
        mid_low, *pair_of(up, pair), *pair_of(down, pair), *pair_of(heads, pair), into, cot, *rows
    )


def ffn_back_kernel(branch_hbm, *refs):
    down_hbm, up_hbm, slope_hbm, refs = refs[0:6], refs[6:12], refs[12:16], refs[16:]
    one_hbm, scale_ref, gain_ref, refs = refs[0], refs[1], refs[2], refs[3:]
    pre_hbm, sum_ref, low_ref, low_t, norm_sum_ref, refs = (
        refs[0:4],
        refs[4],
        refs[5],
        refs[6],
        refs[7],
        refs[8:],
    )
    branch, down, up, slope, total, one, low, low_turned, sems = refs
    size = up.shape[1]
    plan = ((0, 0), (0, 1), (1, 0), (1, 1), (2, None), (3, None), (4, None), (5, None))
    first = pltpu.make_async_copy(branch_hbm, branch, sems.at[0])
    first.start()
    copies = []
    for j, (piece, which) in enumerate(plan):
        if which is None:
            down_part, up_part = down_hbm[piece], up_hbm[piece]
        else:
            down_part, up_part = down_hbm[piece].at[which], up_hbm[piece].at[which]
        columns = slice((j % 2) * size, (j % 2 + 1) * size)
        group = [
            pltpu.make_async_copy(down_part, down.at[j], sems.at[1 + 3 * j]),
            pltpu.make_async_copy(
                slope_hbm[j // 2].at[:, columns], slope.at[j], sems.at[2 + 3 * j]
            ),
            pltpu.make_async_copy(up_part, up.at[j], sems.at[3 + 3 * j]),
        ]
        for copy in group:
            copy.start()
        copies.append(group)
    last = pltpu.make_async_copy(one_hbm, one, sems.at[25])
    last.start()
    first.wait()
    stores = []
    norm_sums = [0.0] * 3
    for j in range(len(plan)):
        for copy in copies[j]:
            copy.wait()
        if j == len(plan) - 1:
            last.wait()
        columns = slice((j % 2) * size, (j % 2 + 1) * size)
        sums = 0.0
        for r in range(LEN // ROWS):
            rows = slice(r * ROWS, (r + 1) * ROWS)
            d_act = dot(branch[rows, :], down[j], NT)
            d_pre = (d_act * slope[j, rows, :].astype(F32)).astype(BF16)
            slope[j, rows, :] = d_pre
            sums = sums + jnp.sum(d_pre.astype(F32), axis=0, keepdims=True)
            part = dot(d_pre, up[j])
            if j == 0:
                total[rows, :] = part
            elif j < len(plan) - 1:
                total[rows, :] += part
            else:
                d_mid = total[rows, :] + part + branch[rows, :].astype(F32)
                normal = one[rows, :].astype(F32)
                part = norm_back(normal, scale_ref[rows, :], d_mid, gain_ref[...]).astype(BF16)
                low[rows, :] = part
                low_turned[:, rows] = part.T
                for k, (source, target) in enumerate(
                    (
                        (low.at[rows, :], low_ref.at[rows, :]),
                        (low_turned.at[:, rows], low_t.at[:, rows]),
                    )
                ):
                    store = pltpu.make_async_copy(source, target, sems.at[34 + 2 * r + k])
                    store.start()
                    stores.append(store)
                for k, v in enumerate((part.astype(F32), d_mid * normal, d_mid)):
                    norm_sums[k] = norm_sums[k] + jnp.sum(v, axis=0, keepdims=True)
        sum_ref[j : j + 1, :] = sums
        store = pltpu.make_async_copy(slope.at[j], pre_hbm[j // 2].at[:, columns], sems.at[26 + j])
        store.start()
        stores.append(store)
    for k in range(3):
        norm_sum_ref[k : k + 1, :] = norm_sums[k]
    for store in stores:
        store.wait()


def ffn_back(branch_two, down, up, slopes, normal_one, scale_one, gain):
    size = down[2].shape[0]
    hbm = pl.BlockSpec(memory_space=pltpu.HBM)
    return pl.pallas_call(
        ffn_back_kernel,
        out_shape=(far((LEN, 2 * size)),) * 4
        + (struct((8, size), F32), far((LEN, D)), far((D, LEN)), struct((8, D), F32)),
        grid=(1,),
        in_specs=[hbm] * 18 + [whole((LEN, 1)), whole((1, D))],
        out_specs=[hbm] * 4 + [whole((8, size)), hbm, hbm, whole((8, D))],
        scratch_shapes=[
            pltpu.VMEM((LEN, D), BF16),
            pltpu.VMEM((8, size, D), BF16),
            pltpu.VMEM((8, size, D), BF16),
            pltpu.VMEM((8, LEN, size), BF16),
            pltpu.VMEM((LEN, D), F32),
            pltpu.VMEM((LEN, D), BF16),
            pltpu.VMEM((LEN, D), BF16),
            pltpu.VMEM((D, LEN), BF16),
            pltpu.SemaphoreType.DMA((42,)),
        ],
        compiler_params=room(52),
        cost_estimate=cost(17e9, 40e6),
    )(branch_two, *down, *up, *slopes, normal_one, scale_one, gain)


class Run(NamedTuple):
    which: int
    first: int
    second: int
    size: int
    base: int
    stride: int


def unit_runs(count, size):
    half = size // 2
    return [Run(0, r * half // count, half + r * half // count, half // count, r * half // count, half) for r in range(count)]


def head_runs(which, count):
    return [Run(which, 2 * j * UNIT, (2 * j + 1) * UNIT, UNIT, 2 * j * UNIT, UNIT) for j in range(count)]


def part_width(part):
    return sum(2 * run.size for run in part)


def grad_kernel(blocks, side_from, outputs, lefts, got_from, left_at, *refs):
    n_right = 3 * lefts
    left_hbm, right_hbm, refs = refs[:lefts], refs[lefts : lefts + n_right], refs[lefts + n_right :]
    got_hbm, refs = (None, refs) if got_from is None else (refs[0], refs[1:])
    out_hbm, (left, right, got, out, sems) = refs[: len(outputs)], refs[len(outputs) :]
    count = [0]

    def copy_of(source, target):
        copy = pltpu.make_async_copy(source, target, sems.at[count[0]])
        copy.start()
        count[0] += 1
        return copy

    ready = {}
    chunks, at = [], 0
    for part, far in blocks:
        for run in part:
            copies = []
            if (run.which, 0) not in ready:
                source = left_hbm[run.which]
                ready[run.which, 0] = copy_of(source.at[:, left_at[0]], left.at[run.which, 0])
            for h in range(2):
                if far:
                    piece, source = 1 + h, run.second if side_from else run.first
                else:
                    piece, source = 0, run.second if h else run.first
                copies.append(
                    copy_of(
                        right_hbm[3 * run.which + piece].at[:, source : source + run.size],
                        right.at[:, at + h * run.size : at + (h + 1) * run.size],
                    )
                )
            columns = slice(at, at + 2 * run.size)
            if got_from is not None:
                source = got_hbm.at[:, :, got_from + at : got_from + at + 2 * run.size]
                copies.append(copy_of(source, got.at[:, :, columns]))
            if (run.which, 1) not in ready:
                source = left_hbm[run.which]
                ready[run.which, 1] = copy_of(source.at[:, left_at[1]], left.at[run.which, 1])
            chunks.append((run.which, at, 2 * run.size, copies))
            at += 2 * run.size
    stores = []
    for which, at, size, copies in chunks:
        for copy in copies:
            copy.wait()
        columns = slice(at, at + size)
        for side in range(2):
            if (which, side) in ready:
                ready.pop((which, side)).wait()
            total = dot(left[which, side].reshape(D // 2, LEN), right[:, columns])
            if got_from is not None:
                total = total + got[side, :, columns].astype(F32)
            out[side, :, columns] = total.astype(BF16)
        for (start, end, side), target in zip(outputs, out_hbm):
            if start <= at < end:
                place = slice(at - start, at - start + size)
                if side is None:
                    stores.append(copy_of(out.at[:, :, columns], target.at[:, :, place]))
                else:
                    stores.append(copy_of(out.at[side, :, columns], target.at[:, place]))
    for copy in stores:
        copy.wait()


def grad_call(info, left_t, rights, blocks, side, outputs, got=None, got_from=None):
    width = sum(part_width(part) for part, _ in blocks)
    hbm = pl.BlockSpec(memory_space=pltpu.HBM)
    lefts = len(left_t)
    operands = [v.reshape(4, 2, D // 8, LEN) for v in left_t] + [v for r in rights for v in r]
    operands += [] if got is None else [got]
    shapes = [
        (2, D // 2, end - start) if at is None else (D // 2, end - start) for start, end, at in outputs
    ]
    return pl.pallas_call(
        functools.partial(grad_kernel, blocks, side, outputs, lefts, got_from),
        out_shape=tuple(far(shape) for shape in shapes),
        grid_spec=pltpu.PrefetchScalarGridSpec(
            num_scalar_prefetch=1,
            grid=(1,),
            in_specs=[hbm] * len(operands),
            out_specs=[hbm] * len(shapes),
            scratch_shapes=[
                pltpu.VMEM((lefts, 2, 4, D // 8, LEN), BF16),
                pltpu.VMEM((LEN, width), BF16),
                pltpu.VMEM((2, D // 2, 128 if got is None else width), BF16),
                pltpu.VMEM((2, D // 2, width), BF16),
                pltpu.SemaphoreType.DMA((48,)),
            ],
        ),
        compiler_params=room(60),
        cost_estimate=cost(2 * D * LEN * width, 10e6),
    )(info, *operands)


def column_runs(part, swap):
    at = 0
    for run in part:
        for h in range(2):
            source = at + (1 - h if swap else h) * run.size
            yield at + h * run.size, source, run.size
        at += 2 * run.size


def add_kernel(part, swap, mine_ref, got_ref, out_ref):
    rows = out_ref.shape[0]
    mine, got = mine_ref[...].reshape(rows, -1), got_ref[...].reshape(rows, -1)
    for at, source, size in column_runs(part, swap):
        total = mine[:, at : at + size].astype(F32) + got[:, source : source + size].astype(F32)
        out_ref[:, at : at + size] = total.astype(BF16)


def block_spec(array, where, width):
    side, column = where
    if len(array.shape) == 3:
        return pl.BlockSpec((1, D // 2, width), lambda *_: (side, 0, column))
    return pl.BlockSpec((D // 2, width), lambda *_: (0, column))


def add_parts(mine, got, part, swap):
    width = part_width(part)
    return pl.pallas_call(
        functools.partial(add_kernel, part, swap),
        out_shape=struct((D // 2, width)),
        grid=(1,),
        in_specs=[block_spec(*v, width) for v in (mine, got)],
        out_specs=whole((D // 2, width)),
        compiler_params=room(24),
        cost_estimate=cost(1e6, 3e6),
    )(mine[0], got[0])


def split_kernel(parts, info_ref, *refs):
    ins, out_refs = refs[: 3 * len(parts)], refs[3 * len(parts) :]
    span = D // 8
    for k in range(4):
        rows = pl.ds(pl.multiple_of((info_ref[2] ^ k) * span, span), span)
        first = 0
        for p, part in enumerate(parts):
            mine, from_x, from_y = [
                (ref[0, rows, :] if len(ref.shape) == 3 else ref[rows, :]).astype(F32)
                for ref in ins[3 * p : 3 * p + 3]
            ]
            for at, source, size in column_runs(part, True):
                total = mine[:, at : at + size] + from_y[:, at : at + size]
                total = total + from_x[:, source : source + size]
                out_refs[k][:, first + at : first + at + size] = total.astype(BF16)
            first += part_width(part)


def split_z(info, parts, sources):
    width = sum(part_width(part) for part in parts)
    specs = [
        block_spec(*v, part_width(part)) for part, triple in zip(parts, sources) for v in triple
    ]
    out = pl.pallas_call(
        functools.partial(split_kernel, parts),
        out_shape=(struct((D // 8, width)),) * 4,
        grid_spec=pltpu.PrefetchScalarGridSpec(
            num_scalar_prefetch=1,
            grid=(1,),
            in_specs=specs,
            out_specs=[whole((D // 8, width))] * 4,
        ),
        compiler_params=room(60),
        cost_estimate=cost(1e6, 4e6),
    )(info, *[v[0] for triple in sources for v in triple])
    return [out[0]] + [send_dp(out[k], 2 * k) for k in (1, 2, 3)]


def finish_kernel(runs, turned, info_ref, *refs):
    parts, outs = refs[:4], refs[4:]
    at = 0
    for run in runs:
        for h in range(2):
            columns = slice(at, at + run.size)
            total = parts[0][:, columns].astype(F32)
            for part in parts[1:]:
                total = total + part[:, columns].astype(F32)
            spot = pl.ds(pl.multiple_of(run.base + info_ref[h] * run.stride, UNIT), run.size)
            if turned[run.which]:
                outs[run.which][spot, :] = total.T
            else:
                outs[run.which][:, spot] = total
            at += run.size


def finish(info, values, parts, turned):
    rows = D // 8
    runs = tuple(run for part in parts for run in part)
    sizes = [sum(2 * r.size for r in runs if r.which == k) for k in range(len(turned))]
    shapes = [(size, rows) if t else (rows, size) for size, t in zip(sizes, turned)]
    return pl.pallas_call(
        functools.partial(finish_kernel, runs, turned),
        out_shape=tuple(struct(shape, F32) for shape in shapes),
        grid_spec=pltpu.PrefetchScalarGridSpec(
            num_scalar_prefetch=1,
            grid=(1,),
            in_specs=[whole((rows, sum(sizes)))] * 4,
            out_specs=[whole(shape) for shape in shapes],
        ),
        compiler_params=room(24),
        cost_estimate=cost(1e6, 4e6),
    )(info, *values)


def input_grad_kernel(branch_ref, *refs):
    grads, heads, (out_ref, sum_ref, weight, sems) = refs[:4], refs[4:10], refs[10:]
    step = pl.program_id(0)
    plan = ((0, 0), (0, 1), (1, 0), (1, 1), (2, None), (3, None), (4, None), (5, None))
    copies = []
    for j, (piece, which) in enumerate(plan):
        source = heads[piece] if which is None else heads[piece].at[which]
        for k in range(3):
            at = ((j // 2) * 6 + 2 * k + j % 2) * UNIT
            copies.append(
                pltpu.make_async_copy(
                    source.at[k * UNIT : (k + 1) * UNIT, :],
                    weight.at[at : at + UNIT, :],
                    sems.at[3 * j + k],
                )
            )

    @pl.when(step == 0)
    def _():
        for copy in copies:
            copy.start()
        sum_ref[...] = jnp.zeros_like(sum_ref)

    total = branch_ref[...].astype(F32)
    for p in range(4):

        @pl.when(step == 0)
        def _():
            for copy in copies[6 * p : 6 * p + 6]:
                copy.wait()

        total = total + dot(grads[p][...], weight[6 * p * UNIT : 6 * (p + 1) * UNIT, :])
    out_ref[...] = total
    sum_ref[0:1, :] += jnp.sum(total, axis=0, keepdims=True)


def input_grad(branch_one, d_qkv, heads):
    tile = pl.BlockSpec((ROWS, D), lambda i: (i, 0))
    width = d_qkv[0].shape[1]
    return pl.pallas_call(
        input_grad_kernel,
        out_shape=(far((LEN, D), F32), struct((8, D), F32)),
        grid=(LEN // ROWS,),
        in_specs=[tile]
        + [pl.BlockSpec((ROWS, width), lambda i: (i, 0))] * 4
        + [pl.BlockSpec(memory_space=pltpu.HBM)] * 6,
        out_specs=[tile, whole((8, D))],
        scratch_shapes=[pltpu.VMEM((4 * width, D), BF16), pltpu.SemaphoreType.DMA((24,))],
        compiler_params=room(60),
        cost_estimate=cost(6.4e9, 20e6),
    )(branch_one, *d_qkv, *heads)


def exchange_kernel(sum_ref, row_ref, total_ref, rows_ref, got, sems_a, sems_b):
    devices = GRID_DP * GRID_MP
    me = lax.axis_index("dp") * GRID_MP + lax.axis_index("mp")

    def place(index):
        return {"dp": index // GRID_MP, "mp": index % GRID_MP}

    barrier = pltpu.get_barrier_semaphore()

    def greet(k, carry):
        target = (me + k) % devices
        pl.semaphore_signal(
            barrier, inc=1, device_id=place(target), device_id_type=pl.DeviceIdType.MESH
        )
        return carry

    lax.fori_loop(1, devices, greet, 0)
    pl.semaphore_wait(barrier, devices - 1)

    def copies(k):
        target = (me + k) % devices
        first = pltpu.make_async_remote_copy(
            src_ref=sum_ref.at[target],
            dst_ref=got.at[k],
            send_sem=sems_a.at[0, k],
            recv_sem=sems_a.at[1, k],
            device_id=place(target),
            device_id_type=pl.DeviceIdType.MESH,
        )
        second = pltpu.make_async_remote_copy(
            src_ref=row_ref,
            dst_ref=rows_ref.at[k],
            send_sem=sems_b.at[0, k],
            recv_sem=sems_b.at[1, k],
            device_id=place(target),
            device_id_type=pl.DeviceIdType.MESH,
        )
        return first, second

    def start(k, carry):
        for copy in copies(k):
            copy.start()
        return carry

    lax.fori_loop(1, devices, start, 0)
    rows_ref[0] = row_ref[...]

    def finish_copy(k, carry):
        for copy in copies(k):
            copy.wait()
        return carry

    lax.fori_loop(1, devices, finish_copy, 0)
    total_ref[...] = sum_ref[me] + jnp.sum(got[1:], axis=0)


def exchange(sums, row):
    devices = GRID_DP * GRID_MP
    vmem = pl.BlockSpec(memory_space=pltpu.VMEM)
    return pl.pallas_call(
        exchange_kernel,
        out_shape=(struct(sums.shape[1:], F32), struct((devices,) + row.shape, F32)),
        in_specs=[vmem, vmem],
        out_specs=[vmem, vmem],
        scratch_shapes=[
            pltpu.VMEM(sums.shape, F32),
            pltpu.SemaphoreType.DMA((2, devices)),
            pltpu.SemaphoreType.DMA((2, devices)),
        ],
        compiler_params=pltpu.CompilerParams(collective_id=0, has_side_effects=True),
        cost_estimate=cost(1e6, 1e6),
    )(sums, row)


def natural_order(x_at, mp_at):
    block, half = jnp.arange(8, dtype=jnp.int32) // 2, jnp.arange(8, dtype=jnp.int32) % 2
    away, at = block ^ mp_at, half ^ x_at
    source = jnp.where(away < 2, 2 * away + at, 2 + away + 2 * at)
    return (source[:, None] == jnp.arange(8, dtype=jnp.int32)[None, :]).astype(F32)


def body_rows(
    tokens,
    segment_ids,
    time_steps,
    w_qkv,
    b_qv,
    w_out,
    b_out,
    gain_one,
    shift_one,
    w_up,
    b_up,
    w_down,
    b_down,
    gain_two,
    shift_two,
    w_time,
    b_time,
    cotangent,
):
    dp_at, mp_at = lax.axis_index("dp"), lax.axis_index("mp")
    x_at, z_at = dp_at % 2, dp_at // 2
    info = jnp.stack([x_at, 1 - x_at, z_at, mp_at]).astype(jnp.int32)
    row = lambda v: v.astype(F32)[None, :]
    width = w_qkv.shape[2]

    heads_own, heads_first = pack_heads(info, w_qkv, w_out, b_qv, b_up)
    heads = fetch(heads_own, heads_first)
    up_own, up_first, down_own, down_first = pack_units(info, w_up, w_down)
    up = fetch(up_own, up_first)
    down = fetch(down_own, down_first)

    own_step = lax.dynamic_slice_in_dim(time_steps, mp_at, 1, 0)
    segment_row = lax.dynamic_index_in_dim(segment_ids, mp_at, 0, keepdims=False)
    features = time_features(own_step)
    embed_row = jnp.dot(features, w_time.astype(F32), precision=HIGHEST_PRECISION)
    embed_row = embed_row + row(b_time)
    hidden_low = (tokens.astype(F32) + embed_row).astype(BF16)
    hotq, hotk = mark_segments(segment_row)
    win_f, win_b = windows(segment_row, TILE_F), windows(segment_row, TILE_B)

    qkv, ctx, lse = [], [], []
    for p in range(4):
        parts = attend_pair(win_f, hidden_low, heads, p, hotq, hotk)
        for kept, part in zip((qkv, ctx, lse), parts):
            kept.append(part)
    normal_one, scale_one, mid_low, mid_t, hidden_t = first_norm(
        tokens, ctx, heads, embed_row, row(b_out), row(gain_one), row(shift_one)
    )

    act, slope, ffn = [], [], ()
    for p in range(3):
        act_p, slope_p, *ffn = ffn_pair(mid_low, up, down, p, heads, ffn)
        act.append(act_p)
        slope.append(slope_p)
    act_p, slope_p, out_rows, branch_two, branch_two_t, sums_two = ffn_last(
        mid_low,
        up,
        down,
        3,
        heads,
        *ffn,
        cotangent,
        *[row(v) for v in (b_down, gain_two, shift_two)],
    )
    act.append(act_p)
    slope.append(slope_p)

    units = act[0].shape[1]
    down_parts = [(run,) for run in unit_runs(2, units)]
    up_parts = [down_parts[0], (down_parts[1][0], *head_runs(1, 1))]
    qkv_part = tuple(head_runs(0, 3))

    def two_way(left_t, rights, parts, cover):
        blocks = tuple((part, far) for part in parts for far in (False, True))
        one, two = (part_width(part) for part in parts)
        every = 2 * (one + two)
        (sent,) = grad_call(info, left_t, [r[1:] for r in rights], blocks, 1, ((0, every, None),))
        got = send_mp(sent, 1)
        covered = cover()
        outputs = (
            (0, one, None),
            (one, 2 * one, None),
            (2 * one, every, 0),
            (2 * one, every, 1),
        )
        result = grad_call(
            info, left_t, [r[:1] + r[2:] for r in rights], blocks, 0, outputs, got, 0
        )
        return covered, result

    def first_sends(blocks):
        own, far, keep, leave = blocks
        return own, keep, send_mp(far, 2), send_dp(leave, 1)

    def second_sends(sums, parts):
        own, keep, from_y, from_x = sums
        low = add_parts((own, (1, 0)), (from_y, (1, 0)), parts[0], False)
        x_two = send_dp(low, 1)
        low = add_parts((keep, (0, 1)), (from_x, (0, 1)), parts[1], True)
        y_two = send_mp(low, 2)
        here = (0, 0)
        return (
            ((own, here), (x_two, here), (from_y, here)),
            ((keep, here), (from_x, here), (y_two, here)),
        )

    def ffn_part():
        return ffn_back(
            branch_two, down, up, slope, normal_one, scale_one, row(gain_one)
        )

    (*d_pre, sums_up, branch_one, branch_one_t, sums_one), down_blocks = two_way(
        [branch_two_t], [act], down_parts, ffn_part
    )
    down_sums = first_sends(down_blocks)
    d_qkv, qkv_sums = [None] * 4, [None] * 4

    def back(p):
        d_qkv[p], qkv_sums[p] = attend_back_pair(
            win_b, qkv[p], hotq, hotk, branch_one, heads, p, ctx[p], lse[p]
        )

    _, up_blocks = two_way([mid_t, branch_one_t], [d_pre, ctx], up_parts, lambda: back(1))
    down_last = second_sends(down_sums, down_parts)
    up_sums = first_sends(up_blocks)
    back(2)
    down_values = split_z(info, down_parts, down_last)
    back(3)
    wide = part_width(qkv_part)
    far_only, own_only = ((qkv_part, True),), ((qkv_part, False),)
    (sent,) = grad_call(
        info, [hidden_t], [d_qkv[1:]], own_only + far_only, 1, ((0, 2 * wide, None),)
    )
    got = send_mp(sent, 1)
    up_last = second_sends(after(up_sums, sent), up_parts)
    sides = ((0, wide, 0), (0, wide, 1))
    far_keep, far_leave = grad_call(
        info, [hidden_t], [[d_qkv[1]] + d_qkv[2:]], far_only, 0, sides, got, wide
    )
    far_x = send_dp(far_leave, 1)
    back(0)
    up_values = split_z(info, up_parts, up_last)
    here = (0, 0)
    far_low = add_parts((far_keep, here), (far_x, here), qkv_part, True)
    far_y = send_mp(far_low, 2)
    own_keep, own_leave = grad_call(
        info, [hidden_t], [d_qkv[:1] + d_qkv[2:]], own_only, 0, sides, got, 0
    )
    own_x = send_dp(own_leave, 1)
    grad_tokens, sums_in = input_grad(branch_one, d_qkv, heads)
    qkv_values = split_z(info, (qkv_part,), (((own_keep, here), (own_x, here), (far_y, here)),))

    devices = GRID_DP * GRID_MP
    heads_sum = jnp.concatenate([v[0:1] for v in qkv_sums]).reshape(4, 3, HALF, UNIT)
    heads_sum = heads_sum.transpose(0, 2, 1, 3).reshape(8, -1)
    blocks = jnp.dot(
        natural_order(x_at, mp_at),
        jnp.concatenate([sums_up, heads_sum], axis=1),
        precision=HIGHEST_PRECISION,
    )

    def spread(v):
        return v.reshape(GRID_MP, GRID_DP, -1).transpose(1, 0, 2).reshape(devices, -1)

    ends = (0, units // 2, units // 2 + UNIT, units // 2 + 3 * UNIT)
    full = jnp.concatenate([sums_two[:3], sums_one[:3]]).reshape(6, devices, -1)
    rows = [full.transpose(1, 0, 2).reshape(devices, -1), spread(blocks[:, : ends[1]])]
    rows += [spread(blocks[:, at : at + UNIT]) for at in (ends[1], ends[3] - UNIT)]
    tail_row = jnp.concatenate(
        [sums_in[0:1], jnp.broadcast_to(own_step.astype(F32)[None, :], (1, UNIT))], axis=1
    )
    totals, all_rows = exchange(jnp.concatenate(rows, axis=1)[:, None, :], tail_row)
    totals, all_rows, down_values, up_values = after(
        (totals, all_rows, down_values, up_values), qkv_values[0]
    )
    all_rows = all_rows[:, 0]
    span = D // (GRID_DP * GRID_MP)
    own = [totals[0, j * span : (j + 1) * span] for j in range(6)]
    device_at = dp_at * GRID_MP + mp_at
    all_grads = all_rows[:, :D]
    dims = device_at * span + jnp.arange(span, dtype=jnp.int32)
    ladder = (dims % (D // 2)).astype(F32)
    frequency = jnp.exp(ladder * (-math.log(10000.0) / (D // 2)))
    angles = all_rows[:, D : D + 1] * frequency[None, :]
    own_features = jnp.where((dims < D // 2)[None, :], jnp.sin(angles), jnp.cos(angles))
    g_w_time = jnp.dot(own_features.T, all_grads, precision=HIGHEST_PRECISION)
    g_b_time = lax.dynamic_slice_in_dim(jnp.sum(all_grads, axis=0), device_at * span, span, 0)

    (g_w_qkv,) = finish(info, qkv_values, (qkv_part,), (False,))
    (g_w_down,) = finish(info, down_values, down_parts, (True,))
    g_w_up, g_w_out = finish(info, up_values, up_parts, (False, True))
    up_end = totals.shape[1] - 2 * span
    return (
        out_rows,
        grad_tokens,
        g_w_qkv.reshape(D // 8, 3, width),
        totals[0, up_end:].reshape(2, 1, -1),
        g_w_out,
        own[3],
        own[4],
        own[5],
        g_w_up,
        totals[:, 6 * span : up_end],
        g_w_down,
        own[0],
        own[1],
        own[2],
        g_w_time,
        g_b_time,
    )


def solution(mesh):
    placed = (
        P(("dp", "mp"), None),
        P("dp", None),
        P("dp"),
        P(None, None, "mp"),
        P(None, "mp"),
        P("mp", None),
        P(),
        P(),
        P(),
        P(None, "mp"),
        P("mp"),
        P("mp", None),
        P(),
        P(),
        P(),
        P(),
        P(),
        P(("dp", "mp"), None),
    )
    rows = mesh.shape["dp"], mesh.shape["mp"]

    def body(*args):
        if args[0].shape[0] != LEN or rows != (GRID_DP, GRID_MP):
            return body_split(*args)
        return body_rows(*args)

    return jax.shard_map(
        body,
        mesh=mesh,
        in_specs=placed,
        out_specs=(
            P(("dp", "mp"), None),
            P(("dp", "mp"), None),
            P("dp", None, "mp"),
            P(None, "mp", "dp"),
            P("mp", "dp"),
            P(("dp", "mp")),
            P(("dp", "mp")),
            P(("dp", "mp")),
            P("dp", "mp"),
            P("mp", "dp"),
            P("mp", "dp"),
            P(("dp", "mp")),
            P(("dp", "mp")),
            P(("dp", "mp")),
            P(("dp", "mp"), None),
            P(("dp", "mp")),
        ),
        check_vma=False,
    )
```

```python
import functools
import math
from typing import NamedTuple

import jax
import jax.numpy as jnp
from jax import lax
from jax.experimental import pallas as pl
from jax.experimental.pallas import tpu as pltpu
from jax.sharding import PartitionSpec as P


D = 1024
HEAD_DIM = 64
LEN = 1024


EPS = 1e-05
HIGHEST_PRECISION = lax.Precision.HIGHEST


def time_features(step_values):
    half_width = D // 2
    ladder = jnp.arange(half_width, dtype=jnp.float32)
    frequency = jnp.exp(ladder * (-math.log(10000.0) / half_width))
    angles = step_values.astype(jnp.float32)[:, None] * frequency[None, :]
    return jnp.concatenate([jnp.sin(angles), jnp.cos(angles)], axis=1)


def layer_norm(values, gain_vec, shift_vec):
    center = values - jnp.mean(values, axis=-1, keepdims=True)
    spread = jnp.mean(center * center, axis=-1, keepdims=True)
    return center * lax.rsqrt(spread + EPS) * gain_vec + shift_vec


def exact_gelu(values):
    return jax.nn.gelu(values, approximate=False)


def project_qkv(hidden_full, w_qkv, b_qv):
    width_local = w_qkv.shape[2]
    w_flat = w_qkv.reshape(w_qkv.shape[0], 3 * width_local)
    bias_row = jnp.concatenate([b_qv[0], jnp.zeros((width_local,), b_qv.dtype), b_qv[1]]).astype(
        jnp.float32
    )
    product = jnp.dot(hidden_full, w_flat, preferred_element_type=jnp.float32)
    return (product + bias_row[None, :]).astype(jnp.bfloat16)


def head_parts(qkv_seq):
    width_local = qkv_seq.shape[1] // 3
    head_local = width_local // HEAD_DIM
    shaped = qkv_seq.reshape(qkv_seq.shape[0], 3, head_local, HEAD_DIM)
    return (shaped[:, 0], shaped[:, 1], shaped[:, 2])


def masked_scores(queries, keys_part, segment_row):
    scores = jnp.einsum("qhd,khd->hqk", queries, keys_part, preferred_element_type=jnp.float32)
    scores = scores * (1.0 / math.sqrt(HEAD_DIM))
    same_doc = segment_row[:, None] == segment_row[None, :]
    return jnp.where(same_doc[None, :, :], scores, -1e30)


def attend_forward(inputs):
    qkv_seq, segment_row = inputs
    queries, keys_part, values_part = head_parts(qkv_seq)
    masked = masked_scores(queries, keys_part, segment_row)
    top_score = jnp.max(masked, axis=2, keepdims=True)
    weights_exp = jnp.exp(masked - top_score)
    totals = jnp.sum(weights_exp, axis=2, keepdims=True)
    probability = weights_exp / totals
    context = jnp.einsum(
        "hqk,khd->qhd",
        probability.astype(jnp.bfloat16),
        values_part,
        preferred_element_type=jnp.float32,
    )
    log_total = (top_score + jnp.log(totals))[:, :, 0]
    return (context.reshape(qkv_seq.shape[0], -1).astype(jnp.bfloat16), log_total)


def attend_backward(inputs):
    qkv_seq, grad_seq, log_total, segment_row = inputs
    queries, keys_part, values_part = head_parts(qkv_seq)
    masked = masked_scores(queries, keys_part, segment_row)
    probability = jnp.exp(masked - log_total[:, :, None])
    grad_heads = grad_seq.reshape(grad_seq.shape[0], -1, HEAD_DIM)
    d_values = jnp.einsum(
        "hqk,qhd->khd",
        probability.astype(jnp.bfloat16),
        grad_heads,
        preferred_element_type=jnp.float32,
    )
    d_probs = jnp.einsum(
        "qhd,khd->hqk", grad_heads, values_part, preferred_element_type=jnp.float32
    )
    row_terms = jnp.sum(probability * d_probs, axis=2, keepdims=True)
    d_scores = (probability * (d_probs - row_terms)).astype(jnp.bfloat16)
    score_scale = 1.0 / math.sqrt(HEAD_DIM)
    d_queries = (
        jnp.einsum("hqk,khd->qhd", d_scores, keys_part, preferred_element_type=jnp.float32)
        * score_scale
    )
    d_keys = (
        jnp.einsum("hqk,qhd->khd", d_scores, queries, preferred_element_type=jnp.float32)
        * score_scale
    )
    stacked = jnp.stack([d_queries, d_keys, d_values], axis=1)
    return stacked.reshape(qkv_seq.shape[0], -1).astype(jnp.bfloat16)


def body_split(
    tokens,
    segment_ids,
    time_steps,
    w_qkv,
    b_qv,
    w_out,
    b_out,
    gain_one,
    shift_one,
    w_up,
    b_up,
    w_down,
    b_down,
    gain_two,
    shift_two,
    w_time,
    b_time,
    cotangent,
):
    row_count = tokens.shape[0]
    seq_local = time_steps.shape[0]
    width_local = w_qkv.shape[2]
    gain_one_f = gain_one.astype(jnp.float32)
    shift_one_f = shift_one.astype(jnp.float32)
    gain_two_f = gain_two.astype(jnp.float32)
    shift_two_f = shift_two.astype(jnp.float32)
    w_flat = w_qkv.reshape(D, 3 * width_local)
    features = time_features(time_steps)
    embed_rows = jnp.dot(features, w_time.astype(jnp.float32), precision=HIGHEST_PRECISION)
    embed_rows = embed_rows + b_time.astype(jnp.float32)[None, :]
    row_seq = (lax.axis_index("mp") * row_count + jnp.arange(row_count, dtype=jnp.int32)) // LEN
    selector = (row_seq[:, None] == jnp.arange(seq_local, dtype=jnp.int32)[None, :]).astype(
        jnp.float32
    )
    hidden_in = tokens.astype(jnp.float32) + jnp.dot(
        selector, embed_rows, precision=HIGHEST_PRECISION
    )
    hidden_low = hidden_in.astype(jnp.bfloat16)
    hidden_full = lax.all_gather(hidden_low, "mp", axis=0, tiled=True)
    qkv_full = project_qkv(hidden_full, w_qkv, b_qv)
    ctx_blocks, log_totals = lax.map(
        attend_forward, (qkv_full.reshape(seq_local, LEN, 3 * width_local), segment_ids)
    )
    context = ctx_blocks.reshape(seq_local * LEN, width_local)
    rows_in = context
    attn_sum = lax.psum_scatter(
        jnp.dot(rows_in, w_out, preferred_element_type=jnp.float32).astype(jnp.bfloat16),
        "mp",
        scatter_dimension=0,
        tiled=True,
    ).astype(jnp.float32)
    attn_out = attn_sum + b_out.astype(jnp.float32)[None, :]
    mid_in = hidden_in + attn_out
    mid_norm = layer_norm(mid_in, gain_one_f, shift_one_f)
    mid_low = mid_norm.astype(jnp.bfloat16)
    mid_full = lax.all_gather(mid_low, "mp", axis=0, tiled=True)
    pre_act = (
        jnp.dot(mid_full, w_up, preferred_element_type=jnp.float32)
        + b_up.astype(jnp.float32)[None, :]
    )
    activated = exact_gelu(pre_act).astype(jnp.bfloat16)
    rows_in = activated
    ffn_part = lax.psum_scatter(
        jnp.dot(rows_in, w_down, preferred_element_type=jnp.float32).astype(jnp.bfloat16),
        "mp",
        scatter_dimension=0,
        tiled=True,
    ).astype(jnp.float32)
    out_in = mid_norm + ffn_part + b_down.astype(jnp.float32)[None, :]
    out_rows, out_back = jax.vjp(layer_norm, out_in, gain_two_f, shift_two_f)
    grad_two, grad_gain_two, grad_shift_two = out_back(cotangent.astype(jnp.float32))
    branch_two = grad_two.astype(jnp.bfloat16)
    grad_b_down = jnp.sum(branch_two.astype(jnp.float32), axis=0)
    _, gelu_back = jax.vjp(exact_gelu, pre_act)
    cot_full = lax.all_gather(branch_two, "mp", axis=0, tiled=True)
    d_act = jnp.dot(cot_full, w_down.T, preferred_element_type=jnp.float32)
    grad_w_down = jnp.dot(activated.T, cot_full, preferred_element_type=jnp.float32)
    d_pre = gelu_back(d_act)[0].astype(jnp.bfloat16)
    grad_w_up = jnp.dot(mid_full.T, d_pre, preferred_element_type=jnp.float32)
    grad_b_up = jnp.sum(d_pre.astype(jnp.float32), axis=0)
    rows_in = d_pre
    d_mid_part = lax.psum_scatter(
        jnp.dot(rows_in, w_up.T, preferred_element_type=jnp.float32).astype(jnp.bfloat16),
        "mp",
        scatter_dimension=0,
        tiled=True,
    ).astype(jnp.float32)
    _, mid_back = jax.vjp(layer_norm, mid_in, gain_one_f, shift_one_f)
    grad_one, grad_gain_one, grad_shift_one = mid_back(grad_two + d_mid_part)
    branch_one = grad_one.astype(jnp.bfloat16)
    grad_b_out = jnp.sum(branch_one.astype(jnp.float32), axis=0)
    cot_attn = lax.all_gather(branch_one, "mp", axis=0, tiled=True)
    d_context = jnp.dot(cot_attn, w_out.T, preferred_element_type=jnp.float32).astype(jnp.bfloat16)
    grad_w_out = jnp.dot(context.T, cot_attn, preferred_element_type=jnp.float32)
    grad_blocks = lax.map(
        attend_backward,
        (
            qkv_full.reshape(seq_local, LEN, 3 * width_local),
            d_context.reshape(seq_local, LEN, width_local),
            log_totals,
            segment_ids,
        ),
    )
    d_qkv = grad_blocks.reshape(seq_local * LEN, 3 * width_local)
    grad_w_qkv = jnp.dot(hidden_full.T, d_qkv, preferred_element_type=jnp.float32).reshape(
        D, 3, width_local
    )
    qkv_sums = jnp.sum(d_qkv.astype(jnp.float32), axis=0).reshape(3, width_local)
    grad_b_qv = jnp.stack([qkv_sums[0], qkv_sums[2]]).reshape(2, 1, width_local)
    rows_in = d_qkv
    input_part = lax.psum_scatter(
        jnp.dot(rows_in, w_flat.T, preferred_element_type=jnp.float32).astype(jnp.bfloat16),
        "mp",
        scatter_dimension=0,
        tiled=True,
    ).astype(jnp.float32)
    grad_tokens = grad_one + input_part
    grad_embed = jnp.dot(selector.T, grad_tokens, precision=HIGHEST_PRECISION)
    grad_w_time = jnp.dot(features.T, grad_embed, precision=HIGHEST_PRECISION)
    grad_b_time = jnp.sum(grad_embed, axis=0)
    sharded = (
        lax.psum_scatter(
            grad_w_qkv.astype(jnp.bfloat16), "dp", scatter_dimension=0, tiled=True
        ).astype(jnp.float32),
        lax.psum_scatter(
            grad_b_qv.astype(jnp.bfloat16), "dp", scatter_dimension=2, tiled=True
        ).astype(jnp.float32),
        lax.psum_scatter(
            grad_w_out.astype(jnp.bfloat16), "dp", scatter_dimension=1, tiled=True
        ).astype(jnp.float32),
        lax.psum_scatter(
            grad_w_up.astype(jnp.bfloat16), "dp", scatter_dimension=0, tiled=True
        ).astype(jnp.float32),
        lax.psum_scatter(
            grad_b_up.reshape(1, -1).astype(jnp.bfloat16), "dp", scatter_dimension=1, tiled=True
        ).astype(jnp.float32),
        lax.psum_scatter(
            grad_w_down.astype(jnp.bfloat16), "dp", scatter_dimension=1, tiled=True
        ).astype(jnp.float32),
    )
    shared = (
        lax.psum_scatter(grad_w_time, ("dp", "mp"), scatter_dimension=0, tiled=True),
        lax.psum_scatter(grad_b_time, ("dp", "mp"), scatter_dimension=0, tiled=True),
        lax.psum_scatter(grad_gain_one, ("dp", "mp"), scatter_dimension=0, tiled=True),
        lax.psum_scatter(grad_shift_one, ("dp", "mp"), scatter_dimension=0, tiled=True),
        lax.psum_scatter(grad_gain_two, ("dp", "mp"), scatter_dimension=0, tiled=True),
        lax.psum_scatter(grad_shift_two, ("dp", "mp"), scatter_dimension=0, tiled=True),
        lax.psum_scatter(grad_b_out, ("dp", "mp"), scatter_dimension=0, tiled=True),
        lax.psum_scatter(grad_b_down, ("dp", "mp"), scatter_dimension=0, tiled=True),
    )
    return (
        out_rows.astype(jnp.bfloat16),
        grad_tokens,
        sharded[0],
        sharded[1],
        sharded[2],
        shared[6],
        shared[2],
        shared[3],
        sharded[3],
        sharded[4],
        sharded[5],
        shared[7],
        shared[4],
        shared[5],
        shared[0],
        shared[1],
    )


GRID_DP = 8
GRID_MP = 4
HALF = 2
UNIT = 128
F32 = jnp.float32
BF16 = jnp.bfloat16
TILE_F = 512
TILE_B = 256
TILE_U = 256
ROWS = 256
GRAIN = 256
STEP = 128
EXTRA = 16
FAR = -(2.0**100)
NN = (((1,), (0,)), ((), ()))
NT = (((1,), (1,)), ((), ()))


def dot(left, right, dims=NN):
    return lax.dot_general(left, right, dims, preferred_element_type=F32)


def after(values, others):
    return lax.optimization_barrier((values, others))[0]


def whole(shape):
    return pl.BlockSpec(shape, lambda *_: (0,) * len(shape))


def struct(shape, kind=BF16):
    return jax.ShapeDtypeStruct(shape, kind)


def far(shape, kind=BF16):
    return pltpu.HBM(shape, kind)


def room(mib):
    return pltpu.CompilerParams(vmem_limit_bytes=mib * 2**20)


def cost(flops, moved):
    return pl.CostEstimate(flops=int(flops), bytes_accessed=int(moved), transcendentals=0)


def send_mp(values, bit):
    return lax.ppermute(values, "mp", [(i, i ^ bit) for i in range(GRID_MP)])


def send_dp(values, bit):
    return lax.ppermute(values, "dp", [(i, i ^ bit) for i in range(GRID_DP)])


def fetch(own, first_half):
    near = send_mp(own, 1)
    far_a = send_mp(first_half, 2)
    near_a = send_mp(far_a, 1)
    far_b = send_dp(far_a, 1)
    near_b = send_mp(far_b, 1)
    return [own, near, far_a, near_a, far_b, near_b]


def pack_heads_kernel(info_ref, qkv_ref, out_ref, qv_ref, up_ref, both_ref, first_ref):
    size = up_ref.shape[1] // 2
    for u in range(HALF):
        at = pl.ds(pl.multiple_of(info_ref[u] * UNIT, UNIT), UNIT)
        for j in range(3):
            both_ref[u, j * UNIT : (j + 1) * UNIT, :] = qkv_ref[j, :, at].T
        both_ref[u, 3 * UNIT : 4 * UNIT, :] = out_ref[at, :]
        hidden = pl.ds(pl.multiple_of(info_ref[u] * size, UNIT), size)
        rest = jnp.zeros((1, D - 2 * UNIT - size), F32)
        qv = qv_ref[:, at].astype(F32)
        parts = [qv[0:1], qv[1:2], up_ref[0:1, hidden], rest]
        bias = jnp.broadcast_to(jnp.concatenate(parts, axis=1), (EXTRA, D))
        both_ref[u, 4 * UNIT :, :] = bias.astype(BF16)
    first_ref[...] = both_ref[0]


def pack_heads(info, w_qkv, w_out, b_qv, b_up):
    rows = 4 * UNIT + EXTRA
    return pl.pallas_call(
        pack_heads_kernel,
        out_shape=(far((HALF, rows, D)), far((rows, D))),
        grid_spec=pltpu.PrefetchScalarGridSpec(
            num_scalar_prefetch=1,
            grid=(1,),
            in_specs=[
                whole((3, D, 2 * UNIT)),
                whole((2 * UNIT, D)),
                whole((2, 2 * UNIT)),
                whole((1, b_up.shape[0])),
            ],
            out_specs=[whole((HALF, rows, D)), whole((rows, D))],
        ),
        compiler_params=room(60),
        cost_estimate=cost(1e6, 5e6),
    )(info, w_qkv.transpose(1, 0, 2), w_out, b_qv, b_up.astype(F32)[None, :])


def pack_units_kernel(info_ref, up_ref, down_ref, up_both, up_first, down_both, down_first):
    step = pl.program_id(0)
    up = up_ref[...].T
    up_both[0] = up
    down_both[0] = down_ref[...]

    @pl.when(step == 0)
    def _():
        up_first[...] = up
        down_first[...] = down_ref[...]


def pack_units(info, w_up, w_down):
    size = w_down.shape[0] // 2
    return pl.pallas_call(
        pack_units_kernel,
        out_shape=(far((HALF, size, D)), far((size, D))) * 2,
        grid_spec=pltpu.PrefetchScalarGridSpec(
            num_scalar_prefetch=1,
            grid=(HALF,),
            in_specs=[
                pl.BlockSpec((D, size), lambda i, info: (0, info[i])),
                pl.BlockSpec((size, D), lambda i, info: (info[i], 0)),
            ],
            out_specs=[pl.BlockSpec((1, size, D), lambda i, info: (i, 0, 0)), whole((size, D))] * 2,
        ),
        compiler_params=room(60),
        cost_estimate=cost(1e6, 10e6),
    )(info, w_up, w_down)


def half_specs(rows, block):
    both = [pl.BlockSpec((1, rows, D), lambda *_, u=u: (u, block, 0)) for u in range(HALF)]
    return both * 2 + [pl.BlockSpec((rows, D), lambda *_: (block, 0))] * 4


def eight(pieces):
    own, near, far_a, near_a, far_b, near_b = pieces
    return [own, own, near, near, far_a, near_a, far_b, near_b]


def pair_specs(rows, block, pair):
    return half_specs(rows, block)[2 * pair : 2 * pair + 2]


def pair_of(pieces, pair):
    return eight(pieces)[2 * pair : 2 * pair + 2]


def rows_of(ref):
    return ref[...].reshape(-1, D)


def mark_segments(segment_row):
    lane = jnp.arange(UNIT, dtype=jnp.int32)[None, :]
    hot = segment_row[:, None] == (lane % HEAD_DIM)
    used = (lane % HEAD_DIM) < 8
    return (
        jnp.where(hot & used, 1.0, 0.0).astype(BF16),
        jnp.where(used & ~hot, FAR, 0.0).astype(BF16),
    )


def windows(segment_row, tile):
    first, last = segment_row[::tile], segment_row[tile - 1 :: tile]
    low = jnp.sum(segment_row[None, :] < first[:, None], axis=1) // STEP * STEP
    high = jnp.sum(segment_row[None, :] <= last[:, None], axis=1)
    count = jnp.maximum((high - low + GRAIN - 1) // GRAIN, tile // GRAIN)
    low = jnp.minimum(low, LEN - count * GRAIN)
    return jnp.stack([low, count]).astype(jnp.int32)


def variants(count, tile, run):
    for n in range(tile // GRAIN, LEN // GRAIN + 1):

        @pl.when(count == n)
        def _(n=n):
            run(n * GRAIN)


def lanes_at(at, base=0):
    return pl.ds(pl.multiple_of(base + at * UNIT, UNIT), UNIT)


def attend_kernel(
    win_ref, x_ref, *refs
):
    weights, biases, (hotq_ref, hotk_ref, qkv_ref, ctx_ref, lse_ref, w_ref, kx) = refs[:2], refs[2:4], refs[4:]
    unit, step = pl.program_id(0), pl.program_id(1)

    @pl.when((unit == 0) & (step == 0))
    def _():
        for u in range(HALF):
            part = rows_of(weights[u])
            for j in range(3):
                at = (2 * j + u) * UNIT
                w_ref[at : at + UNIT, :] = part[j * UNIT : (j + 1) * UNIT]
        first, second = [rows_of(ref)[0:1].astype(F32) for ref in biases]
        none = jnp.zeros((1, 2 * UNIT), F32)
        bias = [first[:, :UNIT], second[:, :UNIT], none]
        bias += [first[:, UNIT : 2 * UNIT], second[:, UNIT : 2 * UNIT]]
        bias = jnp.concatenate(bias, axis=1)
        for r in range(LEN // ROWS):
            rows = slice(r * ROWS, (r + 1) * ROWS)
            qkv_ref[rows, :] = (dot(x_ref[rows, :], w_ref[...], NT) + bias).astype(BF16)

    @pl.when(step == 0)
    def _():
        lane = lax.broadcasted_iota(jnp.int32, (LEN, UNIT), 1)
        keys = qkv_ref[:, lanes_at(unit, 2 * UNIT)]
        for h in range(HALF):
            kx[h] = jnp.where((lane // HEAD_DIM) == h, keys, hotk_ref[...])

    lane = lax.broadcasted_iota(jnp.int32, (TILE_F, UNIT), 1)
    rows = pl.ds(pl.multiple_of(step * TILE_F, TILE_F), TILE_F)
    queries = qkv_ref[rows, lanes_at(unit)] * jnp.asarray(1.0 / math.sqrt(HEAD_DIM), BF16)
    start = pl.multiple_of(win_ref[0, step], STEP)

    def run(width):
        window = pl.ds(start, width)
        values = qkv_ref[window, lanes_at(unit, 4 * UNIT)]
        scores = [
            dot(
                jnp.where((lane // HEAD_DIM) == h, queries, hotq_ref[...]), kx[h, window, :], NT
            )
            for h in range(HALF)
        ]
        outs = []
        for h in range(HALF):
            top = jnp.max(scores[h], axis=1, keepdims=True)
            weight = jnp.exp(scores[h] - top)
            total = jnp.sum(weight, axis=1, keepdims=True)
            outs.append(dot(weight.astype(BF16), values) * (1.0 / total))
            lse_ref[0, h : h + 1, :] = (top + jnp.log(total)).T
        ctx_ref[...] = jnp.where(lane < HEAD_DIM, outs[0], outs[1]).astype(BF16)

    variants(win_ref[1, step], TILE_F, run)


def attend_pair(win, hidden_low, heads, pair, hotq, hotk):
    return pl.pallas_call(
        attend_kernel,
        out_shape=(
            far((LEN, 6 * UNIT)),
            far((LEN, 2 * UNIT)),
            far((HALF, 8, LEN), F32),
        ),
        grid_spec=pltpu.PrefetchScalarGridSpec(
            num_scalar_prefetch=1,
            grid=(HALF, LEN // TILE_F),
            in_specs=[whole((LEN, D))]
            + pair_specs(4 * UNIT, 0, pair)
            + pair_specs(EXTRA, 4 * UNIT // EXTRA, pair)
            + [
                pl.BlockSpec((TILE_F, UNIT), lambda n, i, win: (i, 0)),
                whole((LEN, UNIT)),
            ],
            out_specs=[
                whole((LEN, 6 * UNIT)),
                pl.BlockSpec((TILE_F, UNIT), lambda n, i, win: (i, n)),
                pl.BlockSpec((1, 8, TILE_F), lambda n, i, win: (n, 0, i)),
            ],
            scratch_shapes=[pltpu.VMEM((6 * UNIT, D), BF16), pltpu.VMEM((HALF, LEN, UNIT), BF16)],
        ),
        compiler_params=room(32),
        cost_estimate=cost(6e9, 8e6),
    )(win, hidden_low, *pair_of(heads, pair) * 2, hotq, hotk)


def attend_back_kernel(
    win_ref,
    qkv_ref,
    hotq_ref,
    hotk_ref,
    branch_ref,
    wa_ref,
    wb_ref,
    ctx_ref,
    lse_ref,
    out_ref,
    sum_ref,
    kx,
    kt,
    grads,
    dk,
    dv,
):
    unit, step = pl.program_id(0), pl.program_id(1)
    scale = jnp.asarray(1.0 / math.sqrt(HEAD_DIM), BF16)

    @pl.when(step == 0)
    def _():
        lane = lax.broadcasted_iota(jnp.int32, (LEN, UNIT), 1)
        keys = qkv_ref[:, lanes_at(unit, 2 * UNIT)]
        for h in range(HALF):
            kx[h] = jnp.where((lane // HEAD_DIM) == h, keys, hotk_ref[...])
        kt[...] = (keys * scale).T
        dk[...] = jnp.zeros_like(dk)
        dv[...] = jnp.zeros_like(dv)

    lane = lax.broadcasted_iota(jnp.int32, (TILE_B, UNIT), 1)
    rows = pl.ds(pl.multiple_of(step * TILE_B, TILE_B), TILE_B)

    @pl.when(unit == 0)
    def _():
        weight = jnp.concatenate([rows_of(wa_ref), rows_of(wb_ref)], axis=0)
        grads[rows, :] = dot(branch_ref[...], weight, NT).astype(BF16)

    queries = qkv_ref[rows, lanes_at(unit)] * scale
    grad = grads[rows, lanes_at(unit)]
    product = (grad.astype(F32) * ctx_ref[...].astype(F32)).T
    start = pl.multiple_of(win_ref[0, step], STEP)

    def run(width):
        window = pl.ds(start, width)
        values = qkv_ref[window, lanes_at(unit, 4 * UNIT)]
        d_queries, d_keys, d_values = [], [], []
        for h in range(HALF):
            mine = (lane // HEAD_DIM) == h
            q_mine = jnp.where(mine, queries, jnp.zeros_like(queries))
            g_mine = jnp.where(mine, grad, jnp.zeros_like(grad))
            scores = dot(kx[h, window, :], jnp.where(mine, queries, hotq_ref[...]), NT)
            weight = jnp.exp(scores - lse_ref[0, h : h + 1, :])
            d_weight = dot(values, g_mine, NT)
            row_term = jnp.sum(
                product[h * HEAD_DIM : (h + 1) * HEAD_DIM], axis=0, keepdims=True
            )
            d_scores = (weight * (d_weight - row_term)).astype(BF16)
            d_values.append(dot(weight.astype(BF16), g_mine))
            d_keys.append(dot(d_scores, q_mine))
            d_queries.append(dot(kt[h * HEAD_DIM : (h + 1) * HEAD_DIM, window], d_scores))
        dv[window, :] += d_values[0] + d_values[1]
        dk[window, :] += d_keys[0] + d_keys[1]
        out_ref[rows, lanes_at(unit)] = jnp.concatenate(d_queries, 0).T.astype(BF16)

    variants(win_ref[1, step], TILE_B, run)

    @pl.when(step == LEN // TILE_B - 1)
    def _():
        out_ref[:, lanes_at(unit, 2 * UNIT)] = dk[...].astype(BF16)
        out_ref[:, lanes_at(unit, 4 * UNIT)] = dv[...].astype(BF16)

    @pl.when((unit == HALF - 1) & (step == LEN // TILE_B - 1))
    def _():
        total = jnp.sum(out_ref[...].astype(F32), axis=0, keepdims=True)
        sum_ref[...] = jnp.broadcast_to(total, sum_ref.shape)


def attend_back_pair(win, qkv, hotq, hotk, branch_one, heads, pair, ctx, lse):
    return pl.pallas_call(
        attend_back_kernel,
        out_shape=(far((LEN, 6 * UNIT)), struct((8, 6 * UNIT), F32)),
        grid_spec=pltpu.PrefetchScalarGridSpec(
            num_scalar_prefetch=1,
            grid=(HALF, LEN // TILE_B),
            in_specs=[
                whole((LEN, 6 * UNIT)),
                pl.BlockSpec((TILE_B, UNIT), lambda n, i, win: (i, 0)),
                whole((LEN, UNIT)),
                pl.BlockSpec((TILE_B, D), lambda n, i, win: (jnp.where(n == 0, i, LEN // TILE_B - 1), 0)),
                *pair_specs(UNIT, 3, pair),
                pl.BlockSpec((TILE_B, UNIT), lambda n, i, win: (i, n)),
                pl.BlockSpec((1, 8, TILE_B), lambda n, i, win: (n, 0, i)),
            ],
            out_specs=[whole((LEN, 6 * UNIT)), whole((8, 6 * UNIT))],
            scratch_shapes=[
                pltpu.VMEM((HALF, LEN, UNIT), BF16),
                pltpu.VMEM((UNIT, LEN), BF16),
                pltpu.VMEM((LEN, 2 * UNIT), BF16),
                pltpu.VMEM((LEN, UNIT), F32),
                pltpu.VMEM((LEN, UNIT), F32),
            ],
        ),
        compiler_params=room(32),
        cost_estimate=cost(8e9, 8e6),
    )(win, qkv, hotq, hotk, branch_one, *pair_of(heads, pair), ctx, lse)


def norm_of(values):
    center = values - jnp.mean(values, axis=-1, keepdims=True)
    spread = jnp.mean(center * center, axis=-1, keepdims=True)
    scale = lax.rsqrt(spread + EPS)
    return center * scale, scale


def norm_back(normal, scale, grad, gain_row):
    scaled = grad * gain_row
    mean_e = jnp.mean(scaled, axis=-1, keepdims=True)
    mean_en = jnp.mean(scaled * normal, axis=-1, keepdims=True)
    return scale * (scaled - mean_e - normal * mean_en)


def first_norm_kernel(tok_ref, *refs):
    ctx_refs, weights, refs = refs[:4], refs[4:12], refs[12:]
    embed_ref, bout_ref, gain_ref, shift_ref, normal_ref, scale_ref, mid_ref, mid_t, hid_t, wout_ref = refs

    @pl.when(pl.program_id(0) == 0)
    def _():
        for j in range(8):
            wout_ref[j * UNIT : (j + 1) * UNIT, :] = rows_of(weights[j])

    hidden = tok_ref[...].astype(F32) + embed_ref[...]
    hid_t[...] = hidden.astype(BF16).T
    total = bout_ref[...]
    for p in range(4):
        total = total + dot(ctx_refs[p][...], wout_ref[2 * p * UNIT : 2 * (p + 1) * UNIT, :])
    normal, scale = norm_of(hidden + total)
    normal_ref[...] = normal.astype(BF16)
    scale_ref[...] = scale
    mid = (normal * gain_ref[...] + shift_ref[...]).astype(BF16)
    mid_ref[...] = mid
    mid_t[...] = mid.T


def first_norm(tokens, contexts, heads, embed_row, b_out, gain, shift):
    tile = pl.BlockSpec((ROWS, D), lambda i: (i, 0))
    column = pl.BlockSpec((D, ROWS), lambda i: (0, i))
    return pl.pallas_call(
        first_norm_kernel,
        out_shape=(
        far((LEN, D)),
        far((LEN, 1), F32),
        struct((LEN, D)),
        far((D, LEN)),
        far((D, LEN)),
        ),
        grid=(LEN // ROWS,),
        in_specs=[tile]
        + [pl.BlockSpec((ROWS, 2 * UNIT), lambda i: (i, 0))] * 4
        + half_specs(UNIT, 3)
        + [whole((1, D))] * 4,
        out_specs=[
            tile,
            pl.BlockSpec((ROWS, 1), lambda i: (i, 0)),
            tile,
            column,
            column,
        ],
        scratch_shapes=[pltpu.VMEM((D, D), BF16)],
        compiler_params=room(24),
        cost_estimate=cost(2.2e9, 20e6),
    )(tokens, *contexts, *eight(heads), embed_row, b_out, gain, shift)


def ffn_tile(mid_ref, up_refs, down_refs, bias_refs, act_ref, slope_ref):
    size = act_ref.shape[1] // 2
    pres = []
    for up, ref in zip(up_refs, bias_refs):
        bias = rows_of(ref)[0:1, 2 * UNIT : 2 * UNIT + size].astype(F32)
        pres.append(dot(mid_ref[...], rows_of(up), NT) + bias)
    total = 0.0
    for u in range(HALF):
        columns = slice(u * size, (u + 1) * size)
        pre = pres[u]
        phi = 0.5 * (1.0 + lax.erf(pre * math.sqrt(0.5)))
        bell = jnp.exp(-0.5 * pre * pre) * (1.0 / math.sqrt(2.0 * math.pi))
        act = (pre * phi).astype(BF16)
        act_ref[:, columns] = act
        slope_ref[:, columns] = (phi + pre * bell).astype(BF16)
        total = total + dot(act, rows_of(down_refs[u]))
    return total


def ffn_kernel(mid_ref, *refs):
    *into, act_ref, slope_ref, total_ref = refs[6:]
    total = ffn_tile(mid_ref, refs[0:2], refs[2:4], refs[4:6], act_ref, slope_ref)
    for ref in into:
        total = total + ref[...]
    total_ref[...] = total


def ffn_specs(size, pair):
    return (
        [pl.BlockSpec((TILE_U, D), lambda i: (i, 0))]
        + pair_specs(size, 0, pair) * 2
        + pair_specs(EXTRA, 4 * UNIT // EXTRA, pair)
    )


def ffn_pair(mid_low, up, down, pair, heads, into):
    size = up[2].shape[0]
    tile = lambda n: pl.BlockSpec((TILE_U, n), lambda i: (i, 0))
    return pl.pallas_call(
        ffn_kernel,
        out_shape=(
            far((LEN, 2 * size)),
            far((LEN, 2 * size)),
            struct((LEN, D), F32),
        ),
        in_specs=ffn_specs(size, pair) + [tile(D)] * len(into),
        out_specs=[tile(2 * size), tile(2 * size), tile(D)],
        grid=(LEN // TILE_U,),
        compiler_params=room(24),
        cost_estimate=cost(4.3e9, 18e6),
    )(mid_low, *pair_of(up, pair), *pair_of(down, pair), *pair_of(heads, pair), *into)


def ffn_last_kernel(mid_ref, *refs):
    into_ref, cot_ref, bias_ref, gain_ref, shift_ref = refs[6:11]
    act_ref, slope_ref, out_ref, low_ref, low_t, sum_ref = refs[11:]

    @pl.when(pl.program_id(0) == 0)
    def _():
        sum_ref[...] = jnp.zeros_like(sum_ref)

    total = ffn_tile(mid_ref, refs[0:2], refs[2:4], refs[4:6], act_ref, slope_ref)
    total = total + into_ref[...] + bias_ref[...]
    normal, scale = norm_of(mid_ref[...].astype(F32) + total)
    out_ref[...] = (normal * gain_ref[...] + shift_ref[...]).astype(BF16)
    cot = cot_ref[...].astype(F32)
    low = norm_back(normal, scale, cot, gain_ref[...]).astype(BF16)
    low_ref[...] = low
    low_t[...] = low.T
    sums = [jnp.sum(v, axis=0, keepdims=True) for v in (low.astype(F32), cot * normal, cot)]
    for j in range(3):
        sum_ref[j : j + 1, :] += sums[j]


def ffn_last(mid_low, up, down, pair, heads, into, cot, *rows):
    size = up[2].shape[0]
    tile = lambda n: pl.BlockSpec((TILE_U, n), lambda i: (i, 0))
    return pl.pallas_call(
        ffn_last_kernel,
        out_shape=(
            far((LEN, 2 * size)),
            far((LEN, 2 * size)),
            far((LEN, D)),
            far((LEN, D)),
            far((D, LEN)),
            struct((8, D), F32),
        ),
        in_specs=ffn_specs(size, pair) + [tile(D)] * 2 + [whole((1, D))] * 3,
        out_specs=[tile(2 * size), tile(2 * size), tile(D), tile(D)]
        + [pl.BlockSpec((D, TILE_U), lambda i: (0, i)), whole((8, D))],
        grid=(LEN // TILE_U,),
        compiler_params=room(30),
        cost_estimate=cost(4.3e9, 30e6),
    )(
        mid_low, *pair_of(up, pair), *pair_of(down, pair), *pair_of(heads, pair), into, cot, *rows
    )


def ffn_back_kernel(branch_hbm, *refs):
    down_hbm, up_hbm, slope_hbm, refs = refs[0:6], refs[6:12], refs[12:16], refs[16:]
    one_hbm, scale_ref, gain_ref, refs = refs[0], refs[1], refs[2], refs[3:]
    pre_hbm, sum_ref, low_ref, low_t, norm_sum_ref, refs = (
        refs[0:4],
        refs[4],
        refs[5],
        refs[6],
        refs[7],
        refs[8:],
    )
    branch, down, up, slope, total, one, low, low_turned, sems = refs
    size = up.shape[1]
    plan = ((0, 0), (0, 1), (1, 0), (1, 1), (2, None), (3, None), (4, None), (5, None))
    first = pltpu.make_async_copy(branch_hbm, branch, sems.at[0])
    first.start()
    copies = []
    for j, (piece, which) in enumerate(plan):
        if which is None:
            down_part, up_part = down_hbm[piece], up_hbm[piece]
        else:
            down_part, up_part = down_hbm[piece].at[which], up_hbm[piece].at[which]
        columns = slice((j % 2) * size, (j % 2 + 1) * size)
        group = [
            pltpu.make_async_copy(down_part, down.at[j], sems.at[1 + 3 * j]),
            pltpu.make_async_copy(
                slope_hbm[j // 2].at[:, columns], slope.at[j], sems.at[2 + 3 * j]
            ),
            pltpu.make_async_copy(up_part, up.at[j], sems.at[3 + 3 * j]),
        ]
        for copy in group:
            copy.start()
        copies.append(group)
    last = pltpu.make_async_copy(one_hbm, one, sems.at[25])
    last.start()
    first.wait()
    stores = []
    norm_sums = [0.0] * 3
    for j in range(len(plan)):
        for copy in copies[j]:
            copy.wait()
        if j == len(plan) - 1:
            last.wait()
        columns = slice((j % 2) * size, (j % 2 + 1) * size)
        sums = 0.0
        for r in range(LEN // ROWS):
            rows = slice(r * ROWS, (r + 1) * ROWS)
            d_act = dot(branch[rows, :], down[j], NT)
            d_pre = (d_act * slope[j, rows, :].astype(F32)).astype(BF16)
            slope[j, rows, :] = d_pre
            sums = sums + jnp.sum(d_pre.astype(F32), axis=0, keepdims=True)
            part = dot(d_pre, up[j])
            if j == 0:
                total[rows, :] = part
            elif j < len(plan) - 1:
                total[rows, :] += part
            else:
                d_mid = total[rows, :] + part + branch[rows, :].astype(F32)
                normal = one[rows, :].astype(F32)
                part = norm_back(normal, scale_ref[rows, :], d_mid, gain_ref[...]).astype(BF16)
                low[rows, :] = part
                low_turned[:, rows] = part.T
                for k, (source, target) in enumerate(
                    (
                        (low.at[rows, :], low_ref.at[rows, :]),
                        (low_turned.at[:, rows], low_t.at[:, rows]),
                    )
                ):
                    store = pltpu.make_async_copy(source, target, sems.at[34 + 2 * r + k])
                    store.start()
                    stores.append(store)
                for k, v in enumerate((part.astype(F32), d_mid * normal, d_mid)):
                    norm_sums[k] = norm_sums[k] + jnp.sum(v, axis=0, keepdims=True)
        sum_ref[j : j + 1, :] = sums
        store = pltpu.make_async_copy(slope.at[j], pre_hbm[j // 2].at[:, columns], sems.at[26 + j])
        store.start()
        stores.append(store)
    for k in range(3):
        norm_sum_ref[k : k + 1, :] = norm_sums[k]
    for store in stores:
        store.wait()


def ffn_back(branch_two, down, up, slopes, normal_one, scale_one, gain):
    size = down[2].shape[0]
    hbm = pl.BlockSpec(memory_space=pltpu.HBM)
    return pl.pallas_call(
        ffn_back_kernel,
        out_shape=(far((LEN, 2 * size)),) * 4
        + (struct((8, size), F32), far((LEN, D)), far((D, LEN)), struct((8, D), F32)),
        grid=(1,),
        in_specs=[hbm] * 18 + [whole((LEN, 1)), whole((1, D))],
        out_specs=[hbm] * 4 + [whole((8, size)), hbm, hbm, whole((8, D))],
        scratch_shapes=[
            pltpu.VMEM((LEN, D), BF16),
            pltpu.VMEM((8, size, D), BF16),
            pltpu.VMEM((8, size, D), BF16),
            pltpu.VMEM((8, LEN, size), BF16),
            pltpu.VMEM((LEN, D), F32),
            pltpu.VMEM((LEN, D), BF16),
            pltpu.VMEM((LEN, D), BF16),
            pltpu.VMEM((D, LEN), BF16),
            pltpu.SemaphoreType.DMA((42,)),
        ],
        compiler_params=room(52),
        cost_estimate=cost(17e9, 40e6),
    )(branch_two, *down, *up, *slopes, normal_one, scale_one, gain)


class Run(NamedTuple):
    which: int
    first: int
    second: int
    size: int
    base: int
    stride: int


def unit_runs(count, size):
    half = size // 2
    return [Run(0, r * half // count, half + r * half // count, half // count, r * half // count, half) for r in range(count)]


def head_runs(which, count):
    return [Run(which, 2 * j * UNIT, (2 * j + 1) * UNIT, UNIT, 2 * j * UNIT, UNIT) for j in range(count)]


def part_width(part):
    return sum(2 * run.size for run in part)


def grad_kernel(blocks, side_from, outputs, lefts, got_from, left_at, *refs):
    n_right = 3 * lefts
    left_hbm, right_hbm, refs = refs[:lefts], refs[lefts : lefts + n_right], refs[lefts + n_right :]
    got_hbm, refs = (None, refs) if got_from is None else (refs[0], refs[1:])
    out_hbm, (left, right, got, out, sems) = refs[: len(outputs)], refs[len(outputs) :]
    count = [0]

    def copy_of(source, target):
        copy = pltpu.make_async_copy(source, target, sems.at[count[0]])
        copy.start()
        count[0] += 1
        return copy

    ready = {}
    chunks, at = [], 0
    for part, far in blocks:
        for run in part:
            copies = []
            if (run.which, 0) not in ready:
                source = left_hbm[run.which]
                ready[run.which, 0] = copy_of(source.at[:, left_at[0]], left.at[run.which, 0])
            for h in range(2):
                if far:
                    piece, source = 1 + h, run.second if side_from else run.first
                else:
                    piece, source = 0, run.second if h else run.first
                copies.append(
                    copy_of(
                        right_hbm[3 * run.which + piece].at[:, source : source + run.size],
                        right.at[:, at + h * run.size : at + (h + 1) * run.size],
                    )
                )
            columns = slice(at, at + 2 * run.size)
            if got_from is not None:
                source = got_hbm.at[:, :, got_from + at : got_from + at + 2 * run.size]
                copies.append(copy_of(source, got.at[:, :, columns]))
            if (run.which, 1) not in ready:
                source = left_hbm[run.which]
                ready[run.which, 1] = copy_of(source.at[:, left_at[1]], left.at[run.which, 1])
            chunks.append((run.which, at, 2 * run.size, copies))
            at += 2 * run.size
    stores = []
    for which, at, size, copies in chunks:
        for copy in copies:
            copy.wait()
        columns = slice(at, at + size)
        for side in range(2):
            if (which, side) in ready:
                ready.pop((which, side)).wait()
            total = dot(left[which, side].reshape(D // 2, LEN), right[:, columns])
            if got_from is not None:
                total = total + got[side, :, columns].astype(F32)
            out[side, :, columns] = total.astype(BF16)
        for (start, end, side), target in zip(outputs, out_hbm):
            if start <= at < end:
                place = slice(at - start, at - start + size)
                if side is None:
                    stores.append(copy_of(out.at[:, :, columns], target.at[:, :, place]))
                else:
                    stores.append(copy_of(out.at[side, :, columns], target.at[:, place]))
    for copy in stores:
        copy.wait()


def grad_call(info, left_t, rights, blocks, side, outputs, got=None, got_from=None):
    width = sum(part_width(part) for part, _ in blocks)
    hbm = pl.BlockSpec(memory_space=pltpu.HBM)
    lefts = len(left_t)
    operands = [v.reshape(4, 2, D // 8, LEN) for v in left_t] + [v for r in rights for v in r]
    operands += [] if got is None else [got]
    shapes = [
        (2, D // 2, end - start) if at is None else (D // 2, end - start) for start, end, at in outputs
    ]
    return pl.pallas_call(
        functools.partial(grad_kernel, blocks, side, outputs, lefts, got_from),
        out_shape=tuple(far(shape) for shape in shapes),
        grid_spec=pltpu.PrefetchScalarGridSpec(
            num_scalar_prefetch=1,
            grid=(1,),
            in_specs=[hbm] * len(operands),
            out_specs=[hbm] * len(shapes),
            scratch_shapes=[
                pltpu.VMEM((lefts, 2, 4, D // 8, LEN), BF16),
                pltpu.VMEM((LEN, width), BF16),
                pltpu.VMEM((2, D // 2, 128 if got is None else width), BF16),
                pltpu.VMEM((2, D // 2, width), BF16),
                pltpu.SemaphoreType.DMA((48,)),
            ],
        ),
        compiler_params=room(60),
        cost_estimate=cost(2 * D * LEN * width, 10e6),
    )(info, *operands)


def column_runs(part, swap):
    at = 0
    for run in part:
        for h in range(2):
            source = at + (1 - h if swap else h) * run.size
            yield at + h * run.size, source, run.size
        at += 2 * run.size


def add_kernel(jobs, *refs):
    ins, outs = refs[: 2 * len(jobs)], refs[2 * len(jobs) :]
    for k, (part, swap) in enumerate(jobs):
        rows = outs[k].shape[0]
        mine, got = [ref[...].reshape(rows, -1) for ref in ins[2 * k : 2 * k + 2]]
        for at, source, size in column_runs(part, swap):
            total = mine[:, at : at + size].astype(F32) + got[:, source : source + size].astype(F32)
            outs[k][:, at : at + size] = total.astype(BF16)


def half_spec(array, where, width):
    side, column = where
    if len(array.shape) == 3:
        return pl.BlockSpec((1, D // 4, width), lambda i: (side, i, column))
    return pl.BlockSpec((D // 4, width), lambda i: (i, column))


def add_parts(*jobs):
    widths = [part_width(job[2]) for job in jobs]
    return pl.pallas_call(
        functools.partial(add_kernel, tuple(job[2:] for job in jobs)),
        out_shape=tuple(struct((D // 2, width)) for width in widths),
        grid=(2,),
        in_specs=[half_spec(*v, width) for job, width in zip(jobs, widths) for v in job[:2]],
        out_specs=[pl.BlockSpec((D // 4, width), lambda i: (i, 0)) for width in widths],
        compiler_params=room(24),
        cost_estimate=cost(1e6, 3e6),
    )(*[v[0] for job in jobs for v in job[:2]])


def block_spec(array, where, width):
    side, column = where
    if len(array.shape) == 3:
        return pl.BlockSpec((1, D // 2, width), lambda *_: (side, 0, column))
    return pl.BlockSpec((D // 2, width), lambda *_: (0, column))


def split_kernel(parts, info_ref, *refs):
    ins, out_refs = refs[: 3 * len(parts)], refs[3 * len(parts) :]
    span = D // 8
    for k in range(4):
        rows = pl.ds(pl.multiple_of((info_ref[2] ^ k) * span, span), span)
        first = 0
        for p, part in enumerate(parts):
            mine, from_x, from_y = [
                (ref[0, rows, :] if len(ref.shape) == 3 else ref[rows, :]).astype(F32)
                for ref in ins[3 * p : 3 * p + 3]
            ]
            for at, source, size in column_runs(part, True):
                total = mine[:, at : at + size] + from_y[:, at : at + size]
                total = total + from_x[:, source : source + size]
                out_refs[k][:, first + at : first + at + size] = total.astype(BF16)
            first += part_width(part)


def split_z(info, parts, sources):
    width = sum(part_width(part) for part in parts)
    specs = [
        block_spec(*v, part_width(part)) for part, triple in zip(parts, sources) for v in triple
    ]
    out = pl.pallas_call(
        functools.partial(split_kernel, parts),
        out_shape=(struct((D // 8, width)),) * 4,
        grid_spec=pltpu.PrefetchScalarGridSpec(
            num_scalar_prefetch=1,
            grid=(1,),
            in_specs=specs,
            out_specs=[whole((D // 8, width))] * 4,
        ),
        compiler_params=room(60),
        cost_estimate=cost(1e6, 4e6),
    )(info, *[v[0] for triple in sources for v in triple])
    return [out[0]] + [send_dp(out[k], 2 * k) for k in (1, 2, 3)]


def finish_kernel(runs, turned, info_ref, *refs):
    parts, outs = refs[:4], refs[4:]
    at = 0
    for run in runs:
        for h in range(2):
            columns = slice(at, at + run.size)
            total = parts[0][:, columns].astype(F32)
            for part in parts[1:]:
                total = total + part[:, columns].astype(F32)
            spot = pl.ds(pl.multiple_of(run.base + info_ref[h] * run.stride, UNIT), run.size)
            if turned[run.which]:
                outs[run.which][spot, :] = total.T
            else:
                outs[run.which][:, spot] = total
            at += run.size


def finish(info, values, parts, turned):
    rows = D // 8
    runs = tuple(run for part in parts for run in part)
    sizes = [sum(2 * r.size for r in runs if r.which == k) for k in range(len(turned))]
    shapes = [(size, rows) if t else (rows, size) for size, t in zip(sizes, turned)]
    return pl.pallas_call(
        functools.partial(finish_kernel, runs, turned),
        out_shape=tuple(struct(shape, F32) for shape in shapes),
        grid_spec=pltpu.PrefetchScalarGridSpec(
            num_scalar_prefetch=1,
            grid=(1,),
            in_specs=[whole((rows, sum(sizes)))] * 4,
            out_specs=[whole(shape) for shape in shapes],
        ),
        compiler_params=room(24),
        cost_estimate=cost(1e6, 4e6),
    )(info, *values)


def input_grad_kernel(branch_ref, *refs):
    grads, heads, (out_ref, sum_ref, weight, sems) = refs[:4], refs[4:10], refs[10:]
    step = pl.program_id(0)
    plan = ((0, 0), (0, 1), (1, 0), (1, 1), (2, None), (3, None), (4, None), (5, None))
    copies = []
    for j, (piece, which) in enumerate(plan):
        source = heads[piece] if which is None else heads[piece].at[which]
        for k in range(3):
            at = ((j // 2) * 6 + 2 * k + j % 2) * UNIT
            copies.append(
                pltpu.make_async_copy(
                    source.at[k * UNIT : (k + 1) * UNIT, :],
                    weight.at[at : at + UNIT, :],
                    sems.at[3 * j + k],
                )
            )

    @pl.when(step == 0)
    def _():
        for copy in copies:
            copy.start()
        sum_ref[...] = jnp.zeros_like(sum_ref)

    total = branch_ref[...].astype(F32)
    for p in range(4):

        @pl.when(step == 0)
        def _():
            for copy in copies[6 * p : 6 * p + 6]:
                copy.wait()

        total = total + dot(grads[p][...], weight[6 * p * UNIT : 6 * (p + 1) * UNIT, :])
    out_ref[...] = total
    sum_ref[0:1, :] += jnp.sum(total, axis=0, keepdims=True)


def input_grad(branch_one, d_qkv, heads):
    tile = pl.BlockSpec((ROWS, D), lambda i: (i, 0))
    width = d_qkv[0].shape[1]
    return pl.pallas_call(
        input_grad_kernel,
        out_shape=(far((LEN, D), F32), struct((8, D), F32)),
        grid=(LEN // ROWS,),
        in_specs=[tile]
        + [pl.BlockSpec((ROWS, width), lambda i: (i, 0))] * 4
        + [pl.BlockSpec(memory_space=pltpu.HBM)] * 6,
        out_specs=[tile, whole((8, D))],
        scratch_shapes=[pltpu.VMEM((4 * width, D), BF16), pltpu.SemaphoreType.DMA((24,))],
        compiler_params=room(60),
        cost_estimate=cost(6.4e9, 20e6),
    )(branch_one, *d_qkv, *heads)


def exchange_kernel(sum_ref, row_ref, total_ref, rows_ref, got, sems_a, sems_b):
    devices = GRID_DP * GRID_MP
    me = lax.axis_index("dp") * GRID_MP + lax.axis_index("mp")

    def place(index):
        return {"dp": index // GRID_MP, "mp": index % GRID_MP}

    barrier = pltpu.get_barrier_semaphore()

    def greet(k, carry):
        target = (me + k) % devices
        pl.semaphore_signal(
            barrier, inc=1, device_id=place(target), device_id_type=pl.DeviceIdType.MESH
        )
        return carry

    lax.fori_loop(1, devices, greet, 0)
    pl.semaphore_wait(barrier, devices - 1)

    def copies(k):
        target = (me + k) % devices
        first = pltpu.make_async_remote_copy(
            src_ref=sum_ref.at[target],
            dst_ref=got.at[k],
            send_sem=sems_a.at[0, k],
            recv_sem=sems_a.at[1, k],
            device_id=place(target),
            device_id_type=pl.DeviceIdType.MESH,
        )
        second = pltpu.make_async_remote_copy(
            src_ref=row_ref,
            dst_ref=rows_ref.at[k],
            send_sem=sems_b.at[0, k],
            recv_sem=sems_b.at[1, k],
            device_id=place(target),
            device_id_type=pl.DeviceIdType.MESH,
        )
        return first, second

    def start(k, carry):
        for copy in copies(k):
            copy.start()
        return carry

    lax.fori_loop(1, devices, start, 0)
    rows_ref[0] = row_ref[...]

    def finish_copy(k, carry):
        for copy in copies(k):
            copy.wait()
        return carry

    lax.fori_loop(1, devices, finish_copy, 0)
    total_ref[...] = sum_ref[me] + jnp.sum(got[1:], axis=0)


def exchange(sums, row):
    devices = GRID_DP * GRID_MP
    vmem = pl.BlockSpec(memory_space=pltpu.VMEM)
    return pl.pallas_call(
        exchange_kernel,
        out_shape=(struct(sums.shape[1:], F32), struct((devices,) + row.shape, F32)),
        in_specs=[vmem, vmem],
        out_specs=[vmem, vmem],
        scratch_shapes=[
            pltpu.VMEM(sums.shape, F32),
            pltpu.SemaphoreType.DMA((2, devices)),
            pltpu.SemaphoreType.DMA((2, devices)),
        ],
        compiler_params=pltpu.CompilerParams(collective_id=0, has_side_effects=True),
        cost_estimate=cost(1e6, 1e6),
    )(sums, row)


def natural_order(x_at, mp_at):
    block, half = jnp.arange(8, dtype=jnp.int32) // 2, jnp.arange(8, dtype=jnp.int32) % 2
    away, at = block ^ mp_at, half ^ x_at
    source = jnp.where(away < 2, 2 * away + at, 2 + away + 2 * at)
    return (source[:, None] == jnp.arange(8, dtype=jnp.int32)[None, :]).astype(F32)


def body_rows(
    tokens,
    segment_ids,
    time_steps,
    w_qkv,
    b_qv,
    w_out,
    b_out,
    gain_one,
    shift_one,
    w_up,
    b_up,
    w_down,
    b_down,
    gain_two,
    shift_two,
    w_time,
    b_time,
    cotangent,
):
    dp_at, mp_at = lax.axis_index("dp"), lax.axis_index("mp")
    x_at, z_at = dp_at % 2, dp_at // 2
    info = jnp.stack([x_at, 1 - x_at, z_at, mp_at]).astype(jnp.int32)
    row = lambda v: v.astype(F32)[None, :]
    width = w_qkv.shape[2]

    heads_own, heads_first = pack_heads(info, w_qkv, w_out, b_qv, b_up)
    heads = fetch(heads_own, heads_first)
    up_own, up_first, down_own, down_first = pack_units(info, w_up, w_down)
    up = fetch(up_own, up_first)
    down = fetch(down_own, down_first)

    own_step = lax.dynamic_slice_in_dim(time_steps, mp_at, 1, 0)
    segment_row = lax.dynamic_index_in_dim(segment_ids, mp_at, 0, keepdims=False)
    features = time_features(own_step)
    embed_row = jnp.dot(features, w_time.astype(F32), precision=HIGHEST_PRECISION)
    embed_row = embed_row + row(b_time)
    hidden_low = (tokens.astype(F32) + embed_row).astype(BF16)
    hotq, hotk = mark_segments(segment_row)
    win_f, win_b = windows(segment_row, TILE_F), windows(segment_row, TILE_B)

    qkv, ctx, lse = [], [], []
    for p in range(4):
        parts = attend_pair(win_f, hidden_low, heads, p, hotq, hotk)
        for kept, part in zip((qkv, ctx, lse), parts):
            kept.append(part)
    normal_one, scale_one, mid_low, mid_t, hidden_t = first_norm(
        tokens, ctx, heads, embed_row, row(b_out), row(gain_one), row(shift_one)
    )

    act, slope, ffn = [], [], ()
    for p in range(3):
        act_p, slope_p, *ffn = ffn_pair(mid_low, up, down, p, heads, ffn)
        act.append(act_p)
        slope.append(slope_p)
    act_p, slope_p, out_rows, branch_two, branch_two_t, sums_two = ffn_last(
        mid_low,
        up,
        down,
        3,
        heads,
        *ffn,
        cotangent,
        *[row(v) for v in (b_down, gain_two, shift_two)],
    )
    act.append(act_p)
    slope.append(slope_p)

    units = act[0].shape[1]
    down_parts = [(run,) for run in unit_runs(2, units)]
    up_parts = [down_parts[0], (down_parts[1][0], *head_runs(1, 1))]
    qkv_part = tuple(head_runs(0, 3))

    def two_way(left_t, rights, parts, cover):
        blocks = tuple((part, far) for part in parts for far in (False, True))
        one, two = (part_width(part) for part in parts)
        every = 2 * (one + two)
        (sent,) = grad_call(info, left_t, [r[1:] for r in rights], blocks, 1, ((0, every, None),))
        got = send_mp(sent, 1)
        covered = cover()
        outputs = (
            (0, one, None),
            (one, 2 * one, None),
            (2 * one, every, 0),
            (2 * one, every, 1),
        )
        result = grad_call(
            info, left_t, [r[:1] + r[2:] for r in rights], blocks, 0, outputs, got, 0
        )
        return covered, result

    def first_sends(blocks):
        own, far, keep, leave = blocks
        return own, keep, send_mp(far, 2), send_dp(leave, 1)

    def second_sends(sums, parts):
        own, keep, from_y, from_x = sums
        low, other = add_parts(
            ((own, (1, 0)), (from_y, (1, 0)), parts[0], False),
            ((keep, (0, 1)), (from_x, (0, 1)), parts[1], True),
        )
        x_two = send_dp(low, 1)
        y_two = send_mp(other, 2)
        here = (0, 0)
        return (
            ((own, here), (x_two, here), (from_y, here)),
            ((keep, here), (from_x, here), (y_two, here)),
        )

    def ffn_part():
        return ffn_back(
            branch_two, down, up, slope, normal_one, scale_one, row(gain_one)
        )

    (*d_pre, sums_up, branch_one, branch_one_t, sums_one), down_blocks = two_way(
        [branch_two_t], [act], down_parts, ffn_part
    )
    down_sums = first_sends(down_blocks)
    d_qkv, qkv_sums = [None] * 4, [None] * 4

    def back(p):
        d_qkv[p], qkv_sums[p] = attend_back_pair(
            win_b, qkv[p], hotq, hotk, branch_one, heads, p, ctx[p], lse[p]
        )

    _, up_blocks = two_way([mid_t, branch_one_t], [d_pre, ctx], up_parts, lambda: back(1))
    down_last = second_sends(down_sums, down_parts)
    up_sums = first_sends(up_blocks)
    back(2)
    down_values = split_z(info, down_parts, down_last)
    back(3)
    wide = part_width(qkv_part)
    far_only, own_only = ((qkv_part, True),), ((qkv_part, False),)
    (sent,) = grad_call(
        info, [hidden_t], [d_qkv[1:]], own_only + far_only, 1, ((0, 2 * wide, None),)
    )
    got = send_mp(sent, 1)
    up_last = second_sends(after(up_sums, sent), up_parts)
    sides = ((0, wide, 0), (0, wide, 1))
    far_keep, far_leave = grad_call(
        info, [hidden_t], [[d_qkv[1]] + d_qkv[2:]], far_only, 0, sides, got, wide
    )
    far_x = send_dp(far_leave, 1)
    back(0)
    up_values = split_z(info, up_parts, up_last)
    here = (0, 0)
    (far_low,) = add_parts(((far_keep, here), (far_x, here), qkv_part, True))
    far_y = send_mp(far_low, 2)
    own_keep, own_leave = grad_call(
        info, [hidden_t], [d_qkv[:1] + d_qkv[2:]], own_only, 0, sides, got, 0
    )
    own_x = send_dp(own_leave, 1)
    grad_tokens, sums_in = input_grad(branch_one, d_qkv, heads)
    qkv_values = split_z(info, (qkv_part,), (((own_keep, here), (own_x, here), (far_y, here)),))

    devices = GRID_DP * GRID_MP
    heads_sum = jnp.concatenate([v[0:1] for v in qkv_sums]).reshape(4, 3, HALF, UNIT)
    heads_sum = heads_sum.transpose(0, 2, 1, 3).reshape(8, -1)
    blocks = jnp.dot(
        natural_order(x_at, mp_at),
        jnp.concatenate([sums_up, heads_sum], axis=1),
        precision=HIGHEST_PRECISION,
    )

    def spread(v):
        return v.reshape(GRID_MP, GRID_DP, -1).transpose(1, 0, 2).reshape(devices, -1)

    ends = (0, units // 2, units // 2 + UNIT, units // 2 + 3 * UNIT)
    full = jnp.concatenate([sums_two[:3], sums_one[:3]]).reshape(6, devices, -1)
    rows = [full.transpose(1, 0, 2).reshape(devices, -1), spread(blocks[:, : ends[1]])]
    rows += [spread(blocks[:, at : at + UNIT]) for at in (ends[1], ends[3] - UNIT)]
    tail_row = jnp.concatenate(
        [sums_in[0:1], jnp.broadcast_to(own_step.astype(F32)[None, :], (1, UNIT))], axis=1
    )
    totals, all_rows = exchange(jnp.concatenate(rows, axis=1)[:, None, :], tail_row)
    totals, all_rows, down_values, up_values = after(
        (totals, all_rows, down_values, up_values), qkv_values[0]
    )
    all_rows = all_rows[:, 0]
    span = D // (GRID_DP * GRID_MP)
    own = [totals[0, j * span : (j + 1) * span] for j in range(6)]
    device_at = dp_at * GRID_MP + mp_at
    all_grads = all_rows[:, :D]
    dims = device_at * span + jnp.arange(span, dtype=jnp.int32)
    ladder = (dims % (D // 2)).astype(F32)
    frequency = jnp.exp(ladder * (-math.log(10000.0) / (D // 2)))
    angles = all_rows[:, D : D + 1] * frequency[None, :]
    own_features = jnp.where((dims < D // 2)[None, :], jnp.sin(angles), jnp.cos(angles))
    g_w_time = jnp.dot(own_features.T, all_grads, precision=HIGHEST_PRECISION)
    g_b_time = lax.dynamic_slice_in_dim(jnp.sum(all_grads, axis=0), device_at * span, span, 0)

    (g_w_qkv,) = finish(info, qkv_values, (qkv_part,), (False,))
    (g_w_down,) = finish(info, down_values, down_parts, (True,))
    g_w_up, g_w_out = finish(info, up_values, up_parts, (False, True))
    up_end = totals.shape[1] - 2 * span
    return (
        out_rows,
        grad_tokens,
        g_w_qkv.reshape(D // 8, 3, width),
        totals[0, up_end:].reshape(2, 1, -1),
        g_w_out,
        own[3],
        own[4],
        own[5],
        g_w_up,
        totals[:, 6 * span : up_end],
        g_w_down,
        own[0],
        own[1],
        own[2],
        g_w_time,
        g_b_time,
    )


def solution(mesh):
    placed = (
        P(("dp", "mp"), None),
        P("dp", None),
        P("dp"),
        P(None, None, "mp"),
        P(None, "mp"),
        P("mp", None),
        P(),
        P(),
        P(),
        P(None, "mp"),
        P("mp"),
        P("mp", None),
        P(),
        P(),
        P(),
        P(),
        P(),
        P(("dp", "mp"), None),
    )
    rows = mesh.shape["dp"], mesh.shape["mp"]

    def body(*args):
        if args[0].shape[0] != LEN or rows != (GRID_DP, GRID_MP):
            return body_split(*args)
        return body_rows(*args)

    return jax.shard_map(
        body,
        mesh=mesh,
        in_specs=placed,
        out_specs=(
            P(("dp", "mp"), None),
            P(("dp", "mp"), None),
            P("dp", None, "mp"),
            P(None, "mp", "dp"),
            P("mp", "dp"),
            P(("dp", "mp")),
            P(("dp", "mp")),
            P(("dp", "mp")),
            P("dp", "mp"),
            P("mp", "dp"),
            P("mp", "dp"),
            P(("dp", "mp")),
            P(("dp", "mp")),
            P(("dp", "mp")),
            P(("dp", "mp"), None),
            P(("dp", "mp")),
        ),
        check_vma=False,
    )
```
